64 devices in a mesh: rep: 8 (over x, y, core), dp: 8 (over z).
Axes of the slice: x: 2, y: 2, z: 8, core: 2. Of those that a mesh axis runs over, the one named last changes fastest.
The devices are a block of a 4x4x8 slice.
Arguments:
- x: bfloat16 [64, 2048, 512], P(('rep', 'dp')), parts along dimension 0
- dy: bfloat16 [64, 2048, 512], P(('rep', 'dp')), parts along dimension 0
- wq: bfloat16 [2, 512, 512], P(None, 'dp')
- wk: bfloat16 [2, 512, 128], P(None, 'dp')
- wv: bfloat16 [2, 512, 128], P(None, 'dp')
- wo: bfloat16 [2, 512, 512], P(None, 'dp')
- w_gate: bfloat16 [2, 512, 1536], P(None, 'dp')
- w_up: bfloat16 [2, 512, 1536], P(None, 'dp')
- w_down: bfloat16 [2, 1536, 512], P(None, 'dp')
- m_wq: float32 [2, 512, 512], P(None, 'dp')
- m_wk: float32 [2, 512, 128], P(None, 'dp')
- m_wv: float32 [2, 512, 128], P(None, 'dp')
- m_wo: float32 [2, 512, 512], P(None, 'dp')
- m_w_gate: float32 [2, 512, 1536], P(None, 'dp')
- m_w_up: float32 [2, 512, 1536], P(None, 'dp')
- m_w_down: float32 [2, 1536, 512], P(None, 'dp')
- v_wq: float32 [2, 512, 512], P(None, 'dp')
- v_wk: float32 [2, 512, 128], P(None, 'dp')
- v_wv: float32 [2, 512, 128], P(None, 'dp')
- v_wo: float32 [2, 512, 512], P(None, 'dp')
- v_w_gate: float32 [2, 512, 1536], P(None, 'dp')
- v_w_up: float32 [2, 512, 1536], P(None, 'dp')
- v_w_down: float32 [2, 1536, 512], P(None, 'dp')
Outputs:
- output 1: bfloat16 [16, 512, 512], P('rep', 'dp'), parts along dimension 0
- output 2: bfloat16 [16, 512, 128], P('rep', 'dp'), parts along dimension 0
- output 3: bfloat16 [16, 512, 128], P('rep', 'dp'), parts along dimension 0
- output 4: bfloat16 [16, 512, 512], P('rep', 'dp'), parts along dimension 0
- output 5: bfloat16 [16, 512, 1536], P('rep', 'dp'), parts along dimension 0
- output 6: bfloat16 [16, 512, 1536], P('rep', 'dp'), parts along dimension 0
- output 7: bfloat16 [16, 1536, 512], P('rep', 'dp'), parts along dimension 0
- output 8: float32 [16, 512, 512], P('rep', 'dp'), parts along dimension 0
- output 9: float32 [16, 512, 128], P('rep', 'dp'), parts along dimension 0
- output 10: float32 [16, 512, 128], P('rep', 'dp'), parts along dimension 0
- output 11: float32 [16, 512, 512], P('rep', 'dp'), parts along dimension 0
- output 12: float32 [16, 512, 1536], P('rep', 'dp'), parts along dimension 0
- output 13: float32 [16, 512, 1536], P('rep', 'dp'), parts along dimension 0
- output 14: float32 [16, 1536, 512], P('rep', 'dp'), parts along dimension 0
- output 15: float32 [16, 512, 512], P('rep', 'dp'), parts along dimension 0
- output 16: float32 [16, 512, 128], P('rep', 'dp'), parts along dimension 0
- output 17: float32 [16, 512, 128], P('rep', 'dp'), parts along dimension 0
- output 18: float32 [16, 512, 512], P('rep', 'dp'), parts along dimension 0
- output 19: float32 [16, 512, 1536], P('rep', 'dp'), parts along dimension 0
- output 20: float32 [16, 512, 1536], P('rep', 'dp'), parts along dimension 0
- output 21: float32 [16, 1536, 512], P('rep', 'dp'), parts along dimension 0
There are 8 independent parts. The reference program is written for one: setup_inputs(seed, part) draws one part's arguments, and reference() takes and returns one part's arrays. A program takes and returns all parts, laid end to end along the dimension named above; an argument that names none is the same for every part.
All inputs are finite; a program needn't handle non-finite values.
Results may differ from the reference program's by a relative error of at most 0.0257.
Values are sent between devices in bfloat16 or wider.
A program may use at most 768 MiB of HBM per device.

```python
import jax
import jax.numpy as jnp
from jax import lax

SEQUENCES = 8
TOKENS = 2048
D = 512
HEADS = 4
KV_HEADS = 1
HEAD = 128
FF = 1536
LAYERS = 2
THETA = 10000
NAMES = ("wq", "wk", "wv", "wo", "w_gate", "w_up", "w_down")
SHAPES = {
    "wq": (LAYERS, D, HEADS * HEAD),
    "wk": (LAYERS, D, KV_HEADS * HEAD),
    "wv": (LAYERS, D, KV_HEADS * HEAD),
    "wo": (LAYERS, HEADS * HEAD, D),
    "w_gate": (LAYERS, D, FF),
    "w_up": (LAYERS, D, FF),
    "w_down": (LAYERS, FF, D),
}


def bump(key, n, height):
    away = (jnp.arange(n, dtype=jnp.int32) - jax.random.randint(key, (), 0, n, jnp.int32)) % n
    return jnp.where(away < n // 8, height, 1.0)


def together(key, own, strength):
    shared = jax.random.normal(key, own.shape[1:], jnp.float32)
    return (own + strength * shared) * lax.rsqrt(1 + strength * strength)


def setup_inputs(seed: int = 0, part: int = 0) -> dict:
    kx, kdy, ka, kb, kz, kf, kh, kl, *keys = jax.random.split(jax.random.key(seed), 8 + 3 * len(NAMES))
    kx, kdy, ka, kb = (jax.random.fold_in(k, part) for k in (kx, kdy, ka, kb))
    kw, km, kv = (keys[i::3] for i in range(3))
    shape = (SEQUENCES, TOKENS, D)
    much_x, much_dy = jax.random.uniform(kz, (2,), jnp.float32, 0.0, 1.0)
    loud = 2.0 ** jax.random.uniform(jax.random.fold_in(kz, 1), (), jnp.float32, -1.0, 2.0)
    layers = 2.0 ** jax.random.uniform(kl, (LAYERS, 1, 1), jnp.float32, -1.0, 1.0)
    times = {"wq": 1.0, "wk": 1.0, "wv": 2.0, "wo": layers, "w_gate": 1.0, "w_up": bump(kh, FF, 4.0), "w_down": layers}
    x = together(ka, jax.random.normal(kx, shape, jnp.float32), much_x) * bump(kf, D, 4.0)
    dy = together(kb, jax.random.normal(kdy, shape, jnp.float32), much_dy)
    drawn = {"x": x.astype(jnp.bfloat16), "dy": (loud * dy * (SEQUENCES * TOKENS) ** -0.5).astype(jnp.bfloat16)}
    for key, name in zip(kw, NAMES, strict=True):
        drawn[name] = (jax.random.normal(key, SHAPES[name], jnp.float32) * SHAPES[name][1] ** -0.5 * times[name]).astype(jnp.bfloat16)
    for key, name in zip(km, NAMES, strict=True):
        drawn[f"m_{name}"] = 0.1 * jax.random.normal(key, SHAPES[name], jnp.float32)
    for key, name in zip(kv, NAMES, strict=True):
        drawn[f"v_{name}"] = loud * loud * jax.random.uniform(key, SHAPES[name], jnp.float32, 0.2, 0.6)
    return drawn


def matmul(a, w):
    return jnp.dot(a, w, preferred_element_type=jnp.float32).astype(jnp.bfloat16)


def normed(h):
    wide = h.astype(jnp.float32)
    scale = lax.rsqrt(jnp.mean(wide**2, -1, keepdims=True) + 1e-6)
    return (wide * scale).astype(jnp.bfloat16)


def turned(t, theta):
    half = t.shape[-1] // 2
    angle = jnp.arange(t.shape[0], dtype=jnp.float32)[:, None] * theta ** (-jnp.arange(half, dtype=jnp.float32) / half)
    cos, sin = jnp.cos(angle)[:, None], jnp.sin(angle)[:, None]
    a, b = t[..., :half].astype(jnp.float32), t[..., half:].astype(jnp.float32)
    return jnp.concatenate([a * cos - b * sin, b * cos + a * sin], -1).astype(jnp.bfloat16)


def seen_by(q, k, v):
    tokens, kv = q.shape[0], k.shape[1]
    q = q.reshape(tokens, kv, -1, q.shape[-1])
    scores = jnp.einsum("tgsd,ugd->gstu", q.astype(jnp.float32), k.astype(jnp.float32)) * q.shape[-1] ** -0.5
    place = jnp.arange(tokens)
    weights = jax.nn.softmax(jnp.where(place[:, None] >= place, scores, -jnp.inf), -1).astype(jnp.bfloat16)
    return jnp.einsum("gstu,ugd->tgsd", weights.astype(jnp.float32), v.astype(jnp.float32)).astype(jnp.bfloat16).reshape(tokens, -1)


def layer(h, w):
    a = normed(h)
    q, k = (turned(matmul(a, w[name]).reshape(h.shape[0], -1, HEAD), THETA) for name in ("wq", "wk"))
    h = h + matmul(seen_by(q, k, matmul(a, w["wv"]).reshape(h.shape[0], -1, HEAD)), w["wo"])
    b = normed(h)
    gate = jnp.dot(b, w["w_gate"], preferred_element_type=jnp.float32)
    up = jnp.dot(b, w["w_up"], preferred_element_type=jnp.float32)
    return h + matmul((jax.nn.silu(gate) * up).astype(jnp.bfloat16), w["w_down"])


def adamw(w, m, v, g):
    m = 0.9 * m + 0.1 * g
    v = 0.95 * v + 0.05 * g * g
    step = m * lax.rsqrt(v + 1e-8) + 0.1 * w
    return (w - 0.02 * step).astype(jnp.bfloat16), m, v


def stack(weights, h):
    return lax.scan(lambda h, w: (layer(h, w), None), h, weights)[0]


def reference(x, dy, wq, wk, wv, wo, w_gate, w_up, w_down, m_wq, m_wk, m_wv, m_wo, m_w_gate, m_w_up, m_w_down, v_wq, v_wk, v_wv, v_wo, v_w_gate, v_w_up, v_w_down):
    weights = dict(zip(NAMES, (wq, wk, wv, wo, w_gate, w_up, w_down), strict=True))

    def take(so_far, sequence):
        h, by_y = sequence
        _, back = jax.vjp(stack, weights, h)
        by_weights, by_h = back(by_y)
        return jax.tree.map(lambda total, term: total + term.astype(jnp.float32), so_far, by_weights), by_h

    none_yet = {name: jnp.zeros(w.shape, jnp.float32) for name, w in weights.items()}
    by_weights, by_x = lax.scan(take, none_yet, (x, dy))
    gradients = [by_weights[name].astype(jnp.bfloat16).astype(jnp.float32) for name in NAMES]
    first = (m_wq, m_wk, m_wv, m_wo, m_w_gate, m_w_up, m_w_down)
    second = (v_wq, v_wk, v_wv, v_wo, v_w_gate, v_w_up, v_w_down)
    new = [adamw(weights[name].astype(jnp.float32), m, v, g) for name, m, v, g in zip(NAMES, first, second, gradients, strict=True)]
    return tuple(one[which] for which in range(3) for one in new)
```

```python
import functools

import jax
import jax.numpy as jnp
import numpy as np
from jax import lax
from jax.experimental import pallas as pl
from jax.experimental.pallas import tpu as pltpu
from jax.sharding import PartitionSpec as P

HEAD = 128
THETA = 10000
NEG = -1e30
HIDDEN = 2 * NEG
LOG2E = 1.4426950408889634
SCALE = HEAD**-0.5
E = SCALE * LOG2E
VMEM = 66_000_000
F32, BF16 = jnp.float32, jnp.bfloat16
ANY = pl.BlockSpec(memory_space=pl.ANY)


def dot(a, b, ca=1, cb=0):
    return lax.dot_general(a, b, (((ca,), (cb,)), ((), ())), preferred_element_type=F32)


def tile(i, n):
    return pl.ds(pl.multiple_of(i * n, n), n)


def loop(n, body):
    lax.fori_loop(0, n, lambda i, _: body(i), None)


def scale_of(wide):
    return lax.rsqrt(jnp.mean(wide * wide, -1, keepdims=True) + 1e-6)


def norm_bwd(wide, scale, g):
    return scale * g - wide * (scale * scale * scale * jnp.mean(wide * g, -1, keepdims=True))


def angles(tokens):
    half = HEAD // 2
    turn = np.float32(THETA) ** (-np.arange(half, dtype=np.float32) / np.float32(half))
    angle = np.arange(tokens, dtype=np.float32)[:, None] * turn.astype(np.float32)
    return np.concatenate([np.cos(angle), np.sin(angle)], -1).astype(np.float32)


def turns(t):
    swapped = pltpu.roll(t, HEAD // 2, 1)
    first = lax.broadcasted_iota(jnp.int32, t.shape, 1) < HEAD // 2
    return jnp.where(first, t, swapped), jnp.where(first, -swapped, t)


def rotated(t, cos, sin):
    return t * cos + pltpu.roll(t, HEAD // 2, 1) * sin


def merged(w):
    return w.reshape(w.shape[0] * w.shape[1], w.shape[2])


def qkv_phase(h, w, table, q, k, v, vt, rows):
    wide_q = q.shape[1]

    def step(i):
        at = tile(i, rows)
        wide = h[at, :].astype(F32)
        a = (wide * scale_of(wide)).astype(BF16)
        y = dot(a, merged(w[...])).astype(BF16)
        cos, sin = turns(table[at, :])
        for n in range(wide_q // HEAD):
            part = slice(n * HEAD, (n + 1) * HEAD)
            q[at, part] = rotated(y[:, part].astype(F32), cos, sin).astype(BF16)
        k[at, :] = rotated(y[:, wide_q : wide_q + HEAD].astype(F32), cos, sin).astype(BF16)
        mine = y[:, wide_q + HEAD :]
        v[at, :] = mine
        vt[:, at] = mine.T

    loop(h.shape[0] // rows, step)


def spans(bq):
    half = bq // 2
    return [(0, half, 0), (half, half, half)]


def seen(keys, first_key, queries, first_query):
    key = lax.broadcasted_iota(jnp.int32, (keys, queries), 0) + first_key
    return lax.broadcasted_iota(jnp.int32, (keys, queries), 1) + first_query >= key


def attend_phase(q, k, vt, o, lse, top_s, mix_s, bq):
    heads = q.shape[1] // HEAD

    def block(iq, start, nk, lo, mask):
        here = pl.ds(start, nk)
        cols = pl.ds(pl.multiple_of(iq * bq + lo, bq - lo), bq - lo)
        keys = k[here, :]
        scores = [dot(keys, q[cols, n * HEAD : (n + 1) * HEAD], 1, 1) for n in range(heads)]
        values = jnp.concatenate([vt[:, here], jnp.ones((8, nk), BF16)], axis=0)
        for n, s in enumerate(scores):
            if mask is not None:
                s = jnp.where(mask, s, HIDDEN)
            old = top_s[n : n + 1, lo:]
            top = jnp.maximum(old, s.max(axis=0, keepdims=True))
            top_s[n : n + 1, lo:] = top
            p = jnp.exp2((s - top) * E).astype(BF16)
            mix_s[n, :, lo:] = mix_s[n, :, lo:] * jnp.exp2((old - top) * E) + dot(values, p)

    def step(iq):
        at = tile(iq, bq)
        top_s[...] = jnp.full(top_s.shape, NEG, F32)
        mix_s[...] = jnp.zeros(mix_s.shape, F32)
        loop(iq, lambda j: block(iq, pl.multiple_of(j * bq, bq), bq, 0, None))
        for first, nk, lo in spans(bq):
            block(iq, pl.multiple_of(iq * bq + first, nk), nk, lo, seen(nk, first, bq - lo, lo))
        for n in range(heads):
            total = mix_s[n, HEAD : HEAD + 1, :]
            o[at, n * HEAD : (n + 1) * HEAD] = (mix_s[n, :HEAD, :] * (1 / total)).T.astype(BF16)
            lse[n : n + 1, at] = top_s[n : n + 1, :] * E + jnp.log2(total)

    loop(q.shape[0] // bq, step)


def mid_phase(h, o, od, hm, rows, r):
    def step(i):
        at = tile(i, rows)
        hm[at, :] = h[at, :] + dot(o[at, :], merged(od[:, :r, :])).astype(BF16)

    loop(h.shape[0] // rows, step)


def ffn_phase(hm, gu, od, out, rows, r):
    def step(i):
        at = tile(i, rows)
        mid = hm[at, :]
        wide = mid.astype(F32)
        b = (wide * scale_of(wide)).astype(BF16)
        y = dot(b, merged(gu[...]))
        half = y.shape[1] // 2
        gate, up = y[:, :half], y[:, half:]
        made = (gate * (1 / (1 + jnp.exp(-gate))) * up).astype(BF16)
        out[at, :] = mid + dot(made, merged(od[:, r:, :])).astype(BF16)

    loop(hm.shape[0] // rows, step)


def ffn_bwd_phase(hm, dy, gu, od, made_s, dgu_s, bt_s, dhm, rows, r):
    def step(i):
        at = tile(i, rows)
        wide = hm[at, :].astype(F32)
        scale = scale_of(wide)
        b = (wide * scale).astype(BF16)
        bt_s[:, at] = b.T
        y = dot(b, merged(gu[...]))
        half = y.shape[1] // 2
        gate, up = y[:, :half], y[:, half:]
        back = dy[at, :]
        d_made = dot(back, merged(od[:, r:, :]), 1, 1).astype(BF16).astype(F32)
        sig = 1 / (1 + jnp.exp(-gate))
        silu = gate * sig
        made_s[at, :] = (silu * up).astype(BF16)
        dgu_s[at, :half] = (d_made * up * (sig * (1 + gate - silu))).astype(BF16)
        dgu_s[at, half:] = (d_made * silu).astype(BF16)
        db = dot(dgu_s[at, :], merged(gu[...]), 1, 1).astype(BF16).astype(F32)
        dhm[at, :] = (back.astype(F32) + norm_bwd(wide, scale, db)).astype(BF16)

    loop(hm.shape[0] // rows, step)


def ffn_weights_phase(made_s, dgu_s, bt_s, dy, p_gu, p_od, wide, r):
    n = p_gu.shape[0]

    def units(i):
        part = tile(i, wide)
        p_gu[:, :, part] = dot(bt_s[...], dgu_s[:, part]).astype(BF16).reshape(n, -1, wide)

    loop(dgu_s.shape[1] // wide, units)
    share = p_od.shape[1] - r
    group = 2
    def downs(i):
        got = dot(made_s[:, tile(i, group * share)], dy[...], 0, 0).astype(BF16)
        p_od[pl.ds(i * group, group), r:, :] = got.reshape(group, share, -1)

    loop(n // group, downs)


def out_bwd_phase(dhm, o, od, p_od, do, rows, r):
    def step(i):
        at = tile(i, rows)
        do[at, :] = dot(dhm[at, :], merged(od[:, :r, :]), 1, 1).astype(BF16)

    loop(dhm.shape[0] // rows, step)
    p_od[:, :r, :] = dot(o[...], dhm[...], 0, 0).astype(BF16).reshape(p_od.shape[0], r, -1)


def attend_bwd_phase(q, k, v, o, do, lse, table, dqkv, dq_s, dk_s, dv_s, kt_s, bq):
    heads = q.shape[1] // HEAD
    wide_q = q.shape[1]
    dk_s[...] = jnp.zeros(dk_s.shape, F32)
    dv_s[...] = jnp.zeros(dv_s.shape, F32)
    kt_s[...] = k[...].T

    def block(iq, start, nk, lo, mask, lses, deltas):
        here = pl.ds(start, nk)
        cols = pl.ds(pl.multiple_of(iq * bq + lo, bq - lo), bq - lo)
        keys, values, keys_t = k[here, :], v[here, :], kt_s[:, here]
        qs = [q[cols, n * HEAD : (n + 1) * HEAD] for n in range(heads)]
        dos = [do[cols, n * HEAD : (n + 1) * HEAD] for n in range(heads)]
        scores = [dot(keys, x, 1, 1) for x in qs]
        dps = [dot(values, x, 1, 1) for x in dos]
        for n in range(heads):
            p = jnp.exp2(scores[n] * E - lses[n][:, lo:])
            if mask is not None:
                p = jnp.where(mask, p, 0.0)
            ds = (p * (dps[n] - deltas[n][:, lo:])).astype(BF16)
            dv_s[here, :] += dot(p.astype(BF16), dos[n])
            dk_s[here, :] += dot(ds, qs[n])
            dq_s[n, :, lo:] += dot(keys_t, ds)

    def step(iq):
        at = tile(iq, bq)
        dq_s[...] = jnp.zeros(dq_s.shape, F32)
        lses = [lse[n : n + 1, at] for n in range(heads)]
        deltas = []
        for n in range(heads):
            part = slice(n * HEAD, (n + 1) * HEAD)
            deltas.append((do[at, part].astype(F32) * o[at, part].astype(F32)).T.sum(axis=0, keepdims=True))
        loop(iq, lambda j: block(iq, pl.multiple_of(j * bq, bq), bq, 0, None, lses, deltas))
        for first, nk, lo in spans(bq):
            block(iq, pl.multiple_of(iq * bq + first, nk), nk, lo, seen(nk, first, bq - lo, lo), lses, deltas)
        cos, sin = turns(table[at, :])
        for n in range(heads):
            back = (dq_s[n] * SCALE).T.astype(BF16).astype(F32)
            dqkv[at, n * HEAD : (n + 1) * HEAD] = rotated(back, cos, -sin).astype(BF16)

    loop(q.shape[0] // bq, step)

    def finish(i):
        at = tile(i, bq)
        cos, sin = turns(table[at, :])
        dqkv[at, wide_q : wide_q + HEAD] = rotated((dk_s[at, :] * SCALE).astype(BF16).astype(F32), cos, -sin).astype(BF16)
        dqkv[at, wide_q + HEAD :] = dv_s[at, :].astype(BF16)

    loop(q.shape[0] // bq, finish)


def qkv_bwd_phase(h, dqkv, w, dhm, p_qkv, a_s, dh, rows):
    def step(i):
        at = tile(i, rows)
        wide = h[at, :].astype(F32)
        scale = scale_of(wide)
        a_s[at, :] = (wide * scale).astype(BF16)
        if dh is not None:
            da = dot(dqkv[at, :], merged(w[...]), 1, 1).astype(BF16).astype(F32)
            dh[at, :] = (dhm[at, :].astype(F32) + norm_bwd(wide, scale, da)).astype(BF16)

    loop(h.shape[0] // rows, step)
    p_qkv[...] = dot(a_s[...], dqkv[...], 0, 0).astype(BF16).reshape(p_qkv.shape)


def forward(sizes, x, table, qkv, gu, od, q_o, k_o, v_o, o_o, lse_o, hm_o, h_o,
            h_s, table_s, qkv_s, gu_s, od_s, q_s, k_s, v_s, vt_s, o_s, lse_s, hm_s, top_s, mix_s, in_sem, out_sem):
    layers, r, bq, rows = sizes
    start = pltpu.make_async_copy(x, h_s.at[0], in_sem.at[0])
    start.start()
    brought = [start, pltpu.make_async_copy(table, table_s, in_sem.at[1])]
    brought[1].start()
    n = 2
    for i in range(layers):
        for src, dst in ((qkv, qkv_s), (od, od_s), (gu, gu_s)):
            brought.append(pltpu.make_async_copy(src.at[:, i], dst.at[i], in_sem.at[n]))
            brought[-1].start()
            n += 1
    out = []

    def keep(src, dst):
        out.append(pltpu.make_async_copy(src, dst, out_sem.at[len(out)]))
        out[-1].start()

    brought[0].wait()
    brought[1].wait()
    for i in range(layers):
        brought[2 + 3 * i].wait()
        qkv_phase(h_s.at[i], qkv_s.at[i], table_s, q_s.at[i], k_s.at[i], v_s.at[i], vt_s, rows)
        keep(q_s.at[i], q_o.at[i])
        keep(k_s.at[i], k_o.at[i])
        keep(v_s.at[i], v_o.at[i])
        attend_phase(q_s.at[i], k_s.at[i], vt_s, o_s.at[i], lse_s.at[i], top_s, mix_s, bq)
        keep(o_s.at[i], o_o.at[i])
        keep(lse_s.at[i], lse_o.at[i])
        brought[3 + 3 * i].wait()
        mid_phase(h_s.at[i], o_s.at[i], od_s.at[i], hm_s.at[i], rows, r)
        keep(hm_s.at[i], hm_o.at[i])
        brought[4 + 3 * i].wait()
        if i + 1 < layers:
            ffn_phase(hm_s.at[i], gu_s.at[i], od_s.at[i], h_s.at[i + 1], rows, r)
            keep(h_s.at[i + 1], h_o.at[i])
    for copy in out:
        copy.wait()


def backward(sizes, x, dy, table, qkv, gu, od, q, k, v, o, lse, hm, h, qkv_g, gu_g, od_g,
             table_s, qkv_s, gu_s, od_s, q_s, k_s, v_s, o_s, lse_s, hm_s, h_s, dh_s, dhm_s, made_s, dgu_s, bt_s, dq_s, dk_s, dv_s, kt_s,
             p_qkv, p_gu, p_od, in_sem, out_sem):
    layers, r, bq, rows, wide = sizes
    split = p_qkv.shape[2]
    dqkv_s, do_s = made_s.at[:, :split], made_s.at[:, split : split + q_s.shape[1]]
    flying = {}

    def bring(name, src, dst):
        flying[name] = pltpu.make_async_copy(src, dst, in_sem.at[sorted(NAMED).index(name)])
        flying[name].start()

    def attention_inputs(i):
        for name, src, dst in (("q", q, q_s), ("k", k, k_s), ("v", v, v_s), ("o", o, o_s), ("lse", lse, lse_s)):
            bring(name, src.at[i], dst)
        bring("h", x if i == 0 else h.at[i - 1], h_s)

    last = layers - 1
    bring("gu", gu.at[:, last], gu_s)
    bring("hm", hm.at[last], hm_s)
    bring("dy", dy, dh_s)
    bring("od", od.at[:, last], od_s)
    bring("table", table, table_s)
    attention_inputs(last)
    bring("qkv", qkv.at[:, last], qkv_s)
    out = []

    def send(src, dst):
        out.append(pltpu.make_async_copy(src, dst, out_sem.at[len(out)]))
        out[-1].start()

    for i in reversed(range(layers)):
        for name in ("gu", "hm", "od"):
            flying[name].wait()
        if i == last:
            flying["dy"].wait()
        ffn_bwd_phase(hm_s, dh_s, gu_s, od_s, made_s, dgu_s, bt_s, dhm_s, rows, r)
        if i:
            bring("gu", gu.at[:, i - 1], gu_s)
            bring("hm", hm.at[i - 1], hm_s)
        else:
            for copy in out:
                copy.wait()
        ffn_weights_phase(made_s, dgu_s, bt_s, dh_s, p_gu, p_od, wide, r)
        send(p_gu, gu_g.at[i])
        flying["o"].wait()
        out_bwd_phase(dhm_s, o_s, od_s, p_od, do_s, rows, r)
        send(p_od, od_g.at[i])
        if i:
            bring("od", od.at[:, i - 1], od_s)
        for name in ("q", "k", "v", "lse") + (("table",) if i == last else ()):
            flying[name].wait()
        attend_bwd_phase(q_s, k_s, v_s, o_s, do_s, lse_s, table_s, dqkv_s, dq_s, dk_s, dv_s, kt_s, bq)
        flying["h"].wait()
        if i == last:
            flying["qkv"].wait()
        qkv_bwd_phase(h_s, dqkv_s, qkv_s, dhm_s, p_qkv, do_s, dh_s if i else None, rows)
        send(p_qkv, qkv_g.at[i])
        if i:
            attention_inputs(i - 1)
    for copy in out[-3:]:
        copy.wait()


NAMED = ("gu", "hm", "dy", "od", "table", "q", "k", "v", "o", "lse", "h", "qkv")


def adamw(w, m, v, g):
    m = 0.9 * m + 0.1 * g
    v = 0.95 * v + 0.05 * g * g
    step = m * lax.rsqrt(v + 1e-8) + 0.1 * w
    return (w - 0.02 * step).astype(BF16), m, v


def solution(mesh):
    n = mesh.shape["dp"]

    def step(x, dy, *arrays):
        weights, m, v = (arrays[i : i + 7] for i in (0, 7, 14))
        wq, wk, wv, wo, wg, wu, wd = weights
        layers, r, wide_q = wq.shape
        x, dy = x[0], dy[0]
        tokens, d = x.shape
        ff = wg.shape[2]
        bq, rows = min(512, tokens), min(256, tokens)
        packs = [jnp.concatenate(p, a) for p, a in (((wq, wk, wv), 2), ((wg, wu), 2), ((wo, wd), 1))]
        qkv, gu, od = (lax.all_gather(p, "dp") for p in packs)
        table = jnp.asarray(angles(tokens))
        wide = qkv.shape[3]
        heads = wide_q // HEAD
        ro = wo.shape[1]
        both = lambda *s: jax.ShapeDtypeStruct((layers, *s), BF16)
        q, k, v_, o, lse, hm, h = pl.pallas_call(
            functools.partial(forward, (layers, ro, bq, rows)),
            out_shape=[both(tokens, wide_q), both(tokens, HEAD), both(tokens, HEAD), both(tokens, wide_q),
                       jax.ShapeDtypeStruct((layers, 8, tokens), F32), both(tokens, d), jax.ShapeDtypeStruct((max(layers - 1, 1), tokens, d), BF16)],
            in_specs=[ANY] * 5,
            out_specs=[ANY] * 7,
            scratch_shapes=[
                pltpu.VMEM((layers, tokens, d), BF16), pltpu.VMEM((tokens, HEAD), F32),
                pltpu.VMEM((layers, n, r, wide), BF16), pltpu.VMEM((layers, n, r, 2 * ff), BF16), pltpu.VMEM((layers, n, od.shape[2], d), BF16),
                pltpu.VMEM((layers, tokens, wide_q), BF16), pltpu.VMEM((layers, tokens, HEAD), BF16), pltpu.VMEM((layers, tokens, HEAD), BF16),
                pltpu.VMEM((HEAD, tokens), BF16), pltpu.VMEM((layers, tokens, wide_q), BF16), pltpu.VMEM((layers, 8, tokens), F32),
                pltpu.VMEM((layers, tokens, d), BF16), pltpu.VMEM((heads, bq), F32), pltpu.VMEM((heads, HEAD + 8, bq), F32),
                pltpu.SemaphoreType.DMA((2 + 3 * layers,)), pltpu.SemaphoreType.DMA((7 * layers,)),
            ],
            compiler_params=pltpu.CompilerParams(vmem_limit_bytes=VMEM),
            name="forward",
        )(x, table, qkv, gu, od)
        grad = lambda a: jax.ShapeDtypeStruct((layers, n, *a.shape[2:]), BF16)
        grads = pl.pallas_call(
            functools.partial(backward, (layers, ro, bq, rows, 512)),
            out_shape=[grad(qkv), grad(gu), grad(od)],
            in_specs=[ANY] * 13,
            out_specs=[ANY] * 3,
            scratch_shapes=[
                pltpu.VMEM((tokens, HEAD), F32),
                pltpu.VMEM((n, r, wide), BF16), pltpu.VMEM((n, r, 2 * ff), BF16), pltpu.VMEM((n, od.shape[2], d), BF16),
                pltpu.VMEM((tokens, wide_q), BF16), pltpu.VMEM((tokens, HEAD), BF16), pltpu.VMEM((tokens, HEAD), BF16),
                pltpu.VMEM((tokens, wide_q), BF16), pltpu.VMEM((8, tokens), F32), pltpu.VMEM((tokens, d), BF16), pltpu.VMEM((tokens, d), BF16),
                pltpu.VMEM((tokens, d), BF16), pltpu.VMEM((tokens, d), BF16),
                pltpu.VMEM((tokens, ff), BF16), pltpu.VMEM((tokens, 2 * ff), BF16), pltpu.VMEM((d, tokens), BF16),
                pltpu.VMEM((heads, HEAD, bq), F32), pltpu.VMEM((tokens, HEAD), F32), pltpu.VMEM((tokens, HEAD), F32), pltpu.VMEM((HEAD, tokens), BF16),
                pltpu.VMEM((n, r, wide), BF16), pltpu.VMEM((n, r, 2 * ff), BF16), pltpu.VMEM((n, od.shape[2], d), BF16),
                pltpu.SemaphoreType.DMA((len(NAMED),)), pltpu.SemaphoreType.DMA((3 * layers,)),
            ],
            compiler_params=pltpu.CompilerParams(vmem_limit_bytes=VMEM),
            name="backward",
        )(x, dy, table, qkv, gu, od, q, k, v_, o, lse, hm, h)
        summed = lambda g: lax.psum_scatter(g.reshape(layers, -1, g.shape[3]), "dp", scatter_dimension=1, tiled=True).astype(F32)
        g_qkv, g_gu, g_od = (summed(g) for g in grads)
        gradients = [g_qkv[..., :wide_q], g_qkv[..., wide_q : wide_q + HEAD], g_qkv[..., wide_q + HEAD :], g_od[:, :ro], g_gu[..., :ff], g_gu[..., ff:], g_od[:, ro:]]
        new = [adamw(w.astype(F32), mm, vv, g) for w, mm, vv, g in zip(weights, m, v, gradients, strict=True)]
        return tuple(one[which] for which in range(3) for one in new)

    states, cut = P(("rep", "dp"), None, None), P(None, "dp", None)
    return jax.shard_map(
        step,
        mesh=mesh,
        in_specs=(states, states) + (cut,) * 21,
        out_specs=(P("rep", "dp", None),) * 21,
        check_vma=False,
    )
```

```python
import functools

import jax
import jax.numpy as jnp
import numpy as np
from jax import lax
from jax.experimental import pallas as pl
from jax.experimental.pallas import tpu as pltpu
from jax.sharding import PartitionSpec as P

HEAD = 128
THETA = 10000
NEG = -1e30
HIDDEN = 2 * NEG
LOG2E = 1.4426950408889634
SCALE = HEAD**-0.5
E = SCALE * LOG2E
VMEM = 66_000_000
F32, BF16 = jnp.float32, jnp.bfloat16
ANY = pl.BlockSpec(memory_space=pl.ANY)
MESH = pl.DeviceIdType.MESH


def dot(a, b, ca=1, cb=0):
    return lax.dot_general(a, b, (((ca,), (cb,)), ((), ())), preferred_element_type=F32)


def tile(i, n):
    return pl.ds(pl.multiple_of(i * n, n), n)


def loop(n, body):
    lax.fori_loop(0, n, lambda i, _: body(i), None)


def polled(events, i):
    for when, what in events.items():
        pl.when(i == when)(what)


def the_rest(events, steps):
    for when, what in events.items():
        if when >= steps:
            what()


def scale_of(wide):
    return lax.rsqrt(jnp.mean(wide * wide, -1, keepdims=True) + 1e-6)


def norm_bwd(wide, scale, g):
    return scale * g - wide * (scale * scale * scale * jnp.mean(wide * g, -1, keepdims=True))


def angles(tokens):
    half = HEAD // 2
    turn = np.float32(THETA) ** (-np.arange(half, dtype=np.float32) / np.float32(half))
    angle = np.arange(tokens, dtype=np.float32)[:, None] * turn.astype(np.float32)
    return np.concatenate([np.cos(angle), np.sin(angle)], -1).astype(np.float32)


def turns(t):
    swapped = pltpu.roll(t, HEAD // 2, 1)
    first = lax.broadcasted_iota(jnp.int32, t.shape, 1) < HEAD // 2
    return jnp.where(first, t, swapped), jnp.where(first, -swapped, t)


def rotated(t, cos, sin):
    return t * cos + pltpu.roll(t, HEAD // 2, 1) * sin


class Ring:
    def __init__(self, n):
        self.n, self.far_a = n, n // 2
        self.far_b = n - 1 - self.far_a
        self.me = lax.axis_index("dp")
        rep = lax.axis_index("rep")
        self.core = lax.rem(rep, 2)
        self.partner = {"rep": rep + 1 - 2 * self.core}
        self.turn = 1 - 2 * self.core

    def at(self, k):
        return lax.rem(self.me + self.n + k * self.turn, self.n)

    def to(self, k):
        return {"dp": self.at(k)}

    def meet(self, partner):
        barrier = pltpu.get_barrier_semaphore()
        others = [self.to(1), self.to(-1)] + [self.partner] * partner
        for other in others:
            pl.semaphore_signal(barrier, inc=1, device_id=other, device_id_type=MESH)
        pl.semaphore_wait(barrier, len(others))


def remote(src, dst, send, recv, to):
    return pltpu.make_async_remote_copy(src_ref=src, dst_ref=dst, send_sem=send, recv_sem=recv, device_id=to, device_id_type=MESH)


class Gather:
    def __init__(self, ring, buf, sems):
        self.ring, self.buf, self.sems = ring, buf, sems
        self.half = buf.shape[1] // 2

    def piece(self, block, half):
        return self.buf.at[block, pl.ds(pl.multiple_of(half * self.half, self.half), self.half), :]

    def copy(self, chain, step, block, to):
        part = self.piece(block, self.ring.core)
        return remote(part, part, self.sems.at[2 * chain, step], self.sems.at[2 * chain + 1, step], to)

    def hop(self, chain, step):
        ring = self.ring
        return self.copy(chain, step, ring.at(-step if chain == 0 else step), ring.to(1 if chain == 0 else -1))

    def arriving(self, chain, step):
        ring = self.ring
        return self.copy(chain, step, ring.at(-step - 1 if chain == 0 else step + 1), ring.to(1 if chain == 0 else -1))

    def handed(self, chain, step):
        ring = self.ring
        block = ring.at(-step - 1 if chain == 0 else step + 1)
        return self.copy(2, step + chain * ring.far_a, block, ring.partner)

    def begin(self):
        self.hop(0, 0).start()
        self.hop(1, 0).start()

    def step(self, s):
        for chain, far in ((0, self.ring.far_a), (1, self.ring.far_b)):
            if s <= far:
                self.arriving(chain, s - 1).wait_recv()
                if s < far:
                    self.hop(chain, s).start()
                self.handed(chain, s - 1).start()

    def complete(self):
        ring = self.ring
        for chain, far in ((0, ring.far_a), (1, ring.far_b)):
            for step in range(far):
                part = self.piece(ring.at(step + 1 if chain == 0 else -step - 1), 1 - ring.core)
                i = step + chain * ring.far_a
                remote(part, part, self.sems.at[4, i], self.sems.at[5, i], ring.partner).wait_recv()

    def drain(self):
        for chain, far in ((0, self.ring.far_a), (1, self.ring.far_b)):
            for step in range(far):
                self.hop(chain, step).wait_send()
                self.handed(chain, step).wait_send()


class Scatter:
    def __init__(self, ring, p, came_a, came_b, sems, free, got):
        self.ring, self.p, self.came, self.sems, self.free, self.got = ring, p, (came_a, came_b), sems, free, got

    def far(self, chain):
        return self.ring.far_b if chain else self.ring.far_a

    def hop(self, chain, step):
        ring = self.ring
        left = self.far(chain) - step
        block = ring.at(left if chain == 0 else -left)
        return remote(self.p.at[block], self.came[chain].at[step], self.sems.at[2 * chain, step], self.sems.at[2 * chain + 1, step],
                      ring.to(1 if chain == 0 else -1))

    def added(self, chain, step):
        ring = self.ring
        left = self.far(chain) - step
        block = ring.at(left if chain == 0 else -left)
        few = 16

        def rows(i):
            at = tile(i, few)
            self.p[block, at, :] = (self.p[block, at, :].astype(F32) + self.came[chain][step - 1, at, :].astype(F32)).astype(BF16)

        loop(self.p.shape[1] // few, rows)

    def begin(self, wait):
        if wait:
            pl.semaphore_wait(self.free, 2)
        self.hop(0, 0).start()
        self.hop(1, 0).start()

    def step(self, s):
        going = [chain for chain in (0, 1) if s < self.far(chain)]
        for chain in (0, 1):
            if s <= self.far(chain):
                self.hop(chain, s - 1).wait_recv()
            if chain in going:
                self.added(chain, s)
        for chain in going:
            self.hop(chain, s).start()
        if s == self.ring.far_a:
            self.end()

    def end(self):
        me, few = self.ring.me, 16
        last_a, last_b = self.ring.far_a - 1, self.ring.far_b - 1

        def rows(i):
            at = tile(i, few)
            total = self.came[0][last_a, at, :].astype(F32) + self.came[1][last_b, at, :].astype(F32) + self.p[me, at, :].astype(F32)
            self.got[at, :] = total.astype(BF16)

        loop(self.p.shape[1] // few, rows)

    def close(self, signal):
        for chain in (0, 1):
            for step in range(self.far(chain)):
                self.hop(chain, step).wait_send()
        if signal:
            for k in (1, -1):
                pl.semaphore_signal(self.free, inc=1, device_id=self.ring.to(k), device_id_type=MESH)


def merged(w):
    return w.reshape(w.shape[0] * w.shape[1], w.shape[2])


def qkv_phase(h, w, table, q, k, v, vt, rows):
    wide_q = q.shape[1]

    def step(i):
        at = tile(i, rows)
        wide = h[at, :].astype(F32)
        a = (wide * scale_of(wide)).astype(BF16)
        y = dot(a, merged(w[...])).astype(BF16)
        cos, sin = turns(table[at, :])
        for n in range(wide_q // HEAD):
            part = slice(n * HEAD, (n + 1) * HEAD)
            q[at, part] = rotated(y[:, part].astype(F32), cos, sin).astype(BF16)
        k[at, :] = rotated(y[:, wide_q : wide_q + HEAD].astype(F32), cos, sin).astype(BF16)
        mine = y[:, wide_q + HEAD :]
        v[at, :] = mine
        vt[:, at] = mine.T

    loop(h.shape[0] // rows, step)


def spans(bq):
    half = bq // 2
    return [(0, half, 0), (half, half, half)]


def seen(keys, first_key, queries, first_query):
    key = lax.broadcasted_iota(jnp.int32, (keys, queries), 0) + first_key
    return lax.broadcasted_iota(jnp.int32, (keys, queries), 1) + first_query >= key


def blocks(tokens, bq):
    return (tokens // bq) * (tokens // bq + 1) // 2


def row_of_blocks(iq, bq, block, events):
    def step(j):
        @pl.when(j < iq)
        def _():
            block(pl.multiple_of(j * bq, bq), bq, 0, None)

        @pl.when(j == iq)
        def _():
            for first, nk, lo in spans(bq):
                block(pl.multiple_of(iq * bq + first, nk), nk, lo, seen(nk, first, bq - lo, lo))

        polled(events, lax.div(iq * (iq + 1), 2) + j)

    loop(iq + 1, step)


def attend_phase(q, k, vt, o, lse, top_s, mix_s, bq, events):
    heads = q.shape[1] // HEAD

    def block(iq, start, nk, lo, mask):
        here = pl.ds(start, nk)
        cols = pl.ds(pl.multiple_of(iq * bq + lo, bq - lo), bq - lo)
        keys = k[here, :]
        scores = [dot(keys, q[cols, n * HEAD : (n + 1) * HEAD], 1, 1) for n in range(heads)]
        values = jnp.concatenate([vt[:, here], jnp.ones((8, nk), BF16)], axis=0)
        for n, s in enumerate(scores):
            if mask is not None:
                s = jnp.where(mask, s, HIDDEN)
            old = top_s[n : n + 1, lo:]
            top = jnp.maximum(old, s.max(axis=0, keepdims=True))
            top_s[n : n + 1, lo:] = top
            p = jnp.exp2((s - top) * E).astype(BF16)
            mix_s[n, :, lo:] = mix_s[n, :, lo:] * jnp.exp2((old - top) * E) + dot(values, p)

    def step(iq):
        at = tile(iq, bq)
        top_s[...] = jnp.full(top_s.shape, NEG, F32)
        mix_s[...] = jnp.zeros(mix_s.shape, F32)
        row_of_blocks(iq, bq, functools.partial(block, iq), events)
        for n in range(heads):
            total = mix_s[n, HEAD : HEAD + 1, :]
            o[at, n * HEAD : (n + 1) * HEAD] = (mix_s[n, :HEAD, :] * (1 / total)).T.astype(BF16)
            lse[n : n + 1, at] = top_s[n : n + 1, :] * E + jnp.log2(total)

    loop(q.shape[0] // bq, step)
    the_rest(events, blocks(q.shape[0], bq))


def mid_phase(h, o, od, hm, rows, r):
    def step(i):
        at = tile(i, rows)
        hm[at, :] = h[at, :] + dot(o[at, :], merged(od[:, :r, :])).astype(BF16)

    loop(h.shape[0] // rows, step)


def ffn_phase(hm, gu, od, out, rows, r, events):
    def step(i):
        at = tile(i, rows)
        mid = hm[at, :]
        wide = mid.astype(F32)
        b = (wide * scale_of(wide)).astype(BF16)
        y = dot(b, merged(gu[...]))
        half = y.shape[1] // 2
        gate, up = y[:, :half], y[:, half:]
        made = (gate * (1 / (1 + jnp.exp(-gate))) * up).astype(BF16)
        out[at, :] = mid + dot(made, merged(od[:, r:, :])).astype(BF16)
        polled(events, i)

    loop(hm.shape[0] // rows, step)
    the_rest(events, hm.shape[0] // rows)


def ffn_bwd_phase(hm, dy, gu, od, made_s, dgu_s, bt_s, dhm, rows, r, events):
    def step(i):
        at = tile(i, rows)
        wide = hm[at, :].astype(F32)
        scale = scale_of(wide)
        b = (wide * scale).astype(BF16)
        bt_s[:, at] = b.T
        y = dot(b, merged(gu[...]))
        half = y.shape[1] // 2
        gate, up = y[:, :half], y[:, half:]
        back = dy[at, :]
        d_made = dot(back, merged(od[:, r:, :]), 1, 1).astype(BF16).astype(F32)
        sig = 1 / (1 + jnp.exp(-gate))
        silu = gate * sig
        made_s[at, :] = (silu * up).astype(BF16)
        dgu_s[at, :half] = (d_made * up * (sig * (1 + gate - silu))).astype(BF16)
        dgu_s[at, half:] = (d_made * silu).astype(BF16)
        db = dot(dgu_s[at, :], merged(gu[...]), 1, 1).astype(BF16).astype(F32)
        dhm[at, :] = (back.astype(F32) + norm_bwd(wide, scale, db)).astype(BF16)
        polled(events, i)

    loop(hm.shape[0] // rows, step)
    the_rest(events, hm.shape[0] // rows)


def units_phase(dgu_s, bt_s, p_gu, wide):
    n = p_gu.shape[0]

    def units(i):
        part = tile(i, wide)
        p_gu[:, :, part] = dot(bt_s[...], dgu_s[:, part]).astype(BF16).reshape(n, -1, wide)

    loop(dgu_s.shape[1] // wide, units)


def downs_phase(made_s, dy, p_od, r):
    n, share, group = p_od.shape[0], p_od.shape[1] - r, 2

    def downs(i):
        got = dot(made_s[:, tile(i, group * share)], dy[...], 0, 0).astype(BF16)
        p_od[pl.ds(i * group, group), r:, :] = got.reshape(group, share, -1)

    loop(n // group, downs)


def out_bwd_phase(dhm, o, od, p_od, do, rows, r):
    def step(i):
        at = tile(i, rows)
        do[at, :] = dot(dhm[at, :], merged(od[:, :r, :]), 1, 1).astype(BF16)

    loop(dhm.shape[0] // rows, step)
    p_od[:, :r, :] = dot(o[...], dhm[...], 0, 0).astype(BF16).reshape(p_od.shape[0], r, -1)


def attend_bwd_phase(q, k, v, o, do, lse, table, dqkv, dq_s, dk_s, dv_s, kt_s, bq, events):
    heads = q.shape[1] // HEAD
    wide_q = q.shape[1]
    dk_s[...] = jnp.zeros(dk_s.shape, F32)
    dv_s[...] = jnp.zeros(dv_s.shape, F32)
    kt_s[...] = k[...].T

    def block(iq, lses, deltas, start, nk, lo, mask):
        here = pl.ds(start, nk)
        cols = pl.ds(pl.multiple_of(iq * bq + lo, bq - lo), bq - lo)
        keys, values, keys_t = k[here, :], v[here, :], kt_s[:, here]
        qs = [q[cols, n * HEAD : (n + 1) * HEAD] for n in range(heads)]
        dos = [do[cols, n * HEAD : (n + 1) * HEAD] for n in range(heads)]
        scores = [dot(keys, x, 1, 1) for x in qs]
        dps = [dot(values, x, 1, 1) for x in dos]
        for n in range(heads):
            p = jnp.exp2(scores[n] * E - lses[n][:, lo:])
            if mask is not None:
                p = jnp.where(mask, p, 0.0)
            ds = (p * (dps[n] - deltas[n][:, lo:])).astype(BF16)
            dv_s[here, :] += dot(p.astype(BF16), dos[n])
            dk_s[here, :] += dot(ds, qs[n])
            dq_s[n, :, lo:] += dot(keys_t, ds)

    def step(iq):
        at = tile(iq, bq)
        dq_s[...] = jnp.zeros(dq_s.shape, F32)
        lses = [lse[n : n + 1, at] for n in range(heads)]
        deltas = []
        for n in range(heads):
            part = slice(n * HEAD, (n + 1) * HEAD)
            deltas.append((do[at, part].astype(F32) * o[at, part].astype(F32)).T.sum(axis=0, keepdims=True))
        row_of_blocks(iq, bq, functools.partial(block, iq, lses, deltas), events)
        cos, sin = turns(table[at, :])
        for n in range(heads):
            back = (dq_s[n] * SCALE).T.astype(BF16).astype(F32)
            dqkv[at, n * HEAD : (n + 1) * HEAD] = rotated(back, cos, -sin).astype(BF16)

    loop(q.shape[0] // bq, step)
    the_rest(events, blocks(q.shape[0], bq))

    def finish(i):
        at = tile(i, bq)
        cos, sin = turns(table[at, :])
        dqkv[at, wide_q : wide_q + HEAD] = rotated((dk_s[at, :] * SCALE).astype(BF16).astype(F32), cos, -sin).astype(BF16)
        dqkv[at, wide_q + HEAD :] = dv_s[at, :].astype(BF16)

    loop(q.shape[0] // bq, finish)


def qkv_bwd_phase(h, dqkv, w, dhm, p_qkv, a_s, dh, rows):
    def step(i):
        at = tile(i, rows)
        wide = h[at, :].astype(F32)
        scale = scale_of(wide)
        a_s[at, :] = (wide * scale).astype(BF16)
        if dh is not None:
            da = dot(dqkv[at, :], merged(w[...]), 1, 1).astype(BF16).astype(F32)
            dh[at, :] = (dhm[at, :].astype(F32) + norm_bwd(wide, scale, da)).astype(BF16)

    loop(h.shape[0] // rows, step)
    p_qkv[...] = dot(a_s[...], dqkv[...], 0, 0).astype(BF16).reshape(p_qkv.shape)


def forward(sizes, x, table, wq, wk, wv, wo, wg, wu, wd, q_o, k_o, v_o, o_o, lse_o, hm_o, h_o, qkv_o, gu_o, od_o,
            h_s, table_s, qkv_s, gu_s, od_s, q_s, k_s, v_s, vt_s, o_s, lse_s, hm_s, top_s, mix_s, own_sem, in_sem, out_sem, gather_sems):
    layers, n, bq, rows = sizes
    ring = Ring(n)
    me = ring.me
    wide_q, ff, ro = wq.shape[2], wg.shape[2], wo.shape[1]
    own = []

    def fetch(i, group, pieces):
        for src, dst in pieces:
            own.append((i, group, pltpu.make_async_copy(src, dst, own_sem.at[len(own)])))
            own[-1][2].start()

    def arrived(i, group):
        for copy in [c for j, g, c in own if (j, g) == (i, group)]:
            copy.wait()

    for i in range(layers):
        fetch(i, 0, [(wq.at[i], qkv_s.at[i, me, :, :wide_q]), (wk.at[i], qkv_s.at[i, me, :, wide_q : wide_q + HEAD]), (wv.at[i], qkv_s.at[i, me, :, wide_q + HEAD :])])
        if i == 0:
            brought = [pltpu.make_async_copy(x, h_s.at[0], in_sem.at[0]), pltpu.make_async_copy(table, table_s, in_sem.at[1])]
            for copy in brought:
                copy.start()
        fetch(i, 1, [(wo.at[i], od_s.at[i, me, :ro, :]), (wd.at[i], od_s.at[i, me, ro:, :])])
        fetch(i, 2, [(wg.at[i], gu_s.at[i, me, :, :ff]), (wu.at[i], gu_s.at[i, me, :, ff:])])
    packs = [[Gather(ring, buf.at[i], gather_sems.at[3 * i + g]) for g, buf in enumerate((qkv_s, od_s, gu_s))] for i in range(layers)]
    out = []

    def keep(src, dst):
        out.append(pltpu.make_async_copy(src, dst, out_sem.at[len(out)]))
        out[-1].start()

    def begin(i, group):
        arrived(i, group)
        packs[i][group].begin()

    def together(*whats):
        def run():
            for what in whats:
                what()

        return run

    far = ring.far_a
    ring.meet(1)
    begin(0, 0)
    for s in range(1, far + 1):
        packs[0][0].step(s)
    begin(0, 1)
    begin(0, 2)
    for copy in brought:
        copy.wait()
    for i in range(layers):
        qkv, od, gu = packs[i]
        qkv.complete()
        keep(qkv_s.at[i], qkv_o.at[i])
        qkv_phase(h_s.at[i], qkv_s.at[i], table_s, q_s.at[i], k_s.at[i], v_s.at[i], vt_s, rows)
        keep(q_s.at[i], q_o.at[i])
        keep(k_s.at[i], k_o.at[i])
        keep(v_s.at[i], v_o.at[i])
        events = {2 * (s - 1) + g: functools.partial(pack.step, s) for s in range(1, far + 1) for g, pack in enumerate((od, gu))}
        attend_phase(q_s.at[i], k_s.at[i], vt_s, o_s.at[i], lse_s.at[i], top_s, mix_s, bq, events)
        keep(o_s.at[i], o_o.at[i])
        keep(lse_s.at[i], lse_o.at[i])
        if i + 1 < layers:
            begin(i + 1, 0)
        od.complete()
        keep(od_s.at[i], od_o.at[i])
        mid_phase(h_s.at[i], o_s.at[i], od_s.at[i], hm_s.at[i], rows, ro)
        keep(hm_s.at[i], hm_o.at[i])
        gu.complete()
        keep(gu_s.at[i], gu_o.at[i])
        if i + 1 < layers:
            later = packs[i + 1][0]
            events = {2 * s - 1: functools.partial(later.step, s) for s in range(1, far + 1)}
            events[2 * far - 3] = together(events[2 * far - 3], functools.partial(begin, i + 1, 1), functools.partial(begin, i + 1, 2))
            ffn_phase(hm_s.at[i], gu_s.at[i], od_s.at[i], h_s.at[i + 1], rows, ro, events)
            keep(h_s.at[i + 1], h_o.at[i])
    for copy in out:
        copy.wait()
    for pack in sum(packs, []):
        pack.drain()


def backward(sizes, x, dy, table, qkv, gu, od, q, k, v, o, lse, hm, h, qkv_g, gu_g, wo_g, wd_g,
             table_s, qkv_s, gu_s, od_s, lse_s, hm_s, dh_s, dhm_s, made_s, dgu_s, bt_s, dq_s, dk_s, dv_s, kt_s,
             p_qkv, p_gu, p_od, a_qkv, a_gu, a_od, b_qkv, b_gu, b_od, got_qkv, got_gu, got_od, in_sem, out_sem, scatter_sems, free_sems):
    layers, n, bq, rows, wide, r = sizes
    ring = Ring(n)
    far = ring.far_a
    split, heads = p_qkv.shape[2], q.shape[2]
    dqkv_s, do_s = made_s.at[:, :split], made_s.at[:, split : split + heads]
    place = 0
    lent = []
    for width in (heads, heads, HEAD, HEAD, x.shape[1]):
        lent.append(dgu_s.at[:, place : place + width])
        place += width
    q_s, o_s, k_s, v_s, h_s = lent
    flying = {}

    def bring(name, src, dst):
        flying[name] = pltpu.make_async_copy(src, dst, in_sem.at[NAMED.index(name)])
        flying[name].start()

    last = layers - 1
    bring("gu", gu.at[last], gu_s)
    bring("hm", hm.at[last], hm_s)
    bring("dy", dy, dh_s)
    bring("od", od.at[last], od_s)
    bring("table", table, table_s)
    bring("qkv", qkv.at[last], qkv_s)
    out = []

    def keep(src, dst):
        out.append(pltpu.make_async_copy(src, dst, out_sem.at[len(out)]))
        out[-1].start()

    def pack(g, p, a, b, got):
        return Scatter(ring, p, a, b, scatter_sems.at[g], free_sems.at[g], got)

    ring.meet(0)
    before = {}
    for i in reversed(range(layers)):
        for name in ("gu", "hm", "od"):
            flying[name].wait()
        if i == last:
            flying["dy"].wait()
        ffn_bwd_phase(hm_s, dh_s, gu_s, od_s, made_s, dgu_s, bt_s, dhm_s, rows, r, before)
        if i:
            bring("gu", gu.at[i - 1], gu_s)
            bring("hm", hm.at[i - 1], hm_s)
        r_qkv, r_gu, r_od = (pack(g, p, a, b, got.at[i]) for g, (p, a, b, got) in enumerate(
            ((p_qkv, a_qkv, b_qkv, got_qkv), (p_gu, a_gu, b_gu, got_gu), (p_od, a_od, b_od, got_od))))
        again = i < last
        units_phase(dgu_s, bt_s, p_gu, wide)
        r_gu.begin(again)
        for name, src, dst in (("o", o.at[i], o_s), ("q", q.at[i], q_s), ("k", k.at[i], k_s), ("v", v.at[i], v_s), ("lse", lse.at[i], lse_s),
                               ("h", x if i == 0 else h.at[i - 1], h_s)):
            bring(name, src, dst)
        downs_phase(made_s, dh_s, p_od, r)
        flying["o"].wait()
        out_bwd_phase(dhm_s, o_s, od_s, p_od, do_s, rows, r)
        r_od.begin(again)
        if i:
            bring("od", od.at[i - 1], od_s)
        for name in ("q", "k", "v", "lse") + (("table",) if i == last else ()):
            flying[name].wait()
        order = [functools.partial(p.step, s) for s in range(1, far + 1) for p in (r_gu, r_od)]
        cut = min(2 * far - 3, (blocks(x.shape[0], bq) + 1) // 2)
        attend_bwd_phase(q_s, k_s, v_s, o_s, do_s, lse_s, table_s, dqkv_s, dq_s, dk_s, dv_s, kt_s, bq, {2 * e: what for e, what in enumerate(order[:cut])})
        flying["h"].wait()
        if i == last:
            flying["qkv"].wait()
        qkv_bwd_phase(h_s, dqkv_s, qkv_s, dhm_s, p_qkv, do_s, dh_s if i else None, rows)
        r_qkv.begin(again)

        def closed(p, signal):
            return lambda: p.close(signal)

        ends = [closed(p, i > 0) for p in (r_gu, r_od, r_qkv)]
        stops = [functools.partial(r_qkv.step, s) for s in range(1, far + 1)]
        left = order[cut:]
        line = []
        while left or stops:
            line += left[:1] + stops[:1]
            left, stops = left[1:], stops[1:]
        before = dict(enumerate(line + ends))
        if i == 0:
            the_rest(before, 0)
            before = {}
    for i in range(layers):
        keep(got_qkv.at[i], qkv_g.at[i])
        keep(got_gu.at[i], gu_g.at[i])
        keep(got_od.at[i, :r, :], wo_g.at[i])
        keep(got_od.at[i, r:, :], wd_g.at[i])
    for copy in out:
        copy.wait()


NAMED = ("gu", "hm", "dy", "od", "table", "q", "k", "v", "o", "lse", "h", "qkv")


def adamw(*refs):
    g_qkv, g_gu, g_wo, g_wd = refs[:4]
    ins, outs = refs[4:25], refs[25:]
    heads, ff = ins[0].shape[2], ins[4].shape[2]
    grads = (g_qkv.at[0, :, :heads], g_qkv.at[0, :, heads : heads + HEAD], g_qkv.at[0, :, heads + HEAD :], g_wo.at[0], g_gu.at[0, :, :ff], g_gu.at[0, :, ff:], g_wd.at[0])
    for i, grad in enumerate(grads):
        g = grad[...].astype(F32)
        w = ins[i][0].astype(F32)
        m = 0.9 * ins[7 + i][0] + 0.1 * g
        v = 0.95 * ins[14 + i][0] + 0.05 * g * g
        outs[i][0] = (w - 0.02 * (m * lax.rsqrt(v + 1e-8) + 0.1 * w)).astype(BF16)
        outs[7 + i][0] = m
        outs[14 + i][0] = v


def solution(mesh):
    n = mesh.shape["dp"]
    far_a, far_b = n // 2, n - 1 - n // 2

    def step(x, dy, *arrays):
        weights = arrays[:7]
        wq, wk, wv, wo, wg, wu, wd = weights
        layers, r, wide_q = wq.shape
        x, dy = x[0], dy[0]
        tokens, d = x.shape
        ff = wg.shape[2]
        bq, rows = min(512, tokens), min(256, tokens)
        table = jnp.asarray(angles(tokens))
        wide = wide_q + 2 * HEAD
        heads = wide_q // HEAD
        ro = wo.shape[1]
        shapes = (r, wide), (r, 2 * ff), (ro + wd.shape[1], d)
        both = lambda *s: jax.ShapeDtypeStruct((layers, *s), BF16)
        whole = [both(n, *s) for s in shapes]
        some = lambda lead, s: pltpu.VMEM((*lead, *s), BF16)
        q, k, v_, o, lse, hm, h, qkv, gu, od = pl.pallas_call(
            functools.partial(forward, (layers, n, bq, rows)),
            out_shape=[both(tokens, wide_q), both(tokens, HEAD), both(tokens, HEAD), both(tokens, wide_q),
                       jax.ShapeDtypeStruct((layers, 8, tokens), F32), both(tokens, d), jax.ShapeDtypeStruct((max(layers - 1, 1), tokens, d), BF16), *whole],
            in_specs=[ANY] * 9,
            out_specs=[ANY] * 10,
            scratch_shapes=[
                pltpu.VMEM((layers, tokens, d), BF16), pltpu.VMEM((tokens, HEAD), F32),
                *(some((layers, n), s) for s in shapes),
                pltpu.VMEM((layers, tokens, wide_q), BF16), pltpu.VMEM((layers, tokens, HEAD), BF16), pltpu.VMEM((layers, tokens, HEAD), BF16),
                pltpu.VMEM((HEAD, tokens), BF16), pltpu.VMEM((layers, tokens, wide_q), BF16), pltpu.VMEM((layers, 8, tokens), F32),
                pltpu.VMEM((layers, tokens, d), BF16), pltpu.VMEM((heads, bq), F32), pltpu.VMEM((heads, HEAD + 8, bq), F32),
                pltpu.SemaphoreType.DMA((7 * layers,)), pltpu.SemaphoreType.DMA((2,)), pltpu.SemaphoreType.DMA((10 * layers,)),
                pltpu.SemaphoreType.DMA((3 * layers, 6, n)),
            ],
            compiler_params=pltpu.CompilerParams(vmem_limit_bytes=VMEM, collective_id=0, has_side_effects=True),
            name="forward",
        )(x, table, *weights)
        grads = pl.pallas_call(
            functools.partial(backward, (layers, n, bq, rows, 512, ro)),
            out_shape=[both(*shapes[0]), both(*shapes[1]), both(ro, d), both(wd.shape[1], d)],
            in_specs=[ANY] * 13,
            out_specs=[ANY] * 4,
            scratch_shapes=[
                pltpu.VMEM((tokens, HEAD), F32), *(some((n,), s) for s in shapes),
                pltpu.VMEM((8, tokens), F32), pltpu.VMEM((tokens, d), BF16), pltpu.VMEM((tokens, d), BF16), pltpu.VMEM((tokens, d), BF16),
                pltpu.VMEM((tokens, ff), BF16), pltpu.VMEM((tokens, 2 * ff), BF16), pltpu.VMEM((d, tokens), BF16),
                pltpu.VMEM((heads, HEAD, bq), F32), pltpu.VMEM((tokens, HEAD), F32), pltpu.VMEM((tokens, HEAD), F32), pltpu.VMEM((HEAD, tokens), BF16),
                *(some((n,), s) for s in shapes), *(some((far_a,), s) for s in shapes), *(some((far_b,), s) for s in shapes), *(some((layers,), s) for s in shapes),
                pltpu.SemaphoreType.DMA((len(NAMED),)), pltpu.SemaphoreType.DMA((4 * layers,)),
                pltpu.SemaphoreType.DMA((3, 4, far_a)), pltpu.SemaphoreType.REGULAR((3,)),
            ],
            compiler_params=pltpu.CompilerParams(vmem_limit_bytes=VMEM, collective_id=1, has_side_effects=True),
            name="backward",
        )(x, dy, table, qkv, gu, od, q, k, v_, o, lse, hm, h)
        parts = 4
        block = lambda a: pl.BlockSpec((1, a.shape[1] // parts, a.shape[2]), lambda i, j: (i, j, 0))
        return pl.pallas_call(
            adamw,
            grid=(layers, parts),
            out_shape=[jax.ShapeDtypeStruct(a.shape, a.dtype) for a in arrays],
            in_specs=[block(a) for a in (*grads, *arrays)],
            out_specs=[block(a) for a in arrays],
            name="adamw",
        )(*grads, *arrays)

    states, cut = P(("rep", "dp"), None, None), P(None, "dp", None)
    return jax.shard_map(
        step,
        mesh=mesh,
        in_specs=(states, states) + (cut,) * 21,
        out_specs=(P("rep", "dp", None),) * 21,
        check_vma=False,
    )
```

```python
import functools

import jax
import jax.numpy as jnp
import numpy as np
from jax import lax
from jax.experimental import pallas as pl
from jax.experimental.pallas import tpu as pltpu
from jax.sharding import PartitionSpec as P

HEAD = 128
THETA = 10000
NEG = -1e30
HIDDEN = 2 * NEG
LOG2E = 1.4426950408889634
SCALE = HEAD**-0.5
E = SCALE * LOG2E
VMEM = 66_000_000
STRETCH = 64
F32, BF16 = jnp.float32, jnp.bfloat16
ANY = pl.BlockSpec(memory_space=pl.ANY)
MESH = pl.DeviceIdType.MESH
A, B = 0, 1


def dot(a, b, ca=1, cb=0):
    return lax.dot_general(a, b, (((ca,), (cb,)), ((), ())), preferred_element_type=F32)


def tile(i, n):
    return pl.ds(pl.multiple_of(i * n, n), n)


def loop(n, body):
    lax.fori_loop(0, n, lambda i, _: body(i), None)


def polled(events, i, steps):
    for when, what in events.items():
        if when < steps:
            pl.when(i == when)(what)


def the_rest(events, steps):
    for when, what in events.items():
        if when >= steps:
            what()


def scale_of(wide):
    return lax.rsqrt(jnp.mean(wide * wide, -1, keepdims=True) + 1e-6)


def norm_bwd(wide, scale, g):
    return scale * g - wide * (scale * scale * scale * jnp.mean(wide * g, -1, keepdims=True))


def angles(tokens):
    half = HEAD // 2
    turn = float(THETA) ** (-np.arange(half) / half)
    place = np.arange(STRETCH)[:, None] * turn
    start = np.arange(0, tokens, STRETCH)[:, None] * turn
    cos, sin = np.cos(start), np.sin(start)
    return np.concatenate([np.concatenate(p, 1) for p in ((np.cos(place), np.sin(place)), (cos, cos), (-sin, sin))]).astype(np.float32)


def table_phase(few, table):
    starts = table.shape[0] // STRETCH

    def step(i):
        place = few[:STRETCH, :]
        row = lambda first: few[pl.ds(first + i, 1), :]
        table[tile(i, STRETCH), :] = place * row(STRETCH) + pltpu.roll(place, HEAD // 2, 1) * row(STRETCH + starts)

    loop(starts, step)


def turns(t):
    swapped = pltpu.roll(t, HEAD // 2, 1)
    first = lax.broadcasted_iota(jnp.int32, t.shape, 1) < HEAD // 2
    return jnp.where(first, t, swapped), jnp.where(first, -swapped, t)


def rotated(t, cos, sin):
    return t * cos + pltpu.roll(t, HEAD // 2, 1) * sin


class Ring:
    def __init__(self, n):
        self.n, self.far_a = n, n // 2
        self.far_b = n - 1 - self.far_a
        self.me = lax.axis_index("dp")
        rep = lax.axis_index("rep")
        self.core = lax.rem(rep, 2)
        self.partner = {"rep": rep + 1 - 2 * self.core}
        self.turn = 1 - 2 * self.core

    def at(self, k):
        return lax.rem(self.me + self.n + k * self.turn, self.n)

    def to(self, k):
        return {"dp": self.at(k)}

    def meet(self, partner):
        barrier = pltpu.get_barrier_semaphore()
        others = [self.to(1), self.to(-1)] + [self.partner] * partner
        for other in others:
            pl.semaphore_signal(barrier, inc=1, device_id=other, device_id_type=MESH)
        pl.semaphore_wait(barrier, len(others))


def remote(src, dst, send, recv, to):
    return pltpu.make_async_remote_copy(src_ref=src, dst_ref=dst, send_sem=send, recv_sem=recv, device_id=to, device_id_type=MESH)


class Chains:
    def far(self, chain):
        return self.ring.far_b if chain else self.ring.far_a

    def now(self, s):
        for stop in range(1, s + 1):
            for chain in (A, B):
                if self.taken[chain] < min(stop, self.far(chain)):
                    self.taken[chain] += 1
                    self.take(chain, self.taken[chain])

    def finish(self):
        self.now(self.ring.far_a)


class Gather(Chains):
    def __init__(self, ring, buf, sems):
        self.taken = [0, 0]
        self.ring, self.buf, self.sems = ring, buf, sems
        self.half = buf.shape[1] // 2

    def piece(self, block, half):
        return self.buf.at[block, pl.ds(pl.multiple_of(half * self.half, self.half), self.half), :]

    def copy(self, chain, step, block, to):
        part = self.piece(block, self.ring.core)
        return remote(part, part, self.sems.at[2 * chain, step], self.sems.at[2 * chain + 1, step], to)

    def hop(self, chain, step):
        ring = self.ring
        return self.copy(chain, step, ring.at(-step if chain == 0 else step), ring.to(1 if chain == 0 else -1))

    def arriving(self, chain, step):
        ring = self.ring
        return self.copy(chain, step, ring.at(-step - 1 if chain == 0 else step + 1), ring.to(1 if chain == 0 else -1))

    def handed(self, chain, step):
        ring = self.ring
        block = ring.at(-step - 1 if chain == 0 else step + 1)
        return self.copy(2, step + chain * ring.far_a, block, ring.partner)

    def begin(self):
        self.hop(0, 0).start()
        self.hop(1, 0).start()

    def take(self, chain, s):
        self.arriving(chain, s - 1).wait_recv()
        if s < self.far(chain):
            self.hop(chain, s).start()
        self.handed(chain, s - 1).start()

    def complete(self):
        ring = self.ring
        for chain, far in ((0, ring.far_a), (1, ring.far_b)):
            for step in range(far):
                part = self.piece(ring.at(step + 1 if chain == 0 else -step - 1), 1 - ring.core)
                i = step + chain * ring.far_a
                remote(part, part, self.sems.at[4, i], self.sems.at[5, i], ring.partner).wait_recv()

    def drain(self):
        for chain, far in ((0, self.ring.far_a), (1, self.ring.far_b)):
            for step in range(far):
                self.hop(chain, step).wait_send()
                self.handed(chain, step).wait_send()


class Scatter(Chains):
    def __init__(self, ring, p, came_a, came_b, sems, free, got, signal, taken=(0, 0)):
        self.signal = signal
        self.ring, self.p, self.came, self.sems, self.free, self.got = ring, p, (came_a, came_b), sems, free, got
        self.taken = list(taken)

    def hop(self, chain, step):
        ring = self.ring
        left = self.far(chain) - step
        block = ring.at(left if chain == 0 else -left)
        return remote(self.p.at[block], self.came[chain].at[step], self.sems.at[2 * chain, step], self.sems.at[2 * chain + 1, step],
                      ring.to(1 if chain == 0 else -1))

    def added(self, chain, step):
        ring = self.ring
        left = self.far(chain) - step
        block = ring.at(left if chain == 0 else -left)
        few = 16

        def rows(i):
            at = tile(i, few)
            self.p[block, at, :] = (self.p[block, at, :].astype(F32) + self.came[chain][step - 1, at, :].astype(F32)).astype(BF16)

        loop(self.p.shape[1] // few, rows)

    def begin(self, wait):
        pl.when(wait)(lambda: pl.semaphore_wait(self.free, 2))
        self.hop(0, 0).start()
        self.hop(1, 0).start()

    def take(self, chain, s):
        self.hop(chain, s - 1).wait_recv()
        if s < self.far(chain):
            self.added(chain, s)
            self.hop(chain, s).start()
        if self.taken == [self.far(A), self.far(B)]:
            self.end()

    def end(self):
        me, few = self.ring.me, 16
        last_a, last_b = self.ring.far_a - 1, self.ring.far_b - 1

        def rows(i):
            at = tile(i, few)
            total = self.came[0][last_a, at, :].astype(F32) + self.came[1][last_b, at, :].astype(F32) + self.p[me, at, :].astype(F32)
            self.got[at, :] = total.astype(BF16)

        loop(self.p.shape[1] // few, rows)
        for chain in (A, B):
            for step in range(self.far(chain)):
                self.hop(chain, step).wait_send()

        @pl.when(self.signal)
        def _():
            for k in (1, -1):
                pl.semaphore_signal(self.free, inc=1, device_id=self.ring.to(k), device_id_type=MESH)


def merged(w):
    return w.reshape(w.shape[0] * w.shape[1], w.shape[2])


def qkv_phase(h, w, table, q, k, v, vt, rows, events):
    wide_q = q.shape[1]

    def step(i):
        at = tile(i, rows)
        wide = h[at, :].astype(F32)
        a = (wide * scale_of(wide)).astype(BF16)
        y = dot(a, merged(w[...])).astype(BF16)
        cos, sin = turns(table[at, :])
        for n in range(wide_q // HEAD):
            part = slice(n * HEAD, (n + 1) * HEAD)
            q[at, part] = rotated(y[:, part].astype(F32), cos, sin).astype(BF16)
        k[at, :] = rotated(y[:, wide_q : wide_q + HEAD].astype(F32), cos, sin).astype(BF16)
        mine = y[:, wide_q + HEAD :]
        v[at, :] = mine
        vt[:, at] = mine.T
        polled(events, i, h.shape[0] // rows)

    loop(h.shape[0] // rows, step)
    the_rest(events, h.shape[0] // rows)


def spans(bq):
    half = bq // 2
    return [(0, half, 0), (half, half, half)]


def seen(keys, first_key, queries, first_query):
    key = lax.broadcasted_iota(jnp.int32, (keys, queries), 0) + first_key
    return lax.broadcasted_iota(jnp.int32, (keys, queries), 1) + first_query >= key


def blocks(tokens, bq):
    return (tokens // bq) * (tokens // bq + 1) // 2


def row_of_blocks(iq, bq, block, events, steps):
    def step(j):
        @pl.when(j < iq)
        def _():
            block(pl.multiple_of(j * bq, bq), bq, 0, None)

        @pl.when(j == iq)
        def _():
            for first, nk, lo in spans(bq):
                block(pl.multiple_of(iq * bq + first, nk), nk, lo, seen(nk, first, bq - lo, lo))

        polled(events, lax.div(iq * (iq + 1), 2) + j, steps)

    loop(iq + 1, step)


def attend_phase(q, k, vt, o, lse, top_s, mix_s, bq, events):
    heads = q.shape[1] // HEAD

    def block(iq, start, nk, lo, mask):
        here = pl.ds(start, nk)
        cols = pl.ds(pl.multiple_of(iq * bq + lo, bq - lo), bq - lo)
        keys = k[here, :]
        scores = [dot(keys, q[cols, n * HEAD : (n + 1) * HEAD], 1, 1) for n in range(heads)]
        values = jnp.concatenate([vt[:, here], jnp.ones((8, nk), BF16)], axis=0)
        for n, s in enumerate(scores):
            if mask is not None:
                s = jnp.where(mask, s, HIDDEN)
            old = top_s[n : n + 1, lo:]
            top = jnp.maximum(old, s.max(axis=0, keepdims=True))
            top_s[n : n + 1, lo:] = top
            p = jnp.exp2((s - top) * E).astype(BF16)
            mix_s[n, :, lo:] = mix_s[n, :, lo:] * jnp.exp2((old - top) * E) + dot(values, p)

    def step(iq):
        at = tile(iq, bq)
        top_s[...] = jnp.full(top_s.shape, NEG, F32)
        mix_s[...] = jnp.zeros(mix_s.shape, F32)
        row_of_blocks(iq, bq, functools.partial(block, iq), events, blocks(q.shape[0], bq))
        for n in range(heads):
            total = mix_s[n, HEAD : HEAD + 1, :]
            o[at, n * HEAD : (n + 1) * HEAD] = (mix_s[n, :HEAD, :] * (1 / total)).T.astype(BF16)
            lse[n : n + 1, at] = top_s[n : n + 1, :] * E + jnp.log2(total)

    loop(q.shape[0] // bq, step)
    the_rest(events, blocks(q.shape[0], bq))


def mid_phase(h, o, od, hm, rows, r):
    def step(i):
        at = tile(i, rows)
        hm[at, :] = h[at, :] + dot(o[at, :], merged(od[:, :r, :])).astype(BF16)

    loop(h.shape[0] // rows, step)


def ffn_phase(hm, gu, od, out, rows, r, events):
    def step(i):
        at = tile(i, rows)
        mid = hm[at, :]
        wide = mid.astype(F32)
        b = (wide * scale_of(wide)).astype(BF16)
        y = dot(b, merged(gu[...]))
        part = y.shape[1] // 4
        pieces = []
        for n in (0, 2 * part):
            gate, up = y[:, n : n + part], y[:, n + part : n + 2 * part]
            pieces.append((gate * (1 / (1 + jnp.exp(-gate))) * up).astype(BF16))
        made = jnp.concatenate(pieces, axis=1)
        out[at, :] = mid + dot(made, merged(od[:, r:, :])).astype(BF16)
        polled(events, i, hm.shape[0] // rows)

    loop(hm.shape[0] // rows, step)
    the_rest(events, hm.shape[0] // rows)


def ffn_bwd_phase(half, hm, dy, gu, od, made_s, dgu_s, bt_s, db_s, dhm, rows, r, events):
    part = dgu_s.shape[1] // 4
    lanes, units = slice(2 * part * half, 2 * part * (half + 1)), slice(part * half, part * (half + 1))
    some = od.shape[0] // 2

    def step(i):
        at = tile(i, rows)
        wide = hm[at, :].astype(F32)
        scale = scale_of(wide)
        b = (wide * scale).astype(BF16)
        if half == 0:
            bt_s[:, at] = b.T
        y = dot(b, merged(gu[:, :, lanes]))
        gate, up = y[:, :part], y[:, part:]
        back = dy[at, :]
        d_made = dot(back, merged(od[some * half : some * (half + 1), r:, :]), 1, 1).astype(BF16).astype(F32)
        sig = 1 / (1 + jnp.exp(-gate))
        silu = gate * sig
        made_s[at, units] = (silu * up).astype(BF16)
        d_gate = (d_made * up * (sig * (1 + gate - silu))).astype(BF16)
        d_up = (d_made * silu).astype(BF16)
        both = jnp.concatenate([d_gate, d_up], axis=1)
        dgu_s[at, lanes] = both
        db = dot(both, merged(gu[:, :, lanes]), 1, 1)
        if half == 0:
            db_s[at, :] = db
        else:
            db = (db_s[at, :] + db).astype(BF16).astype(F32)
            dhm[at, :] = (back.astype(F32) + norm_bwd(wide, scale, db)).astype(BF16)
        polled(events, i, hm.shape[0] // rows)

    loop(hm.shape[0] // rows, step)
    the_rest(events, hm.shape[0] // rows)


def units_phase(half, dgu_s, bt_s, p):
    n, _, columns = p.shape
    wide = next(w for w in (512, 256, 128) if columns % w == 0)

    def units(i):
        here = pl.ds(pl.multiple_of(columns * half + i * wide, wide), wide)
        p[:, :, tile(i, wide)] = dot(bt_s[...], dgu_s[:, here]).astype(BF16).reshape(n, -1, wide)

    loop(columns // wide, units)


def downs_phase(made_s, dy, p):
    n, share, group = p.shape[0], p.shape[1], 2

    def downs(i):
        got = dot(made_s[:, tile(i, group * share)], dy[...], 0, 0).astype(BF16)
        p[pl.ds(i * group, group)] = got.reshape(group, share, -1)

    loop(n // group, downs)


def out_bwd_phase(dhm, o, od, p, do, rows, r):
    def step(i):
        at = tile(i, rows)
        do[at, :] = dot(dhm[at, :], merged(od[:, :r, :]), 1, 1).astype(BF16)

    loop(dhm.shape[0] // rows, step)
    p[...] = dot(o[...], dhm[...], 0, 0).astype(BF16).reshape(p.shape)


def attend_bwd_phase(q, k, v, o, do, lse, table, dqkv, dq_s, dk_s, dv_s, kt_s, bq, events):
    heads = q.shape[1] // HEAD
    wide_q = q.shape[1]
    dk_s[...] = jnp.zeros(dk_s.shape, F32)
    dv_s[...] = jnp.zeros(dv_s.shape, F32)
    kt_s[...] = k[...].T

    def block(iq, lses, deltas, start, nk, lo, mask):
        here = pl.ds(start, nk)
        cols = pl.ds(pl.multiple_of(iq * bq + lo, bq - lo), bq - lo)
        keys, values, keys_t = k[here, :], v[here, :], kt_s[:, here]
        qs = [q[cols, n * HEAD : (n + 1) * HEAD] for n in range(heads)]
        dos = [do[cols, n * HEAD : (n + 1) * HEAD] for n in range(heads)]
        scores = [dot(keys, x, 1, 1) for x in qs]
        dps = [dot(values, x, 1, 1) for x in dos]
        for n in range(heads):
            p = jnp.exp2(scores[n] * E - lses[n][:, lo:])
            if mask is not None:
                p = jnp.where(mask, p, 0.0)
            ds = (p * (dps[n] - deltas[n][:, lo:])).astype(BF16)
            dv_s[here, :] += dot(p.astype(BF16), dos[n])
            dk_s[here, :] += dot(ds, qs[n])
            dq_s[n, :, lo:] += dot(keys_t, ds)

    def step(iq):
        at = tile(iq, bq)
        dq_s[...] = jnp.zeros(dq_s.shape, F32)
        lses = [lse[n : n + 1, at] for n in range(heads)]
        deltas = []
        for n in range(heads):
            part = slice(n * HEAD, (n + 1) * HEAD)
            deltas.append((do[at, part].astype(F32) * o[at, part].astype(F32)).T.sum(axis=0, keepdims=True))
        row_of_blocks(iq, bq, functools.partial(block, iq, lses, deltas), events, blocks(q.shape[0], bq))
        cos, sin = turns(table[at, :])
        for n in range(heads):
            back = (dq_s[n] * SCALE).T.astype(BF16).astype(F32)
            dqkv[at, n * HEAD : (n + 1) * HEAD] = rotated(back, cos, -sin).astype(BF16)

    loop(q.shape[0] // bq, step)
    the_rest(events, blocks(q.shape[0], bq))

    def finish(i):
        at = tile(i, bq)
        cos, sin = turns(table[at, :])
        dqkv[at, wide_q : wide_q + HEAD] = rotated((dk_s[at, :] * SCALE).astype(BF16).astype(F32), cos, -sin).astype(BF16)
        dqkv[at, wide_q + HEAD :] = dv_s[at, :].astype(BF16)

    loop(q.shape[0] // bq, finish)


def qkv_bwd_phase(h, dqkv, w, dhm, p_qkv, a_s, dh, rows, further):
    def step(i):
        at = tile(i, rows)
        wide = h[at, :].astype(F32)
        scale = scale_of(wide)
        a_s[at, :] = (wide * scale).astype(BF16)

        @pl.when(further)
        def _():
            da = dot(dqkv[at, :], merged(w[...]), 1, 1).astype(BF16).astype(F32)
            dh[at, :] = (dhm[at, :].astype(F32) + norm_bwd(wide, scale, da)).astype(BF16)

    loop(h.shape[0] // rows, step)
    p_qkv[...] = dot(a_s[...], dqkv[...], 0, 0).astype(BF16).reshape(p_qkv.shape)


QKV, OD, GU = range(3)
OWN, OLD = range(2)
NEXT = OLD
PLAN = {
    "qkv": ((0, OD, OWN, 2), (0, QKV, NEXT, 0), (6, GU, OWN, 2)),
    "attend": ((1, OD, OWN, 3), (2, QKV, NEXT, 1), (2, OD, NEXT, 0), (4, GU, OWN, 3), (6, OD, OWN, 4), (6, GU, NEXT, 0), (7, QKV, NEXT, 2), (8, OD, NEXT, 1)),
    "ffn": ((1, GU, NEXT, 1), (2, QKV, NEXT, 3), (3, OD, NEXT, 2), (7, QKV, NEXT, 4), (7, GU, NEXT, 2)),
}
LAST_PLAN = {"qkv": ((1, OD, OWN, 3),), "attend": ((2, GU, OWN, 3), (3, OD, OWN, 4), (6, GU, OWN, 4))}
HEAD_PLAN = ((QKV, 0), (OD, 0), (QKV, 1), (GU, 0), (QKV, 2), (OD, 1), (QKV, 3), (GU, 1), (QKV, 4))


def planned(act, entries):
    by_step = {}
    for when, *what in entries:
        by_step.setdefault(when, []).append(what)
    return {when: functools.partial(act, whats) for when, whats in by_step.items()}


def forward(sizes, x, few, wq, wk, wv, wo, wg, wu, wd, q_o, k_o, v_o, o_o, lse_o, hm_o, h_o, qkv_o, gu_o, od_o, table_o,
            h_s, few_s, table_s, qkv_s, gu_s, od_s, q_s, k_s, v_s, vt_s, o_s, lse_s, hm_s, top_s, mix_s, own_sem, in_sem, out_sem, gather_sems):
    layers, n, bq, rows = sizes
    ring = Ring(n)
    me = ring.me
    wide_q, ff, ro = wq.shape[2], wg.shape[2], wo.shape[1]
    half = ff // 2
    own = {}

    def fetch(i, group, pieces):
        for src, dst in pieces:
            copy = pltpu.make_async_copy(src, dst, own_sem.at[sum(map(len, own.values()))])
            own.setdefault((i, group), []).append(copy)
            copy.start()

    for i in range(layers):
        fetch(i, QKV, [(wq.at[i], qkv_s.at[i, me, :, :wide_q]), (wk.at[i], qkv_s.at[i, me, :, wide_q : wide_q + HEAD]), (wv.at[i], qkv_s.at[i, me, :, wide_q + HEAD :])])
        fetch(i, OD, [(wo.at[i], od_s.at[i, me, :ro, :]), (wd.at[i], od_s.at[i, me, ro:, :])])
        if i == 0:
            brought = [pltpu.make_async_copy(x, h_s.at[0], in_sem.at[0]), pltpu.make_async_copy(few, few_s, in_sem.at[1])]
            for copy in brought:
                copy.start()
        fetch(i, GU, [(w.at[i, :, half * j : half * (j + 1)], gu_s.at[i, me, :, half * (2 * j + k) : half * (2 * j + k + 1)]) for j in (0, 1) for k, w in enumerate((wg, wu))])
    packs = {(g, i): Gather(ring, buf.at[i], gather_sems.at[3 * i + g]) for g, buf in enumerate((qkv_s, od_s, gu_s)) for i in range(layers)}
    begun = set()
    out = []

    def keep(src, dst):
        out.append(pltpu.make_async_copy(src, dst, out_sem.at[len(out)]))
        out[-1].start()

    def begin(group, i):
        if (group, i) not in begun:
            begun.add((group, i))
            for copy in own[i, group]:
                copy.wait()
            packs[group, i].begin()

    def act(i, whats):
        for group, which, stop in whats:
            if i + which < layers:
                begin(group, i + which)
                packs[group, i + which].now(stop)

    def plan(phase, i):
        return planned(functools.partial(act, i), (PLAN if i + 1 < layers else LAST_PLAN).get(phase, ()))

    def whole(group, i):
        begin(group, i)
        packs[group, i].finish()
        packs[group, i].complete()

    ring.meet(1)
    begin(QKV, 0)
    begin(OD, 0)
    for copy in brought:
        copy.wait()
    table_phase(few_s, table_s)
    keep(table_s, table_o)
    act(0, [(group, OWN, stop) for group, stop in HEAD_PLAN])
    for i in range(layers):
        keep(h_s.at[i], h_o.at[i])
        whole(QKV, i)
        keep(qkv_s.at[i], qkv_o.at[i])
        qkv_phase(h_s.at[i], qkv_s.at[i], table_s, q_s.at[i], k_s.at[i], v_s.at[i], vt_s, rows, plan("qkv", i))
        keep(q_s.at[i], q_o.at[i])
        keep(k_s.at[i], k_o.at[i])
        keep(v_s.at[i], v_o.at[i])
        attend_phase(q_s.at[i], k_s.at[i], vt_s, o_s.at[i], lse_s.at[i], top_s, mix_s, bq, plan("attend", i))
        keep(o_s.at[i], o_o.at[i])
        keep(lse_s.at[i], lse_o.at[i])
        whole(OD, i)
        keep(od_s.at[i], od_o.at[i])
        mid_phase(h_s.at[i], o_s.at[i], od_s.at[i], hm_s.at[i], rows, ro)
        keep(hm_s.at[i], hm_o.at[i])
        whole(GU, i)
        keep(gu_s.at[i], gu_o.at[i])
        if i + 1 < layers:
            ffn_phase(hm_s.at[i], gu_s.at[i], od_s.at[i], h_s.at[i + 1], rows, ro, plan("ffn", i))
    for copy in out:
        copy.wait()
    for pack in packs.values():
        pack.drain()


PACKS = 5
QKV_G, GA_G, GB_G, WD_G, WO_G = range(PACKS)
BACK = {
    "first": ((3, QKV_G, OLD, 1), (5, WD_G, OLD, 4), (5, WO_G, OLD, 4), (7, QKV_G, OLD, 2)),
    "second": ((1, QKV_G, OLD, 3), (5, GA_G, OWN, 1), (6, QKV_G, OLD, 4)),
    "downs": ((0, GA_G, OWN, 2),),
    "attend": ((0, GB_G, OWN, 1), (1, WD_G, OWN, 1), (2, GA_G, OWN, 3), (3, WO_G, OWN, 1), (4, GB_G, OWN, 2), (6, WD_G, OWN, 2), (7, GA_G, OWN, 4), (8, WO_G, OWN, 2),
               (9, GB_G, OWN, 3)),
    "end": ((0, GB_G, OWN, 4), (0, WD_G, OWN, 3), (0, WO_G, OWN, 3)),
}
TAIL = ((QKV_G, 1), (WD_G, 4), (WO_G, 4), (QKV_G, 4))
NAMED = ("gu", "hm", "dy", "od", "table", "q", "k", "v", "o", "lse", "h", "qkv")


def backward(sizes, dy, table, qkv, gu, od, q, k, v, o, lse, hm, h, *refs):
    layers, n, bq, rows, r = sizes
    results, refs = refs[:PACKS], refs[PACKS:]
    table_s, qkv_s, gu_s, od_s, lse_s, hm_s, dh_s, dhm_s, made_s, dgu_s, bt_s, db_s, dq_s, kt_s = refs[:14]
    refs = refs[14:]
    terms, came_a, came_b, got = (refs[PACKS * i : PACKS * (i + 1)] for i in range(4))
    in_sem, out_sem, scatter_sems, free_sems = refs[PACKS * 4 :]
    ring = Ring(n)
    split, heads = qkv_s.shape[2], q.shape[2]
    dqkv_s, do_s = made_s.at[:, :split], made_s.at[:, split : split + heads]
    dk_s, dv_s = db_s.at[:, :HEAD], db_s.at[:, HEAD : 2 * HEAD]
    place = 0
    lent = []
    for width in (heads, heads, HEAD, HEAD, h.shape[2]):
        lent.append(dgu_s.at[:, place : place + width])
        place += width
    q_s, o_s, k_s, v_s, h_s = lent
    places = {"gu": (gu, gu_s), "hm": (hm, hm_s), "dy": (dy, dh_s), "od": (od, od_s), "table": (table, table_s), "q": (q, q_s), "k": (k, k_s), "v": (v, v_s),
              "o": (o, o_s), "lse": (lse, lse_s), "h": (h, h_s), "qkv": (qkv, qkv_s)}

    def copy_of(name, *i):
        src, dst = places[name]
        return pltpu.make_async_copy(src.at[i] if i else src, dst, in_sem.at[NAMED.index(name)])

    def bring(names, *i):
        for name in names:
            copy_of(name, *i).start()

    def need(names, *i):
        for name in names:
            copy_of(name, *i).wait()

    last = layers - 1
    bring(("gu", "hm"), last)
    bring(("dy",))
    bring(("od",), last)
    bring(("table",))
    bring(("qkv",), last)
    ring.meet(0)

    def pack(group, i, signal, taken=(0, 0)):
        return Scatter(ring, terms[group], came_a[group], came_b[group], scatter_sems.at[group], free_sems.at[group], got[group].at[i], signal, taken)

    reached = {}
    for entries in BACK.values():
        for _, group, old, stop in entries:
            if old == OWN:
                reached[group] = max(stop, reached.get(group, 0))
    taken = {group: (min(stop, ring.far_a), min(stop, ring.far_b)) for group, stop in reached.items()}

    def layer(step):
        i = last - step
        later = step > 0
        own = {group: pack(group, i, i > 0) for group in range(PACKS)}
        old = {group: pack(group, i + 1, i >= 0, taken.get(group, (0, 0))) for group in range(PACKS)}

        def act(whats):
            for group, which, stop in whats:
                if which == OWN:
                    own[group].now(stop)
                else:
                    pl.when(later)(functools.partial(old[group].now, stop))

        def plan(phase):
            return planned(act, BACK[phase])

        def before(group):
            pl.when(later)(old[group].finish)

        need(("gu", "hm", "od"), i)
        pl.when(step == 0)(functools.partial(need, ("dy",)))
        for half, group, phase in ((0, GA_G, "first"), (1, GB_G, "second")):
            ffn_bwd_phase(half, hm_s, dh_s, gu_s, od_s, made_s, dgu_s, bt_s, db_s, dhm_s, rows, r, plan(phase))
            if half == 1:
                pl.when(i > 0)(functools.partial(bring, ("gu", "hm"), i - 1))
            before(group)
            units_phase(half, dgu_s, bt_s, terms[group])
            own[group].begin(later)
        bring(("o", "q", "k", "v", "lse", "h"), i)
        before(WD_G)
        downs_phase(made_s, dh_s, terms[WD_G])
        own[WD_G].begin(later)
        the_rest(plan("downs"), 0)
        need(("o",), i)
        before(WO_G)
        out_bwd_phase(dhm_s, o_s, od_s, terms[WO_G], do_s, rows, r)
        own[WO_G].begin(later)
        pl.when(i > 0)(functools.partial(bring, ("od",), i - 1))
        need(("q", "k", "v", "lse"), i)
        pl.when(step == 0)(functools.partial(need, ("table",)))
        attend_bwd_phase(q_s, k_s, v_s, o_s, do_s, lse_s, table_s, dqkv_s, dq_s, dk_s, dv_s, kt_s, bq, plan("attend"))
        need(("h",), i)
        pl.when(step == 0)(functools.partial(need, ("qkv",), last))
        before(QKV_G)
        qkv_bwd_phase(h_s, dqkv_s, qkv_s, dhm_s, terms[QKV_G], do_s, dh_s, rows, i > 0)
        own[QKV_G].begin(later)
        the_rest(plan("end"), 0)

        @pl.when(jnp.logical_and(i > 1, i < layers))
        def _():
            copy_of("qkv", i - 1).start()
            copy_of("qkv", i - 1).wait()

    loop(layers, layer)
    final = {group: pack(group, 0, False, taken.get(group, (0, 0))) for group in range(PACKS)}
    for group, stop in TAIL:
        final[group].now(stop)
    for p in final.values():
        p.finish()
    out = []
    for group in range(PACKS):
        for i in range(layers):
            out.append(pltpu.make_async_copy(got[group].at[i], results[group].at[i], out_sem.at[len(out)]))
            out[-1].start()
    for copy in out:
        copy.wait()


SEVEN = 7


def adamw(*refs):
    count = 3 * SEVEN
    grads, refs = refs[:PACKS], refs[PACKS:]
    ins, outs, refs = refs[:count], refs[count : 2 * count], refs[2 * count :]
    grads_s, refs = refs[:PACKS], refs[PACKS:]
    ins_s, outs_s, (grad_sem, in_sem, out_sem) = refs[:count], refs[count : 2 * count], refs[2 * count :]
    kinds = range(0, count, SEVEN)
    layers = ins[0].shape[0]
    heads, half, few = ins[0].shape[2], ins[4].shape[2] // 2, 16
    waits = []
    for i in range(layers):
        copies = [pltpu.make_async_copy(src.at[i], dst.at[i], grad_sem.at[g, i]) for g, (src, dst) in enumerate(zip(grads, grads_s, strict=True))]
        copies += [pltpu.make_async_copy(ins[a].at[i], ins_s[a].at[i], in_sem.at[a, i]) for w in range(SEVEN) for a in (w + kind for kind in kinds)]
        for copy in copies:
            copy.start()
        waits.append(copies)
    parts = (
        [(0, 0, 0, heads)], [(0, heads, 0, HEAD)], [(0, heads + HEAD, 0, HEAD)], [(4, 0, 0, ins[3].shape[2])],
        [(1, 0, 0, half), (2, 0, half, half)], [(1, half, 0, half), (2, half, half, half)], [(3, 0, 0, ins[6].shape[2])],
    )
    out = []
    for i in range(layers):
        for copy in waits[i][:PACKS]:
            copy.wait()
        for w in range(SEVEN):
            for copy in waits[i][PACKS + 3 * w : PACKS + 3 * (w + 1)]:
                copy.wait()

            def step(j, i=i, w=w):
                at = tile(j, few)
                for grad, first, start, wide in parts[w]:
                    here = slice(start, start + wide)
                    g = grads_s[grad][i, at, first : first + wide].astype(F32)
                    weight = ins_s[w][i, at, here].astype(F32)
                    of_m, of_v = w + SEVEN, w + 2 * SEVEN
                    m = 0.9 * ins_s[of_m][i, at, here] + 0.1 * g
                    v = 0.95 * ins_s[of_v][i, at, here] + 0.05 * g * g
                    outs_s[w][i, at, here] = (weight - 0.02 * (m * lax.rsqrt(v + 1e-8) + 0.1 * weight)).astype(BF16)
                    outs_s[of_m][i, at, here] = m
                    outs_s[of_v][i, at, here] = v

            loop(ins[w].shape[1] // few, step)
            for a in (w + kind for kind in kinds):
                out.append(pltpu.make_async_copy(outs_s[a].at[i], outs[a].at[i], out_sem.at[a, i]))
                out[-1].start()
    for copy in out:
        copy.wait()


def solution(mesh):
    n = mesh.shape["dp"]
    far_a, far_b = n // 2, n - 1 - n // 2

    def step(x, dy, *arrays):
        weights = arrays[:SEVEN]
        wq, wk, wv, wo, wg, wu, wd = weights
        layers, r, wide_q = wq.shape
        x, dy = x[0], dy[0]
        tokens, d = x.shape
        ff = wg.shape[2]
        bq, rows = min(512, tokens), min(256, tokens)
        few = jnp.asarray(angles(tokens))
        wide = wide_q + 2 * HEAD
        heads = wide_q // HEAD
        ro = wo.shape[1]
        shapes = (r, wide), (r, 2 * ff), (ro + wd.shape[1], d)
        terms = (r, wide), (r, ff), (r, ff), (wd.shape[1], d), (ro, d)
        both = lambda *s: jax.ShapeDtypeStruct((layers, *s), BF16)
        some = lambda lead, s: pltpu.VMEM((*lead, *s), BF16)
        q, k, v_, o, lse, hm, h, qkv, gu, od, table = pl.pallas_call(
            functools.partial(forward, (layers, n, bq, rows)),
            out_shape=[both(tokens, wide_q), both(tokens, HEAD), both(tokens, HEAD), both(tokens, wide_q), jax.ShapeDtypeStruct((layers, 8, tokens), F32),
                       both(tokens, d), both(tokens, d), *(both(n, *s) for s in shapes), jax.ShapeDtypeStruct((tokens, HEAD), F32)],
            in_specs=[ANY] * 9,
            out_specs=[ANY] * 11,
            scratch_shapes=[
                pltpu.VMEM((layers, tokens, d), BF16), pltpu.VMEM(few.shape, F32), pltpu.VMEM((tokens, HEAD), F32),
                *(some((layers, n), s) for s in shapes),
                pltpu.VMEM((layers, tokens, wide_q), BF16), pltpu.VMEM((layers, tokens, HEAD), BF16), pltpu.VMEM((layers, tokens, HEAD), BF16),
                pltpu.VMEM((HEAD, tokens), BF16), pltpu.VMEM((layers, tokens, wide_q), BF16), pltpu.VMEM((layers, 8, tokens), F32),
                pltpu.VMEM((layers, tokens, d), BF16), pltpu.VMEM((heads, bq), F32), pltpu.VMEM((heads, HEAD + 8, bq), F32),
                pltpu.SemaphoreType.DMA((9 * layers,)), pltpu.SemaphoreType.DMA((2,)), pltpu.SemaphoreType.DMA((10 * layers + 1,)),
                pltpu.SemaphoreType.DMA((3 * layers, 6, n)),
            ],
            compiler_params=pltpu.CompilerParams(vmem_limit_bytes=VMEM, collective_id=0, has_side_effects=True),
            name="forward",
        )(x, few, *weights)
        grads = pl.pallas_call(
            functools.partial(backward, (layers, n, bq, rows, ro)),
            out_shape=[both(*s) for s in terms],
            in_specs=[ANY] * 12,
            out_specs=[ANY] * 5,
            scratch_shapes=[
                pltpu.VMEM((tokens, HEAD), F32), *(some((n,), s) for s in shapes),
                pltpu.VMEM((8, tokens), F32), pltpu.VMEM((tokens, d), BF16), pltpu.VMEM((tokens, d), BF16), pltpu.VMEM((tokens, d), BF16),
                pltpu.VMEM((tokens, ff), BF16), pltpu.VMEM((tokens, 2 * ff), BF16), pltpu.VMEM((d, tokens), BF16),
                pltpu.VMEM((tokens, d), F32), pltpu.VMEM((heads, HEAD, bq), F32), pltpu.VMEM((HEAD, tokens), BF16),
                *(some((lead,), s) for lead in (n, far_a, far_b, layers) for s in terms),
                pltpu.SemaphoreType.DMA((len(NAMED),)), pltpu.SemaphoreType.DMA((5 * layers,)),
                pltpu.SemaphoreType.DMA((5, 4, far_a)), pltpu.SemaphoreType.REGULAR((5,)),
            ],
            compiler_params=pltpu.CompilerParams(vmem_limit_bytes=VMEM, collective_id=1, has_side_effects=True),
            name="backward",
        )(dy, table, qkv, gu, od, q, k, v_, o, lse, hm, h)
        in_vmem = lambda a: pltpu.VMEM(a.shape, a.dtype)
        return pl.pallas_call(
            adamw,
            out_shape=[jax.ShapeDtypeStruct(a.shape, a.dtype) for a in arrays],
            in_specs=[ANY] * (PACKS + 3 * SEVEN),
            out_specs=[ANY] * (3 * SEVEN),
            scratch_shapes=[*map(in_vmem, grads), *map(in_vmem, arrays), *map(in_vmem, arrays),
                            pltpu.SemaphoreType.DMA((PACKS, layers)), *(pltpu.SemaphoreType.DMA((3 * SEVEN, layers)) for _ in arrays[:2])],
            compiler_params=pltpu.CompilerParams(vmem_limit_bytes=VMEM),
            name="adamw",
        )(*grads, *arrays)

    states, cut = P(("rep", "dp"), None, None), P(None, "dp", None)
    return jax.shard_map(
        step,
        mesh=mesh,
        in_specs=(states, states) + (cut,) * (3 * SEVEN),
        out_specs=(P("rep", "dp", None),) * (3 * SEVEN),
        check_vma=False,
    )
```

```python
import functools

import jax
import jax.numpy as jnp
import numpy as np
from jax import lax
from jax.experimental import pallas as pl
from jax.experimental.pallas import tpu as pltpu
from jax.sharding import PartitionSpec as P

HEAD = 128
THETA = 10000
NEG = -1e30
HIDDEN = 2 * NEG
LOG2E = 1.4426950408889634
SCALE = HEAD**-0.5
E = SCALE * LOG2E
VMEM = 66_000_000
STRETCH = 64
F32, BF16 = jnp.float32, jnp.bfloat16
ANY = pl.BlockSpec(memory_space=pl.ANY)
MESH = pl.DeviceIdType.MESH
A, B = 0, 1


def dot(a, b, ca=1, cb=0):
    return lax.dot_general(a, b, (((ca,), (cb,)), ((), ())), preferred_element_type=F32)


def tile(i, n):
    return pl.ds(pl.multiple_of(i * n, n), n)


def loop(n, body):
    lax.fori_loop(0, n, lambda i, _: body(i), None)


def polled(events, i, steps):
    for when, what in events.items():
        if when < steps:
            pl.when(i == when)(what)


def the_rest(events, steps):
    for when, what in events.items():
        if when >= steps:
            what()


def scale_of(wide):
    return lax.rsqrt(jnp.mean(wide * wide, -1, keepdims=True) + 1e-6)


def norm_bwd(wide, scale, g):
    return scale * g - wide * (scale * scale * scale * jnp.mean(wide * g, -1, keepdims=True))


def angles(tokens):
    half = HEAD // 2
    turn = float(THETA) ** (-np.arange(half) / half)
    place = np.arange(STRETCH)[:, None] * turn
    start = np.arange(0, tokens, STRETCH)[:, None] * turn
    cos, sin = np.cos(start), np.sin(start)
    return np.concatenate([np.concatenate(p, 1) for p in ((np.cos(place), np.sin(place)), (cos, cos), (-sin, sin))]).astype(np.float32)


def table_phase(few, table):
    starts = table.shape[0] // STRETCH

    def step(i):
        place = few[:STRETCH, :]
        row = lambda first: few[pl.ds(first + i, 1), :]
        table[tile(i, STRETCH), :] = place * row(STRETCH) + pltpu.roll(place, HEAD // 2, 1) * row(STRETCH + starts)

    loop(starts, step)


def turns(t):
    swapped = pltpu.roll(t, HEAD // 2, 1)
    first = lax.broadcasted_iota(jnp.int32, t.shape, 1) < HEAD // 2
    return jnp.where(first, t, swapped), jnp.where(first, -swapped, t)


def rotated(t, cos, sin):
    return t * cos + pltpu.roll(t, HEAD // 2, 1) * sin


class Ring:
    def __init__(self, n):
        self.n, self.far_a = n, n // 2
        self.far_b = n - 1 - self.far_a
        self.me = lax.axis_index("dp")
        rep = lax.axis_index("rep")
        self.core = lax.rem(rep, 2)
        self.partner = {"rep": rep + 1 - 2 * self.core}
        self.turn = 1 - 2 * self.core
        self.near = 1, -1, 2, -2

    def at(self, k):
        return lax.rem(self.me + self.n + k * self.turn, self.n)

    def to(self, k):
        return {"dp": self.at(k)}

    def meet(self, partner):
        barrier = pltpu.get_barrier_semaphore()
        others = [self.to(k) for k in self.near] + [self.partner] * partner
        for other in others:
            pl.semaphore_signal(barrier, inc=1, device_id=other, device_id_type=MESH)
        pl.semaphore_wait(barrier, len(others))


def remote(src, dst, send, recv, to):
    return pltpu.make_async_remote_copy(src_ref=src, dst_ref=dst, send_sem=send, recv_sem=recv, device_id=to, device_id_type=MESH)


class Chains:
    def far(self, chain):
        return self.ring.far_b if chain else self.ring.far_a

    def stops(self, chain):
        return range(1, self.far(chain) + 1)

    def now(self, s):
        for count in range(1, s + 1):
            for chain in (A, B):
                if self.taken[chain] < min(count, len(self.stops(chain))):
                    self.taken[chain] += 1
                    self.take(chain, self.stops(chain)[self.taken[chain] - 1])

    def finish(self):
        self.now(self.ring.far_a)


class Gather(Chains):
    def __init__(self, ring, buf, sems, handed_sems, quick):
        self.taken = [0, 0]
        self.ring, self.buf, self.sems, self.handed_sems, self.quick = ring, buf, sems, handed_sems, quick
        self.half = buf.shape[1] // 2
        self.last_handed = None

    def stops(self, chain):
        some = [*super().stops(chain)]
        return some[1::-1] + some[2:] if self.quick else some

    def piece(self, block, half):
        return self.buf.at[block, pl.ds(pl.multiple_of(half * self.half, self.half), self.half), :]

    def hop(self, chain, step):
        ring = self.ring
        along = 1 if chain == A else -1
        done = step // 2 * 2 if self.quick else step
        part = self.piece(ring.at(-along * done), ring.core)
        return remote(part, part, self.sems.at[2 * chain, step], self.sems.at[2 * chain + 1, step], ring.to(along * (step + 1 - done)))

    def handed(self, chain, step):
        ring = self.ring
        part = self.piece(ring.at(-step - 1 if chain == A else step + 1), ring.core)
        return remote(part, part, self.handed_sems.at[ring.n - 1], self.handed_sems.at[step + chain * ring.far_a], ring.partner)

    def begin(self):
        for chain in (A, B):
            for step in (1, 0) if self.quick else (0,):
                self.hop(chain, step).start()

    def take(self, chain, s):
        ring = self.ring
        part = self.piece(ring.at(-s if chain == A else s), ring.core)
        remote(part, part, self.sems.at[2 * chain, s - 1], self.sems.at[2 * chain + 1, s - 1], ring.to(1)).wait_recv()
        for step in (range(s + 1, s - 1, -1) if s == 2 else ()) if self.quick else (s,):
            if step < self.far(chain):
                self.hop(chain, step).start()
        if self.last_handed:
            self.handed(*self.last_handed).wait_send()
        self.last_handed = chain, s - 1
        self.handed(*self.last_handed).start()

    def complete(self):
        ring = self.ring
        for chain in (A, B):
            for step in range(self.far(chain)):
                part = self.piece(ring.at(step + 1 if chain == A else -step - 1), 1 - ring.core)
                remote(part, part, self.handed_sems.at[ring.n - 1], self.handed_sems.at[step + chain * ring.far_a], ring.partner).wait_recv()

    def drain(self):
        for chain in (A, B):
            for step in range(self.far(chain)):
                self.hop(chain, step).wait_send()
        self.handed(*self.last_handed).wait_send()


class Scatter(Chains):
    def __init__(self, ring, p, came_a, came_b, sems, free, got, signal, taken=(0, 0)):
        self.signal = signal
        self.ring, self.p, self.came, self.sems, self.free, self.got = ring, p, (came_a, came_b), sems, free, got
        self.taken = list(taken)

    def hop(self, chain, step):
        ring = self.ring
        left = self.far(chain) - step
        block = ring.at(left if chain == 0 else -left)
        return remote(self.p.at[block], self.came[chain].at[step], self.sems.at[2 * chain, step], self.sems.at[2 * chain + 1, step],
                      ring.to(1 if chain == 0 else -1))

    def added(self, chain, step):
        ring = self.ring
        left = self.far(chain) - step
        block = ring.at(left if chain == 0 else -left)
        few = 16

        def rows(i):
            at = tile(i, few)
            self.p[block, at, :] = (self.p[block, at, :].astype(F32) + self.came[chain][step - 1, at, :].astype(F32)).astype(BF16)

        loop(self.p.shape[1] // few, rows)

    def begin(self, wait):
        pl.when(wait)(lambda: pl.semaphore_wait(self.free, len(self.ring.near)))
        self.hop(A, 0).start()
        self.hop(B, 0).start()

    def take(self, chain, s):
        self.hop(chain, s - 1).wait_recv()
        if s < self.far(chain):
            self.added(chain, s)
            self.hop(chain, s).start()
        if self.taken == [self.far(A), self.far(B)]:
            self.end()

    def arrived(self):
        return [(chain, self.far(chain) - 1) for chain in (A, B)]

    def end(self):
        me, few = self.ring.me, 16

        def rows(i):
            at = tile(i, few)
            total = self.p[me, at, :].astype(F32)
            for chain, slot in self.arrived():
                total += self.came[chain][slot, at, :].astype(F32)
            self.got[at, :] = total.astype(BF16)

        loop(self.p.shape[1] // few, rows)
        for chain in (A, B):
            for step in range(self.far(chain)):
                self.hop(chain, step).wait_send()

        @pl.when(self.signal)
        def _():
            for k in self.ring.near:
                pl.semaphore_signal(self.free, inc=1, device_id=self.ring.to(k), device_id_type=MESH)


class QuickScatter(Scatter):
    def hop(self, chain, step):
        ring = self.ring
        kind = step + self.far(A) - self.far(chain)
        block, reach = ((4, 2), (3, 1), (1, 1), (2, 2))[kind]
        along = 1 if chain == A else -1
        return remote(self.p.at[ring.at(along * block)], self.came[chain].at[step], self.sems.at[2 * chain, step], self.sems.at[2 * chain + 1, step],
                      ring.to(along * reach))

    def begin(self, wait):
        pl.when(wait)(lambda: pl.semaphore_wait(self.free, len(self.ring.near)))
        for step in range(self.far(A) - 1):
            for chain in (A, B):
                if step < self.far(chain) - 1:
                    self.hop(chain, step).start()

    def take(self, chain, s):
        self.hop(chain, s - 1).wait_recv()
        beyond = self.far(chain) - 2
        if s == beyond:
            block, few = self.ring.at(2 if chain == A else -2), 16

            def rows(i):
                at = tile(i, few)
                total = self.p[block, at, :].astype(F32)
                for slot in range(beyond):
                    total += self.came[chain][slot, at, :].astype(F32)
                self.p[block, at, :] = total.astype(BF16)

            loop(self.p.shape[1] // few, rows)
            self.hop(chain, self.far(chain) - 1).start()
        if self.taken == [self.far(A), self.far(B)]:
            self.end()

    def arrived(self):
        return [(chain, self.far(chain) - back) for chain in (A, B) for back in (1, 2)]


def merged(w):
    return w.reshape(w.shape[0] * w.shape[1], w.shape[2])


def qkv_phase(h, w, table, q, k, v, vt, rows, events):
    wide_q = q.shape[1]

    def step(i):
        at = tile(i, rows)
        wide = h[at, :].astype(F32)
        a = (wide * scale_of(wide)).astype(BF16)
        y = dot(a, merged(w[...])).astype(BF16)
        cos, sin = turns(table[at, :])
        for n in range(wide_q // HEAD):
            part = slice(n * HEAD, (n + 1) * HEAD)
            q[at, part] = rotated(y[:, part].astype(F32), cos, sin).astype(BF16)
        k[at, :] = rotated(y[:, wide_q : wide_q + HEAD].astype(F32), cos, sin).astype(BF16)
        mine = y[:, wide_q + HEAD :]
        v[at, :] = mine
        vt[:, at] = mine.T
        polled(events, i, h.shape[0] // rows)

    loop(h.shape[0] // rows, step)
    the_rest(events, h.shape[0] // rows)


def spans(bq):
    half = bq // 2
    return [(0, half, 0), (half, half, half)]


def seen(keys, first_key, queries, first_query):
    key = lax.broadcasted_iota(jnp.int32, (keys, queries), 0) + first_key
    return lax.broadcasted_iota(jnp.int32, (keys, queries), 1) + first_query >= key


def blocks(tokens, bq):
    return (tokens // bq) * (tokens // bq + 1) // 2


def row_of_blocks(iq, bq, block, events, steps):
    def step(j):
        @pl.when(j < iq)
        def _():
            block(pl.multiple_of(j * bq, bq), bq, 0, None)

        @pl.when(j == iq)
        def _():
            for first, nk, lo in spans(bq):
                block(pl.multiple_of(iq * bq + first, nk), nk, lo, seen(nk, first, bq - lo, lo))

        polled(events, lax.div(iq * (iq + 1), 2) + j, steps)

    loop(iq + 1, step)


def attend_phase(q, k, vt, o, lse, top_s, mix_s, bq, events):
    heads = q.shape[1] // HEAD

    def block(iq, start, nk, lo, mask):
        here = pl.ds(start, nk)
        cols = pl.ds(pl.multiple_of(iq * bq + lo, bq - lo), bq - lo)
        keys = k[here, :]
        scores = [dot(keys, q[cols, n * HEAD : (n + 1) * HEAD], 1, 1) for n in range(heads)]
        values = jnp.concatenate([vt[:, here], jnp.ones((8, nk), BF16)], axis=0)
        for n, s in enumerate(scores):
            if mask is not None:
                s = jnp.where(mask, s, HIDDEN)
            old = top_s[n : n + 1, lo:]
            top = jnp.maximum(old, s.max(axis=0, keepdims=True))
            top_s[n : n + 1, lo:] = top
            p = jnp.exp2((s - top) * E).astype(BF16)
            mix_s[n, :, lo:] = mix_s[n, :, lo:] * jnp.exp2((old - top) * E) + dot(values, p)

    def step(iq):
        at = tile(iq, bq)
        top_s[...] = jnp.full(top_s.shape, NEG, F32)
        mix_s[...] = jnp.zeros(mix_s.shape, F32)
        row_of_blocks(iq, bq, functools.partial(block, iq), events, blocks(q.shape[0], bq))
        for n in range(heads):
            total = mix_s[n, HEAD : HEAD + 1, :]
            o[at, n * HEAD : (n + 1) * HEAD] = (mix_s[n, :HEAD, :] * (1 / total)).T.astype(BF16)
            lse[n : n + 1, at] = top_s[n : n + 1, :] * E + jnp.log2(total)

    loop(q.shape[0] // bq, step)
    the_rest(events, blocks(q.shape[0], bq))


def mid_phase(h, o, od, hm, rows, r):
    def step(i):
        at = tile(i, rows)
        hm[at, :] = h[at, :] + dot(o[at, :], merged(od[:, :r, :])).astype(BF16)

    loop(h.shape[0] // rows, step)


def ffn_phase(hm, gu, od, out, rows, r, events):
    def step(i):
        at = tile(i, rows)
        mid = hm[at, :]
        wide = mid.astype(F32)
        b = (wide * scale_of(wide)).astype(BF16)
        y = dot(b, merged(gu[...]))
        part = y.shape[1] // 4
        pieces = []
        for n in (0, 2 * part):
            gate, up = y[:, n : n + part], y[:, n + part : n + 2 * part]
            pieces.append((gate * (1 / (1 + jnp.exp(-gate))) * up).astype(BF16))
        made = jnp.concatenate(pieces, axis=1)
        out[at, :] = mid + dot(made, merged(od[:, r:, :])).astype(BF16)
        polled(events, i, hm.shape[0] // rows)

    loop(hm.shape[0] // rows, step)
    the_rest(events, hm.shape[0] // rows)


def ffn_bwd_phase(half, hm, dy, gu, od, made_s, dgu_s, bt_s, db_s, dhm, rows, r, events):
    part = dgu_s.shape[1] // 4
    lanes, units = slice(2 * part * half, 2 * part * (half + 1)), slice(part * half, part * (half + 1))
    some = od.shape[0] // 2

    def step(i):
        at = tile(i, rows)
        wide = hm[at, :].astype(F32)
        scale = scale_of(wide)
        b = (wide * scale).astype(BF16)
        if half == 0:
            bt_s[:, at] = b.T
        y = dot(b, merged(gu[:, :, lanes]))
        gate, up = y[:, :part], y[:, part:]
        back = dy[at, :]
        d_made = dot(back, merged(od[some * half : some * (half + 1), r:, :]), 1, 1).astype(BF16).astype(F32)
        sig = 1 / (1 + jnp.exp(-gate))
        silu = gate * sig
        made_s[at, units] = (silu * up).astype(BF16)
        d_gate = (d_made * up * (sig * (1 + gate - silu))).astype(BF16)
        d_up = (d_made * silu).astype(BF16)
        both = jnp.concatenate([d_gate, d_up], axis=1)
        dgu_s[at, lanes] = both
        db = dot(both, merged(gu[:, :, lanes]), 1, 1)
        if half == 0:
            db_s[at, :] = db
        else:
            db = (db_s[at, :] + db).astype(BF16).astype(F32)
            dhm[at, :] = (back.astype(F32) + norm_bwd(wide, scale, db)).astype(BF16)
        polled(events, i, hm.shape[0] // rows)

    loop(hm.shape[0] // rows, step)
    the_rest(events, hm.shape[0] // rows)


def units_phase(half, dgu_s, bt_s, p):
    n, _, columns = p.shape
    wide = next(w for w in (512, 256, 128) if columns % w == 0)

    def units(i):
        here = pl.ds(pl.multiple_of(columns * half + i * wide, wide), wide)
        p[:, :, tile(i, wide)] = dot(bt_s[...], dgu_s[:, here]).astype(BF16).reshape(n, -1, wide)

    loop(columns // wide, units)


def downs_phase(made_s, dy, p):
    n, share, group = p.shape[0], p.shape[1], 2

    def downs(i):
        got = dot(made_s[:, tile(i, group * share)], dy[...], 0, 0).astype(BF16)
        p[pl.ds(i * group, group)] = got.reshape(group, share, -1)

    loop(n // group, downs)


def out_bwd_phase(dhm, o, od, p, do, rows, r):
    def step(i):
        at = tile(i, rows)
        do[at, :] = dot(dhm[at, :], merged(od[:, :r, :]), 1, 1).astype(BF16)

    loop(dhm.shape[0] // rows, step)
    p[...] = dot(o[...], dhm[...], 0, 0).astype(BF16).reshape(p.shape)


def attend_bwd_phase(q, k, v, o, do, lse, table, dqkv, dq_s, dk_s, dv_s, kt_s, bq, events):
    heads = q.shape[1] // HEAD
    wide_q = q.shape[1]
    dk_s[...] = jnp.zeros(dk_s.shape, F32)
    dv_s[...] = jnp.zeros(dv_s.shape, F32)
    kt_s[...] = k[...].T

    def block(iq, lses, deltas, start, nk, lo, mask):
        here = pl.ds(start, nk)
        cols = pl.ds(pl.multiple_of(iq * bq + lo, bq - lo), bq - lo)
        keys, values, keys_t = k[here, :], v[here, :], kt_s[:, here]
        qs = [q[cols, n * HEAD : (n + 1) * HEAD] for n in range(heads)]
        dos = [do[cols, n * HEAD : (n + 1) * HEAD] for n in range(heads)]
        scores = [dot(keys, x, 1, 1) for x in qs]
        dps = [dot(values, x, 1, 1) for x in dos]
        for n in range(heads):
            p = jnp.exp2(scores[n] * E - lses[n][:, lo:])
            if mask is not None:
                p = jnp.where(mask, p, 0.0)
            ds = (p * (dps[n] - deltas[n][:, lo:])).astype(BF16)
            dv_s[here, :] += dot(p.astype(BF16), dos[n])
            dk_s[here, :] += dot(ds, qs[n])
            dq_s[n, :, lo:] += dot(keys_t, ds)

    def step(iq):
        at = tile(iq, bq)
        dq_s[...] = jnp.zeros(dq_s.shape, F32)
        lses = [lse[n : n + 1, at] for n in range(heads)]
        deltas = []
        for n in range(heads):
            part = slice(n * HEAD, (n + 1) * HEAD)
            deltas.append((do[at, part].astype(F32) * o[at, part].astype(F32)).T.sum(axis=0, keepdims=True))
        row_of_blocks(iq, bq, functools.partial(block, iq, lses, deltas), events, blocks(q.shape[0], bq))
        cos, sin = turns(table[at, :])
        for n in range(heads):
            back = (dq_s[n] * SCALE).T.astype(BF16).astype(F32)
            dqkv[at, n * HEAD : (n + 1) * HEAD] = rotated(back, cos, -sin).astype(BF16)

    loop(q.shape[0] // bq, step)
    the_rest(events, blocks(q.shape[0], bq))

    def finish(i):
        at = tile(i, bq)
        cos, sin = turns(table[at, :])
        dqkv[at, wide_q : wide_q + HEAD] = rotated((dk_s[at, :] * SCALE).astype(BF16).astype(F32), cos, -sin).astype(BF16)
        dqkv[at, wide_q + HEAD :] = dv_s[at, :].astype(BF16)

    loop(q.shape[0] // bq, finish)


def qkv_bwd_phase(h, dqkv, w, dhm, p_qkv, a_s, dh, rows, further):
    def step(i):
        at = tile(i, rows)
        wide = h[at, :].astype(F32)
        scale = scale_of(wide)
        a_s[at, :] = (wide * scale).astype(BF16)

        @pl.when(further)
        def _():
            da = dot(dqkv[at, :], merged(w[...]), 1, 1).astype(BF16).astype(F32)
            dh[at, :] = (dhm[at, :].astype(F32) + norm_bwd(wide, scale, da)).astype(BF16)

    loop(h.shape[0] // rows, step)
    p_qkv[...] = dot(a_s[...], dqkv[...], 0, 0).astype(BF16).reshape(p_qkv.shape)


QKV, OD, GU = range(3)
OWN, OLD = range(2)
NEXT = OLD
PLAN = {
    "qkv": ((0, OD, OWN, 2), (0, QKV, NEXT, 0), (3, GU, OWN, 2)),
    "attend": ((1, OD, OWN, 3), (2, QKV, NEXT, 1), (2, OD, NEXT, 0), (4, GU, OWN, 3), (6, OD, OWN, 4), (6, GU, NEXT, 0), (7, QKV, NEXT, 2), (8, OD, NEXT, 1)),
    "ffn": ((0, GU, NEXT, 1), (1, QKV, NEXT, 4), (1, OD, NEXT, 2), (3, GU, NEXT, 2)),
}
LAST_PLAN = {"qkv": ((0, OD, OWN, 3),), "attend": ((2, GU, OWN, 3), (3, OD, OWN, 4), (6, GU, OWN, 4))}
HEAD_PLAN = ((QKV, 1), (QKV, 2), (GU, 0), (QKV, 3), (OD, 1), (QKV, 4))


def planned(act, entries):
    by_step = {}
    for when, *what in entries:
        by_step.setdefault(when, []).append(what)
    return {when: functools.partial(act, whats) for when, whats in by_step.items()}


def forward(sizes, x, few, wq, wk, wv, wo, wg, wu, wd, q_o, k_o, v_o, o_o, lse_o, hm_o, h_o, qkv_o, gu_o, od_o, table_o,
            h_s, few_s, table_s, qkv_s, gu_s, od_s, q_s, k_s, v_s, vt_s, o_s, lse_s, hm_s, top_s, mix_s, own_sem, in_sem, out_sem, gather_sems, handed_sems):
    layers, n, bq, rows = sizes
    ring = Ring(n)
    me = ring.me
    wide_q, ff, ro = wq.shape[2], wg.shape[2], wo.shape[1]
    half = ff // 2
    own = {}

    def fetch(i, group, pieces):
        for src, dst in pieces:
            copy = pltpu.make_async_copy(src, dst, own_sem.at[sum(map(len, own.values()))])
            own.setdefault((i, group), []).append(copy)
            copy.start()

    for i in range(layers):
        fetch(i, QKV, [(wq.at[i], qkv_s.at[i, me, :, :wide_q]), (wk.at[i], qkv_s.at[i, me, :, wide_q : wide_q + HEAD]), (wv.at[i], qkv_s.at[i, me, :, wide_q + HEAD :])])
        fetch(i, OD, [(wo.at[i], od_s.at[i, me, :ro, :]), (wd.at[i], od_s.at[i, me, ro:, :])])
        if i == 0:
            brought = [pltpu.make_async_copy(x, h_s.at[0], in_sem.at[0]), pltpu.make_async_copy(few, few_s, in_sem.at[1])]
            for copy in brought:
                copy.start()
        fetch(i, GU, [(w.at[i, :, half * j : half * (j + 1)], gu_s.at[i, me, :, half * (2 * j + k) : half * (2 * j + k + 1)]) for j in (0, 1) for k, w in enumerate((wg, wu))])
    packs = {(g, i): Gather(ring, buf.at[i], gather_sems.at[3 * i + g], handed_sems.at[3 * i + g], g == QKV) for g, buf in enumerate((qkv_s, od_s, gu_s)) for i in range(layers)}
    begun = set()
    out = []

    def keep(src, dst):
        out.append(pltpu.make_async_copy(src, dst, out_sem.at[len(out)]))
        out[-1].start()

    def begin(group, i):
        if (group, i) not in begun:
            begun.add((group, i))
            for copy in own[i, group]:
                copy.wait()
            packs[group, i].begin()

    def act(i, whats):
        for group, which, stop in whats:
            if i + which < layers:
                begin(group, i + which)
                packs[group, i + which].now(stop)

    def plan(phase, i):
        return planned(functools.partial(act, i), (PLAN if i + 1 < layers else LAST_PLAN).get(phase, ()))

    def whole(group, i):
        begin(group, i)
        packs[group, i].finish()
        packs[group, i].complete()

    ring.meet(1)
    begin(QKV, 0)
    begin(OD, 0)
    for copy in brought:
        copy.wait()
    table_phase(few_s, table_s)
    keep(table_s, table_o)
    act(0, [(group, OWN, stop) for group, stop in HEAD_PLAN])
    for i in range(layers):
        keep(h_s.at[i], h_o.at[i])
        whole(QKV, i)
        keep(qkv_s.at[i], qkv_o.at[i])
        qkv_phase(h_s.at[i], qkv_s.at[i], table_s, q_s.at[i], k_s.at[i], v_s.at[i], vt_s, rows, plan("qkv", i))
        keep(q_s.at[i], q_o.at[i])
        keep(k_s.at[i], k_o.at[i])
        keep(v_s.at[i], v_o.at[i])
        attend_phase(q_s.at[i], k_s.at[i], vt_s, o_s.at[i], lse_s.at[i], top_s, mix_s, bq, plan("attend", i))
        keep(o_s.at[i], o_o.at[i])
        keep(lse_s.at[i], lse_o.at[i])
        whole(OD, i)
        keep(od_s.at[i], od_o.at[i])
        mid_phase(h_s.at[i], o_s.at[i], od_s.at[i], hm_s.at[i], rows, ro)
        keep(hm_s.at[i], hm_o.at[i])
        whole(GU, i)
        keep(gu_s.at[i], gu_o.at[i])
        if i + 1 < layers:
            ffn_phase(hm_s.at[i], gu_s.at[i], od_s.at[i], h_s.at[i + 1], rows, ro, plan("ffn", i))
    for copy in out:
        copy.wait()
    for pack in packs.values():
        pack.drain()


PACKS = 5
QKV_G, GA_G, GB_G, WD_G, WO_G = range(PACKS)
BACK = {
    "first": ((1, QKV_G, OLD, 2), (2, WD_G, OLD, 4), (2, WO_G, OLD, 4), (3, QKV_G, OLD, 4)),
    "second": ((2, GA_G, OWN, 1),),
    "downs": ((0, GA_G, OWN, 2),),
    "attend": ((0, GB_G, OWN, 1), (1, WD_G, OWN, 1), (2, GA_G, OWN, 3), (3, WO_G, OWN, 1), (4, GB_G, OWN, 2), (6, WD_G, OWN, 2), (7, GA_G, OWN, 4), (8, WO_G, OWN, 2),
               (9, GB_G, OWN, 3)),
    "end": ((0, GB_G, OWN, 4), (0, WD_G, OWN, 3), (0, WO_G, OWN, 3)),
}
TAIL = ((QKV_G, 2), (WD_G, 4), (WO_G, 4), (QKV_G, 4))
NAMED = ("gu", "hm", "dy", "od", "table", "q", "k", "v", "o", "lse", "h", "qkv")


def backward(sizes, dy, table, qkv, gu, od, q, k, v, o, lse, hm, h, *refs):
    layers, n, bq, rows, r = sizes
    results, refs = refs[:PACKS], refs[PACKS:]
    table_s, qkv_s, gu_s, od_s, lse_s, hm_s, dh_s, dhm_s, made_s, dgu_s, bt_s, db_s, dq_s, kt_s = refs[:14]
    refs = refs[14:]
    terms, came_a, came_b, got = (refs[PACKS * i : PACKS * (i + 1)] for i in range(4))
    in_sem, out_sem, scatter_sems, free_sems = refs[PACKS * 4 :]
    ring = Ring(n)
    split, heads = qkv_s.shape[2], q.shape[2]
    dqkv_s, do_s = made_s.at[:, :split], made_s.at[:, split : split + heads]
    dk_s, dv_s = db_s.at[:, :HEAD], db_s.at[:, HEAD : 2 * HEAD]
    place = 0
    lent = []
    for width in (heads, heads, HEAD, HEAD, h.shape[2]):
        lent.append(dgu_s.at[:, place : place + width])
        place += width
    q_s, o_s, k_s, v_s, h_s = lent
    places = {"gu": (gu, gu_s), "hm": (hm, hm_s), "dy": (dy, dh_s), "od": (od, od_s), "table": (table, table_s), "q": (q, q_s), "k": (k, k_s), "v": (v, v_s),
              "o": (o, o_s), "lse": (lse, lse_s), "h": (h, h_s), "qkv": (qkv, qkv_s)}

    def copy_of(name, *i):
        src, dst = places[name]
        return pltpu.make_async_copy(src.at[i] if i else src, dst, in_sem.at[NAMED.index(name)])

    def bring(names, *i):
        for name in names:
            copy_of(name, *i).start()

    def need(names, *i):
        for name in names:
            copy_of(name, *i).wait()

    last = layers - 1
    bring(("gu", "hm"), last)
    bring(("dy",))
    bring(("od",), last)
    bring(("table",))
    bring(("qkv",), last)
    ring.meet(0)

    def pack(group, i, signal, taken=(0, 0)):
        return (QuickScatter if group == QKV_G else Scatter)(ring, terms[group], came_a[group], came_b[group], scatter_sems.at[group], free_sems.at[group], got[group].at[i], signal, taken)

    reached = {}
    for entries in BACK.values():
        for _, group, old, stop in entries:
            if old == OWN:
                reached[group] = max(stop, reached.get(group, 0))
    taken = {group: (min(stop, ring.far_a), min(stop, ring.far_b)) for group, stop in reached.items()}

    def layer(step):
        i = last - step
        later = step > 0
        own = {group: pack(group, i, i > 0) for group in range(PACKS)}
        old = {group: pack(group, i + 1, i >= 0, taken.get(group, (0, 0))) for group in range(PACKS)}

        def act(whats):
            for group, which, stop in whats:
                if which == OWN:
                    own[group].now(stop)
                else:
                    pl.when(later)(functools.partial(old[group].now, stop))

        def plan(phase):
            return planned(act, BACK[phase])

        def before(group):
            pl.when(later)(old[group].finish)

        need(("gu", "hm", "od"), i)
        pl.when(step == 0)(functools.partial(need, ("dy",)))
        for half, group, phase in ((0, GA_G, "first"), (1, GB_G, "second")):
            ffn_bwd_phase(half, hm_s, dh_s, gu_s, od_s, made_s, dgu_s, bt_s, db_s, dhm_s, rows, r, plan(phase))
            if half == 1:
                pl.when(i > 0)(functools.partial(bring, ("gu", "hm"), i - 1))
            before(group)
            units_phase(half, dgu_s, bt_s, terms[group])
            own[group].begin(later)
        bring(("o", "q", "k", "v", "lse", "h"), i)
        before(WD_G)
        downs_phase(made_s, dh_s, terms[WD_G])
        own[WD_G].begin(later)
        the_rest(plan("downs"), 0)
        need(("o",), i)
        before(WO_G)
        out_bwd_phase(dhm_s, o_s, od_s, terms[WO_G], do_s, rows, r)
        own[WO_G].begin(later)
        pl.when(i > 0)(functools.partial(bring, ("od",), i - 1))
        need(("q", "k", "v", "lse"), i)
        pl.when(step == 0)(functools.partial(need, ("table",)))
        attend_bwd_phase(q_s, k_s, v_s, o_s, do_s, lse_s, table_s, dqkv_s, dq_s, dk_s, dv_s, kt_s, bq, plan("attend"))
        need(("h",), i)
        pl.when(step == 0)(functools.partial(need, ("qkv",), last))
        before(QKV_G)
        qkv_bwd_phase(h_s, dqkv_s, qkv_s, dhm_s, terms[QKV_G], do_s, dh_s, rows, i > 0)
        own[QKV_G].begin(later)
        the_rest(plan("end"), 0)

        @pl.when(jnp.logical_and(i > 1, i < layers))
        def _():
            copy_of("qkv", i - 1).start()
            copy_of("qkv", i - 1).wait()

    loop(layers, layer)
    final = {group: pack(group, 0, False, taken.get(group, (0, 0))) for group in range(PACKS)}
    for group, stop in TAIL:
        final[group].now(stop)
    for p in final.values():
        p.finish()
    out = []
    for group in range(PACKS):
        for i in range(layers):
            out.append(pltpu.make_async_copy(got[group].at[i], results[group].at[i], out_sem.at[len(out)]))
            out[-1].start()
    for copy in out:
        copy.wait()


SEVEN = 7
START = 0


def adamw(*refs):
    count = 3 * SEVEN
    grads, refs = refs[:PACKS], refs[PACKS:]
    ins, outs, refs = refs[:count], refs[count : 2 * count], refs[2 * count :]
    grads_s, refs = refs[:PACKS], refs[PACKS:]
    ins_s, outs_s, (grad_sem, in_sem, out_sem) = refs[:count], refs[count : 2 * count], refs[2 * count :]
    kinds = range(0, count, SEVEN)
    layers = ins[0].shape[0]
    heads, half, whole, few = ins[0].shape[2], ins[4].shape[2] // 2, ins[3].shape[2], 16
    waits = []
    for i in range(layers):
        copies = [pltpu.make_async_copy(src.at[i], dst.at[i], grad_sem.at[g, i]) for g, (src, dst) in enumerate(zip(grads, grads_s, strict=True))]
        copies += [pltpu.make_async_copy(ins[a].at[i], ins_s[a].at[i], in_sem.at[a, i]) for w in range(SEVEN) for a in (w + kind for kind in kinds)]
        for copy in copies:
            copy.start()
        waits.append(copies)
    parts = (
        [(QKV_G, START, START, heads)], [(QKV_G, heads, START, HEAD)], [(QKV_G, heads + HEAD, START, HEAD)], [(WO_G, START, START, whole)],
        [(GA_G, START, START, half), (GB_G, START, half, half)], [(GA_G, half, START, half), (GB_G, half, half, half)], [(WD_G, START, START, whole)],
    )
    out = []
    for i in range(layers):
        for copy in waits[i][:PACKS]:
            copy.wait()
        for w in range(SEVEN):
            for copy in waits[i][PACKS + 3 * w : PACKS + 3 * (w + 1)]:
                copy.wait()

            def step(j, i=i, w=w):
                at = tile(j, few)
                for grad, first, start, wide in parts[w]:
                    here = slice(start, start + wide)
                    g = grads_s[grad][i, at, first : first + wide].astype(F32)
                    weight = ins_s[w][i, at, here].astype(F32)
                    of_m, of_v = w + SEVEN, w + 2 * SEVEN
                    m = 0.9 * ins_s[of_m][i, at, here] + 0.1 * g
                    v = 0.95 * ins_s[of_v][i, at, here] + 0.05 * g * g
                    outs_s[w][i, at, here] = (weight - 0.02 * (m * lax.rsqrt(v + 1e-8) + 0.1 * weight)).astype(BF16)
                    outs_s[of_m][i, at, here] = m
                    outs_s[of_v][i, at, here] = v

            loop(ins[w].shape[1] // few, step)
            for a in (w + kind for kind in kinds):
                out.append(pltpu.make_async_copy(outs_s[a].at[i], outs[a].at[i], out_sem.at[a, i]))
                out[-1].start()
    for copy in out:
        copy.wait()


def solution(mesh):
    n = mesh.shape["dp"]
    far_a, far_b = n // 2, n - 1 - n // 2

    def step(x, dy, *arrays):
        weights = arrays[:SEVEN]
        wq, wk, wv, wo, wg, wu, wd = weights
        layers, r, wide_q = wq.shape
        x, dy = x[0], dy[0]
        tokens, d = x.shape
        ff = wg.shape[2]
        bq, rows = (min(512, tokens),) * 2
        few = jnp.asarray(angles(tokens))
        wide = wide_q + 2 * HEAD
        heads = wide_q // HEAD
        ro = wo.shape[1]
        shapes = (r, wide), (r, 2 * ff), (ro + wd.shape[1], d)
        terms = (r, wide), (r, ff), (r, ff), (wd.shape[1], d), (ro, d)
        both = lambda *s: jax.ShapeDtypeStruct((layers, *s), BF16)
        some = lambda lead, s: pltpu.VMEM((*lead, *s), BF16)
        q, k, v_, o, lse, hm, h, qkv, gu, od, table = pl.pallas_call(
            functools.partial(forward, (layers, n, bq, rows)),
            out_shape=[both(tokens, wide_q), both(tokens, HEAD), both(tokens, HEAD), both(tokens, wide_q), jax.ShapeDtypeStruct((layers, 8, tokens), F32),
                       both(tokens, d), both(tokens, d), *(both(n, *s) for s in shapes), jax.ShapeDtypeStruct((tokens, HEAD), F32)],
            in_specs=[ANY] * 9,
            out_specs=[ANY] * 11,
            scratch_shapes=[
                pltpu.VMEM((layers, tokens, d), BF16), pltpu.VMEM(few.shape, F32), pltpu.VMEM((tokens, HEAD), F32),
                *(some((layers, n), s) for s in shapes),
                pltpu.VMEM((layers, tokens, wide_q), BF16), pltpu.VMEM((layers, tokens, HEAD), BF16), pltpu.VMEM((layers, tokens, HEAD), BF16),
                pltpu.VMEM((HEAD, tokens), BF16), pltpu.VMEM((layers, tokens, wide_q), BF16), pltpu.VMEM((layers, 8, tokens), F32),
                pltpu.VMEM((layers, tokens, d), BF16), pltpu.VMEM((heads, bq), F32), pltpu.VMEM((heads, HEAD + 8, bq), F32),
                pltpu.SemaphoreType.DMA((9 * layers,)), pltpu.SemaphoreType.DMA((2,)), pltpu.SemaphoreType.DMA((10 * layers + 1,)),
                pltpu.SemaphoreType.DMA((3 * layers, 4, far_a)), pltpu.SemaphoreType.DMA((3 * layers, n)),
            ],
            compiler_params=pltpu.CompilerParams(vmem_limit_bytes=VMEM, collective_id=0, has_side_effects=True),
            name="forward",
        )(x, few, *weights)
        grads = pl.pallas_call(
            functools.partial(backward, (layers, n, bq, rows, ro)),
            out_shape=[both(*s) for s in terms],
            in_specs=[ANY] * 12,
            out_specs=[ANY] * 5,
            scratch_shapes=[
                pltpu.VMEM((tokens, HEAD), F32), *(some((n,), s) for s in shapes),
                pltpu.VMEM((8, tokens), F32), pltpu.VMEM((tokens, d), BF16), pltpu.VMEM((tokens, d), BF16), pltpu.VMEM((tokens, d), BF16),
                pltpu.VMEM((tokens, ff), BF16), pltpu.VMEM((tokens, 2 * ff), BF16), pltpu.VMEM((d, tokens), BF16),
                pltpu.VMEM((tokens, d), F32), pltpu.VMEM((heads, HEAD, bq), F32), pltpu.VMEM((HEAD, tokens), BF16),
                *(some((lead,), s) for lead in (n, far_a, far_b, layers) for s in terms),
                pltpu.SemaphoreType.DMA((len(NAMED),)), pltpu.SemaphoreType.DMA((5 * layers,)),
                pltpu.SemaphoreType.DMA((5, 4, far_a)), pltpu.SemaphoreType.REGULAR((5,)),
            ],
            compiler_params=pltpu.CompilerParams(vmem_limit_bytes=VMEM, collective_id=1, has_side_effects=True),
            name="backward",
        )(dy, table, qkv, gu, od, q, k, v_, o, lse, hm, h)
        in_vmem = lambda a: pltpu.VMEM(a.shape, a.dtype)
        return pl.pallas_call(
            adamw,
            out_shape=[jax.ShapeDtypeStruct(a.shape, a.dtype) for a in arrays],
            in_specs=[ANY] * (PACKS + 3 * SEVEN),
            out_specs=[ANY] * (3 * SEVEN),
            scratch_shapes=[*map(in_vmem, grads), *map(in_vmem, arrays), *map(in_vmem, arrays),
                            pltpu.SemaphoreType.DMA((PACKS, layers)), *(pltpu.SemaphoreType.DMA((3 * SEVEN, layers)) for _ in arrays[:2])],
            compiler_params=pltpu.CompilerParams(vmem_limit_bytes=VMEM),
            name="adamw",
        )(*grads, *arrays)

    states, cut = P(("rep", "dp"), None, None), P(None, "dp", None)
    return jax.shard_map(
        step,
        mesh=mesh,
        in_specs=(states, states) + (cut,) * (3 * SEVEN),
        out_specs=(P("rep", "dp", None),) * (3 * SEVEN),
        check_vma=False,
    )
```

```python
import functools

import jax
import jax.numpy as jnp
import numpy as np
from jax import lax
from jax.experimental import pallas as pl
from jax.experimental.pallas import tpu as pltpu
from jax.sharding import PartitionSpec as P

HEAD = 128
THETA = 10000
NEG = -1e30
HIDDEN = 2 * NEG
LOG2E = 1.4426950408889634
SCALE = HEAD**-0.5
E = SCALE * LOG2E
VMEM = 66_000_000
STRETCH = 64
F32, BF16 = jnp.float32, jnp.bfloat16
ANY = pl.BlockSpec(memory_space=pl.ANY)
MESH = pl.DeviceIdType.MESH
A, B = 0, 1


def dot(a, b, ca=1, cb=0):
    return lax.dot_general(a, b, (((ca,), (cb,)), ((), ())), preferred_element_type=F32)


def scoped(name, what, *args):
    with jax.named_scope(name):
        return what(*args)


def tile(i, n):
    return pl.ds(pl.multiple_of(i * n, n), n)


def loop(n, body):
    lax.fori_loop(0, n, lambda i, _: body(i), None)


def polled(events, i, steps):
    for when, what in events.items():
        if when < steps:
            pl.when(i == when)(functools.partial(scoped, f"ev{when}", what))


def the_rest(events, steps):
    for when, what in events.items():
        if when >= steps:
            what()


def scale_of(wide):
    return lax.rsqrt(jnp.mean(wide * wide, -1, keepdims=True) + 1e-6)


def norm_bwd(wide, scale, g):
    return scale * g - wide * (scale * scale * scale * jnp.mean(wide * g, -1, keepdims=True))


def angles(tokens):
    half = HEAD // 2
    turn = float(THETA) ** (-np.arange(half) / half)
    place = np.arange(STRETCH)[:, None] * turn
    start = np.arange(0, tokens, STRETCH)[:, None] * turn
    cos, sin = np.cos(start), np.sin(start)
    return np.concatenate([np.concatenate(p, 1) for p in ((np.cos(place), np.sin(place)), (cos, cos), (-sin, sin))]).astype(np.float32)


def table_phase(few, table):
    starts = table.shape[0] // STRETCH

    def step(i):
        place = few[:STRETCH, :]
        row = lambda first: few[pl.ds(first + i, 1), :]
        table[tile(i, STRETCH), :] = place * row(STRETCH) + pltpu.roll(place, HEAD // 2, 1) * row(STRETCH + starts)

    loop(starts, step)


def turns(t):
    swapped = pltpu.roll(t, HEAD // 2, 1)
    first = lax.broadcasted_iota(jnp.int32, t.shape, 1) < HEAD // 2
    return jnp.where(first, t, swapped), jnp.where(first, -swapped, t)


def rotated(t, cos, sin):
    return t * cos + pltpu.roll(t, HEAD // 2, 1) * sin


class Ring:
    def __init__(self, n):
        self.n, self.far_a = n, n // 2
        self.far_b = n - 1 - self.far_a
        self.me = lax.axis_index("dp")
        rep = lax.axis_index("rep")
        self.core = lax.rem(rep, 2)
        self.partner = {"rep": rep + 1 - 2 * self.core}
        self.turn = 1 - 2 * self.core
        self.near = 1, -1, 2, -2

    def at(self, k):
        return lax.rem(self.me + self.n + k * self.turn, self.n)

    def to(self, k):
        return {"dp": self.at(k)}

    def meet(self, partner):
        barrier = pltpu.get_barrier_semaphore()
        others = [self.to(k) for k in self.near] + [self.partner] * partner
        for other in others:
            pl.semaphore_signal(barrier, inc=1, device_id=other, device_id_type=MESH)
        pl.semaphore_wait(barrier, len(others))


def remote(src, dst, send, recv, to):
    return pltpu.make_async_remote_copy(src_ref=src, dst_ref=dst, send_sem=send, recv_sem=recv, device_id=to, device_id_type=MESH)


class Chains:
    def far(self, chain):
        return self.ring.far_b if chain else self.ring.far_a

    def stops(self, chain):
        return range(1, self.far(chain) + 1)

    def now(self, s):
        for count in range(1, s + 1):
            for chain in (A, B):
                if self.taken[chain] < min(count, len(self.stops(chain))):
                    self.taken[chain] += 1
                    self.take(chain, self.stops(chain)[self.taken[chain] - 1])

    def finish(self):
        self.now(self.ring.far_a)


class Gather(Chains):
    def __init__(self, ring, buf, sems, handed_sems, quick):
        self.taken = [0, 0]
        self.ring, self.buf, self.sems, self.handed_sems, self.quick = ring, buf, sems, handed_sems, quick
        self.half = buf.shape[1] // 2
        self.last_handed = None

    def stops(self, chain):
        some = [*super().stops(chain)]
        return some[1::-1] + some[2:] if self.quick else some

    def piece(self, block, half):
        return self.buf.at[block, pl.ds(pl.multiple_of(half * self.half, self.half), self.half), :]

    def hop(self, chain, step):
        ring = self.ring
        along = 1 if chain == A else -1
        done = step // 2 * 2 if self.quick else step
        part = self.piece(ring.at(-along * done), ring.core)
        return remote(part, part, self.sems.at[2 * chain, step], self.sems.at[2 * chain + 1, step], ring.to(along * (step + 1 - done)))

    def handed(self, chain, step):
        ring = self.ring
        part = self.piece(ring.at(-step - 1 if chain == A else step + 1), ring.core)
        return remote(part, part, self.handed_sems.at[ring.n - 1], self.handed_sems.at[step + chain * ring.far_a], ring.partner)

    def begin(self):
        for chain in (A, B):
            for step in (1, 0) if self.quick else (0,):
                self.hop(chain, step).start()

    def take(self, chain, s):
        ring = self.ring
        part = self.piece(ring.at(-s if chain == A else s), ring.core)
        remote(part, part, self.sems.at[2 * chain, s - 1], self.sems.at[2 * chain + 1, s - 1], ring.to(1)).wait_recv()
        for step in (range(s + 1, s - 1, -1) if s == 2 else ()) if self.quick else (s,):
            if step < self.far(chain):
                self.hop(chain, step).start()
        if self.last_handed:
            self.handed(*self.last_handed).wait_send()
        self.last_handed = chain, s - 1
        self.handed(*self.last_handed).start()

    def complete(self):
        ring = self.ring
        for chain in (A, B):
            for step in range(self.far(chain)):
                part = self.piece(ring.at(step + 1 if chain == A else -step - 1), 1 - ring.core)
                remote(part, part, self.handed_sems.at[ring.n - 1], self.handed_sems.at[step + chain * ring.far_a], ring.partner).wait_recv()

    def drain(self):
        for chain in (A, B):
            for step in range(self.far(chain)):
                self.hop(chain, step).wait_send()
        self.handed(*self.last_handed).wait_send()


class Scatter(Chains):
    def __init__(self, ring, p, came_a, came_b, sems, free, got, signal, taken=(0, 0)):
        self.signal = signal
        self.ring, self.p, self.came, self.sems, self.free, self.got = ring, p, (came_a, came_b), sems, free, got
        self.taken = list(taken)

    def hop(self, chain, step):
        ring = self.ring
        left = self.far(chain) - step
        block = ring.at(left if chain == 0 else -left)
        return remote(self.p.at[block], self.came[chain].at[step], self.sems.at[2 * chain, step], self.sems.at[2 * chain + 1, step],
                      ring.to(1 if chain == 0 else -1))

    def added(self, chain, step):
        ring = self.ring
        left = self.far(chain) - step
        block = ring.at(left if chain == 0 else -left)
        few = 16

        def rows(i):
            at = tile(i, few)
            self.p[block, at, :] = (self.p[block, at, :].astype(F32) + self.came[chain][step - 1, at, :].astype(F32)).astype(BF16)

        loop(self.p.shape[1] // few, rows)

    def begin(self, wait):
        pl.when(wait)(lambda: pl.semaphore_wait(self.free, len(self.ring.near)))
        self.hop(A, 0).start()
        self.hop(B, 0).start()

    def take(self, chain, s):
        self.hop(chain, s - 1).wait_recv()
        if s < self.far(chain):
            self.added(chain, s)
            self.hop(chain, s).start()
        if self.taken == [self.far(A), self.far(B)]:
            self.end()

    def arrived(self):
        return [(chain, self.far(chain) - 1) for chain in (A, B)]

    def end(self):
        me, few = self.ring.me, 16

        def rows(i):
            at = tile(i, few)
            total = self.p[me, at, :].astype(F32)
            for chain, slot in self.arrived():
                total += self.came[chain][slot, at, :].astype(F32)
            self.got[at, :] = total.astype(BF16)

        loop(self.p.shape[1] // few, rows)
        for chain in (A, B):
            for step in range(self.far(chain)):
                self.hop(chain, step).wait_send()

        @pl.when(self.signal)
        def _():
            for k in self.ring.near:
                pl.semaphore_signal(self.free, inc=1, device_id=self.ring.to(k), device_id_type=MESH)


class QuickScatter(Scatter):
    def hop(self, chain, step):
        ring = self.ring
        kind = step + self.far(A) - self.far(chain)
        block, reach = ((4, 2), (3, 1), (1, 1), (2, 2))[kind]
        along = 1 if chain == A else -1
        return remote(self.p.at[ring.at(along * block)], self.came[chain].at[step], self.sems.at[2 * chain, step], self.sems.at[2 * chain + 1, step],
                      ring.to(along * reach))

    def begin(self, wait):
        pl.when(wait)(lambda: pl.semaphore_wait(self.free, len(self.ring.near)))
        for step in range(self.far(A) - 1):
            for chain in (A, B):
                if step < self.far(chain) - 1:
                    self.hop(chain, step).start()

    def take(self, chain, s):
        self.hop(chain, s - 1).wait_recv()
        beyond = self.far(chain) - 2
        if s == beyond:
            block, few = self.ring.at(2 if chain == A else -2), 16

            def rows(i):
                at = tile(i, few)
                total = self.p[block, at, :].astype(F32)
                for slot in range(beyond):
                    total += self.came[chain][slot, at, :].astype(F32)
                self.p[block, at, :] = total.astype(BF16)

            loop(self.p.shape[1] // few, rows)
            self.hop(chain, self.far(chain) - 1).start()
        if self.taken == [self.far(A), self.far(B)]:
            self.end()

    def arrived(self):
        return [(chain, self.far(chain) - back) for chain in (A, B) for back in (1, 2)]


def merged(w):
    return w.reshape(w.shape[0] * w.shape[1], w.shape[2])


def qkv_phase(h, w, table, q, k, v, vt, rows, events):
    wide_q = q.shape[1]

    def step(i):
        at = tile(i, rows)
        wide = h[at, :].astype(F32)
        a = (wide * scale_of(wide)).astype(BF16)
        y = dot(a, merged(w[...])).astype(BF16)
        cos, sin = turns(table[at, :])
        for n in range(wide_q // HEAD):
            part = slice(n * HEAD, (n + 1) * HEAD)
            q[at, part] = rotated(y[:, part].astype(F32), cos, sin).astype(BF16)
        k[at, :] = rotated(y[:, wide_q : wide_q + HEAD].astype(F32), cos, sin).astype(BF16)
        mine = y[:, wide_q + HEAD :]
        v[at, :] = mine
        vt[:, at] = mine.T
        polled(events, i, h.shape[0] // rows)

    loop(h.shape[0] // rows, step)
    the_rest(events, h.shape[0] // rows)


def spans(bq):
    half = bq // 2
    return [(0, half, 0), (half, half, half)]


def seen(keys, first_key, queries, first_query):
    key = lax.broadcasted_iota(jnp.int32, (keys, queries), 0) + first_key
    return lax.broadcasted_iota(jnp.int32, (keys, queries), 1) + first_query >= key


def blocks(tokens, bq):
    return (tokens // bq) * (tokens // bq + 1) // 2


def row_of_blocks(iq, bq, block, events, steps):
    def step(j):
        @pl.when(j < iq)
        def _():
            block(pl.multiple_of(j * bq, bq), bq, 0, None)

        @pl.when(j == iq)
        def _():
            for first, nk, lo in spans(bq):
                block(pl.multiple_of(iq * bq + first, nk), nk, lo, seen(nk, first, bq - lo, lo))

        polled(events, lax.div(iq * (iq + 1), 2) + j, steps)

    loop(iq + 1, step)


def attend_phase(q, k, vt, o, lse, top_s, mix_s, bq, events):
    heads = q.shape[1] // HEAD

    def block(iq, start, nk, lo, mask):
        here = pl.ds(start, nk)
        cols = pl.ds(pl.multiple_of(iq * bq + lo, bq - lo), bq - lo)
        keys = k[here, :]
        scores = [dot(keys, q[cols, n * HEAD : (n + 1) * HEAD], 1, 1) for n in range(heads)]
        values = jnp.concatenate([vt[:, here], jnp.ones((8, nk), BF16)], axis=0)
        for n, s in enumerate(scores):
            if mask is not None:
                s = jnp.where(mask, s, HIDDEN)
            old = top_s[n : n + 1, lo:]
            top = jnp.maximum(old, s.max(axis=0, keepdims=True))
            top_s[n : n + 1, lo:] = top
            p = jnp.exp2((s - top) * E).astype(BF16)
            mix_s[n, :, lo:] = mix_s[n, :, lo:] * jnp.exp2((old - top) * E) + dot(values, p)

    def step(iq):
        at = tile(iq, bq)
        top_s[...] = jnp.full(top_s.shape, NEG, F32)
        mix_s[...] = jnp.zeros(mix_s.shape, F32)
        row_of_blocks(iq, bq, functools.partial(block, iq), events, blocks(q.shape[0], bq))
        for n in range(heads):
            total = mix_s[n, HEAD : HEAD + 1, :]
            o[at, n * HEAD : (n + 1) * HEAD] = (mix_s[n, :HEAD, :] * (1 / total)).T.astype(BF16)
            lse[n : n + 1, at] = top_s[n : n + 1, :] * E + jnp.log2(total)

    loop(q.shape[0] // bq, step)
    the_rest(events, blocks(q.shape[0], bq))


def mid_phase(h, o, od, hm, rows, r):
    def step(i):
        at = tile(i, rows)
        hm[at, :] = h[at, :] + dot(o[at, :], merged(od[:, :r, :])).astype(BF16)

    loop(h.shape[0] // rows, step)


def ffn_phase(hm, gu, od, out, rows, r, events):
    def step(i):
        at = tile(i, rows)
        mid = hm[at, :]
        wide = mid.astype(F32)
        b = (wide * scale_of(wide)).astype(BF16)
        y = dot(b, merged(gu[...]))
        part = y.shape[1] // 4
        pieces = []
        for n in (0, 2 * part):
            gate, up = y[:, n : n + part], y[:, n + part : n + 2 * part]
            pieces.append((gate * (1 / (1 + jnp.exp(-gate))) * up).astype(BF16))
        made = jnp.concatenate(pieces, axis=1)
        out[at, :] = mid + dot(made, merged(od[:, r:, :])).astype(BF16)
        polled(events, i, hm.shape[0] // rows)

    loop(hm.shape[0] // rows, step)
    the_rest(events, hm.shape[0] // rows)


def ffn_bwd_phase(half, hm, dy, gu, od, made_s, dgu_s, bt_s, db_s, dhm, rows, r, events):
    part = dgu_s.shape[1] // 4
    lanes, units = slice(2 * part * half, 2 * part * (half + 1)), slice(part * half, part * (half + 1))
    some = od.shape[0] // 2

    def step(i):
        at = tile(i, rows)
        wide = hm[at, :].astype(F32)
        scale = scale_of(wide)
        b = (wide * scale).astype(BF16)
        if half == 0:
            bt_s[:, at] = b.T
        y = dot(b, merged(gu[:, :, lanes]))
        gate, up = y[:, :part], y[:, part:]
        back = dy[at, :]
        d_made = dot(back, merged(od[some * half : some * (half + 1), r:, :]), 1, 1).astype(BF16).astype(F32)
        sig = 1 / (1 + jnp.exp(-gate))
        silu = gate * sig
        made_s[at, units] = (silu * up).astype(BF16)
        d_gate = (d_made * up * (sig * (1 + gate - silu))).astype(BF16)
        d_up = (d_made * silu).astype(BF16)
        both = jnp.concatenate([d_gate, d_up], axis=1)
        dgu_s[at, lanes] = both
        db = dot(both, merged(gu[:, :, lanes]), 1, 1)
        if half == 0:
            db_s[at, :] = db
        else:
            db = (db_s[at, :] + db).astype(BF16).astype(F32)
            dhm[at, :] = (back.astype(F32) + norm_bwd(wide, scale, db)).astype(BF16)
        polled(events, i, hm.shape[0] // rows)

    loop(hm.shape[0] // rows, step)
    the_rest(events, hm.shape[0] // rows)


def units_phase(half, dgu_s, bt_s, p):
    n, _, columns = p.shape
    wide = next(w for w in (512, 256, 128) if columns % w == 0)

    def units(i):
        here = pl.ds(pl.multiple_of(columns * half + i * wide, wide), wide)
        p[:, :, tile(i, wide)] = dot(bt_s[...], dgu_s[:, here]).astype(BF16).reshape(n, -1, wide)

    loop(columns // wide, units)


def downs_phase(made_s, dy, p):
    n, share, group = p.shape[0], p.shape[1], 2

    def downs(i):
        got = dot(made_s[:, tile(i, group * share)], dy[...], 0, 0).astype(BF16)
        p[pl.ds(i * group, group)] = got.reshape(group, share, -1)

    loop(n // group, downs)


def out_bwd_phase(dhm, o, od, p, do, rows, r):
    def step(i):
        at = tile(i, rows)
        do[at, :] = dot(dhm[at, :], merged(od[:, :r, :]), 1, 1).astype(BF16)

    loop(dhm.shape[0] // rows, step)
    p[...] = dot(o[...], dhm[...], 0, 0).astype(BF16).reshape(p.shape)


def attend_bwd_phase(q, k, v, o, do, lse, table, dqkv, dq_s, dk_s, dv_s, kt_s, bq, events):
    heads = q.shape[1] // HEAD
    wide_q = q.shape[1]
    dk_s[...] = jnp.zeros(dk_s.shape, F32)
    dv_s[...] = jnp.zeros(dv_s.shape, F32)
    kt_s[...] = k[...].T

    def block(iq, lses, deltas, start, nk, lo, mask):
        here = pl.ds(start, nk)
        cols = pl.ds(pl.multiple_of(iq * bq + lo, bq - lo), bq - lo)
        keys, values, keys_t = k[here, :], v[here, :], kt_s[:, here]
        qs = [q[cols, n * HEAD : (n + 1) * HEAD] for n in range(heads)]
        dos = [do[cols, n * HEAD : (n + 1) * HEAD] for n in range(heads)]
        scores = [dot(keys, x, 1, 1) for x in qs]
        dps = [dot(values, x, 1, 1) for x in dos]
        for n in range(heads):
            p = jnp.exp2(scores[n] * E - lses[n][:, lo:])
            if mask is not None:
                p = jnp.where(mask, p, 0.0)
            ds = (p * (dps[n] - deltas[n][:, lo:])).astype(BF16)
            dv_s[here, :] += dot(p.astype(BF16), dos[n])
            dk_s[here, :] += dot(ds, qs[n])
            dq_s[n, :, lo:] += dot(keys_t, ds)

    def step(iq):
        at = tile(iq, bq)
        dq_s[...] = jnp.zeros(dq_s.shape, F32)
        lses = [lse[n : n + 1, at] for n in range(heads)]
        deltas = []
        for n in range(heads):
            part = slice(n * HEAD, (n + 1) * HEAD)
            deltas.append((do[at, part].astype(F32) * o[at, part].astype(F32)).T.sum(axis=0, keepdims=True))
        row_of_blocks(iq, bq, functools.partial(block, iq, lses, deltas), events, blocks(q.shape[0], bq))
        cos, sin = turns(table[at, :])
        for n in range(heads):
            back = (dq_s[n] * SCALE).T.astype(BF16).astype(F32)
            dqkv[at, n * HEAD : (n + 1) * HEAD] = rotated(back, cos, -sin).astype(BF16)

    loop(q.shape[0] // bq, step)
    the_rest(events, blocks(q.shape[0], bq))

    def finish(i):
        at = tile(i, bq)
        cos, sin = turns(table[at, :])
        dqkv[at, wide_q : wide_q + HEAD] = rotated((dk_s[at, :] * SCALE).astype(BF16).astype(F32), cos, -sin).astype(BF16)
        dqkv[at, wide_q + HEAD :] = dv_s[at, :].astype(BF16)

    loop(q.shape[0] // bq, finish)


def qkv_bwd_phase(h, dqkv, w, dhm, p_qkv, a_s, dh, rows, further):
    def step(i):
        at = tile(i, rows)
        wide = h[at, :].astype(F32)
        scale = scale_of(wide)
        a_s[at, :] = (wide * scale).astype(BF16)

        @pl.when(further)
        def _():
            da = dot(dqkv[at, :], merged(w[...]), 1, 1).astype(BF16).astype(F32)
            dh[at, :] = (dhm[at, :].astype(F32) + norm_bwd(wide, scale, da)).astype(BF16)

    loop(h.shape[0] // rows, step)
    p_qkv[...] = dot(a_s[...], dqkv[...], 0, 0).astype(BF16).reshape(p_qkv.shape)


QKV, OD, GU = range(3)
OWN, OLD = range(2)
NEXT = OLD
PLAN = {
    "qkv": ((0, OD, OWN, 2), (0, QKV, NEXT, 0), (3, GU, OWN, 2)),
    "attend": ((1, OD, OWN, 3), (2, QKV, NEXT, 1), (2, OD, NEXT, 0), (4, GU, OWN, 3), (6, OD, OWN, 4), (6, GU, NEXT, 0), (7, QKV, NEXT, 2), (8, OD, NEXT, 1)),
    "ffn": ((0, GU, NEXT, 1), (1, QKV, NEXT, 3), (1, OD, NEXT, 2), (3, QKV, NEXT, 4), (3, GU, NEXT, 2)),
}
LAST_PLAN = {"qkv": ((0, OD, OWN, 3),), "attend": ((2, GU, OWN, 3), (3, OD, OWN, 4), (6, GU, OWN, 4))}
HEAD_PLAN = ((QKV, 1), (GU, 0), (QKV, 2), (OD, 1), (QKV, 3), (GU, 1), (QKV, 4))


def planned(act, entries):
    by_step = {}
    for when, *what in entries:
        by_step.setdefault(when, []).append(what)
    return {when: functools.partial(act, whats) for when, whats in by_step.items()}


def forward(sizes, x, few, wq, wk, wv, wo, wg, wu, wd, q_o, k_o, v_o, o_o, lse_o, hm_o, h_o, qkv_o, gu_o, od_o, table_o,
            h_s, few_s, table_s, qkv_s, gu_s, od_s, q_s, k_s, v_s, vt_s, o_s, lse_s, hm_s, top_s, mix_s, own_sem, in_sem, out_sem, gather_sems, handed_sems):
    layers, n, bq, rows = sizes
    ring = Ring(n)
    me = ring.me
    wide_q, ff, ro = wq.shape[2], wg.shape[2], wo.shape[1]
    half = ff // 2
    own = {}

    def fetch(i, group, pieces):
        for src, dst in pieces:
            copy = pltpu.make_async_copy(src, dst, own_sem.at[sum(map(len, own.values()))])
            own.setdefault((i, group), []).append(copy)
            copy.start()

    for i in range(layers):
        fetch(i, QKV, [(wq.at[i], qkv_s.at[i, me, :, :wide_q]), (wk.at[i], qkv_s.at[i, me, :, wide_q : wide_q + HEAD]), (wv.at[i], qkv_s.at[i, me, :, wide_q + HEAD :])])
        fetch(i, OD, [(wo.at[i], od_s.at[i, me, :ro, :]), (wd.at[i], od_s.at[i, me, ro:, :])])
        if i == 0:
            brought = [pltpu.make_async_copy(x, h_s.at[0], in_sem.at[0]), pltpu.make_async_copy(few, few_s, in_sem.at[1])]
            for copy in brought:
                copy.start()
        fetch(i, GU, [(w.at[i, :, half * j : half * (j + 1)], gu_s.at[i, me, :, half * (2 * j + k) : half * (2 * j + k + 1)]) for j in (0, 1) for k, w in enumerate((wg, wu))])
    packs = {(g, i): Gather(ring, buf.at[i], gather_sems.at[3 * i + g], handed_sems.at[3 * i + g], False) for g, buf in enumerate((qkv_s, od_s, gu_s)) for i in range(layers)}
    begun = set()
    out = []

    def keep(src, dst):
        out.append(pltpu.make_async_copy(src, dst, out_sem.at[len(out)]))
        out[-1].start()

    def begin(group, i):
        if (group, i) not in begun:
            begun.add((group, i))
            for copy in own[i, group]:
                copy.wait()
            packs[group, i].begin()

    def act(i, whats):
        for group, which, stop in whats:
            if i + which < layers:
                begin(group, i + which)
                packs[group, i + which].now(stop)

    def plan(phase, i):
        return planned(functools.partial(act, i), (PLAN if i + 1 < layers else LAST_PLAN).get(phase, ()))

    def whole(group, i):
        begin(group, i)
        packs[group, i].finish()
        packs[group, i].complete()

    scoped('meet', ring.meet, 1)
    begin(QKV, 0)
    begin(OD, 0)
    for copy in brought:
        copy.wait()
    table_phase(few_s, table_s)
    keep(table_s, table_o)
    for group, stop in HEAD_PLAN:
        scoped(f'head{group}_{stop}', act, 0, [(group, OWN, stop)])
    for i in range(layers):
        keep(h_s.at[i], h_o.at[i])
        scoped('whole_QKV', whole, QKV, i)
        keep(qkv_s.at[i], qkv_o.at[i])
        scoped('qkv_phase', qkv_phase, h_s.at[i], qkv_s.at[i], table_s, q_s.at[i], k_s.at[i], v_s.at[i], vt_s, rows, plan("qkv", i))
        keep(q_s.at[i], q_o.at[i])
        keep(k_s.at[i], k_o.at[i])
        keep(v_s.at[i], v_o.at[i])
        scoped('attend_phase', attend_phase, q_s.at[i], k_s.at[i], vt_s, o_s.at[i], lse_s.at[i], top_s, mix_s, bq, plan("attend", i))
        keep(o_s.at[i], o_o.at[i])
        keep(lse_s.at[i], lse_o.at[i])
        scoped('whole_OD', whole, OD, i)
        keep(od_s.at[i], od_o.at[i])
        scoped('mid_phase', mid_phase, h_s.at[i], o_s.at[i], od_s.at[i], hm_s.at[i], rows, ro)
        keep(hm_s.at[i], hm_o.at[i])
        scoped('whole_GU', whole, GU, i)
        keep(gu_s.at[i], gu_o.at[i])
        if i + 1 < layers:
            scoped('ffn_phase', ffn_phase, hm_s.at[i], gu_s.at[i], od_s.at[i], h_s.at[i + 1], rows, ro, plan("ffn", i))
    with jax.named_scope('flush'):
        for copy in out:
            copy.wait()
        for pack in packs.values():
            pack.drain()


PACKS = 5
QKV_G, GA_G, GB_G, WD_G, WO_G = range(PACKS)
BACK = {
    "first": ((1, QKV_G, OLD, 2), (2, WD_G, OLD, 4), (2, WO_G, OLD, 4), (3, QKV_G, OLD, 4)),
    "second": ((2, GA_G, OWN, 1),),
    "downs": ((0, GA_G, OWN, 2),),
    "attend": ((0, GB_G, OWN, 1), (1, WD_G, OWN, 1), (2, GA_G, OWN, 3), (3, WO_G, OWN, 1), (4, GB_G, OWN, 2), (6, WD_G, OWN, 2), (7, GA_G, OWN, 4), (8, WO_G, OWN, 2),
               (9, GB_G, OWN, 3)),
    "end": ((0, GB_G, OWN, 4), (0, WD_G, OWN, 3), (0, WO_G, OWN, 3)),
}
TAIL = ((QKV_G, 2), (WD_G, 4), (WO_G, 4), (QKV_G, 4))
NAMED = ("gu", "hm", "dy", "od", "table", "q", "k", "v", "o", "lse", "h", "qkv")


def backward(sizes, dy, table, qkv, gu, od, q, k, v, o, lse, hm, h, *refs):
    layers, n, bq, rows, r = sizes
    results, refs = refs[:PACKS], refs[PACKS:]
    table_s, qkv_s, gu_s, od_s, lse_s, hm_s, dh_s, dhm_s, made_s, dgu_s, bt_s, db_s, dq_s, kt_s = refs[:14]
    refs = refs[14:]
    terms, came_a, came_b, got = (refs[PACKS * i : PACKS * (i + 1)] for i in range(4))
    in_sem, out_sem, scatter_sems, free_sems = refs[PACKS * 4 :]
    ring = Ring(n)
    split, heads = qkv_s.shape[2], q.shape[2]
    dqkv_s, do_s = made_s.at[:, :split], made_s.at[:, split : split + heads]
    dk_s, dv_s = db_s.at[:, :HEAD], db_s.at[:, HEAD : 2 * HEAD]
    place = 0
    lent = []
    for width in (heads, heads, HEAD, HEAD, h.shape[2]):
        lent.append(dgu_s.at[:, place : place + width])
        place += width
    q_s, o_s, k_s, v_s, h_s = lent
    places = {"gu": (gu, gu_s), "hm": (hm, hm_s), "dy": (dy, dh_s), "od": (od, od_s), "table": (table, table_s), "q": (q, q_s), "k": (k, k_s), "v": (v, v_s),
              "o": (o, o_s), "lse": (lse, lse_s), "h": (h, h_s), "qkv": (qkv, qkv_s)}

    def copy_of(name, *i):
        src, dst = places[name]
        return pltpu.make_async_copy(src.at[i] if i else src, dst, in_sem.at[NAMED.index(name)])

    def bring(names, *i):
        for name in names:
            copy_of(name, *i).start()

    def need(names, *i):
        for name in names:
            copy_of(name, *i).wait()

    last = layers - 1
    bring(("gu", "hm"), last)
    bring(("dy",))
    bring(("od",), last)
    bring(("table",))
    bring(("qkv",), last)
    scoped('meet', ring.meet, 0)

    def pack(group, i, signal, taken=(0, 0)):
        return (QuickScatter if group == QKV_G else Scatter)(ring, terms[group], came_a[group], came_b[group], scatter_sems.at[group], free_sems.at[group], got[group].at[i], signal, taken)

    reached = {}
    for entries in BACK.values():
        for _, group, old, stop in entries:
            if old == OWN:
                reached[group] = max(stop, reached.get(group, 0))
    taken = {group: (min(stop, ring.far_a), min(stop, ring.far_b)) for group, stop in reached.items()}

    def layer(step):
        i = last - step
        later = step > 0
        own = {group: pack(group, i, i > 0) for group in range(PACKS)}
        old = {group: pack(group, i + 1, i >= 0, taken.get(group, (0, 0))) for group in range(PACKS)}

        def act(whats):
            for group, which, stop in whats:
                if which == OWN:
                    own[group].now(stop)
                else:
                    pl.when(later)(functools.partial(old[group].now, stop))

        def plan(phase):
            return planned(act, BACK[phase])

        def before(group):
            pl.when(later)(old[group].finish)

        scoped('need', need, ("gu", "hm", "od"), i)
        pl.when(step == 0)(functools.partial(need, ("dy",)))
        for half, group, phase in ((0, GA_G, "first"), (1, GB_G, "second")):
            scoped('ffn_bwd', ffn_bwd_phase, half, hm_s, dh_s, gu_s, od_s, made_s, dgu_s, bt_s, db_s, dhm_s, rows, r, plan(phase))
            if half == 1:
                pl.when(i > 0)(functools.partial(bring, ("gu", "hm"), i - 1))
            before(group)
            scoped('units', units_phase, half, dgu_s, bt_s, terms[group])
            scoped('begin', own[group].begin, later)
        bring(("o", "q", "k", "v", "lse", "h"), i)
        before(WD_G)
        scoped('downs', downs_phase, made_s, dh_s, terms[WD_G])
        own[WD_G].begin(later)
        scoped('downs_ev', the_rest, plan("downs"), 0)
        need(("o",), i)
        before(WO_G)
        scoped('out_bwd', out_bwd_phase, dhm_s, o_s, od_s, terms[WO_G], do_s, rows, r)
        own[WO_G].begin(later)
        pl.when(i > 0)(functools.partial(bring, ("od",), i - 1))
        need(("q", "k", "v", "lse"), i)
        pl.when(step == 0)(functools.partial(need, ("table",)))
        scoped('attend_bwd', attend_bwd_phase, q_s, k_s, v_s, o_s, do_s, lse_s, table_s, dqkv_s, dq_s, dk_s, dv_s, kt_s, bq, plan("attend"))
        need(("h",), i)
        pl.when(step == 0)(functools.partial(need, ("qkv",), last))
        before(QKV_G)
        scoped('qkv_bwd', qkv_bwd_phase, h_s, dqkv_s, qkv_s, dhm_s, terms[QKV_G], do_s, dh_s, rows, i > 0)
        own[QKV_G].begin(later)
        scoped('end_ev', the_rest, plan("end"), 0)

        @pl.when(jnp.logical_and(i > 1, i < layers))
        def _():
            copy_of("qkv", i - 1).start()
            copy_of("qkv", i - 1).wait()

    loop(layers, layer)
    final = {group: pack(group, 0, False, taken.get(group, (0, 0))) for group in range(PACKS)}
    for group, stop in TAIL:
        scoped(f'tail{group}_{stop}', final[group].now, stop)
    for p in final.values():
        p.finish()
    out = []
    for group in range(PACKS):
        for i in range(layers):
            out.append(pltpu.make_async_copy(got[group].at[i], results[group].at[i], out_sem.at[len(out)]))
            out[-1].start()
    for copy in out:
        copy.wait()


SEVEN = 7
START = 0


def adamw(*refs):
    count = 3 * SEVEN
    grads, refs = refs[:PACKS], refs[PACKS:]
    ins, outs, refs = refs[:count], refs[count : 2 * count], refs[2 * count :]
    grads_s, refs = refs[:PACKS], refs[PACKS:]
    ins_s, outs_s, (grad_sem, in_sem, out_sem) = refs[:count], refs[count : 2 * count], refs[2 * count :]
    kinds = range(0, count, SEVEN)
    layers = ins[0].shape[0]
    heads, half, whole, few = ins[0].shape[2], ins[4].shape[2] // 2, ins[3].shape[2], 16
    waits = []
    for i in range(layers):
        copies = [pltpu.make_async_copy(src.at[i], dst.at[i], grad_sem.at[g, i]) for g, (src, dst) in enumerate(zip(grads, grads_s, strict=True))]
        copies += [pltpu.make_async_copy(ins[a].at[i], ins_s[a].at[i], in_sem.at[a, i]) for w in range(SEVEN) for a in (w + kind for kind in kinds)]
        for copy in copies:
            copy.start()
        waits.append(copies)
    parts = (
        [(QKV_G, START, START, heads)], [(QKV_G, heads, START, HEAD)], [(QKV_G, heads + HEAD, START, HEAD)], [(WO_G, START, START, whole)],
        [(GA_G, START, START, half), (GB_G, START, half, half)], [(GA_G, half, START, half), (GB_G, half, half, half)], [(WD_G, START, START, whole)],
    )
    out = []
    for i in range(layers):
        for copy in waits[i][:PACKS]:
            copy.wait()
        for w in range(SEVEN):
            for copy in waits[i][PACKS + 3 * w : PACKS + 3 * (w + 1)]:
                copy.wait()

            def step(j, i=i, w=w):
                at = tile(j, few)
                for grad, first, start, wide in parts[w]:
                    here = slice(start, start + wide)
                    g = grads_s[grad][i, at, first : first + wide].astype(F32)
                    weight = ins_s[w][i, at, here].astype(F32)
                    of_m, of_v = w + SEVEN, w + 2 * SEVEN
                    m = 0.9 * ins_s[of_m][i, at, here] + 0.1 * g
                    v = 0.95 * ins_s[of_v][i, at, here] + 0.05 * g * g
                    outs_s[w][i, at, here] = (weight - 0.02 * (m * lax.rsqrt(v + 1e-8) + 0.1 * weight)).astype(BF16)
                    outs_s[of_m][i, at, here] = m
                    outs_s[of_v][i, at, here] = v

            loop(ins[w].shape[1] // few, step)
            for a in (w + kind for kind in kinds):
                out.append(pltpu.make_async_copy(outs_s[a].at[i], outs[a].at[i], out_sem.at[a, i]))
                out[-1].start()
    for copy in out:
        copy.wait()


def solution(mesh):
    n = mesh.shape["dp"]
    far_a, far_b = n // 2, n - 1 - n // 2

    def step(x, dy, *arrays):
        weights = arrays[:SEVEN]
        wq, wk, wv, wo, wg, wu, wd = weights
        layers, r, wide_q = wq.shape
        x, dy = x[0], dy[0]
        tokens, d = x.shape
        ff = wg.shape[2]
        bq, rows = (min(512, tokens),) * 2
        few = jnp.asarray(angles(tokens))
        wide = wide_q + 2 * HEAD
        heads = wide_q // HEAD
        ro = wo.shape[1]
        shapes = (r, wide), (r, 2 * ff), (ro + wd.shape[1], d)
        terms = (r, wide), (r, ff), (r, ff), (wd.shape[1], d), (ro, d)
        both = lambda *s: jax.ShapeDtypeStruct((layers, *s), BF16)
        some = lambda lead, s: pltpu.VMEM((*lead, *s), BF16)
        q, k, v_, o, lse, hm, h, qkv, gu, od, table = pl.pallas_call(
            functools.partial(forward, (layers, n, bq, rows)),
            out_shape=[both(tokens, wide_q), both(tokens, HEAD), both(tokens, HEAD), both(tokens, wide_q), jax.ShapeDtypeStruct((layers, 8, tokens), F32),
                       both(tokens, d), both(tokens, d), *(both(n, *s) for s in shapes), jax.ShapeDtypeStruct((tokens, HEAD), F32)],
            in_specs=[ANY] * 9,
            out_specs=[ANY] * 11,
            scratch_shapes=[
                pltpu.VMEM((layers, tokens, d), BF16), pltpu.VMEM(few.shape, F32), pltpu.VMEM((tokens, HEAD), F32),
                *(some((layers, n), s) for s in shapes),
                pltpu.VMEM((layers, tokens, wide_q), BF16), pltpu.VMEM((layers, tokens, HEAD), BF16), pltpu.VMEM((layers, tokens, HEAD), BF16),
                pltpu.VMEM((HEAD, tokens), BF16), pltpu.VMEM((layers, tokens, wide_q), BF16), pltpu.VMEM((layers, 8, tokens), F32),
                pltpu.VMEM((layers, tokens, d), BF16), pltpu.VMEM((heads, bq), F32), pltpu.VMEM((heads, HEAD + 8, bq), F32),
                pltpu.SemaphoreType.DMA((9 * layers,)), pltpu.SemaphoreType.DMA((2,)), pltpu.SemaphoreType.DMA((10 * layers + 1,)),
                pltpu.SemaphoreType.DMA((3 * layers, 4, far_a)), pltpu.SemaphoreType.DMA((3 * layers, n)),
            ],
            compiler_params=pltpu.CompilerParams(vmem_limit_bytes=VMEM, collective_id=0, has_side_effects=True),
            name="forward",
        )(x, few, *weights)
        grads = pl.pallas_call(
            functools.partial(backward, (layers, n, bq, rows, ro)),
            out_shape=[both(*s) for s in terms],
            in_specs=[ANY] * 12,
            out_specs=[ANY] * 5,
            scratch_shapes=[
                pltpu.VMEM((tokens, HEAD), F32), *(some((n,), s) for s in shapes),
                pltpu.VMEM((8, tokens), F32), pltpu.VMEM((tokens, d), BF16), pltpu.VMEM((tokens, d), BF16), pltpu.VMEM((tokens, d), BF16),
                pltpu.VMEM((tokens, ff), BF16), pltpu.VMEM((tokens, 2 * ff), BF16), pltpu.VMEM((d, tokens), BF16),
                pltpu.VMEM((tokens, d), F32), pltpu.VMEM((heads, HEAD, bq), F32), pltpu.VMEM((HEAD, tokens), BF16),
                *(some((lead,), s) for lead in (n, far_a, far_b, layers) for s in terms),
                pltpu.SemaphoreType.DMA((len(NAMED),)), pltpu.SemaphoreType.DMA((5 * layers,)),
                pltpu.SemaphoreType.DMA((5, 4, far_a)), pltpu.SemaphoreType.REGULAR((5,)),
            ],
            compiler_params=pltpu.CompilerParams(vmem_limit_bytes=VMEM, collective_id=1, has_side_effects=True),
            name="backward",
        )(dy, table, qkv, gu, od, q, k, v_, o, lse, hm, h)
        in_vmem = lambda a: pltpu.VMEM(a.shape, a.dtype)
        return pl.pallas_call(
            adamw,
            out_shape=[jax.ShapeDtypeStruct(a.shape, a.dtype) for a in arrays],
            in_specs=[ANY] * (PACKS + 3 * SEVEN),
            out_specs=[ANY] * (3 * SEVEN),
            scratch_shapes=[*map(in_vmem, grads), *map(in_vmem, arrays), *map(in_vmem, arrays),
                            pltpu.SemaphoreType.DMA((PACKS, layers)), *(pltpu.SemaphoreType.DMA((3 * SEVEN, layers)) for _ in arrays[:2])],
            compiler_params=pltpu.CompilerParams(vmem_limit_bytes=VMEM),
            name="adamw",
        )(*grads, *arrays)

    states, cut = P(("rep", "dp"), None, None), P(None, "dp", None)
    return jax.shard_map(
        step,
        mesh=mesh,
        in_specs=(states, states) + (cut,) * (3 * SEVEN),
        out_specs=(P("rep", "dp", None),) * (3 * SEVEN),
        check_vma=False,
    )
```

```python
import functools

import jax
import jax.numpy as jnp
import numpy as np
from jax import lax
from jax.experimental import pallas as pl
from jax.experimental.pallas import tpu as pltpu
from jax.sharding import PartitionSpec as P

HEAD = 128
THETA = 10000
NEG = -1e30
HIDDEN = 2 * NEG
LOG2E = 1.4426950408889634
SCALE = HEAD**-0.5
E = SCALE * LOG2E
VMEM = 66_000_000
STRETCH = 64
F32, BF16 = jnp.float32, jnp.bfloat16
ANY = pl.BlockSpec(memory_space=pl.ANY)
MESH = pl.DeviceIdType.MESH
A, B = 0, 1


def dot(a, b, ca=1, cb=0):
    return lax.dot_general(a, b, (((ca,), (cb,)), ((), ())), preferred_element_type=F32)


def scoped(name, what, *args):
    with jax.named_scope(name):
        return what(*args)


def tile(i, n):
    return pl.ds(pl.multiple_of(i * n, n), n)


def loop(n, body):
    lax.fori_loop(0, n, lambda i, _: body(i), None)


def polled(events, i, steps):
    for when, what in events.items():
        if when < steps:
            pl.when(i == when)(functools.partial(scoped, f"ev{when}", what))


def the_rest(events, steps):
    for when, what in events.items():
        if when >= steps:
            what()


def scale_of(wide):
    return lax.rsqrt(jnp.mean(wide * wide, -1, keepdims=True) + 1e-6)


def norm_bwd(wide, scale, g):
    return scale * g - wide * (scale * scale * scale * jnp.mean(wide * g, -1, keepdims=True))


def angles(tokens):
    half = HEAD // 2
    turn = float(THETA) ** (-np.arange(half) / half)
    place = np.arange(STRETCH)[:, None] * turn
    start = np.arange(0, tokens, STRETCH)[:, None] * turn
    cos, sin = np.cos(start), np.sin(start)
    return np.concatenate([np.concatenate(p, 1) for p in ((np.cos(place), np.sin(place)), (cos, cos), (-sin, sin))]).astype(np.float32)


def table_phase(few, table):
    starts = table.shape[0] // STRETCH

    def step(i):
        place = few[:STRETCH, :]
        row = lambda first: few[pl.ds(first + i, 1), :]
        table[tile(i, STRETCH), :] = place * row(STRETCH) + pltpu.roll(place, HEAD // 2, 1) * row(STRETCH + starts)

    loop(starts, step)


def turns(t):
    swapped = pltpu.roll(t, HEAD // 2, 1)
    first = lax.broadcasted_iota(jnp.int32, t.shape, 1) < HEAD // 2
    return jnp.where(first, t, swapped), jnp.where(first, -swapped, t)


def rotated(t, cos, sin):
    return t * cos + pltpu.roll(t, HEAD // 2, 1) * sin


class Ring:
    def __init__(self, n):
        self.n, self.far_a = n, n // 2
        self.far_b = n - 1 - self.far_a
        self.me = lax.axis_index("dp")
        rep = lax.axis_index("rep")
        self.core = lax.rem(rep, 2)
        self.partner = {"rep": rep + 1 - 2 * self.core}
        self.turn = 1 - 2 * self.core
        self.near = 1, -1, 2, -2

    def at(self, k):
        return lax.rem(self.me + self.n + k * self.turn, self.n)

    def to(self, k):
        return {"dp": self.at(k)}

    def meet(self, partner):
        barrier = pltpu.get_barrier_semaphore()
        others = [self.to(k) for k in self.near] + [self.partner] * partner
        for other in others:
            pl.semaphore_signal(barrier, inc=1, device_id=other, device_id_type=MESH)
        pl.semaphore_wait(barrier, len(others))


def remote(src, dst, send, recv, to):
    return pltpu.make_async_remote_copy(src_ref=src, dst_ref=dst, send_sem=send, recv_sem=recv, device_id=to, device_id_type=MESH)


class Chains:
    def far(self, chain):
        return self.ring.far_b if chain else self.ring.far_a

    def stops(self, chain):
        return range(1, self.far(chain) + 1)

    def now(self, s):
        for count in range(1, s + 1):
            for chain in (A, B):
                if self.taken[chain] < min(count, len(self.stops(chain))):
                    self.taken[chain] += 1
                    self.take(chain, self.stops(chain)[self.taken[chain] - 1])

    def finish(self):
        self.now(self.ring.far_a)


class Gather(Chains):
    def __init__(self, ring, buf, sems, handed_sems, quick):
        self.taken = [0, 0]
        self.ring, self.buf, self.sems, self.handed_sems, self.quick = ring, buf, sems, handed_sems, quick
        self.half = buf.shape[1] // 2
        self.last_handed = {}

    def stops(self, chain):
        some = [*super().stops(chain)]
        return some[1::-1] + some[2:] if self.quick else some

    def piece(self, block, half):
        return self.buf.at[block, pl.ds(pl.multiple_of(half * self.half, self.half), self.half), :]

    def hop(self, chain, step):
        ring = self.ring
        along = 1 if chain == A else -1
        done = step // 2 * 2 if self.quick else step
        part = self.piece(ring.at(-along * done), ring.core)
        return remote(part, part, self.sems.at[2 * chain, step], self.sems.at[2 * chain + 1, step], ring.to(along * (step + 1 - done)))

    def handed(self, chain, step):
        ring = self.ring
        part = self.piece(ring.at(-step - 1 if chain == A else step + 1), ring.core)
        return remote(part, part, self.handed_sems.at[ring.n - 1 + chain], self.handed_sems.at[step + chain * ring.far_a], ring.partner)

    def begin(self):
        for chain in (A, B):
            for step in (1, 0) if self.quick else (0,):
                self.hop(chain, step).start()

    def take(self, chain, s):
        ring = self.ring
        part = self.piece(ring.at(-s if chain == A else s), ring.core)
        remote(part, part, self.sems.at[2 * chain, s - 1], self.sems.at[2 * chain + 1, s - 1], ring.to(1)).wait_recv()
        for step in (range(s + 1, s - 1, -1) if s == 2 else ()) if self.quick else (s,):
            if step < self.far(chain):
                self.hop(chain, step).start()
        if chain in self.last_handed:
            self.handed(chain, self.last_handed[chain]).wait_send()
        self.last_handed[chain] = s - 1
        self.handed(chain, s - 1).start()

    def complete(self):
        ring = self.ring
        for chain in (A, B):
            for step in range(self.far(chain)):
                part = self.piece(ring.at(step + 1 if chain == A else -step - 1), 1 - ring.core)
                remote(part, part, self.handed_sems.at[ring.n - 1], self.handed_sems.at[step + chain * ring.far_a], ring.partner).wait_recv()

    def drain(self):
        for chain in (A, B):
            for step in range(self.far(chain)):
                self.hop(chain, step).wait_send()
        for chain, step in self.last_handed.items():
            self.handed(chain, step).wait_send()


class Scatter(Chains):
    def __init__(self, ring, p, came_a, came_b, sems, free, got, signal, taken=(0, 0)):
        self.signal = signal
        self.ring, self.p, self.came, self.sems, self.free, self.got = ring, p, (came_a, came_b), sems, free, got
        self.taken = list(taken)

    def hop(self, chain, step):
        ring = self.ring
        left = self.far(chain) - step
        block = ring.at(left if chain == 0 else -left)
        return remote(self.p.at[block], self.came[chain].at[step], self.sems.at[2 * chain, step], self.sems.at[2 * chain + 1, step],
                      ring.to(1 if chain == 0 else -1))

    def added(self, chain, step):
        ring = self.ring
        left = self.far(chain) - step
        block = ring.at(left if chain == 0 else -left)
        few = 16

        def rows(i):
            at = tile(i, few)
            self.p[block, at, :] = (self.p[block, at, :].astype(F32) + self.came[chain][step - 1, at, :].astype(F32)).astype(BF16)

        loop(self.p.shape[1] // few, rows)

    def begin(self, wait):
        pl.when(wait)(lambda: pl.semaphore_wait(self.free, len(self.ring.near)))
        self.hop(A, 0).start()
        self.hop(B, 0).start()

    def take(self, chain, s):
        self.hop(chain, s - 1).wait_recv()
        if s < self.far(chain):
            self.added(chain, s)
            self.hop(chain, s).start()
        if self.taken == [self.far(A), self.far(B)]:
            self.end()

    def arrived(self):
        return [(chain, self.far(chain) - 1) for chain in (A, B)]

    def end(self):
        me, few = self.ring.me, 16

        def rows(i):
            at = tile(i, few)
            total = self.p[me, at, :].astype(F32)
            for chain, slot in self.arrived():
                total += self.came[chain][slot, at, :].astype(F32)
            self.got[at, :] = total.astype(BF16)

        loop(self.p.shape[1] // few, rows)
        for chain in (A, B):
            for step in range(self.far(chain)):
                self.hop(chain, step).wait_send()

        @pl.when(self.signal)
        def _():
            for k in self.ring.near:
                pl.semaphore_signal(self.free, inc=1, device_id=self.ring.to(k), device_id_type=MESH)


class QuickScatter(Scatter):
    def hop(self, chain, step):
        ring = self.ring
        kind = step + self.far(A) - self.far(chain)
        block, reach = ((4, 2), (3, 1), (1, 1), (2, 2))[kind]
        along = 1 if chain == A else -1
        return remote(self.p.at[ring.at(along * block)], self.came[chain].at[step], self.sems.at[2 * chain, step], self.sems.at[2 * chain + 1, step],
                      ring.to(along * reach))

    def begin(self, wait):
        pl.when(wait)(lambda: pl.semaphore_wait(self.free, len(self.ring.near)))
        for step in range(self.far(A) - 1):
            for chain in (A, B):
                if step < self.far(chain) - 1:
                    self.hop(chain, step).start()

    def take(self, chain, s):
        self.hop(chain, s - 1).wait_recv()
        beyond = self.far(chain) - 2
        if s == beyond:
            block, few = self.ring.at(2 if chain == A else -2), 16

            def rows(i):
                at = tile(i, few)
                total = self.p[block, at, :].astype(F32)
                for slot in range(beyond):
                    total += self.came[chain][slot, at, :].astype(F32)
                self.p[block, at, :] = total.astype(BF16)

            loop(self.p.shape[1] // few, rows)
            self.hop(chain, self.far(chain) - 1).start()
        if self.taken == [self.far(A), self.far(B)]:
            self.end()

    def arrived(self):
        return [(chain, self.far(chain) - back) for chain in (A, B) for back in (1, 2)]


def merged(w):
    return w.reshape(w.shape[0] * w.shape[1], w.shape[2])


def qkv_phase(h, w, table, q, k, v, vt, rows, events):
    wide_q = q.shape[1]

    def step(i):
        at = tile(i, rows)
        wide = h[at, :].astype(F32)
        a = (wide * scale_of(wide)).astype(BF16)
        y = dot(a, merged(w[...])).astype(BF16)
        cos, sin = turns(table[at, :])
        for n in range(wide_q // HEAD):
            part = slice(n * HEAD, (n + 1) * HEAD)
            q[at, part] = rotated(y[:, part].astype(F32), cos, sin).astype(BF16)
        k[at, :] = rotated(y[:, wide_q : wide_q + HEAD].astype(F32), cos, sin).astype(BF16)
        mine = y[:, wide_q + HEAD :]
        v[at, :] = mine
        vt[:, at] = mine.T
        polled(events, i, h.shape[0] // rows)

    loop(h.shape[0] // rows, step)
    the_rest(events, h.shape[0] // rows)


def spans(bq):
    half = bq // 2
    return [(0, half, 0), (half, half, half)]


def seen(keys, first_key, queries, first_query):
    key = lax.broadcasted_iota(jnp.int32, (keys, queries), 0) + first_key
    return lax.broadcasted_iota(jnp.int32, (keys, queries), 1) + first_query >= key


def blocks(tokens, bq):
    return (tokens // bq) * (tokens // bq + 1) // 2


def row_of_blocks(iq, bq, block, events, steps):
    def step(j):
        @pl.when(j < iq)
        def _():
            block(pl.multiple_of(j * bq, bq), bq, 0, None)

        @pl.when(j == iq)
        def _():
            for first, nk, lo in spans(bq):
                block(pl.multiple_of(iq * bq + first, nk), nk, lo, seen(nk, first, bq - lo, lo))

        polled(events, lax.div(iq * (iq + 1), 2) + j, steps)

    loop(iq + 1, step)


def attend_phase(q, k, vt, o, lse, top_s, mix_s, bq, events):
    heads = q.shape[1] // HEAD

    def block(iq, start, nk, lo, mask):
        here = pl.ds(start, nk)
        cols = pl.ds(pl.multiple_of(iq * bq + lo, bq - lo), bq - lo)
        keys = k[here, :]
        scores = [dot(keys, q[cols, n * HEAD : (n + 1) * HEAD], 1, 1) for n in range(heads)]
        values = jnp.concatenate([vt[:, here], jnp.ones((8, nk), BF16)], axis=0)
        for n, s in enumerate(scores):
            if mask is not None:
                s = jnp.where(mask, s, HIDDEN)
            old = top_s[n : n + 1, lo:]
            top = jnp.maximum(old, s.max(axis=0, keepdims=True))
            top_s[n : n + 1, lo:] = top
            p = jnp.exp2((s - top) * E).astype(BF16)
            mix_s[n, :, lo:] = mix_s[n, :, lo:] * jnp.exp2((old - top) * E) + dot(values, p)

    def step(iq):
        at = tile(iq, bq)
        top_s[...] = jnp.full(top_s.shape, NEG, F32)
        mix_s[...] = jnp.zeros(mix_s.shape, F32)
        row_of_blocks(iq, bq, functools.partial(block, iq), events, blocks(q.shape[0], bq))
        for n in range(heads):
            total = mix_s[n, HEAD : HEAD + 1, :]
            o[at, n * HEAD : (n + 1) * HEAD] = (mix_s[n, :HEAD, :] * (1 / total)).T.astype(BF16)
            lse[n : n + 1, at] = top_s[n : n + 1, :] * E + jnp.log2(total)

    loop(q.shape[0] // bq, step)
    the_rest(events, blocks(q.shape[0], bq))


def mid_phase(h, o, od, hm, rows, r):
    def step(i):
        at = tile(i, rows)
        hm[at, :] = h[at, :] + dot(o[at, :], merged(od[:, :r, :])).astype(BF16)

    loop(h.shape[0] // rows, step)


def ffn_phase(hm, gu, od, out, rows, r, events):
    def step(i):
        at = tile(i, rows)
        mid = hm[at, :]
        wide = mid.astype(F32)
        b = (wide * scale_of(wide)).astype(BF16)
        y = dot(b, merged(gu[...]))
        part = y.shape[1] // 4
        pieces = []
        for n in (0, 2 * part):
            gate, up = y[:, n : n + part], y[:, n + part : n + 2 * part]
            pieces.append((gate * (1 / (1 + jnp.exp(-gate))) * up).astype(BF16))
        made = jnp.concatenate(pieces, axis=1)
        out[at, :] = mid + dot(made, merged(od[:, r:, :])).astype(BF16)
        polled(events, i, hm.shape[0] // rows)

    loop(hm.shape[0] // rows, step)
    the_rest(events, hm.shape[0] // rows)


def ffn_bwd_phase(half, hm, dy, gu, od, made_s, dgu_s, bt_s, db_s, dhm, rows, r, events):
    part = dgu_s.shape[1] // 4
    lanes, units = slice(2 * part * half, 2 * part * (half + 1)), slice(part * half, part * (half + 1))
    some = od.shape[0] // 2

    def step(i):
        at = tile(i, rows)
        wide = hm[at, :].astype(F32)
        scale = scale_of(wide)
        b = (wide * scale).astype(BF16)
        if half == 0:
            bt_s[:, at] = b.T
        y = dot(b, merged(gu[:, :, lanes]))
        gate, up = y[:, :part], y[:, part:]
        back = dy[at, :]
        d_made = dot(back, merged(od[some * half : some * (half + 1), r:, :]), 1, 1).astype(BF16).astype(F32)
        sig = 1 / (1 + jnp.exp(-gate))
        silu = gate * sig
        made_s[at, units] = (silu * up).astype(BF16)
        d_gate = (d_made * up * (sig * (1 + gate - silu))).astype(BF16)
        d_up = (d_made * silu).astype(BF16)
        both = jnp.concatenate([d_gate, d_up], axis=1)
        dgu_s[at, lanes] = both
        db = dot(both, merged(gu[:, :, lanes]), 1, 1)
        if half == 0:
            db_s[at, :] = db
        else:
            db = (db_s[at, :] + db).astype(BF16).astype(F32)
            dhm[at, :] = (back.astype(F32) + norm_bwd(wide, scale, db)).astype(BF16)
        polled(events, i, hm.shape[0] // rows)

    loop(hm.shape[0] // rows, step)
    the_rest(events, hm.shape[0] // rows)


def units_phase(half, dgu_s, bt_s, p):
    n, _, columns = p.shape
    wide = next(w for w in (512, 256, 128) if columns % w == 0)

    def units(i):
        here = pl.ds(pl.multiple_of(columns * half + i * wide, wide), wide)
        p[:, :, tile(i, wide)] = dot(bt_s[...], dgu_s[:, here]).astype(BF16).reshape(n, -1, wide)

    loop(columns // wide, units)


def downs_phase(made_s, dy, p):
    n, share, group = p.shape[0], p.shape[1], 2

    def downs(i):
        got = dot(made_s[:, tile(i, group * share)], dy[...], 0, 0).astype(BF16)
        p[pl.ds(i * group, group)] = got.reshape(group, share, -1)

    loop(n // group, downs)


def out_bwd_phase(dhm, o, od, p, do, rows, r):
    def step(i):
        at = tile(i, rows)
        do[at, :] = dot(dhm[at, :], merged(od[:, :r, :]), 1, 1).astype(BF16)

    loop(dhm.shape[0] // rows, step)
    p[...] = dot(o[...], dhm[...], 0, 0).astype(BF16).reshape(p.shape)


def attend_bwd_phase(q, k, v, o, do, lse, table, dqkv, dq_s, dk_s, dv_s, kt_s, bq, events):
    heads = q.shape[1] // HEAD
    wide_q = q.shape[1]
    dk_s[...] = jnp.zeros(dk_s.shape, F32)
    dv_s[...] = jnp.zeros(dv_s.shape, F32)
    kt_s[...] = k[...].T

    def block(iq, lses, deltas, start, nk, lo, mask):
        here = pl.ds(start, nk)
        cols = pl.ds(pl.multiple_of(iq * bq + lo, bq - lo), bq - lo)
        keys, values, keys_t = k[here, :], v[here, :], kt_s[:, here]
        qs = [q[cols, n * HEAD : (n + 1) * HEAD] for n in range(heads)]
        dos = [do[cols, n * HEAD : (n + 1) * HEAD] for n in range(heads)]
        scores = [dot(keys, x, 1, 1) for x in qs]
        dps = [dot(values, x, 1, 1) for x in dos]
        for n in range(heads):
            p = jnp.exp2(scores[n] * E - lses[n][:, lo:])
            if mask is not None:
                p = jnp.where(mask, p, 0.0)
            ds = (p * (dps[n] - deltas[n][:, lo:])).astype(BF16)
            dv_s[here, :] += dot(p.astype(BF16), dos[n])
            dk_s[here, :] += dot(ds, qs[n])
            dq_s[n, :, lo:] += dot(keys_t, ds)

    def step(iq):
        at = tile(iq, bq)
        dq_s[...] = jnp.zeros(dq_s.shape, F32)
        lses = [lse[n : n + 1, at] for n in range(heads)]
        deltas = []
        for n in range(heads):
            part = slice(n * HEAD, (n + 1) * HEAD)
            deltas.append((do[at, part].astype(F32) * o[at, part].astype(F32)).T.sum(axis=0, keepdims=True))
        row_of_blocks(iq, bq, functools.partial(block, iq, lses, deltas), events, blocks(q.shape[0], bq))
        cos, sin = turns(table[at, :])
        for n in range(heads):
            back = (dq_s[n] * SCALE).T.astype(BF16).astype(F32)
            dqkv[at, n * HEAD : (n + 1) * HEAD] = rotated(back, cos, -sin).astype(BF16)

    loop(q.shape[0] // bq, step)
    the_rest(events, blocks(q.shape[0], bq))

    def finish(i):
        at = tile(i, bq)
        cos, sin = turns(table[at, :])
        dqkv[at, wide_q : wide_q + HEAD] = rotated((dk_s[at, :] * SCALE).astype(BF16).astype(F32), cos, -sin).astype(BF16)
        dqkv[at, wide_q + HEAD :] = dv_s[at, :].astype(BF16)

    loop(q.shape[0] // bq, finish)


def qkv_bwd_phase(h, dqkv, w, dhm, p_qkv, a_s, dh, rows, further):
    def step(i):
        at = tile(i, rows)
        wide = h[at, :].astype(F32)
        scale = scale_of(wide)
        a_s[at, :] = (wide * scale).astype(BF16)

        @pl.when(further)
        def _():
            da = dot(dqkv[at, :], merged(w[...]), 1, 1).astype(BF16).astype(F32)
            dh[at, :] = (dhm[at, :].astype(F32) + norm_bwd(wide, scale, da)).astype(BF16)

    loop(h.shape[0] // rows, step)
    p_qkv[...] = dot(a_s[...], dqkv[...], 0, 0).astype(BF16).reshape(p_qkv.shape)


QKV, OD, GU = range(3)
OWN, OLD = range(2)
NEXT = OLD
PLAN = {
    "qkv": ((0, OD, OWN, 2), (0, QKV, NEXT, 0), (0, OD, NEXT, 0), (3, GU, OWN, 2)),
    "attend": ((1, OD, OWN, 3), (2, QKV, NEXT, 1), (3, OD, NEXT, 1), (6, GU, OWN, 3), (8, OD, OWN, 4), (8, QKV, NEXT, 2), (8, GU, NEXT, 0), (9, OD, NEXT, 2)),
    "ffn": ((0, QKV, NEXT, 3), (1, GU, NEXT, 1), (2, QKV, NEXT, 4), (2, OD, NEXT, 3)),
}
LAST_PLAN = {"qkv": ((1, GU, OWN, 2), (2, OD, OWN, 4)), "attend": ((3, GU, OWN, 3), (7, GU, OWN, 4))}
HEAD_PLAN = ((QKV, 1), (GU, 0), (QKV, 2), (OD, 1), (QKV, 3), (GU, 1), (QKV, 4))


def planned(act, entries):
    by_step = {}
    for when, *what in entries:
        by_step.setdefault(when, []).append(what)
    return {when: functools.partial(act, whats) for when, whats in by_step.items()}


def forward(sizes, x, few, wq, wk, wv, wo, wg, wu, wd, q_o, k_o, v_o, o_o, lse_o, hm_o, h_o, qkv_o, gu_o, od_o, table_o,
            h_s, few_s, table_s, qkv_s, gu_s, od_s, q_s, k_s, v_s, vt_s, o_s, lse_s, hm_s, top_s, mix_s, own_sem, in_sem, out_sem, gather_sems, handed_sems):
    layers, n, bq, rows = sizes
    ring = Ring(n)
    me = ring.me
    wide_q, ff, ro = wq.shape[2], wg.shape[2], wo.shape[1]
    half = ff // 2
    own = {}

    def fetch(i, group, pieces):
        for src, dst in pieces:
            copy = pltpu.make_async_copy(src, dst, own_sem.at[sum(map(len, own.values()))])
            own.setdefault((i, group), []).append(copy)
            copy.start()

    for i in range(layers):
        fetch(i, QKV, [(wq.at[i], qkv_s.at[i, me, :, :wide_q]), (wk.at[i], qkv_s.at[i, me, :, wide_q : wide_q + HEAD]), (wv.at[i], qkv_s.at[i, me, :, wide_q + HEAD :])])
        fetch(i, OD, [(wo.at[i], od_s.at[i, me, :ro, :]), (wd.at[i], od_s.at[i, me, ro:, :])])
        if i == 0:
            brought = [pltpu.make_async_copy(x, h_s.at[0], in_sem.at[0]), pltpu.make_async_copy(few, few_s, in_sem.at[1])]
            for copy in brought:
                copy.start()
        fetch(i, GU, [(w.at[i, :, half * j : half * (j + 1)], gu_s.at[i, me, :, half * (2 * j + k) : half * (2 * j + k + 1)]) for j in (0, 1) for k, w in enumerate((wg, wu))])
    packs = {(g, i): Gather(ring, buf.at[i], gather_sems.at[3 * i + g], handed_sems.at[3 * i + g], False) for g, buf in enumerate((qkv_s, od_s, gu_s)) for i in range(layers)}
    begun = set()
    out = []

    def keep(src, dst):
        out.append(pltpu.make_async_copy(src, dst, out_sem.at[len(out)]))
        out[-1].start()

    def begin(group, i):
        if (group, i) not in begun:
            begun.add((group, i))
            for copy in own[i, group]:
                copy.wait()
            packs[group, i].begin()

    def act(i, whats):
        for group, which, stop in whats:
            if i + which < layers:
                begin(group, i + which)
                packs[group, i + which].now(stop)

    def plan(phase, i):
        return planned(functools.partial(act, i), (PLAN if i + 1 < layers else LAST_PLAN).get(phase, ()))

    def whole(group, i):
        begin(group, i)
        packs[group, i].finish()
        packs[group, i].complete()

    scoped('meet', ring.meet, 1)
    begin(QKV, 0)
    begin(OD, 0)
    for copy in brought:
        copy.wait()
    table_phase(few_s, table_s)
    keep(table_s, table_o)
    for group, stop in HEAD_PLAN:
        scoped(f'head{group}_{stop}', act, 0, [(group, OWN, stop)])
    for i in range(layers):
        keep(h_s.at[i], h_o.at[i])
        scoped('whole_QKV', whole, QKV, i)
        keep(qkv_s.at[i], qkv_o.at[i])
        scoped('qkv_phase', qkv_phase, h_s.at[i], qkv_s.at[i], table_s, q_s.at[i], k_s.at[i], v_s.at[i], vt_s, rows, plan("qkv", i))
        keep(q_s.at[i], q_o.at[i])
        keep(k_s.at[i], k_o.at[i])
        keep(v_s.at[i], v_o.at[i])
        scoped('attend_phase', attend_phase, q_s.at[i], k_s.at[i], vt_s, o_s.at[i], lse_s.at[i], top_s, mix_s, bq, plan("attend", i))
        keep(o_s.at[i], o_o.at[i])
        keep(lse_s.at[i], lse_o.at[i])
        scoped('whole_OD', whole, OD, i)
        keep(od_s.at[i], od_o.at[i])
        if i + 1 == layers:
            scoped('whole_GU', whole, GU, i)
            keep(gu_s.at[i], gu_o.at[i])
        scoped('mid_phase', mid_phase, h_s.at[i], o_s.at[i], od_s.at[i], hm_s.at[i], rows, ro)
        keep(hm_s.at[i], hm_o.at[i])
        if i + 1 < layers:
            scoped('whole_GU', whole, GU, i)
            keep(gu_s.at[i], gu_o.at[i])
            scoped('ffn_phase', ffn_phase, hm_s.at[i], gu_s.at[i], od_s.at[i], h_s.at[i + 1], rows, ro, plan("ffn", i))
    with jax.named_scope('flush'):
        for copy in out:
            copy.wait()
        for pack in packs.values():
            pack.drain()


PACKS = 5
QKV_G, GA_G, GB_G, WD_G, WO_G = range(PACKS)
BACK = {
    "first": ((2, QKV_G, OLD, 2), (3, WD_G, OLD, 4), (3, WO_G, OLD, 4)),
    "second": ((0, QKV_G, OLD, 4), (2, GA_G, OWN, 1)),
    "downs": ((0, GA_G, OWN, 2),),
    "attend": ((0, GB_G, OWN, 1), (1, WD_G, OWN, 1), (2, GA_G, OWN, 3), (3, WO_G, OWN, 1), (4, GB_G, OWN, 2), (6, WD_G, OWN, 2), (7, GA_G, OWN, 4), (8, WO_G, OWN, 2),
               (9, GB_G, OWN, 3)),
    "late": ((0, WD_G, OWN, 3), (0, WO_G, OWN, 3)),
    "end": ((0, GB_G, OWN, 4),),
}
TAIL = ((QKV_G, 2), (WD_G, 4), (WO_G, 4), (QKV_G, 4))
NAMED = ("gu", "hm", "dy", "od", "table", "q", "k", "v", "o", "lse", "h", "qkv")


def backward(sizes, dy, table, qkv, gu, od, q, k, v, o, lse, hm, h, *refs):
    layers, n, bq, rows, r = sizes
    results, refs = refs[:PACKS], refs[PACKS:]
    table_s, qkv_s, gu_s, od_s, lse_s, hm_s, dh_s, dhm_s, made_s, dgu_s, bt_s, db_s, dq_s, kt_s = refs[:14]
    refs = refs[14:]
    terms, came_a, came_b, got = (refs[PACKS * i : PACKS * (i + 1)] for i in range(4))
    in_sem, out_sem, scatter_sems, free_sems = refs[PACKS * 4 :]
    ring = Ring(n)
    split, heads = qkv_s.shape[2], q.shape[2]
    dqkv_s, do_s = made_s.at[:, :split], made_s.at[:, split : split + heads]
    dk_s, dv_s = db_s.at[:, :HEAD], db_s.at[:, HEAD : 2 * HEAD]
    place = 0
    lent = []
    for width in (heads, heads, HEAD, HEAD, h.shape[2]):
        lent.append(dgu_s.at[:, place : place + width])
        place += width
    q_s, o_s, k_s, v_s, h_s = lent
    places = {"gu": (gu, gu_s), "hm": (hm, hm_s), "dy": (dy, dh_s), "od": (od, od_s), "table": (table, table_s), "q": (q, q_s), "k": (k, k_s), "v": (v, v_s),
              "o": (o, o_s), "lse": (lse, lse_s), "h": (h, h_s), "qkv": (qkv, qkv_s)}

    def copy_of(name, *i):
        src, dst = places[name]
        return pltpu.make_async_copy(src.at[i] if i else src, dst, in_sem.at[NAMED.index(name)])

    def bring(names, *i):
        for name in names:
            copy_of(name, *i).start()

    def need(names, *i):
        for name in names:
            copy_of(name, *i).wait()

    last = layers - 1
    bring(("gu", "hm"), last)
    bring(("dy",))
    bring(("od",), last)
    bring(("table",))
    bring(("qkv",), last)
    scoped('meet', ring.meet, 0)

    def pack(group, i, signal, taken=(0, 0)):
        return (QuickScatter if group == QKV_G else Scatter)(ring, terms[group], came_a[group], came_b[group], scatter_sems.at[group], free_sems.at[group], got[group].at[i], signal, taken)

    reached = {}
    for entries in BACK.values():
        for _, group, old, stop in entries:
            if old == OWN:
                reached[group] = max(stop, reached.get(group, 0))
    taken = {group: (min(stop, ring.far_a), min(stop, ring.far_b)) for group, stop in reached.items()}

    def layer(step):
        i = last - step
        later = step > 0
        own = {group: pack(group, i, i > 0) for group in range(PACKS)}
        old = {group: pack(group, i + 1, i >= 0, taken.get(group, (0, 0))) for group in range(PACKS)}

        def act(whats):
            for group, which, stop in whats:
                if which == OWN:
                    own[group].now(stop)
                else:
                    pl.when(later)(functools.partial(old[group].now, stop))

        def plan(phase):
            return planned(act, BACK[phase])

        def before(group):
            pl.when(later)(old[group].finish)

        scoped('need', need, ("gu", "hm", "od"), i)
        pl.when(step == 0)(functools.partial(need, ("dy",)))
        for half, group, phase in ((0, GA_G, "first"), (1, GB_G, "second")):
            scoped('ffn_bwd', ffn_bwd_phase, half, hm_s, dh_s, gu_s, od_s, made_s, dgu_s, bt_s, db_s, dhm_s, rows, r, plan(phase))
            if half == 1:
                pl.when(i > 0)(functools.partial(bring, ("gu", "hm"), i - 1))
            before(group)
            scoped('units', units_phase, half, dgu_s, bt_s, terms[group])
            scoped('begin', own[group].begin, later)
        bring(("o", "q", "k", "v", "lse", "h"), i)
        before(WD_G)
        scoped('downs', downs_phase, made_s, dh_s, terms[WD_G])
        own[WD_G].begin(later)
        scoped('downs_ev', the_rest, plan("downs"), 0)
        need(("o",), i)
        before(WO_G)
        scoped('out_bwd', out_bwd_phase, dhm_s, o_s, od_s, terms[WO_G], do_s, rows, r)
        own[WO_G].begin(later)
        pl.when(i > 0)(functools.partial(bring, ("od",), i - 1))
        need(("q", "k", "v", "lse"), i)
        pl.when(step == 0)(functools.partial(need, ("table",)))
        scoped('attend_bwd', attend_bwd_phase, q_s, k_s, v_s, o_s, do_s, lse_s, table_s, dqkv_s, dq_s, dk_s, dv_s, kt_s, bq, plan("attend"))
        scoped('late_ev', the_rest, plan("late"), 0)
        need(("h",), i)
        pl.when(step == 0)(functools.partial(need, ("qkv",), last))
        before(QKV_G)
        scoped('qkv_bwd', qkv_bwd_phase, h_s, dqkv_s, qkv_s, dhm_s, terms[QKV_G], do_s, dh_s, rows, i > 0)
        own[QKV_G].begin(later)
        scoped('end_ev', the_rest, plan("end"), 0)

        @pl.when(jnp.logical_and(i > 1, i < layers))
        def _():
            copy_of("qkv", i - 1).start()
            copy_of("qkv", i - 1).wait()

    loop(layers, layer)
    final = {group: pack(group, 0, False, taken.get(group, (0, 0))) for group in range(PACKS)}
    for group, stop in TAIL:
        scoped(f'tail{group}_{stop}', final[group].now, stop)
    for p in final.values():
        p.finish()
    out = []
    for group in range(PACKS):
        for i in range(layers):
            out.append(pltpu.make_async_copy(got[group].at[i], results[group].at[i], out_sem.at[len(out)]))
            out[-1].start()
    for copy in out:
        copy.wait()


SEVEN = 7
START = 0


def adamw(*refs):
    count = 3 * SEVEN
    grads, refs = refs[:PACKS], refs[PACKS:]
    ins, outs, refs = refs[:count], refs[count : 2 * count], refs[2 * count :]
    grads_s, refs = refs[:PACKS], refs[PACKS:]
    ins_s, outs_s, (grad_sem, in_sem, out_sem) = refs[:count], refs[count : 2 * count], refs[2 * count :]
    kinds = range(0, count, SEVEN)
    layers = ins[0].shape[0]
    heads, half, whole, few = ins[0].shape[2], ins[4].shape[2] // 2, ins[3].shape[2], 16
    waits = []
    for i in range(layers):
        copies = [pltpu.make_async_copy(src.at[i], dst.at[i], grad_sem.at[g, i]) for g, (src, dst) in enumerate(zip(grads, grads_s, strict=True))]
        copies += [pltpu.make_async_copy(ins[a].at[i], ins_s[a].at[i], in_sem.at[a, i]) for w in range(SEVEN) for a in (w + kind for kind in kinds)]
        for copy in copies:
            copy.start()
        waits.append(copies)
    parts = (
        [(QKV_G, START, START, heads)], [(QKV_G, heads, START, HEAD)], [(QKV_G, heads + HEAD, START, HEAD)], [(WO_G, START, START, whole)],
        [(GA_G, START, START, half), (GB_G, START, half, half)], [(GA_G, half, START, half), (GB_G, half, half, half)], [(WD_G, START, START, whole)],
    )
    out = []
    for i in range(layers):
        for copy in waits[i][:PACKS]:
            copy.wait()
        for w in range(SEVEN):
            for copy in waits[i][PACKS + 3 * w : PACKS + 3 * (w + 1)]:
                copy.wait()

            def step(j, i=i, w=w):
                at = tile(j, few)
                for grad, first, start, wide in parts[w]:
                    here = slice(start, start + wide)
                    g = grads_s[grad][i, at, first : first + wide].astype(F32)
                    weight = ins_s[w][i, at, here].astype(F32)
                    of_m, of_v = w + SEVEN, w + 2 * SEVEN
                    m = 0.9 * ins_s[of_m][i, at, here] + 0.1 * g
                    v = 0.95 * ins_s[of_v][i, at, here] + 0.05 * g * g
                    outs_s[w][i, at, here] = (weight - 0.02 * (m * lax.rsqrt(v + 1e-8) + 0.1 * weight)).astype(BF16)
                    outs_s[of_m][i, at, here] = m
                    outs_s[of_v][i, at, here] = v

            loop(ins[w].shape[1] // few, step)
            for a in (w + kind for kind in kinds):
                out.append(pltpu.make_async_copy(outs_s[a].at[i], outs[a].at[i], out_sem.at[a, i]))
                out[-1].start()
    for copy in out:
        copy.wait()


def solution(mesh):
    n = mesh.shape["dp"]
    far_a, far_b = n // 2, n - 1 - n // 2

    def step(x, dy, *arrays):
        weights = arrays[:SEVEN]
        wq, wk, wv, wo, wg, wu, wd = weights
        layers, r, wide_q = wq.shape
        x, dy = x[0], dy[0]
        tokens, d = x.shape
        ff = wg.shape[2]
        bq, rows = (min(512, tokens),) * 2
        few = jnp.asarray(angles(tokens))
        wide = wide_q + 2 * HEAD
        heads = wide_q // HEAD
        ro = wo.shape[1]
        shapes = (r, wide), (r, 2 * ff), (ro + wd.shape[1], d)
        terms = (r, wide), (r, ff), (r, ff), (wd.shape[1], d), (ro, d)
        both = lambda *s: jax.ShapeDtypeStruct((layers, *s), BF16)
        some = lambda lead, s: pltpu.VMEM((*lead, *s), BF16)
        q, k, v_, o, lse, hm, h, qkv, gu, od, table = pl.pallas_call(
            functools.partial(forward, (layers, n, bq, rows)),
            out_shape=[both(tokens, wide_q), both(tokens, HEAD), both(tokens, HEAD), both(tokens, wide_q), jax.ShapeDtypeStruct((layers, 8, tokens), F32),
                       both(tokens, d), both(tokens, d), *(both(n, *s) for s in shapes), jax.ShapeDtypeStruct((tokens, HEAD), F32)],
            in_specs=[ANY] * 9,
            out_specs=[ANY] * 11,
            scratch_shapes=[
                pltpu.VMEM((layers, tokens, d), BF16), pltpu.VMEM(few.shape, F32), pltpu.VMEM((tokens, HEAD), F32),
                *(some((layers, n), s) for s in shapes),
                pltpu.VMEM((layers, tokens, wide_q), BF16), pltpu.VMEM((layers, tokens, HEAD), BF16), pltpu.VMEM((layers, tokens, HEAD), BF16),
                pltpu.VMEM((HEAD, tokens), BF16), pltpu.VMEM((layers, tokens, wide_q), BF16), pltpu.VMEM((layers, 8, tokens), F32),
                pltpu.VMEM((layers, tokens, d), BF16), pltpu.VMEM((heads, bq), F32), pltpu.VMEM((heads, HEAD + 8, bq), F32),
                pltpu.SemaphoreType.DMA((9 * layers,)), pltpu.SemaphoreType.DMA((2,)), pltpu.SemaphoreType.DMA((10 * layers + 1,)),
                pltpu.SemaphoreType.DMA((3 * layers, 4, far_a)), pltpu.SemaphoreType.DMA((3 * layers, n + 1)),
            ],
            compiler_params=pltpu.CompilerParams(vmem_limit_bytes=VMEM, collective_id=0, has_side_effects=True),
            name="forward",
        )(x, few, *weights)
        grads = pl.pallas_call(
            functools.partial(backward, (layers, n, bq, rows, ro)),
            out_shape=[both(*s) for s in terms],
            in_specs=[ANY] * 12,
            out_specs=[ANY] * 5,
            scratch_shapes=[
                pltpu.VMEM((tokens, HEAD), F32), *(some((n,), s) for s in shapes),
                pltpu.VMEM((8, tokens), F32), pltpu.VMEM((tokens, d), BF16), pltpu.VMEM((tokens, d), BF16), pltpu.VMEM((tokens, d), BF16),
                pltpu.VMEM((tokens, ff), BF16), pltpu.VMEM((tokens, 2 * ff), BF16), pltpu.VMEM((d, tokens), BF16),
                pltpu.VMEM((tokens, d), F32), pltpu.VMEM((heads, HEAD, bq), F32), pltpu.VMEM((HEAD, tokens), BF16),
                *(some((lead,), s) for lead in (n, far_a, far_b, layers) for s in terms),
                pltpu.SemaphoreType.DMA((len(NAMED),)), pltpu.SemaphoreType.DMA((5 * layers,)),
                pltpu.SemaphoreType.DMA((5, 4, far_a)), pltpu.SemaphoreType.REGULAR((5,)),
            ],
            compiler_params=pltpu.CompilerParams(vmem_limit_bytes=VMEM, collective_id=1, has_side_effects=True),
            name="backward",
        )(dy, table, qkv, gu, od, q, k, v_, o, lse, hm, h)
        in_vmem = lambda a: pltpu.VMEM(a.shape, a.dtype)
        return pl.pallas_call(
            adamw,
            out_shape=[jax.ShapeDtypeStruct(a.shape, a.dtype) for a in arrays],
            in_specs=[ANY] * (PACKS + 3 * SEVEN),
            out_specs=[ANY] * (3 * SEVEN),
            scratch_shapes=[*map(in_vmem, grads), *map(in_vmem, arrays), *map(in_vmem, arrays),
                            pltpu.SemaphoreType.DMA((PACKS, layers)), *(pltpu.SemaphoreType.DMA((3 * SEVEN, layers)) for _ in arrays[:2])],
            compiler_params=pltpu.CompilerParams(vmem_limit_bytes=VMEM),
            name="adamw",
        )(*grads, *arrays)

    states, cut = P(("rep", "dp"), None, None), P(None, "dp", None)
    return jax.shard_map(
        step,
        mesh=mesh,
        in_specs=(states, states) + (cut,) * (3 * SEVEN),
        out_specs=(P("rep", "dp", None),) * (3 * SEVEN),
        check_vma=False,
    )
```

```python
import functools

import jax
import jax.numpy as jnp
import numpy as np
from jax import lax
from jax.experimental import pallas as pl
from jax.experimental.pallas import tpu as pltpu
from jax.sharding import PartitionSpec as P

HEAD = 128
THETA = 10000
NEG = -1e30
HIDDEN = 2 * NEG
LOG2E = 1.4426950408889634
SCALE = HEAD**-0.5
E = SCALE * LOG2E
VMEM = 66_000_000
STRETCH = 64
F32, BF16 = jnp.float32, jnp.bfloat16
ANY = pl.BlockSpec(memory_space=pl.ANY)
MESH = pl.DeviceIdType.MESH
A, B = 0, 1


def dot(a, b, ca=1, cb=0):
    return lax.dot_general(a, b, (((ca,), (cb,)), ((), ())), preferred_element_type=F32)


def scoped(name, what, *args):
    with jax.named_scope(name):
        return what(*args)


def tile(i, n):
    return pl.ds(pl.multiple_of(i * n, n), n)


def loop(n, body):
    lax.fori_loop(0, n, lambda i, _: body(i), None)


def polled(events, i, steps):
    for when, what in events.items():
        if when < steps:
            pl.when(i == when)(functools.partial(scoped, f"ev{when}", what))


def the_rest(events, steps):
    for when, what in events.items():
        if when >= steps:
            what()


def scale_of(wide):
    return lax.rsqrt(jnp.mean(wide * wide, -1, keepdims=True) + 1e-6)


def norm_bwd(wide, scale, g):
    return scale * g - wide * (scale * scale * scale * jnp.mean(wide * g, -1, keepdims=True))


def angles(tokens):
    half = HEAD // 2
    turn = float(THETA) ** (-np.arange(half) / half)
    place = np.arange(STRETCH)[:, None] * turn
    start = np.arange(0, tokens, STRETCH)[:, None] * turn
    cos, sin = np.cos(start), np.sin(start)
    return np.concatenate([np.concatenate(p, 1) for p in ((np.cos(place), np.sin(place)), (cos, cos), (-sin, sin))]).astype(np.float32)


def table_phase(few, table):
    starts = table.shape[0] // STRETCH

    def step(i):
        place = few[:STRETCH, :]
        row = lambda first: few[pl.ds(first + i, 1), :]
        table[tile(i, STRETCH), :] = place * row(STRETCH) + pltpu.roll(place, HEAD // 2, 1) * row(STRETCH + starts)

    loop(starts, step)


def turns(t):
    swapped = pltpu.roll(t, HEAD // 2, 1)
    first = lax.broadcasted_iota(jnp.int32, t.shape, 1) < HEAD // 2
    return jnp.where(first, t, swapped), jnp.where(first, -swapped, t)


def rotated(t, cos, sin):
    return t * cos + pltpu.roll(t, HEAD // 2, 1) * sin


class Ring:
    def __init__(self, n):
        self.n, self.far_a = n, n // 2
        self.far_b = n - 1 - self.far_a
        self.me = lax.axis_index("dp")
        rep = lax.axis_index("rep")
        self.core = lax.rem(rep, 2)
        self.partner = {"rep": rep + 1 - 2 * self.core}
        self.turn = 1 - 2 * self.core
        self.near = 1, -1, 2, -2

    def at(self, k):
        return lax.rem(self.me + self.n + k * self.turn, self.n)

    def to(self, k):
        return {"dp": self.at(k)}

    def meet(self):
        barrier = pltpu.get_barrier_semaphore()
        others = [self.to(k) for k in self.near] + [self.partner]
        for other in others:
            pl.semaphore_signal(barrier, inc=1, device_id=other, device_id_type=MESH)
        pl.semaphore_wait(barrier, len(others))


def remote(src, dst, send, recv, to):
    return pltpu.make_async_remote_copy(src_ref=src, dst_ref=dst, send_sem=send, recv_sem=recv, device_id=to, device_id_type=MESH)


class Chains:
    def far(self, chain):
        return self.ring.far_b if chain else self.ring.far_a

    def now(self, s):
        for count in range(1, s + 1):
            for chain in (A, B):
                if self.taken[chain] < min(count, self.far(chain)):
                    self.taken[chain] += 1
                    self.take(chain, self.taken[chain])

    def finish(self):
        self.now(self.ring.far_a)


class Blocks:
    def __init__(self, ref, rows):
        self.ref, self.rows = ref, rows

    def part(self, block, first, count, columns=slice(None)):
        if len(self.ref.shape) == 2:
            return self.ref.at[pl.ds(pl.multiple_of(block * self.rows + first, 16), count), columns]
        return self.ref.at[block, pl.ds(pl.multiple_of(first, 16), count), columns]

    def all(self, first, end, share=slice(None)):
        return jnp.concatenate([self.ref[at + first : at + end, :] for at in range(0, self.ref.shape[0], self.rows)[share]])


class Gather(Chains):
    def __init__(self, ring, blocks, sems, handed_sems):
        self.taken = [0, 0]
        self.ring, self.blocks, self.sems, self.handed_sems = ring, blocks, sems, handed_sems
        self.half = blocks.rows // 2
        self.last_handed = {}

    def piece(self, block, half):
        return self.blocks.part(block, half * self.half, self.half)

    def hop(self, chain, step):
        ring = self.ring
        along = 1 if chain == A else -1
        part = self.piece(ring.at(-along * step), ring.core)
        return remote(part, part, self.sems.at[2 * chain, step], self.sems.at[2 * chain + 1, step], ring.to(along))

    def handed(self, chain, step):
        ring = self.ring
        part = self.piece(ring.at(-step - 1 if chain == A else step + 1), ring.core)
        return remote(part, part, self.handed_sems.at[ring.n - 1 + chain], self.handed_sems.at[step + chain * ring.far_a], ring.partner)

    def begin(self):
        for chain in (A, B):
            self.hop(chain, 0).start()

    def take(self, chain, s):
        ring = self.ring
        part = self.piece(ring.at(-s if chain == A else s), ring.core)
        remote(part, part, self.sems.at[2 * chain, s - 1], self.sems.at[2 * chain + 1, s - 1], ring.to(1)).wait_recv()
        if s < self.far(chain):
            self.hop(chain, s).start()
        if chain in self.last_handed:
            self.handed(chain, self.last_handed[chain]).wait_send()
        self.last_handed[chain] = s - 1
        self.handed(chain, s - 1).start()

    def complete(self):
        ring = self.ring
        for chain in (A, B):
            for step in range(self.far(chain)):
                part = self.piece(ring.at(step + 1 if chain == A else -step - 1), 1 - ring.core)
                remote(part, part, self.handed_sems.at[ring.n - 1], self.handed_sems.at[step + chain * ring.far_a], ring.partner).wait_recv()

    def drain(self):
        for chain in (A, B):
            for step in range(self.far(chain)):
                self.hop(chain, step).wait_send()
        for chain, step in self.last_handed.items():
            self.handed(chain, step).wait_send()


class Scatter(Chains):
    def __init__(self, ring, p, came_a, came_b, sems, free, got, signal, taken=(0, 0)):
        self.signal = signal
        self.ring, self.p, self.came, self.sems, self.free, self.got = ring, p, (came_a, came_b), sems, free, got
        self.taken = list(taken)

    def hop(self, chain, step):
        ring = self.ring
        left = self.far(chain) - step
        block = ring.at(left if chain == 0 else -left)
        return remote(self.p.at[block], self.came[chain].at[step], self.sems.at[2 * chain, step], self.sems.at[2 * chain + 1, step],
                      ring.to(1 if chain == 0 else -1))

    def added(self, chain, step):
        ring = self.ring
        left = self.far(chain) - step
        block = ring.at(left if chain == 0 else -left)
        few = 16

        def rows(i):
            at = tile(i, few)
            self.p[block, at, :] = (self.p[block, at, :].astype(F32) + self.came[chain][step - 1, at, :].astype(F32)).astype(BF16)

        loop(self.p.shape[1] // few, rows)

    def begin(self, wait):
        pl.when(wait)(lambda: pl.semaphore_wait(self.free, len(self.ring.near)))
        self.hop(A, 0).start()
        self.hop(B, 0).start()

    def take(self, chain, s):
        self.hop(chain, s - 1).wait_recv()
        if s < self.far(chain):
            self.added(chain, s)
            self.hop(chain, s).start()
        if self.taken == [self.far(A), self.far(B)]:
            self.end()

    def arrived(self):
        return [(chain, self.far(chain) - 1) for chain in (A, B)]

    def end(self):
        me, few = self.ring.me, 16

        def rows(i):
            at = tile(i, few)
            total = self.p[me, at, :].astype(F32)
            for chain, slot in self.arrived():
                total += self.came[chain][slot, at, :].astype(F32)
            self.got[at, :] = total.astype(BF16)

        loop(self.p.shape[1] // few, rows)
        for chain in (A, B):
            for step in range(self.far(chain)):
                self.hop(chain, step).wait_send()

        @pl.when(self.signal)
        def _():
            for k in self.ring.near:
                pl.semaphore_signal(self.free, inc=1, device_id=self.ring.to(k), device_id_type=MESH)


class QuickScatter(Scatter):
    def hop(self, chain, step):
        ring = self.ring
        kind = step + self.far(A) - self.far(chain)
        block, reach = ((4, 2), (3, 1), (1, 1), (2, 2))[kind]
        along = 1 if chain == A else -1
        return remote(self.p.at[ring.at(along * block)], self.came[chain].at[step], self.sems.at[2 * chain, step], self.sems.at[2 * chain + 1, step],
                      ring.to(along * reach))

    def begin(self, wait):
        pl.when(wait)(lambda: pl.semaphore_wait(self.free, len(self.ring.near)))
        for step in range(self.far(A) - 1):
            for chain in (A, B):
                if step < self.far(chain) - 1:
                    self.hop(chain, step).start()

    def take(self, chain, s):
        self.hop(chain, s - 1).wait_recv()
        beyond = self.far(chain) - 2
        if s == beyond:
            block, few = self.ring.at(2 if chain == A else -2), 16

            def rows(i):
                at = tile(i, few)
                total = self.p[block, at, :].astype(F32)
                for slot in range(beyond):
                    total += self.came[chain][slot, at, :].astype(F32)
                self.p[block, at, :] = total.astype(BF16)

            loop(self.p.shape[1] // few, rows)
            self.hop(chain, self.far(chain) - 1).start()
        if self.taken == [self.far(A), self.far(B)]:
            self.end()

    def arrived(self):
        return [(chain, self.far(chain) - back) for chain in (A, B) for back in (1, 2)]


def merged(w):
    return w.reshape(w.shape[0] * w.shape[1], w.shape[2])


def qkv_phase(h, w, table, q, k, v, vt, rows, events):
    wide_q = q.shape[1]

    def step(i):
        at = tile(i, rows)
        wide = h[at, :].astype(F32)
        a = (wide * scale_of(wide)).astype(BF16)
        y = dot(a, merged(w[...])).astype(BF16)
        cos, sin = turns(table[at, :])
        for n in range(wide_q // HEAD):
            part = slice(n * HEAD, (n + 1) * HEAD)
            q[at, part] = rotated(y[:, part].astype(F32), cos, sin).astype(BF16)
        k[at, :] = rotated(y[:, wide_q : wide_q + HEAD].astype(F32), cos, sin).astype(BF16)
        mine = y[:, wide_q + HEAD :]
        v[at, :] = mine
        vt[:, at] = mine.T
        polled(events, i, h.shape[0] // rows)

    loop(h.shape[0] // rows, step)
    the_rest(events, h.shape[0] // rows)


def spans(bq):
    half = bq // 2
    return [(0, half, 0), (half, half, half)]


def seen(keys, first_key, queries, first_query):
    key = lax.broadcasted_iota(jnp.int32, (keys, queries), 0) + first_key
    return lax.broadcasted_iota(jnp.int32, (keys, queries), 1) + first_query >= key


def blocks(tokens, bq):
    return (tokens // bq) * (tokens // bq + 1) // 2


def row_of_blocks(iq, bq, block, events, steps):
    def step(j):
        @pl.when(j < iq)
        def _():
            block(pl.multiple_of(j * bq, bq), bq, 0, None)

        @pl.when(j == iq)
        def _():
            for first, nk, lo in spans(bq):
                block(pl.multiple_of(iq * bq + first, nk), nk, lo, seen(nk, first, bq - lo, lo))

        polled(events, lax.div(iq * (iq + 1), 2) + j, steps)

    loop(iq + 1, step)


def attend_phase(q, k, vt, o, lse, top_s, mix_s, bq, events):
    heads = q.shape[1] // HEAD

    def block(iq, start, nk, lo, mask):
        here = pl.ds(start, nk)
        cols = pl.ds(pl.multiple_of(iq * bq + lo, bq - lo), bq - lo)
        keys = k[here, :]
        scores = [dot(keys, q[cols, n * HEAD : (n + 1) * HEAD], 1, 1) for n in range(heads)]
        values = jnp.concatenate([vt[:, here], jnp.ones((8, nk), BF16)], axis=0)
        for n, s in enumerate(scores):
            if mask is not None:
                s = jnp.where(mask, s, HIDDEN)
            old = top_s[n : n + 1, lo:]
            top = jnp.maximum(old, s.max(axis=0, keepdims=True))
            top_s[n : n + 1, lo:] = top
            p = jnp.exp2((s - top) * E).astype(BF16)
            mix_s[n, :, lo:] = mix_s[n, :, lo:] * jnp.exp2((old - top) * E) + dot(values, p)

    def step(iq):
        at = tile(iq, bq)
        top_s[...] = jnp.full(top_s.shape, NEG, F32)
        mix_s[...] = jnp.zeros(mix_s.shape, F32)
        row_of_blocks(iq, bq, functools.partial(block, iq), events, blocks(q.shape[0], bq))
        for n in range(heads):
            total = mix_s[n, HEAD : HEAD + 1, :]
            o[at, n * HEAD : (n + 1) * HEAD] = (mix_s[n, :HEAD, :] * (1 / total)).T.astype(BF16)
            lse[n : n + 1, at] = top_s[n : n + 1, :] * E + jnp.log2(total)

    loop(q.shape[0] // bq, step)
    the_rest(events, blocks(q.shape[0], bq))


def mid_phase(h, o, od, hm, rows, r):
    def step(i):
        at = tile(i, rows)
        hm[at, :] = h[at, :] + dot(o[at, :], od.all(0, r)).astype(BF16)

    loop(h.shape[0] // rows, step)


def ffn_phase(hm, gu, od, out, rows, r, events):
    def step(i):
        at = tile(i, rows)
        mid = hm[at, :]
        wide = mid.astype(F32)
        b = (wide * scale_of(wide)).astype(BF16)
        y = dot(b, gu.ref[...])
        part = y.shape[1] // 4
        pieces = []
        for n in (0, 2 * part):
            gate, up = y[:, n : n + part], y[:, n + part : n + 2 * part]
            pieces.append((gate * (1 / (1 + jnp.exp(-gate))) * up).astype(BF16))
        made = jnp.concatenate(pieces, axis=1)
        out[at, :] = mid + dot(made, od.all(r, od.rows)).astype(BF16)
        polled(events, i, hm.shape[0] // rows)

    loop(hm.shape[0] // rows, step)
    the_rest(events, hm.shape[0] // rows)


def ffn_bwd_phase(half, hm, dy, gu, od, made_s, dgu_s, bt_s, db_s, dhm, rows, r, events):
    part = dgu_s.shape[1] // 4
    lanes, units = slice(2 * part * half, 2 * part * (half + 1)), slice(part * half, part * (half + 1))
    some = od.ref.shape[0] // od.rows // 2
    share = slice(some * half, some * (half + 1))

    def step(i):
        at = tile(i, rows)
        wide = hm[at, :].astype(F32)
        scale = scale_of(wide)
        b = (wide * scale).astype(BF16)
        if half == 0:
            bt_s[:, at] = b.T
        y = dot(b, gu[:, lanes])
        gate, up = y[:, :part], y[:, part:]
        back = dy[at, :]
        d_made = dot(back, od.all(r, od.rows, share), 1, 1).astype(BF16).astype(F32)
        sig = 1 / (1 + jnp.exp(-gate))
        silu = gate * sig
        made_s[at, units] = (silu * up).astype(BF16)
        d_gate = (d_made * up * (sig * (1 + gate - silu))).astype(BF16)
        d_up = (d_made * silu).astype(BF16)
        both = jnp.concatenate([d_gate, d_up], axis=1)
        dgu_s[at, lanes] = both
        db = dot(both, gu[:, lanes], 1, 1)
        if half == 0:
            db_s[at, :] = db
        else:
            db = (db_s[at, :] + db).astype(BF16).astype(F32)
            dhm[at, :] = (back.astype(F32) + norm_bwd(wide, scale, db)).astype(BF16)
        polled(events, i, hm.shape[0] // rows)

    loop(hm.shape[0] // rows, step)
    the_rest(events, hm.shape[0] // rows)


def units_phase(half, dgu_s, bt_s, p):
    n, _, columns = p.shape
    wide = next(w for w in (512, 256, 128) if columns % w == 0)

    def units(i):
        here = pl.ds(pl.multiple_of(columns * half + i * wide, wide), wide)
        p[:, :, tile(i, wide)] = dot(bt_s[...], dgu_s[:, here]).astype(BF16).reshape(n, -1, wide)

    loop(columns // wide, units)


def downs_phase(made_s, dy, p):
    n, share, group = p.shape[0], p.shape[1], 2

    def downs(i):
        got = dot(made_s[:, tile(i, group * share)], dy[...], 0, 0).astype(BF16)
        p[pl.ds(i * group, group)] = got.reshape(group, share, -1)

    loop(n // group, downs)


def out_bwd_phase(dhm, o, od, p, do, rows, r):
    def step(i):
        at = tile(i, rows)
        do[at, :] = dot(dhm[at, :], od.all(0, r), 1, 1).astype(BF16)

    loop(dhm.shape[0] // rows, step)
    p[...] = dot(o[...], dhm[...], 0, 0).astype(BF16).reshape(p.shape)


def attend_bwd_phase(q, k, v, o, do, lse, table, dqkv, dq_s, dk_s, dv_s, kt_s, bq, events):
    heads = q.shape[1] // HEAD
    wide_q = q.shape[1]
    dk_s[...] = jnp.zeros(dk_s.shape, F32)
    dv_s[...] = jnp.zeros(dv_s.shape, F32)
    kt_s[...] = k[...].T

    def block(iq, lses, deltas, start, nk, lo, mask):
        here = pl.ds(start, nk)
        cols = pl.ds(pl.multiple_of(iq * bq + lo, bq - lo), bq - lo)
        keys, values, keys_t = k[here, :], v[here, :], kt_s[:, here]
        qs = [q[cols, n * HEAD : (n + 1) * HEAD] for n in range(heads)]
        dos = [do[cols, n * HEAD : (n + 1) * HEAD] for n in range(heads)]
        scores = [dot(keys, x, 1, 1) for x in qs]
        dps = [dot(values, x, 1, 1) for x in dos]
        for n in range(heads):
            p = jnp.exp2(scores[n] * E - lses[n][:, lo:])
            if mask is not None:
                p = jnp.where(mask, p, 0.0)
            ds = (p * (dps[n] - deltas[n][:, lo:])).astype(BF16)
            dv_s[here, :] += dot(p.astype(BF16), dos[n])
            dk_s[here, :] += dot(ds, qs[n])
            dq_s[n, :, lo:] += dot(keys_t, ds)

    def step(iq):
        at = tile(iq, bq)
        dq_s[...] = jnp.zeros(dq_s.shape, F32)
        lses = [lse[n : n + 1, at] for n in range(heads)]
        deltas = []
        for n in range(heads):
            part = slice(n * HEAD, (n + 1) * HEAD)
            deltas.append((do[at, part].astype(F32) * o[at, part].astype(F32)).T.sum(axis=0, keepdims=True))
        row_of_blocks(iq, bq, functools.partial(block, iq, lses, deltas), events, blocks(q.shape[0], bq))
        cos, sin = turns(table[at, :])
        for n in range(heads):
            back = (dq_s[n] * SCALE).T.astype(BF16).astype(F32)
            dqkv[at, n * HEAD : (n + 1) * HEAD] = rotated(back, cos, -sin).astype(BF16)

    loop(q.shape[0] // bq, step)
    the_rest(events, blocks(q.shape[0], bq))

    def finish(i):
        at = tile(i, bq)
        cos, sin = turns(table[at, :])
        dqkv[at, wide_q : wide_q + HEAD] = rotated((dk_s[at, :] * SCALE).astype(BF16).astype(F32), cos, -sin).astype(BF16)
        dqkv[at, wide_q + HEAD :] = dv_s[at, :].astype(BF16)

    loop(q.shape[0] // bq, finish)


def qkv_bwd_phase(h, dqkv, w, dhm, p_qkv, a_s, dh, rows, further):
    def step(i):
        at = tile(i, rows)
        wide = h[at, :].astype(F32)
        scale = scale_of(wide)
        a_s[at, :] = (wide * scale).astype(BF16)

        @pl.when(further)
        def _():
            da = dot(dqkv[at, :], merged(w[...]), 1, 1).astype(BF16).astype(F32)
            dh[at, :] = (dhm[at, :].astype(F32) + norm_bwd(wide, scale, da)).astype(BF16)

    loop(h.shape[0] // rows, step)
    p_qkv[...] = dot(a_s[...], dqkv[...], 0, 0).astype(BF16).reshape(p_qkv.shape)


SEVEN = 7
START = 0
QKV, OD, GU = range(3)
OWN, OLD = range(2)
NEXT = OLD
PLAN = {
    "qkv": ((0, OD, OWN, 2), (0, QKV, NEXT, 0), (0, OD, NEXT, 0), (3, GU, OWN, 2)),
    "attend": ((1, OD, OWN, 3), (2, QKV, NEXT, 1), (3, OD, NEXT, 1), (6, GU, OWN, 3), (8, OD, OWN, 4), (8, QKV, NEXT, 2), (8, GU, NEXT, 0), (9, OD, NEXT, 2)),
    "ffn": ((0, QKV, NEXT, 3), (1, GU, NEXT, 1), (2, QKV, NEXT, 4), (2, OD, NEXT, 3)),
}
LAST_PLAN = {"qkv": ((1, GU, OWN, 2), (2, OD, OWN, 4)), "attend": ((3, GU, OWN, 3), (7, GU, OWN, 4))}
HEAD_PLAN = ((QKV, 1), (GU, 0), (QKV, 2), (OD, 1), (QKV, 3), (GU, 1), (QKV, 4))


def planned(act, entries):
    by_step = {}
    for when, *what in entries:
        by_step.setdefault(when, []).append(what)
    return {when: functools.partial(act, whats) for when, whats in by_step.items()}


def forward(ring, sizes, x, few, weights, spaces, h_s, few_s, table_s, packs_s, q_s, k_s, v_s, vt_s, o_s, lse_s, hm_s, top_s, mix_s,
            own_sem, in_sem, out_sem, gather_sems, handed_sems):
    layers, bq, rows = sizes
    me = ring.me
    wq, wk, wv, wo, wg, wu, wd = weights
    wide_q, r, ro, rd = wq.shape[2], wq.shape[1], wo.shape[1], wd.shape[1]
    half = wg.shape[2] // 2
    own = {}

    def fetch(i, group, pieces):
        for src, first, count, start, wide in pieces:
            copy = pltpu.make_async_copy(src, packs_s[i][group].part(me, first, count, slice(start, start + wide)), own_sem.at[sum(map(len, own.values()))])
            own.setdefault((i, group), []).append(copy)
            copy.start()

    for i in range(layers):
        fetch(i, QKV, [(wq.at[i], 0, r, 0, wide_q), (wk.at[i], 0, r, wide_q, HEAD), (wv.at[i], 0, r, wide_q + HEAD, HEAD)])
        fetch(i, OD, [(wo.at[i], 0, ro, 0, wo.shape[2]), (wd.at[i], ro, rd, 0, wd.shape[2])])
        if i == 0:
            brought = [pltpu.make_async_copy(x, h_s, in_sem.at[0]), pltpu.make_async_copy(few, few_s, in_sem.at[1])]
            for copy in brought:
                copy.start()
        fetch(i, GU, [(w.at[i, :, half * j : half * (j + 1)], 0, r, half * (2 * j + k), half) for j in (0, 1) for k, w in enumerate((wg, wu))])
    packs = {(g, i): Gather(ring, packs_s[i][g], gather_sems.at[3 * i + g], handed_sems.at[3 * i + g]) for g in (QKV, OD, GU) for i in range(layers)}
    begun = set()
    kept = {}

    def keep(name, src, i):
        kept[name] = pltpu.make_async_copy(src, spaces[name].at[i], out_sem.at[KEPT.index(name)])
        kept[name].start()

    def reuse(*names):
        for name in names:
            if name in kept:
                kept.pop(name).wait()

    def begin(group, i):
        if (group, i) not in begun:
            begun.add((group, i))
            for copy in own[i, group]:
                copy.wait()
            packs[group, i].begin()

    def act(i, whats):
        for group, which, stop in whats:
            if i + which < layers:
                begin(group, i + which)
                packs[group, i + which].now(stop)

    def plan(phase, i):
        return planned(functools.partial(act, i), (PLAN if i + 1 < layers else LAST_PLAN).get(phase, ()))

    def whole(group, i):
        begin(group, i)
        packs[group, i].finish()
        packs[group, i].complete()

    scoped('meet', ring.meet)
    begin(QKV, 0)
    begin(OD, 0)
    for copy in brought:
        copy.wait()
    table_phase(few_s, table_s)
    for group, stop in HEAD_PLAN:
        scoped(f'head{group}_{stop}', act, 0, [(group, OWN, stop)])
    for i in range(layers):
        qkv, od, gu = packs_s[i]
        last = i + 1 == layers
        keep("h", h_s, i)
        scoped('whole_QKV', whole, QKV, i)
        reuse("q", "k", "v")
        scoped('qkv_phase', qkv_phase, h_s, qkv.ref, table_s, q_s, k_s, v_s, vt_s, rows, plan("qkv", i))
        keep("q", q_s, i)
        keep("k", k_s, i)
        keep("v", v_s, i)
        reuse("o", "lse")
        scoped('attend_phase', attend_phase, q_s, k_s, vt_s, o_s, lse_s, top_s, mix_s, bq, plan("attend", i))
        keep("o", o_s, i)
        keep("lse", lse_s, i)
        scoped('whole_OD', whole, OD, i)
        if last:
            scoped('whole_GU', whole, GU, i)
        else:
            keep("od", od.ref, i)
        reuse("hm")
        scoped('mid_phase', mid_phase, h_s, o_s, od, hm_s, rows, ro)
        if not last:
            keep("hm", hm_s, i)
            scoped('whole_GU', whole, GU, i)
            keep("gu", gu.ref, i)
            reuse("h")
            scoped('ffn_phase', ffn_phase, hm_s, gu, od, h_s, rows, ro, plan("ffn", i))
    with jax.named_scope('flush'):
        reuse(*KEPT)
        for pack in packs.values():
            pack.drain()


KEPT = ("q", "k", "v", "o", "lse", "hm", "h", "od", "gu")
PACKS = 5
QKV_G, GA_G, GB_G, WD_G, WO_G = range(PACKS)
BACK = {
    "first": ((2, QKV_G, OLD, 2), (3, WD_G, OLD, 4), (3, WO_G, OLD, 4)),
    "second": ((0, QKV_G, OLD, 4), (2, GA_G, OWN, 1)),
    "downs": ((0, GA_G, OWN, 2),),
    "attend": ((0, GB_G, OWN, 1), (1, WD_G, OWN, 1), (2, GA_G, OWN, 3), (3, WO_G, OWN, 1), (4, GB_G, OWN, 2), (6, WD_G, OWN, 2), (7, GA_G, OWN, 4), (8, WO_G, OWN, 2),
               (9, GB_G, OWN, 3)),
    "late": ((0, WD_G, OWN, 3), (0, WO_G, OWN, 3)),
    "end": ((0, GB_G, OWN, 4),),
}
TAIL = ((QKV_G, 2), (WD_G, 4), (WO_G, 4), (QKV_G, 4))


def train(sizes, x, few, dy, *refs):
    layers, n, bq, rows, r = sizes
    weights, refs = refs[:SEVEN], refs[SEVEN:]
    results, refs = refs[:PACKS], refs[PACKS:]
    spaces, refs = dict(zip(KEPT, refs)), refs[len(KEPT) :]
    few_s, table_s, qkv_s, gu_s, od_s, k_s, v_s, lse_s, hm_s, dh_s, dhm_s, made_s, dgu_s, bt_s, db_s, mix_s, top_s, kt_s = refs[:18]
    refs = refs[18:]
    terms, came_a, came_b, got = (refs[PACKS * i : PACKS * (i + 1)] for i in range(4))
    forward_sems, (in_sem, result_sem, scatter_sems, free_sems) = refs[PACKS * 4 : -4], refs[-4:]
    ring = Ring(n)
    split, heads = qkv_s.shape[2], spaces["q"].shape[2]
    d = dh_s.shape[1]
    depth = qkv_s.shape[1]
    early = Blocks(terms[QKV_G], depth), Blocks(made_s.at[:, :d], od_s.shape[0] // n), Blocks(dgu_s.at[: n * depth, :], depth)
    late = Blocks(qkv_s, depth), Blocks(od_s, od_s.shape[0] // n), Blocks(gu_s, depth)
    od = late[OD]
    dq_s = mix_s.at[:, :HEAD, :]
    dqkv_s, do_s = made_s.at[:, :split], made_s.at[:, split : split + heads]
    dk_s, dv_s = db_s.at[:, :HEAD], db_s.at[:, HEAD : 2 * HEAD]
    q_s, o_s, h_s = dgu_s.at[:, :heads], dgu_s.at[:, heads : 2 * heads], dgu_s.at[:, 2 * heads : 2 * heads + d]
    places = {"gu": gu_s, "hm": hm_s, "od": od_s, "q": q_s, "k": k_s, "v": v_s, "o": o_s, "lse": lse_s, "h": h_s}

    def copy_of(name, i):
        return pltpu.make_async_copy(spaces[name].at[i], places[name], in_sem.at[KEPT.index(name)])

    def bring(names, i):
        for name in names:
            copy_of(name, i).start()

    def need(names, i):
        for name in names:
            copy_of(name, i).wait()

    back = pltpu.make_async_copy(dy, dh_s, in_sem.at[len(KEPT)])
    back.start()
    forward(ring, (layers, bq, rows), x, few, weights, spaces, made_s.at[:, d : 2 * d], few_s, table_s, [early] * (layers - 1) + [late], dhm_s, k_s, v_s, bt_s.at[:HEAD, :],
            made_s.at[:, 2 * d : 2 * d + heads], lse_s, hm_s, top_s, mix_s, *forward_sems)
    back.wait()
    last = layers - 1

    def pack(group, i, signal, taken=(0, 0)):
        return (QuickScatter if group == QKV_G else Scatter)(ring, terms[group], came_a[group], came_b[group], scatter_sems.at[group], free_sems.at[group], got[group].at[i], signal, taken)

    reached = {}
    for entries in BACK.values():
        for _, group, old, stop in entries:
            if old == OWN:
                reached[group] = max(stop, reached.get(group, 0))
    taken = {group: (min(stop, ring.far_a), min(stop, ring.far_b)) for group, stop in reached.items()}

    def layer(step):
        i = last - step
        later = step > 0
        own = {group: pack(group, i, i > 0) for group in range(PACKS)}
        old = {group: pack(group, i + 1, i >= 0, taken.get(group, (0, 0))) for group in range(PACKS)}

        def act(whats):
            for group, which, stop in whats:
                if which == OWN:
                    own[group].now(stop)
                else:
                    pl.when(later)(functools.partial(old[group].now, stop))

        def plan(phase):
            return planned(act, BACK[phase])

        def before(group):
            pl.when(later)(old[group].finish)

        pl.when(later)(functools.partial(need, ("gu", "hm", "od"), i))
        for half, group, phase in ((0, GA_G, "first"), (1, GB_G, "second")):
            scoped('ffn_bwd', ffn_bwd_phase, half, hm_s, dh_s, gu_s, od, made_s, dgu_s, bt_s, db_s, dhm_s, rows, r, plan(phase))
            if half == 1:
                pl.when(i > 0)(functools.partial(bring, ("gu", "hm"), i - 1))
            before(group)
            scoped('units', units_phase, half, dgu_s, bt_s, terms[group])
            scoped('begin', own[group].begin, later)
        bring(("o", "q", "k", "v", "lse", "h"), i)
        before(WD_G)
        scoped('downs', downs_phase, made_s, dh_s, terms[WD_G])
        own[WD_G].begin(later)
        scoped('downs_ev', the_rest, plan("downs"), 0)
        need(("o",), i)
        before(WO_G)
        scoped('out_bwd', out_bwd_phase, dhm_s, o_s, od, terms[WO_G], do_s, rows, r)
        own[WO_G].begin(later)
        pl.when(i > 0)(functools.partial(bring, ("od",), i - 1))
        need(("q", "k", "v", "lse"), i)
        scoped('attend_bwd', attend_bwd_phase, q_s, k_s, v_s, o_s, do_s, lse_s, table_s, dqkv_s, dq_s, dk_s, dv_s, kt_s, bq, plan("attend"))
        scoped('late_ev', the_rest, plan("late"), 0)
        need(("h",), i)
        before(QKV_G)
        scoped('qkv_bwd', qkv_bwd_phase, h_s, dqkv_s, qkv_s, dhm_s, terms[QKV_G], do_s, dh_s, rows, i > 0)
        own[QKV_G].begin(later)
        scoped('end_ev', the_rest, plan("end"), 0)

    loop(layers, layer)
    final = {group: pack(group, 0, False, taken.get(group, (0, 0))) for group in range(PACKS)}
    for group, stop in TAIL:
        scoped(f'tail{group}_{stop}', final[group].now, stop)
    for p in final.values():
        p.finish()
    out = []
    for group in range(PACKS):
        for i in range(layers):
            out.append(pltpu.make_async_copy(got[group].at[i], results[group].at[i], result_sem.at[len(out)]))
            out[-1].start()
    for copy in out:
        copy.wait()


def adamw(*refs):
    count = 3 * SEVEN
    grads, refs = refs[:PACKS], refs[PACKS:]
    ins, outs, refs = refs[:count], refs[count : 2 * count], refs[2 * count :]
    grads_s, refs = refs[:PACKS], refs[PACKS:]
    ins_s, outs_s, (grad_sem, in_sem, out_sem) = refs[:count], refs[count : 2 * count], refs[2 * count :]
    kinds = range(0, count, SEVEN)
    layers = ins[0].shape[0]
    heads, half, whole, few = ins[0].shape[2], ins[4].shape[2] // 2, ins[3].shape[2], 16
    waits = []
    for i in range(layers):
        copies = [pltpu.make_async_copy(src.at[i], dst.at[i], grad_sem.at[g, i]) for g, (src, dst) in enumerate(zip(grads, grads_s, strict=True))]
        copies += [pltpu.make_async_copy(ins[a].at[i], ins_s[a].at[i], in_sem.at[a, i]) for w in range(SEVEN) for a in (w + kind for kind in kinds)]
        for copy in copies:
            copy.start()
        waits.append(copies)
    parts = (
        [(QKV_G, START, START, heads)], [(QKV_G, heads, START, HEAD)], [(QKV_G, heads + HEAD, START, HEAD)], [(WO_G, START, START, whole)],
        [(GA_G, START, START, half), (GB_G, START, half, half)], [(GA_G, half, START, half), (GB_G, half, half, half)], [(WD_G, START, START, whole)],
    )
    out = []
    for i in range(layers):
        for copy in waits[i][:PACKS]:
            copy.wait()
        for w in range(SEVEN):
            for copy in waits[i][PACKS + 3 * w : PACKS + 3 * (w + 1)]:
                copy.wait()

            def step(j, i=i, w=w):
                at = tile(j, few)
                for grad, first, start, wide in parts[w]:
                    here = slice(start, start + wide)
                    g = grads_s[grad][i, at, first : first + wide].astype(F32)
                    weight = ins_s[w][i, at, here].astype(F32)
                    of_m, of_v = w + SEVEN, w + 2 * SEVEN
                    m = 0.9 * ins_s[of_m][i, at, here] + 0.1 * g
                    v = 0.95 * ins_s[of_v][i, at, here] + 0.05 * g * g
                    outs_s[w][i, at, here] = (weight - 0.02 * (m * lax.rsqrt(v + 1e-8) + 0.1 * weight)).astype(BF16)
                    outs_s[of_m][i, at, here] = m
                    outs_s[of_v][i, at, here] = v

            loop(ins[w].shape[1] // few, step)
            for a in (w + kind for kind in kinds):
                out.append(pltpu.make_async_copy(outs_s[a].at[i], outs[a].at[i], out_sem.at[a, i]))
                out[-1].start()
    for copy in out:
        copy.wait()


def solution(mesh):
    n = mesh.shape["dp"]
    far_a, far_b = n // 2, n - 1 - n // 2

    def step(x, dy, *arrays):
        weights = arrays[:SEVEN]
        wq, wk, wv, wo, wg, wu, wd = weights
        layers, r, wide_q = wq.shape
        x, dy = x[0], dy[0]
        tokens, d = x.shape
        ff = wg.shape[2]
        bq, rows = (min(512, tokens),) * 2
        few = jnp.asarray(angles(tokens))
        wide = wide_q + 2 * HEAD
        heads = wide_q // HEAD
        ro = wo.shape[1]
        shapes = (r, wide), (r, 2 * ff), (ro + wd.shape[1], d)
        terms = (r, wide), (r, ff), (r, ff), (wd.shape[1], d), (ro, d)
        both = lambda *s: jax.ShapeDtypeStruct((layers, *s), BF16)
        some = lambda lead, s: pltpu.VMEM((*lead, *s), BF16)
        grads = pl.pallas_call(
            functools.partial(train, (layers, n, bq, rows, ro)),
            out_shape=[*(both(*s) for s in terms), both(tokens, wide_q), both(tokens, HEAD), both(tokens, HEAD), both(tokens, wide_q),
                       jax.ShapeDtypeStruct((layers, 8, tokens), F32), both(tokens, d), both(tokens, d),
                       jax.ShapeDtypeStruct((layers, n * shapes[2][0], d), BF16), jax.ShapeDtypeStruct((layers, n * r, 2 * ff), BF16)],
            in_specs=[ANY] * (3 + SEVEN),
            out_specs=[ANY] * (PACKS + len(KEPT)),
            scratch_shapes=[
                pltpu.VMEM(few.shape, F32), pltpu.VMEM((tokens, HEAD), F32), some((n,), shapes[0]), *(some((n * s[0],), s[1:]) for s in shapes[1:]),
                some((tokens,), (HEAD,)), some((tokens,), (HEAD,)), pltpu.VMEM((8, tokens), F32), *(some((tokens,), (d,)) for _ in terms[:3]),
                some((tokens,), (ff,)), some((tokens,), (2 * ff,)), some((d,), (tokens,)),
                pltpu.VMEM((tokens, d), F32), pltpu.VMEM((heads, HEAD + 8, bq), F32), pltpu.VMEM((heads, bq), F32), some((HEAD,), (tokens,)),
                *(some((lead,), s) for lead in (n, far_a, far_b, layers) for s in terms),
                pltpu.SemaphoreType.DMA((9 * layers,)), pltpu.SemaphoreType.DMA((2,)), pltpu.SemaphoreType.DMA((len(KEPT),)),
                pltpu.SemaphoreType.DMA((3 * layers, 4, far_a)), pltpu.SemaphoreType.DMA((3 * layers, n + 1)),
                pltpu.SemaphoreType.DMA((len(KEPT) + 1,)), pltpu.SemaphoreType.DMA((PACKS * layers,)),
                pltpu.SemaphoreType.DMA((PACKS, 4, far_a)), pltpu.SemaphoreType.REGULAR((PACKS,)),
            ],
            compiler_params=pltpu.CompilerParams(vmem_limit_bytes=VMEM, collective_id=0, has_side_effects=True),
            name="train",
        )(x, few, dy, *weights)[:PACKS]
        in_vmem = lambda a: pltpu.VMEM(a.shape, a.dtype)
        return pl.pallas_call(
            adamw,
            out_shape=[jax.ShapeDtypeStruct(a.shape, a.dtype) for a in arrays],
            in_specs=[ANY] * (PACKS + 3 * SEVEN),
            out_specs=[ANY] * (3 * SEVEN),
            scratch_shapes=[*map(in_vmem, grads), *map(in_vmem, arrays), *map(in_vmem, arrays),
                            pltpu.SemaphoreType.DMA((PACKS, layers)), *(pltpu.SemaphoreType.DMA((3 * SEVEN, layers)) for _ in arrays[:2])],
            compiler_params=pltpu.CompilerParams(vmem_limit_bytes=VMEM),
            name="adamw",
        )(*grads, *arrays)

    states, cut = P(("rep", "dp"), None, None), P(None, "dp", None)
    return jax.shard_map(
        step,
        mesh=mesh,
        in_specs=(states, states) + (cut,) * (3 * SEVEN),
        out_specs=(P("rep", "dp", None),) * (3 * SEVEN),
        check_vma=False,
    )
```

```python
import functools

import jax
import jax.numpy as jnp
import numpy as np
from jax import lax
from jax.experimental import pallas as pl
from jax.experimental.pallas import tpu as pltpu
from jax.sharding import PartitionSpec as P

HEAD = 128
THETA = 10000
NEG = -1e30
HIDDEN = 2 * NEG
LOG2E = 1.4426950408889634
SCALE = HEAD**-0.5
E = SCALE * LOG2E
VMEM = 66_000_000
STRETCH = 64
F32, BF16 = jnp.float32, jnp.bfloat16
ANY = pl.BlockSpec(memory_space=pl.ANY)
MESH = pl.DeviceIdType.MESH
A, B = range(2)
FEW = 16


def dot(a, b, ca=1, cb=0):
    return lax.dot_general(a, b, (((ca,), (cb,)), ((), ())), preferred_element_type=F32)


def scoped(name, what, *args):
    with jax.named_scope(name):
        return what(*args)


def tile(i, n):
    return pl.ds(pl.multiple_of(i * n, n), n)


def loop(n, body):
    lax.fori_loop(0, n, lambda i, _: body(i), None)


def polled(events, i, steps):
    for when, what in events.items():
        if when < steps:
            pl.when(i == when)(functools.partial(scoped, f"ev{when}", what))


def the_rest(events, steps):
    for when, what in events.items():
        if when >= steps:
            what()


def scale_of(wide):
    return lax.rsqrt(jnp.mean(wide * wide, -1, keepdims=True) + 1e-6)


def norm_bwd(wide, scale, g):
    return scale * g - wide * (scale * scale * scale * jnp.mean(wide * g, -1, keepdims=True))


def angles(tokens):
    half = HEAD // 2
    turn = float(THETA) ** (-np.arange(half) / half)
    place = np.arange(STRETCH)[:, None] * turn
    start = np.arange(0, tokens, STRETCH)[:, None] * turn
    cos, sin = np.cos(start), np.sin(start)
    return np.concatenate([np.concatenate(p, 1) for p in ((np.cos(place), np.sin(place)), (cos, cos), (-sin, sin))]).astype(np.float32)


def table_phase(few, table):
    starts = table.shape[0] // STRETCH

    def step(i):
        place = few[:STRETCH, :]
        row = lambda first: few[pl.ds(first + i, 1), :]
        table[tile(i, STRETCH), :] = place * row(STRETCH) + pltpu.roll(place, HEAD // 2, 1) * row(STRETCH + starts)

    loop(starts, step)


def turns(t):
    swapped = pltpu.roll(t, HEAD // 2, 1)
    first = lax.broadcasted_iota(jnp.int32, t.shape, 1) < HEAD // 2
    return jnp.where(first, t, swapped), jnp.where(first, -swapped, t)


def rotated(t, cos, sin):
    return t * cos + pltpu.roll(t, HEAD // 2, 1) * sin


class Ring:
    def __init__(self, n):
        self.n, self.far_a = n, n // 2
        self.far_b = n - 1 - self.far_a
        self.me = lax.axis_index("dp")
        rep = lax.axis_index("rep")
        self.core = lax.rem(rep, 2)
        self.partner = {"rep": rep + 1 - 2 * self.core}
        self.turn = 1 - 2 * self.core
        self.near = 1, -1, 2, -2

    def at(self, k):
        return lax.rem(self.me + self.n + k * self.turn, self.n)

    def to(self, k):
        return {"dp": self.at(k)}

    def meet(self):
        barrier = pltpu.get_barrier_semaphore()
        others = [self.to(k) for k in self.near] + [self.partner]
        for other in others:
            pl.semaphore_signal(barrier, inc=1, device_id=other, device_id_type=MESH)
        pl.semaphore_wait(barrier, len(others))


def remote(src, dst, send, recv, to):
    return pltpu.make_async_remote_copy(src_ref=src, dst_ref=dst, send_sem=send, recv_sem=recv, device_id=to, device_id_type=MESH)


class Chains:
    def far(self, chain):
        return self.ring.far_b if chain else self.ring.far_a

    def now(self, s):
        for count in range(1, s + 1):
            for chain in (A, B):
                if self.taken[chain] < min(count, self.far(chain)):
                    self.taken[chain] += 1
                    self.take(chain, self.taken[chain])

    def finish(self):
        self.now(self.ring.far_a)


class Blocks:
    def __init__(self, ref, rows):
        self.ref, self.rows = ref, rows

    def part(self, block, first, count, columns=slice(None)):
        if len(self.ref.shape) == 2:
            return self.ref.at[pl.ds(pl.multiple_of(block * self.rows + first, FEW), count), columns]
        return self.ref.at[block, pl.ds(pl.multiple_of(first, FEW), count), columns]

    def all(self, first, end, share=slice(None)):
        return jnp.concatenate([self.ref[at + first : at + end, :] for at in range(0, self.ref.shape[0], self.rows)[share]])


class Gather(Chains):
    def __init__(self, ring, blocks, sems, handed_sems):
        self.taken = [0, 0]
        self.ring, self.blocks, self.sems, self.handed_sems = ring, blocks, sems, handed_sems
        self.half = blocks.rows // 2
        self.last_handed = {}

    def piece(self, block, half):
        return self.blocks.part(block, half * self.half, self.half)

    def hop(self, chain, step):
        ring = self.ring
        along = 1 if chain == A else -1
        part = self.piece(ring.at(-along * step), ring.core)
        return remote(part, part, self.sems.at[2 * chain, step], self.sems.at[2 * chain + 1, step], ring.to(along))

    def handed(self, chain, step):
        ring = self.ring
        part = self.piece(ring.at(-step - 1 if chain == A else step + 1), ring.core)
        return remote(part, part, self.handed_sems.at[ring.n - 1 + chain], self.handed_sems.at[step + chain * ring.far_a], ring.partner)

    def begin(self):
        for chain in (A, B):
            self.hop(chain, 0).start()

    def take(self, chain, s):
        ring = self.ring
        part = self.piece(ring.at(-s if chain == A else s), ring.core)
        remote(part, part, self.sems.at[2 * chain, s - 1], self.sems.at[2 * chain + 1, s - 1], ring.to(1)).wait_recv()
        if s < self.far(chain):
            self.hop(chain, s).start()
        if chain in self.last_handed:
            self.handed(chain, self.last_handed[chain]).wait_send()
        self.last_handed[chain] = s - 1
        self.handed(chain, s - 1).start()

    def complete(self):
        ring = self.ring
        for chain in (A, B):
            for step in range(self.far(chain)):
                part = self.piece(ring.at(step + 1 if chain == A else -step - 1), 1 - ring.core)
                remote(part, part, self.handed_sems.at[ring.n - 1], self.handed_sems.at[step + chain * ring.far_a], ring.partner).wait_recv()

    def drain(self):
        for chain in (A, B):
            for step in range(self.far(chain)):
                self.hop(chain, step).wait_send()
        for chain, step in self.last_handed.items():
            self.handed(chain, step).wait_send()


class Scatter(Chains):
    def __init__(self, ring, p, came_a, came_b, sems, free, got, signal, taken=(0, 0)):
        self.signal = signal
        self.ring, self.p, self.came, self.sems, self.free, self.got = ring, p, (came_a, came_b), sems, free, got
        self.taken = list(taken)

    def hop(self, chain, step):
        ring = self.ring
        left = self.far(chain) - step
        block = ring.at(left if chain == 0 else -left)
        return remote(self.p.at[block], self.came[chain].at[step], self.sems.at[2 * chain, step], self.sems.at[2 * chain + 1, step],
                      ring.to(1 if chain == 0 else -1))

    def added(self, chain, step):
        ring = self.ring
        left = self.far(chain) - step
        block = ring.at(left if chain == 0 else -left)
        few = FEW

        def rows(i):
            at = tile(i, few)
            self.p[block, at, :] = (self.p[block, at, :].astype(F32) + self.came[chain][step - 1, at, :].astype(F32)).astype(BF16)

        loop(self.p.shape[1] // few, rows)

    def begin(self, wait):
        pl.when(wait)(lambda: pl.semaphore_wait(self.free, len(self.ring.near)))
        self.hop(A, 0).start()
        self.hop(B, 0).start()

    def take(self, chain, s):
        self.hop(chain, s - 1).wait_recv()
        if s < self.far(chain):
            self.added(chain, s)
            self.hop(chain, s).start()
        if self.taken == [self.far(A), self.far(B)]:
            self.end()

    def arrived(self):
        return [(chain, self.far(chain) - 1) for chain in (A, B)]

    def end(self):
        me, few = self.ring.me, FEW

        def rows(i):
            at = tile(i, few)
            total = self.p[me, at, :].astype(F32)
            for chain, slot in self.arrived():
                total += self.came[chain][slot, at, :].astype(F32)
            self.got[at, :] = total.astype(BF16)

        loop(self.p.shape[1] // few, rows)
        for chain in (A, B):
            for step in range(self.far(chain)):
                self.hop(chain, step).wait_send()

        @pl.when(self.signal)
        def _():
            for k in self.ring.near:
                pl.semaphore_signal(self.free, inc=1, device_id=self.ring.to(k), device_id_type=MESH)


class QuickScatter(Scatter):
    def hop(self, chain, step):
        ring = self.ring
        kind = step + self.far(A) - self.far(chain)
        block, reach = ((4, 2), (3, 1), (1, 1), (2, 2))[kind]
        along = 1 if chain == A else -1
        return remote(self.p.at[ring.at(along * block)], self.came[chain].at[step], self.sems.at[2 * chain, step], self.sems.at[2 * chain + 1, step],
                      ring.to(along * reach))

    def begin(self, wait):
        pl.when(wait)(lambda: pl.semaphore_wait(self.free, len(self.ring.near)))
        for step in range(self.far(A) - 1):
            for chain in (A, B):
                if step < self.far(chain) - 1:
                    self.hop(chain, step).start()

    def take(self, chain, s):
        self.hop(chain, s - 1).wait_recv()
        beyond = self.far(chain) - 2
        if s == beyond:
            block, few = self.ring.at(2 if chain == A else -2), FEW

            def rows(i):
                at = tile(i, few)
                total = self.p[block, at, :].astype(F32)
                for slot in range(beyond):
                    total += self.came[chain][slot, at, :].astype(F32)
                self.p[block, at, :] = total.astype(BF16)

            loop(self.p.shape[1] // few, rows)
            self.hop(chain, self.far(chain) - 1).start()
        if self.taken == [self.far(A), self.far(B)]:
            self.end()

    def arrived(self):
        return [(chain, self.far(chain) - back) for chain in (A, B) for back in (1, 2)]


def merged(w):
    return w.reshape(w.shape[0] * w.shape[1], w.shape[2])


def qkv_phase(h, w, table, q, k, v, vt, rows, events):
    wide_q = q.shape[1]

    def step(i):
        at = tile(i, rows)
        wide = h[at, :].astype(F32)
        a = (wide * scale_of(wide)).astype(BF16)
        y = dot(a, merged(w[...])).astype(BF16)
        cos, sin = turns(table[at, :])
        for n in range(wide_q // HEAD):
            part = slice(n * HEAD, (n + 1) * HEAD)
            q[at, part] = rotated(y[:, part].astype(F32), cos, sin).astype(BF16)
        k[at, :] = rotated(y[:, wide_q : wide_q + HEAD].astype(F32), cos, sin).astype(BF16)
        mine = y[:, wide_q + HEAD :]
        v[at, :] = mine
        vt[:, at] = mine.T
        polled(events, i, h.shape[0] // rows)

    loop(h.shape[0] // rows, step)
    the_rest(events, h.shape[0] // rows)


def spans(bq):
    half = bq // 2
    return [(0, half, 0), (half, half, half)]


def seen(keys, first_key, queries, first_query):
    key = lax.broadcasted_iota(jnp.int32, (keys, queries), 0) + first_key
    return lax.broadcasted_iota(jnp.int32, (keys, queries), 1) + first_query >= key


def blocks(tokens, bq):
    return (tokens // bq) * (tokens // bq + 1) // 2


def row_of_blocks(iq, bq, block, events, steps):
    def step(j):
        @pl.when(j < iq)
        def _():
            block(pl.multiple_of(j * bq, bq), bq, 0, None)

        @pl.when(j == iq)
        def _():
            for first, nk, lo in spans(bq):
                block(pl.multiple_of(iq * bq + first, nk), nk, lo, seen(nk, first, bq - lo, lo))

        polled(events, lax.div(iq * (iq + 1), 2) + j, steps)

    loop(iq + 1, step)


def attend_phase(q, k, vt, o, lse, top_s, mix_s, bq, events):
    heads = q.shape[1] // HEAD

    def block(iq, start, nk, lo, mask):
        here = pl.ds(start, nk)
        cols = pl.ds(pl.multiple_of(iq * bq + lo, bq - lo), bq - lo)
        keys = k[here, :]
        scores = [dot(keys, q[cols, n * HEAD : (n + 1) * HEAD], 1, 1) for n in range(heads)]
        values = jnp.concatenate([vt[:, here], jnp.ones((8, nk), BF16)], axis=0)
        for n, s in enumerate(scores):
            if mask is not None:
                s = jnp.where(mask, s, HIDDEN)
            old = top_s[n : n + 1, lo:]
            top = jnp.maximum(old, s.max(axis=0, keepdims=True))
            top_s[n : n + 1, lo:] = top
            p = jnp.exp2((s - top) * E).astype(BF16)
            mix_s[n, :, lo:] = mix_s[n, :, lo:] * jnp.exp2((old - top) * E) + dot(values, p)

    def step(iq):
        at = tile(iq, bq)
        top_s[...] = jnp.full(top_s.shape, NEG, F32)
        mix_s[...] = jnp.zeros(mix_s.shape, F32)
        row_of_blocks(iq, bq, functools.partial(block, iq), events, blocks(q.shape[0], bq))
        for n in range(heads):
            total = mix_s[n, HEAD : HEAD + 1, :]
            o[at, n * HEAD : (n + 1) * HEAD] = (mix_s[n, :HEAD, :] * (1 / total)).T.astype(BF16)
            lse[n : n + 1, at] = top_s[n : n + 1, :] * E + jnp.log2(total)

    loop(q.shape[0] // bq, step)
    the_rest(events, blocks(q.shape[0], bq))


def mid_phase(h, o, od, hm, rows, r):
    def step(i):
        at = tile(i, rows)
        hm[at, :] = h[at, :] + dot(o[at, :], od.all(0, r)).astype(BF16)

    loop(h.shape[0] // rows, step)


def ffn_phase(hm, gu, od, out, rows, r, events):
    def step(i):
        at = tile(i, rows)
        mid = hm[at, :]
        wide = mid.astype(F32)
        b = (wide * scale_of(wide)).astype(BF16)
        y = dot(b, gu.ref[...])
        part = y.shape[1] // 4
        pieces = []
        for n in (0, 2 * part):
            gate, up = y[:, n : n + part], y[:, n + part : n + 2 * part]
            pieces.append((gate * (1 / (1 + jnp.exp(-gate))) * up).astype(BF16))
        made = jnp.concatenate(pieces, axis=1)
        out[at, :] = mid + dot(made, od.all(r, od.rows)).astype(BF16)
        polled(events, i, hm.shape[0] // rows)

    loop(hm.shape[0] // rows, step)
    the_rest(events, hm.shape[0] // rows)


def ffn_bwd_phase(half, hm, dy, gu, od, made_s, dgu_s, bt_s, db_s, dhm, rows, r, events):
    part = dgu_s.shape[1] // 4
    lanes, units = slice(2 * part * half, 2 * part * (half + 1)), slice(part * half, part * (half + 1))
    some = od.ref.shape[0] // od.rows // 2
    share = slice(some * half, some * (half + 1))

    def step(i):
        at = tile(i, rows)
        wide = hm[at, :].astype(F32)
        scale = scale_of(wide)
        b = (wide * scale).astype(BF16)
        if half == 0:
            bt_s[:, at] = b.T
        y = dot(b, gu[:, lanes])
        gate, up = y[:, :part], y[:, part:]
        back = dy[at, :]
        d_made = dot(back, od.all(r, od.rows, share), 1, 1).astype(BF16).astype(F32)
        sig = 1 / (1 + jnp.exp(-gate))
        silu = gate * sig
        made_s[at, units] = (silu * up).astype(BF16)
        d_gate = (d_made * up * (sig * (1 + gate - silu))).astype(BF16)
        d_up = (d_made * silu).astype(BF16)
        both = jnp.concatenate([d_gate, d_up], axis=1)
        dgu_s[at, lanes] = both
        db = dot(both, gu[:, lanes], 1, 1)
        if half == 0:
            db_s[at, :] = db
        else:
            db = (db_s[at, :] + db).astype(BF16).astype(F32)
            dhm[at, :] = (back.astype(F32) + norm_bwd(wide, scale, db)).astype(BF16)
        polled(events, i, hm.shape[0] // rows)

    loop(hm.shape[0] // rows, step)
    the_rest(events, hm.shape[0] // rows)


def units_phase(half, dgu_s, bt_s, p):
    n, _, columns = p.shape
    wide = next(w for w in (512, 256, 128) if columns % w == 0)

    def units(i):
        here = pl.ds(pl.multiple_of(columns * half + i * wide, wide), wide)
        p[:, :, tile(i, wide)] = dot(bt_s[...], dgu_s[:, here]).astype(BF16).reshape(n, -1, wide)

    loop(columns // wide, units)


def downs_phase(made_s, dy, p):
    n, share, group = p.shape[0], p.shape[1], 2

    def downs(i):
        got = dot(made_s[:, tile(i, group * share)], dy[...], 0, 0).astype(BF16)
        p[pl.ds(i * group, group)] = got.reshape(group, share, -1)

    loop(n // group, downs)


def out_bwd_phase(dhm, o, od, p, do, rows, r):
    def step(i):
        at = tile(i, rows)
        do[at, :] = dot(dhm[at, :], od.all(0, r), 1, 1).astype(BF16)

    loop(dhm.shape[0] // rows, step)
    p[...] = dot(o[...], dhm[...], 0, 0).astype(BF16).reshape(p.shape)


def attend_bwd_phase(q, k, v, o, do, lse, table, dqkv, dq_s, dk_s, dv_s, kt_s, bq, events):
    heads = q.shape[1] // HEAD
    wide_q = q.shape[1]
    dk_s[...] = jnp.zeros(dk_s.shape, F32)
    dv_s[...] = jnp.zeros(dv_s.shape, F32)
    kt_s[...] = k[...].T

    def block(iq, lses, deltas, start, nk, lo, mask):
        here = pl.ds(start, nk)
        cols = pl.ds(pl.multiple_of(iq * bq + lo, bq - lo), bq - lo)
        keys, values, keys_t = k[here, :], v[here, :], kt_s[:, here]
        for pair in range(0, heads, 2):
            some = range(pair, min(pair + 2, heads))
            qs = [q[cols, n * HEAD : (n + 1) * HEAD] for n in some]
            dos = [do[cols, n * HEAD : (n + 1) * HEAD] for n in some]
            products = [(dot(keys, x, 1, 1), dot(values, y, 1, 1)) for x, y in zip(qs, dos)]
            for n, x, y, (score, dp) in zip(some, qs, dos, products):
                p = jnp.exp2(score * E - lses[n][:, lo:])
                if mask is not None:
                    p = jnp.where(mask, p, 0.0)
                ds = (p * (dp - deltas[n][:, lo:])).astype(BF16)
                dv_s[here, :] += dot(p.astype(BF16), y)
                dk_s[here, :] += dot(ds, x)
                dq_s[n, :, lo:] += dot(keys_t, ds)

    def step(iq):
        at = tile(iq, bq)
        dq_s[...] = jnp.zeros(dq_s.shape, F32)
        lses = [lse[n : n + 1, at] for n in range(heads)]
        deltas = []
        for n in range(heads):
            part = slice(n * HEAD, (n + 1) * HEAD)
            deltas.append((do[at, part].astype(F32) * o[at, part].astype(F32)).T.sum(axis=0, keepdims=True))
        row_of_blocks(iq, bq, functools.partial(block, iq, lses, deltas), events, blocks(q.shape[0], bq))
        cos, sin = turns(table[at, :])
        for n in range(heads):
            back = (dq_s[n] * SCALE).T.astype(BF16).astype(F32)
            dqkv[at, n * HEAD : (n + 1) * HEAD] = rotated(back, cos, -sin).astype(BF16)

    loop(q.shape[0] // bq, step)
    the_rest(events, blocks(q.shape[0], bq))

    def finish(i):
        at = tile(i, bq)
        cos, sin = turns(table[at, :])
        dqkv[at, wide_q : wide_q + HEAD] = rotated((dk_s[at, :] * SCALE).astype(BF16).astype(F32), cos, -sin).astype(BF16)
        dqkv[at, wide_q + HEAD :] = dv_s[at, :].astype(BF16)

    loop(q.shape[0] // bq, finish)


def qkv_bwd_phase(h, dqkv, w, dhm, p_qkv, a_s, dh, rows, further):
    def step(i):
        at = tile(i, rows)
        wide = h[at, :].astype(F32)
        scale = scale_of(wide)
        a_s[at, :] = (wide * scale).astype(BF16)

        @pl.when(further)
        def _():
            da = dot(dqkv[at, :], merged(w[...]), 1, 1).astype(BF16).astype(F32)
            dh[at, :] = (dhm[at, :].astype(F32) + norm_bwd(wide, scale, da)).astype(BF16)

    loop(h.shape[0] // rows, step)
    p_qkv[...] = dot(a_s[...], dqkv[...], 0, 0).astype(BF16).reshape(p_qkv.shape)


SEVEN = 7
START = 0
QKV, OD, GU = range(3)
OWN, OLD = range(2)
NEXT = OLD
PLAN = {
    "qkv": ((0, OD, OWN, 2), (0, QKV, NEXT, 0), (3, GU, OWN, 2), (3, OD, NEXT, 0)),
    "attend": ((2, OD, OWN, 3), (2, QKV, NEXT, 1), (5, GU, OWN, 3), (7, OD, NEXT, 1), (7, GU, NEXT, 0), (8, OD, OWN, 4), (8, QKV, NEXT, 2), (9, GU, OWN, 4)),
    "ffn": ((0, OD, NEXT, 2), (1, QKV, NEXT, 3), (1, GU, NEXT, 1), (3, QKV, NEXT, 4), (3, OD, NEXT, 3)),
}
LAST_PLAN = {"qkv": ((2, GU, OWN, 2),), "attend": ((0, OD, OWN, 4), (4, GU, OWN, 3), (8, GU, OWN, 4))}
HEAD_PLAN = ((QKV, 1), (GU, 0), (QKV, 2), (OD, 1), (QKV, 3), (GU, 1), (QKV, 4))


def planned(act, entries):
    by_step = {}
    for when, *what in entries:
        by_step.setdefault(when, []).append(what)
    return {when: functools.partial(act, whats) for when, whats in by_step.items()}


def forward(ring, sizes, x, few, weights, spaces, h_s, few_s, table_s, packs_s, q_s, k_s, v_s, vt_s, o_s, lse_s, hm_s, top_s, mix_s,
            own_sem, in_sem, out_sem, gather_sems, handed_sems):
    layers, bq, rows = sizes
    me = ring.me
    wq, wk, wv, wo, wg, wu, wd = weights
    wide_q, r, ro, rd = wq.shape[2], wq.shape[1], wo.shape[1], wd.shape[1]
    half = wg.shape[2] // 2
    own = {}

    def fetch(i, group, pieces):
        for src, first, count, start, wide in pieces:
            copy = pltpu.make_async_copy(src, packs_s[i][group].part(me, first, count, slice(start, start + wide)), own_sem.at[sum(map(len, own.values()))])
            own.setdefault((i, group), []).append(copy)
            copy.start()

    for i in range(layers):
        fetch(i, QKV, [(wq.at[i], 0, r, 0, wide_q), (wk.at[i], 0, r, wide_q, HEAD), (wv.at[i], 0, r, wide_q + HEAD, HEAD)])
        fetch(i, OD, [(wo.at[i], 0, ro, 0, wo.shape[2]), (wd.at[i], ro, rd, 0, wd.shape[2])])
        if i == 0:
            brought = [pltpu.make_async_copy(x, h_s, in_sem.at[0]), pltpu.make_async_copy(few, few_s, in_sem.at[1])]
            for copy in brought:
                copy.start()
        fetch(i, GU, [(w.at[i, :, half * j : half * (j + 1)], 0, r, half * (2 * j + k), half) for j in (0, 1) for k, w in enumerate((wg, wu))])
    packs = {(g, i): Gather(ring, packs_s[i][g], gather_sems.at[3 * i + g], handed_sems.at[3 * i + g]) for g in (QKV, OD, GU) for i in range(layers)}
    begun = set()
    kept = {}

    def keep(name, src, i):
        kept[name] = pltpu.make_async_copy(src, spaces[name].at[i], out_sem.at[KEPT.index(name)])
        kept[name].start()

    def reuse(*names):
        for name in names:
            if name in kept:
                kept.pop(name).wait()

    def begin(group, i):
        if (group, i) not in begun:
            begun.add((group, i))
            for copy in own[i, group]:
                copy.wait()
            packs[group, i].begin()

    def act(i, whats):
        for group, which, stop in whats:
            if i + which < layers:
                begin(group, i + which)
                packs[group, i + which].now(stop)

    def plan(phase, i):
        return planned(functools.partial(act, i), (PLAN if i + 1 < layers else LAST_PLAN).get(phase, ()))

    def whole(group, i):
        begin(group, i)
        packs[group, i].finish()
        packs[group, i].complete()

    scoped('meet', ring.meet)
    begin(QKV, 0)
    begin(OD, 0)
    for copy in brought:
        copy.wait()
    table_phase(few_s, table_s)
    for group, stop in HEAD_PLAN:
        scoped(f'head{group}_{stop}', act, 0, [(group, OWN, stop)])
    for i in range(layers):
        qkv, od, gu = packs_s[i]
        last = i + 1 == layers
        keep("h", h_s, i)
        scoped('whole_QKV', whole, QKV, i)
        reuse("q", "k", "v")
        scoped('qkv_phase', qkv_phase, h_s, qkv.ref, table_s, q_s, k_s, v_s, vt_s, rows, plan("qkv", i))
        keep("q", q_s, i)
        keep("k", k_s, i)
        keep("v", v_s, i)
        reuse("o", "lse")
        scoped('attend_phase', attend_phase, q_s, k_s, vt_s, o_s, lse_s, top_s, mix_s, bq, plan("attend", i))
        keep("o", o_s, i)
        keep("lse", lse_s, i)
        scoped('whole_OD', whole, OD, i)
        if last:
            scoped('whole_GU', whole, GU, i)
        else:
            keep("od", od.ref, i)
        reuse("hm")
        scoped('mid_phase', mid_phase, h_s, o_s, od, hm_s, rows, ro)
        if not last:
            keep("hm", hm_s, i)
            scoped('whole_GU', whole, GU, i)
            keep("gu", gu.ref, i)
            reuse("h")
            scoped('ffn_phase', ffn_phase, hm_s, gu, od, h_s, rows, ro, plan("ffn", i))
    with jax.named_scope('flush'):
        reuse(*KEPT)
        for pack in packs.values():
            pack.drain()


KEPT = ("q", "k", "v", "o", "lse", "hm", "h", "od", "gu")
PACKS = 5
QKV_G, GA_G, GB_G, WD_G, WO_G = range(PACKS)
BACK = {
    "first": ((2, QKV_G, OLD, 2), (3, WD_G, OLD, 4), (3, WO_G, OLD, 4)),
    "second": ((0, QKV_G, OLD, 4), (2, GA_G, OWN, 1)),
    "downs": ((0, GA_G, OWN, 2),),
    "attend": ((0, GB_G, OWN, 1), (1, WD_G, OWN, 1), (2, GA_G, OWN, 3), (3, WO_G, OWN, 1), (4, GB_G, OWN, 2), (6, WD_G, OWN, 2), (7, GA_G, OWN, 4), (8, WO_G, OWN, 2),
               (9, GB_G, OWN, 3)),
    "late": ((0, WD_G, OWN, 3), (0, WO_G, OWN, 3)),
    "end": ((0, GB_G, OWN, 4),),
}
TAIL = ((GA_G, 4), (GB_G, 4), (QKV_G, 2), (WD_G, 4), (WO_G, 4))


def train(sizes, x, few, dy, *refs):
    layers, n, bq, rows, r = sizes
    weights, refs = refs[:SEVEN], refs[SEVEN:]
    results, refs = refs[:PACKS], refs[PACKS:]
    spaces, refs = dict(zip(KEPT, refs)), refs[len(KEPT) :]
    few_s, table_s, qkv_s, gu_s, od_s, k_s, v_s, lse_s, hm_s, dh_s, dhm_s, made_s, dgu_s, bt_s, db_s, mix_s, top_s, kt_s = refs[:18]
    refs = refs[18:]
    terms, came_a, came_b, got = (refs[PACKS * i : PACKS * (i + 1)] for i in range(4))
    forward_sems, (in_sem, result_sem, scatter_sems, free_sems) = refs[PACKS * 4 : -4], refs[-4:]
    ring = Ring(n)
    split, heads = qkv_s.shape[2], spaces["q"].shape[2]
    d = dh_s.shape[1]
    depth = qkv_s.shape[1]
    early = Blocks(terms[QKV_G], depth), Blocks(made_s.at[:, :d], od_s.shape[0] // n), Blocks(dgu_s.at[: n * depth, :], depth)
    late = Blocks(qkv_s, depth), Blocks(od_s, od_s.shape[0] // n), Blocks(gu_s, depth)
    od = late[OD]
    dq_s = mix_s.at[:, :HEAD, :]
    dqkv_s, do_s = made_s.at[:, :split], made_s.at[:, split : split + heads]
    dk_s, dv_s = db_s.at[:, :HEAD], db_s.at[:, HEAD : 2 * HEAD]
    q_s, o_s, h_s = dgu_s.at[:, :heads], dgu_s.at[:, heads : 2 * heads], dgu_s.at[:, 2 * heads : 2 * heads + d]
    places = {"gu": gu_s, "hm": hm_s, "od": od_s, "q": q_s, "k": k_s, "v": v_s, "o": o_s, "lse": lse_s, "h": h_s}

    def copy_of(name, i):
        return pltpu.make_async_copy(spaces[name].at[i], places[name], in_sem.at[KEPT.index(name)])

    def bring(names, i):
        for name in names:
            copy_of(name, i).start()

    def need(names, i):
        for name in names:
            copy_of(name, i).wait()

    back = pltpu.make_async_copy(dy, dh_s, in_sem.at[len(KEPT)])
    back.start()
    forward(ring, (layers, bq, rows), x, few, weights, spaces, made_s.at[:, d : 2 * d], few_s, table_s, [early] * (layers - 1) + [late], dhm_s, k_s, v_s, bt_s.at[:HEAD, :],
            made_s.at[:, 2 * d : 2 * d + heads], lse_s, hm_s, top_s, mix_s, *forward_sems)
    back.wait()
    last = layers - 1

    def pack(group, i, signal, taken=(0, 0)):
        return (QuickScatter if group == QKV_G else Scatter)(ring, terms[group], came_a[group], came_b[group], scatter_sems.at[group], free_sems.at[group], got[group].at[i], signal, taken)

    reached = {}
    for entries in BACK.values():
        for _, group, old, stop in entries:
            if old == OWN:
                reached[group] = max(stop, reached.get(group, 0))
    taken = {group: (min(stop, ring.far_a), min(stop, ring.far_b)) for group, stop in reached.items()}

    def layer(step):
        i = last - step
        later = step > 0
        own = {group: pack(group, i, i > 0) for group in range(PACKS)}
        old = {group: pack(group, i + 1, i >= 0, taken.get(group, (0, 0))) for group in range(PACKS)}

        def act(whats):
            for group, which, stop in whats:
                if which == OWN:
                    own[group].now(stop)
                else:
                    pl.when(later)(functools.partial(old[group].now, stop))

        def plan(phase):
            return planned(act, BACK[phase])

        def before(group):
            pl.when(later)(old[group].finish)

        pl.when(later)(functools.partial(need, ("gu", "hm", "od"), i))
        for half, group, phase in ((0, GA_G, "first"), (1, GB_G, "second")):
            scoped('ffn_bwd', ffn_bwd_phase, half, hm_s, dh_s, gu_s, od, made_s, dgu_s, bt_s, db_s, dhm_s, rows, r, plan(phase))
            if half == 1:
                pl.when(i > 0)(functools.partial(bring, ("gu", "hm"), i - 1))
            before(group)
            scoped('units', units_phase, half, dgu_s, bt_s, terms[group])
            scoped('begin', own[group].begin, later)
        bring(("o", "q", "k", "v", "lse", "h"), i)
        before(WD_G)
        scoped('downs', downs_phase, made_s, dh_s, terms[WD_G])
        own[WD_G].begin(later)
        scoped('downs_ev', the_rest, plan("downs"), 0)
        need(("o",), i)
        before(WO_G)
        scoped('out_bwd', out_bwd_phase, dhm_s, o_s, od, terms[WO_G], do_s, rows, r)
        own[WO_G].begin(later)
        pl.when(i > 0)(functools.partial(bring, ("od",), i - 1))
        need(("q", "k", "v", "lse"), i)
        scoped('attend_bwd', attend_bwd_phase, q_s, k_s, v_s, o_s, do_s, lse_s, table_s, dqkv_s, dq_s, dk_s, dv_s, kt_s, bq, plan("attend"))
        scoped('late_ev', the_rest, plan("late"), 0)
        need(("h",), i)
        before(QKV_G)
        scoped('qkv_bwd', qkv_bwd_phase, h_s, dqkv_s, qkv_s, dhm_s, terms[QKV_G], do_s, dh_s, rows, i > 0)
        own[QKV_G].begin(later)
        scoped('end_ev', the_rest, plan("end"), 0)

    loop(layers, layer)
    final = {group: pack(group, 0, False, taken.get(group, (0, 0))) for group in range(PACKS)}
    out = []

    def leave(group, i):
        out.append(pltpu.make_async_copy(got[group].at[i], results[group].at[i], result_sem.at[group, i]))
        out[-1].start()

    for i in range(1, layers):
        for group in range(PACKS):
            leave(group, i)
    for group, stop in TAIL:
        scoped(f'tail{group}_{stop}', final[group].now, stop)
        if group != QKV_G:
            final[group].finish()
            leave(group, 0)
    scoped('tail0_4', final[QKV_G].finish)
    leave(QKV_G, 0)
    for copy in out:
        copy.wait()


def adamw(*refs):
    count = 3 * SEVEN
    grads, refs = refs[:PACKS], refs[PACKS:]
    ins, outs, refs = refs[:count], refs[count : 2 * count], refs[2 * count :]
    grads_s, refs = refs[:PACKS], refs[PACKS:]
    ins_s, outs_s, (grad_sem, in_sem, out_sem) = refs[:count], refs[count : 2 * count], refs[2 * count :]
    kinds = range(0, count, SEVEN)
    layers = ins[0].shape[0]
    heads, half, whole, few = ins[0].shape[2], ins[4].shape[2] // 2, ins[3].shape[2], FEW
    first = [pltpu.make_async_copy(src.at[i], dst.at[i], grad_sem.at[g, i]) for i in range(layers) for g, (src, dst) in enumerate(zip(grads, grads_s, strict=True))]
    order = [(i, w) for i in range(layers) for w in sorted(range(SEVEN), key=lambda w: -ins[w].shape[1] * ins[w].shape[2])]
    loads = [[pltpu.make_async_copy(ins[w + kind].at[i], ins_s[w + kind].at[i], in_sem.at[w + kind, i]) for kind in kinds] for i, w in order]

    def load(at):
        for copy in loads[at] if at < len(order) else ():
            copy.start()

    for copy in first[:PACKS]:
        copy.start()
    ahead = 4
    for at in range(ahead):
        load(at)
    for copy in first[PACKS:]:
        copy.start()
    parts = (
        [(QKV_G, START, START, heads)], [(QKV_G, heads, START, HEAD)], [(QKV_G, heads + HEAD, START, HEAD)], [(WO_G, START, START, whole)],
        [(GA_G, START, START, half), (GB_G, START, half, half)], [(GA_G, half, START, half), (GB_G, half, half, half)], [(WD_G, START, START, whole)],
    )
    out = []
    for at_now, (i, w) in enumerate(order):
        if at_now % SEVEN == 0:
            for copy in first[PACKS * i : PACKS * (i + 1)]:
                copy.wait()
        for copy in loads[at_now]:
            copy.wait()
        load(at_now + ahead)

        def step(j, i=i, w=w):
            at = tile(j, few)
            for grad, first, start, wide in parts[w]:
                here = slice(start, start + wide)
                g = grads_s[grad][i, at, first : first + wide].astype(F32)
                weight = ins_s[w][i, at, here].astype(F32)
                of_m, of_v = w + SEVEN, w + 2 * SEVEN
                m = 0.9 * ins_s[of_m][i, at, here] + 0.1 * g
                v = 0.95 * ins_s[of_v][i, at, here] + 0.05 * g * g
                outs_s[w][i, at, here] = (weight - 0.02 * (m * lax.rsqrt(v + 1e-8) + 0.1 * weight)).astype(BF16)
                outs_s[of_m][i, at, here] = m
                outs_s[of_v][i, at, here] = v

        loop(ins[w].shape[1] // few, step)
        for a in (w + kind for kind in kinds):
            out.append(pltpu.make_async_copy(outs_s[a].at[i], outs[a].at[i], out_sem.at[a, i]))
            out[-1].start()
    for copy in out:
        copy.wait()


def solution(mesh):
    n = mesh.shape["dp"]
    far_a, far_b = n // 2, n - 1 - n // 2

    def step(x, dy, *arrays):
        weights = arrays[:SEVEN]
        wq, wk, wv, wo, wg, wu, wd = weights
        layers, r, wide_q = wq.shape
        x, dy = x[0], dy[0]
        tokens, d = x.shape
        ff = wg.shape[2]
        bq, rows = (min(512, tokens),) * 2
        few = jnp.asarray(angles(tokens))
        wide = wide_q + 2 * HEAD
        heads = wide_q // HEAD
        ro = wo.shape[1]
        shapes = (r, wide), (r, 2 * ff), (ro + wd.shape[1], d)
        terms = (r, wide), (r, ff), (r, ff), (wd.shape[1], d), (ro, d)
        both = lambda *s: jax.ShapeDtypeStruct((layers, *s), BF16)
        some = lambda lead, s: pltpu.VMEM((*lead, *s), BF16)
        grads = pl.pallas_call(
            functools.partial(train, (layers, n, bq, rows, ro)),
            out_shape=[*(both(*s) for s in terms), both(tokens, wide_q), both(tokens, HEAD), both(tokens, HEAD), both(tokens, wide_q),
                       jax.ShapeDtypeStruct((layers, 8, tokens), F32), both(tokens, d), both(tokens, d),
                       jax.ShapeDtypeStruct((layers, n * shapes[2][0], d), BF16), jax.ShapeDtypeStruct((layers, n * r, 2 * ff), BF16)],
            in_specs=[ANY] * (3 + SEVEN),
            out_specs=[ANY] * (PACKS + len(KEPT)),
            scratch_shapes=[
                pltpu.VMEM(few.shape, F32), pltpu.VMEM((tokens, HEAD), F32), some((n,), shapes[0]), *(some((n * s[0],), s[1:]) for s in shapes[1:]),
                some((tokens,), (HEAD,)), some((tokens,), (HEAD,)), pltpu.VMEM((8, tokens), F32), *(some((tokens,), (d,)) for _ in terms[:3]),
                some((tokens,), (ff,)), some((tokens,), (2 * ff,)), some((d,), (tokens,)),
                pltpu.VMEM((tokens, d), F32), pltpu.VMEM((heads, HEAD + 8, bq), F32), pltpu.VMEM((heads, bq), F32), some((HEAD,), (tokens,)),
                *(some((lead,), s) for lead in (n, far_a, far_b, layers) for s in terms),
                pltpu.SemaphoreType.DMA((9 * layers,)), pltpu.SemaphoreType.DMA((2,)), pltpu.SemaphoreType.DMA((len(KEPT),)),
                pltpu.SemaphoreType.DMA((3 * layers, 4, far_a)), pltpu.SemaphoreType.DMA((3 * layers, n + 1)),
                pltpu.SemaphoreType.DMA((len(KEPT) + 1,)), pltpu.SemaphoreType.DMA((PACKS, layers)),
                pltpu.SemaphoreType.DMA((PACKS, 4, far_a)), pltpu.SemaphoreType.REGULAR((PACKS,)),
            ],
            compiler_params=pltpu.CompilerParams(vmem_limit_bytes=VMEM, collective_id=0, has_side_effects=True),
            name="train",
        )(x, few, dy, *weights)[:PACKS]
        in_vmem = lambda a: pltpu.VMEM(a.shape, a.dtype)
        return pl.pallas_call(
            adamw,
            out_shape=[jax.ShapeDtypeStruct(a.shape, a.dtype) for a in arrays],
            in_specs=[ANY] * (PACKS + 3 * SEVEN),
            out_specs=[ANY] * (3 * SEVEN),
            scratch_shapes=[*map(in_vmem, grads), *map(in_vmem, arrays), *map(in_vmem, arrays),
                            pltpu.SemaphoreType.DMA((PACKS, layers)), *(pltpu.SemaphoreType.DMA((3 * SEVEN, layers)) for _ in arrays[:2])],
            compiler_params=pltpu.CompilerParams(vmem_limit_bytes=VMEM),
            name="adamw",
        )(*grads, *arrays)

    states, cut = P(("rep", "dp"), None, None), P(None, "dp", None)
    return jax.shard_map(
        step,
        mesh=mesh,
        in_specs=(states, states) + (cut,) * (3 * SEVEN),
        out_specs=(P("rep", "dp", None),) * (3 * SEVEN),
        check_vma=False,
    )
```

```python
import functools

import jax
import jax.numpy as jnp
import numpy as np
from jax import lax
from jax.experimental import pallas as pl
from jax.experimental.pallas import tpu as pltpu
from jax.sharding import PartitionSpec as P

HEAD = 128
THETA = 10000
NEG = -1e30
HIDDEN = 2 * NEG
LOG2E = 1.4426950408889634
SCALE = HEAD**-0.5
E = SCALE * LOG2E
VMEM = 66_000_000
STRETCH = 64
F32, BF16 = jnp.float32, jnp.bfloat16
ANY = pl.BlockSpec(memory_space=pl.ANY)
MESH = pl.DeviceIdType.MESH
A, B = range(2)
FEW = 16


def dot(a, b, ca=1, cb=0):
    return lax.dot_general(a, b, (((ca,), (cb,)), ((), ())), preferred_element_type=F32)


def scoped(name, what, *args):
    with jax.named_scope(name):
        return what(*args)


def tile(i, n):
    return pl.ds(pl.multiple_of(i * n, n), n)


def loop(n, body):
    lax.fori_loop(0, n, lambda i, _: body(i), None)


def polled(events, i, steps):
    for when, what in events.items():
        if when < steps:
            pl.when(i == when)(functools.partial(scoped, f"ev{when}", what))


def the_rest(events, steps):
    for when, what in events.items():
        if when >= steps:
            what()


def scale_of(wide):
    return lax.rsqrt(jnp.mean(wide * wide, -1, keepdims=True) + 1e-6)


def norm_bwd(wide, scale, g):
    return scale * g - wide * (scale * scale * scale * jnp.mean(wide * g, -1, keepdims=True))


def angles(tokens):
    half = HEAD // 2
    turn = float(THETA) ** (-np.arange(half) / half)
    place = np.arange(STRETCH)[:, None] * turn
    start = np.arange(0, tokens, STRETCH)[:, None] * turn
    cos, sin = np.cos(start), np.sin(start)
    return np.concatenate([np.concatenate(p, 1) for p in ((np.cos(place), np.sin(place)), (cos, cos), (-sin, sin))]).astype(np.float32)


def table_phase(few, table):
    starts = table.shape[0] // STRETCH

    def step(i):
        place = few[:STRETCH, :]
        row = lambda first: few[pl.ds(first + i, 1), :]
        table[tile(i, STRETCH), :] = place * row(STRETCH) + pltpu.roll(place, HEAD // 2, 1) * row(STRETCH + starts)

    loop(starts, step)


def turns(t):
    swapped = pltpu.roll(t, HEAD // 2, 1)
    first = lax.broadcasted_iota(jnp.int32, t.shape, 1) < HEAD // 2
    return jnp.where(first, t, swapped), jnp.where(first, -swapped, t)


def rotated(t, cos, sin):
    return t * cos + pltpu.roll(t, HEAD // 2, 1) * sin


class Ring:
    def __init__(self, n):
        self.n, self.far_a = n, n // 2
        self.far_b = n - 1 - self.far_a
        self.me = lax.axis_index("dp")
        rep = lax.axis_index("rep")
        self.core = lax.rem(rep, 2)
        self.partner = {"rep": rep + 1 - 2 * self.core}
        self.turn = 1 - 2 * self.core
        self.beside = 1, -1
        self.near = *self.beside, 2, -2

    def at(self, k):
        return lax.rem(self.me + self.n + k * self.turn, self.n)

    def to(self, k):
        return {"dp": self.at(k)}

    def meet(self):
        barrier = pltpu.get_barrier_semaphore()
        others = [self.to(k) for k in self.beside] + [self.partner]
        for other in others:
            pl.semaphore_signal(barrier, inc=1, device_id=other, device_id_type=MESH)
        pl.semaphore_wait(barrier, len(others))


def remote(src, dst, send, recv, to):
    return pltpu.make_async_remote_copy(src_ref=src, dst_ref=dst, send_sem=send, recv_sem=recv, device_id=to, device_id_type=MESH)


class Chains:
    def far(self, chain):
        return self.ring.far_b if chain else self.ring.far_a

    def now(self, s):
        for count in range(1, s + 1):
            for chain in (A, B):
                if self.taken[chain] < min(count, self.far(chain)):
                    self.taken[chain] += 1
                    self.take(chain, self.taken[chain])

    def finish(self):
        self.now(self.ring.far_a)


class Blocks:
    def __init__(self, ref, rows):
        self.ref, self.rows = ref, rows

    def part(self, block, first, count, columns=slice(None)):
        if len(self.ref.shape) == 2:
            return self.ref.at[pl.ds(pl.multiple_of(block * self.rows + first, FEW), count), columns]
        return self.ref.at[block, pl.ds(pl.multiple_of(first, FEW), count), columns]

    def all(self, first, end, share=slice(None)):
        return jnp.concatenate([self.ref[at + first : at + end, :] for at in range(0, self.ref.shape[0], self.rows)[share]])


class Gather(Chains):
    def __init__(self, ring, blocks, sems, handed_sems):
        self.taken = [0, 0]
        self.ring, self.blocks, self.sems, self.handed_sems = ring, blocks, sems, handed_sems
        self.half = blocks.rows // 2
        self.last_handed = {}

    def piece(self, block, half):
        return self.blocks.part(block, half * self.half, self.half)

    def hop(self, chain, step):
        ring = self.ring
        along = 1 if chain == A else -1
        part = self.piece(ring.at(-along * step), ring.core)
        return remote(part, part, self.sems.at[2 * chain, step], self.sems.at[2 * chain + 1, step], ring.to(along))

    def handed(self, chain, step):
        ring = self.ring
        part = self.piece(ring.at(-step - 1 if chain == A else step + 1), ring.core)
        return remote(part, part, self.handed_sems.at[ring.n - 1 + chain], self.handed_sems.at[step + chain * ring.far_a], ring.partner)

    def begin(self):
        for chain in (A, B):
            self.hop(chain, 0).start()

    def take(self, chain, s):
        ring = self.ring
        part = self.piece(ring.at(-s if chain == A else s), ring.core)
        remote(part, part, self.sems.at[2 * chain, s - 1], self.sems.at[2 * chain + 1, s - 1], ring.to(1)).wait_recv()
        if s < self.far(chain):
            self.hop(chain, s).start()
        if chain in self.last_handed:
            self.handed(chain, self.last_handed[chain]).wait_send()
        self.last_handed[chain] = s - 1
        self.handed(chain, s - 1).start()

    def complete(self):
        ring = self.ring
        for chain in (A, B):
            for step in range(self.far(chain)):
                part = self.piece(ring.at(step + 1 if chain == A else -step - 1), 1 - ring.core)
                remote(part, part, self.handed_sems.at[ring.n - 1], self.handed_sems.at[step + chain * ring.far_a], ring.partner).wait_recv()

    def drain(self):
        for chain in (A, B):
            for step in range(self.far(chain)):
                self.hop(chain, step).wait_send()
        for chain, step in self.last_handed.items():
            self.handed(chain, step).wait_send()


class Scatter(Chains):
    def __init__(self, ring, p, came_a, came_b, sems, free, got, signal, taken=(0, 0)):
        self.signal = signal
        self.ring, self.p, self.came, self.sems, self.free, self.got = ring, p, (came_a, came_b), sems, free, got
        self.taken = list(taken)

    def hop(self, chain, step):
        ring = self.ring
        left = self.far(chain) - step
        block = ring.at(left if chain == 0 else -left)
        return remote(self.p.at[block], self.came[chain].at[step], self.sems.at[2 * chain, step], self.sems.at[2 * chain + 1, step],
                      ring.to(1 if chain == 0 else -1))

    def added(self, chain, step):
        ring = self.ring
        left = self.far(chain) - step
        block = ring.at(left if chain == 0 else -left)
        few = FEW

        def rows(i):
            at = tile(i, few)
            self.p[block, at, :] = (self.p[block, at, :].astype(F32) + self.came[chain][step - 1, at, :].astype(F32)).astype(BF16)

        loop(self.p.shape[1] // few, rows)

    def begin(self, wait):
        pl.when(wait)(lambda: pl.semaphore_wait(self.free, len(self.ring.near)))
        self.hop(A, 0).start()
        self.hop(B, 0).start()

    def take(self, chain, s):
        self.hop(chain, s - 1).wait_recv()
        if s < self.far(chain):
            self.added(chain, s)
            self.hop(chain, s).start()
        if self.taken == [self.far(A), self.far(B)]:
            self.end()

    def arrived(self):
        return [(chain, self.far(chain) - 1) for chain in (A, B)]

    def end(self):
        me, few = self.ring.me, FEW

        def rows(i):
            at = tile(i, few)
            total = self.p[me, at, :].astype(F32)
            for chain, slot in self.arrived():
                total += self.came[chain][slot, at, :].astype(F32)
            self.got[at, :] = total.astype(BF16)

        loop(self.p.shape[1] // few, rows)
        for chain in (A, B):
            for step in range(self.far(chain)):
                self.hop(chain, step).wait_send()

        @pl.when(self.signal)
        def _():
            for k in self.ring.near:
                pl.semaphore_signal(self.free, inc=1, device_id=self.ring.to(k), device_id_type=MESH)


class QuickScatter(Scatter):
    def hop(self, chain, step):
        ring = self.ring
        kind = step + self.far(A) - self.far(chain)
        block, reach = ((4, 2), (3, 1), (1, 1), (2, 2))[kind]
        along = 1 if chain == A else -1
        return remote(self.p.at[ring.at(along * block)], self.came[chain].at[step], self.sems.at[2 * chain, step], self.sems.at[2 * chain + 1, step],
                      ring.to(along * reach))

    def begin(self, wait):
        pl.when(wait)(lambda: pl.semaphore_wait(self.free, len(self.ring.near)))
        for step in range(self.far(A) - 1):
            for chain in (A, B):
                if step < self.far(chain) - 1:
                    self.hop(chain, step).start()

    def take(self, chain, s):
        self.hop(chain, s - 1).wait_recv()
        beyond = self.far(chain) - 2
        if s == beyond:
            block, few = self.ring.at(2 if chain == A else -2), FEW

            def rows(i):
                at = tile(i, few)
                total = self.p[block, at, :].astype(F32)
                for slot in range(beyond):
                    total += self.came[chain][slot, at, :].astype(F32)
                self.p[block, at, :] = total.astype(BF16)

            loop(self.p.shape[1] // few, rows)
            self.hop(chain, self.far(chain) - 1).start()
        if self.taken == [self.far(A), self.far(B)]:
            self.end()

    def arrived(self):
        return [(chain, self.far(chain) - back) for chain in (A, B) for back in (1, 2)]


def merged(w):
    return w.reshape(w.shape[0] * w.shape[1], w.shape[2])


def qkv_phase(h, w, table, q, k, v, vt, rows, events):
    wide_q = q.shape[1]

    def step(i):
        at = tile(i, rows)
        wide = h[at, :].astype(F32)
        a = (wide * scale_of(wide)).astype(BF16)
        y = dot(a, merged(w[...])).astype(BF16)
        cos, sin = turns(table[at, :])
        for n in range(wide_q // HEAD):
            part = slice(n * HEAD, (n + 1) * HEAD)
            q[at, part] = rotated(y[:, part].astype(F32), cos, sin).astype(BF16)
        k[at, :] = rotated(y[:, wide_q : wide_q + HEAD].astype(F32), cos, sin).astype(BF16)
        mine = y[:, wide_q + HEAD :]
        v[at, :] = mine
        vt[:, at] = mine.T
        polled(events, i, h.shape[0] // rows)

    loop(h.shape[0] // rows, step)
    the_rest(events, h.shape[0] // rows)


def spans(bq):
    half = bq // 2
    return [(0, half, 0), (half, half, half)]


def seen(keys, first_key, queries, first_query):
    key = lax.broadcasted_iota(jnp.int32, (keys, queries), 0) + first_key
    return lax.broadcasted_iota(jnp.int32, (keys, queries), 1) + first_query >= key


def blocks(tokens, bq):
    return (tokens // bq) * (tokens // bq + 1) // 2


def row_of_blocks(iq, bq, block, events, steps):
    def step(j):
        @pl.when(j < iq)
        def _():
            block(pl.multiple_of(j * bq, bq), bq, 0, None)

        @pl.when(j == iq)
        def _():
            for first, nk, lo in spans(bq):
                block(pl.multiple_of(iq * bq + first, nk), nk, lo, seen(nk, first, bq - lo, lo))

        polled(events, lax.div(iq * (iq + 1), 2) + j, steps)

    loop(iq + 1, step)


def attend_phase(q, k, vt, o, lse, top_s, mix_s, bq, events):
    heads = q.shape[1] // HEAD

    def block(iq, start, nk, lo, mask):
        here = pl.ds(start, nk)
        cols = pl.ds(pl.multiple_of(iq * bq + lo, bq - lo), bq - lo)
        keys = k[here, :]
        scores = [dot(keys, q[cols, n * HEAD : (n + 1) * HEAD], 1, 1) for n in range(heads)]
        values = jnp.concatenate([vt[:, here], jnp.ones((8, nk), BF16)], axis=0)
        for n, s in enumerate(scores):
            if mask is not None:
                s = jnp.where(mask, s, HIDDEN)
            old = top_s[n : n + 1, lo:]
            top = jnp.maximum(old, s.max(axis=0, keepdims=True))
            top_s[n : n + 1, lo:] = top
            p = jnp.exp2((s - top) * E).astype(BF16)
            mix_s[n, :, lo:] = mix_s[n, :, lo:] * jnp.exp2((old - top) * E) + dot(values, p)

    def step(iq):
        at = tile(iq, bq)
        top_s[...] = jnp.full(top_s.shape, NEG, F32)
        mix_s[...] = jnp.zeros(mix_s.shape, F32)
        row_of_blocks(iq, bq, functools.partial(block, iq), events, blocks(q.shape[0], bq))
        for n in range(heads):
            total = mix_s[n, HEAD : HEAD + 1, :]
            o[at, n * HEAD : (n + 1) * HEAD] = (mix_s[n, :HEAD, :] * (1 / total)).T.astype(BF16)
            lse[n : n + 1, at] = top_s[n : n + 1, :] * E + jnp.log2(total)

    loop(q.shape[0] // bq, step)
    the_rest(events, blocks(q.shape[0], bq))


def mid_phase(h, o, od, hm, rows, r):
    def step(i):
        at = tile(i, rows)
        hm[at, :] = h[at, :] + dot(o[at, :], od.all(0, r)).astype(BF16)

    loop(h.shape[0] // rows, step)


def ffn_phase(hm, gu, od, out, rows, r, events):
    def step(i):
        at = tile(i, rows)
        mid = hm[at, :]
        wide = mid.astype(F32)
        b = (wide * scale_of(wide)).astype(BF16)
        y = dot(b, gu.ref[...])
        part = y.shape[1] // 4
        pieces = []
        for n in (0, 2 * part):
            gate, up = y[:, n : n + part], y[:, n + part : n + 2 * part]
            pieces.append((gate * (1 / (1 + jnp.exp(-gate))) * up).astype(BF16))
        made = jnp.concatenate(pieces, axis=1)
        out[at, :] = mid + dot(made, od.all(r, od.rows)).astype(BF16)
        polled(events, i, hm.shape[0] // rows)

    loop(hm.shape[0] // rows, step)
    the_rest(events, hm.shape[0] // rows)


def ffn_bwd_phase(half, hm, dy, gu, od, made_s, dgu_s, bt_s, db_s, dhm, rows, r, events):
    part = dgu_s.shape[1] // 4
    lanes, units = slice(2 * part * half, 2 * part * (half + 1)), slice(part * half, part * (half + 1))
    some = od.ref.shape[0] // od.rows // 2
    share = slice(some * half, some * (half + 1))

    def step(i):
        at = tile(i, rows)
        wide = hm[at, :].astype(F32)
        scale = scale_of(wide)
        b = (wide * scale).astype(BF16)
        if half == 0:
            bt_s[:, at] = b.T
        y = dot(b, gu[:, lanes])
        gate, up = y[:, :part], y[:, part:]
        back = dy[at, :]
        d_made = dot(back, od.all(r, od.rows, share), 1, 1).astype(BF16).astype(F32)
        sig = 1 / (1 + jnp.exp(-gate))
        silu = gate * sig
        made_s[at, units] = (silu * up).astype(BF16)
        d_gate = (d_made * up * (sig * (1 + gate - silu))).astype(BF16)
        d_up = (d_made * silu).astype(BF16)
        both = jnp.concatenate([d_gate, d_up], axis=1)
        dgu_s[at, lanes] = both
        db = dot(both, gu[:, lanes], 1, 1)
        if half == 0:
            db_s[at, :] = db
        else:
            db = (db_s[at, :] + db).astype(BF16).astype(F32)
            dhm[at, :] = (back.astype(F32) + norm_bwd(wide, scale, db)).astype(BF16)
        polled(events, i, hm.shape[0] // rows)

    loop(hm.shape[0] // rows, step)
    the_rest(events, hm.shape[0] // rows)


def units_phase(half, dgu_s, bt_s, p):
    n, _, columns = p.shape
    wide = next(w for w in (512, 256, 128) if columns % w == 0)

    def units(i):
        here = pl.ds(pl.multiple_of(columns * half + i * wide, wide), wide)
        p[:, :, tile(i, wide)] = dot(bt_s[...], dgu_s[:, here]).astype(BF16).reshape(n, -1, wide)

    loop(columns // wide, units)


def downs_phase(made_s, dy, p):
    n, share, group = p.shape[0], p.shape[1], 2

    def downs(i):
        got = dot(made_s[:, tile(i, group * share)], dy[...], 0, 0).astype(BF16)
        p[pl.ds(i * group, group)] = got.reshape(group, share, -1)

    loop(n // group, downs)


def out_bwd_phase(dhm, o, od, p, do, delta, rows, r):
    def step(i):
        at = tile(i, rows)
        back = dot(dhm[at, :], od.all(0, r), 1, 1).astype(BF16)
        do[at, :] = back
        both = back.astype(F32) * o[at, :].astype(F32)
        for n in range(o.shape[1] // HEAD):
            delta[n : n + 1, at] = both[:, n * HEAD : (n + 1) * HEAD].T.sum(axis=0, keepdims=True)

    loop(dhm.shape[0] // rows, step)
    p[...] = dot(o[...], dhm[...], 0, 0).astype(BF16).reshape(p.shape)


def attend_bwd_phase(q, k, v, do, lse, delta, table, dqkv, dq_s, dk_s, dv_s, kt_s, bq, events):
    heads = q.shape[1] // HEAD
    wide_q = q.shape[1]
    dk_s[...] = jnp.zeros(dk_s.shape, F32)
    dv_s[...] = jnp.zeros(dv_s.shape, F32)
    kt_s[...] = k[...].T

    def block(iq, lses, deltas, start, nk, lo, mask):
        here = pl.ds(start, nk)
        cols = pl.ds(pl.multiple_of(iq * bq + lo, bq - lo), bq - lo)
        keys, values, keys_t = k[here, :], v[here, :], kt_s[:, here]
        for pair in range(0, heads, 2):
            some = range(pair, min(pair + 2, heads))
            qs = [q[cols, n * HEAD : (n + 1) * HEAD] for n in some]
            dos = [do[cols, n * HEAD : (n + 1) * HEAD] for n in some]
            products = [(dot(keys, x, 1, 1), dot(values, y, 1, 1)) for x, y in zip(qs, dos)]
            for n, x, y, (score, dp) in zip(some, qs, dos, products):
                p = jnp.exp2(score * E - lses[n][:, lo:])
                if mask is not None:
                    p = jnp.where(mask, p, 0.0)
                ds = (p * (dp - deltas[n][:, lo:])).astype(BF16)
                dv_s[here, :] += dot(p.astype(BF16), y)
                dk_s[here, :] += dot(ds, x)
                dq_s[n, :, lo:] += dot(keys_t, ds)

    def step(iq):
        at = tile(iq, bq)
        dq_s[...] = jnp.zeros(dq_s.shape, F32)
        lses = [lse[n : n + 1, at] for n in range(heads)]
        deltas = [delta[n : n + 1, at] for n in range(heads)]
        row_of_blocks(iq, bq, functools.partial(block, iq, lses, deltas), events, blocks(q.shape[0], bq))
        cos, sin = turns(table[at, :])
        for n in range(heads):
            back = (dq_s[n] * SCALE).T.astype(BF16).astype(F32)
            dqkv[at, n * HEAD : (n + 1) * HEAD] = rotated(back, cos, -sin).astype(BF16)

    loop(q.shape[0] // bq, step)
    the_rest(events, blocks(q.shape[0], bq))

    def finish(i):
        at = tile(i, bq)
        cos, sin = turns(table[at, :])
        dqkv[at, wide_q : wide_q + HEAD] = rotated((dk_s[at, :] * SCALE).astype(BF16).astype(F32), cos, -sin).astype(BF16)
        dqkv[at, wide_q + HEAD :] = dv_s[at, :].astype(BF16)

    loop(q.shape[0] // bq, finish)


def qkv_bwd_phase(h, dqkv, w, dhm, p_qkv, a_s, dh, rows, further):
    def normed(at):
        wide = h[at, :].astype(F32)
        scale = scale_of(wide)
        a_s[at, :] = (wide * scale).astype(BF16)
        return wide, scale

    def step(i):
        at = tile(i, rows)

        @pl.when(further)
        def _():
            wide, scale = normed(at)
            da = dot(dqkv[at, :], merged(w[...]), 1, 1).astype(BF16).astype(F32)
            dh[at, :] = (dhm[at, :].astype(F32) + norm_bwd(wide, scale, da)).astype(BF16)

        @pl.when(jnp.logical_not(further))
        def _():
            normed(at)

    loop(h.shape[0] // rows, step)
    p_qkv[...] = dot(a_s[...], dqkv[...], 0, 0).astype(BF16).reshape(p_qkv.shape)


SEVEN = 7
START = 0
QKV, OD, GU = range(3)
OWN, OLD = range(2)
NEXT = OLD
PLAN = {
    "qkv": ((0, OD, OWN, 2), (0, QKV, NEXT, 0), (3, GU, OWN, 2), (3, OD, NEXT, 0)),
    "attend": ((2, OD, OWN, 3), (2, QKV, NEXT, 1), (5, GU, OWN, 3), (7, OD, NEXT, 1), (7, GU, NEXT, 0), (8, OD, OWN, 4), (8, QKV, NEXT, 2), (9, GU, OWN, 4)),
    "ffn": ((0, OD, NEXT, 2), (0, QKV, NEXT, 3), (1, GU, NEXT, 1), (2, QKV, NEXT, 4), (3, OD, NEXT, 3)),
}
LAST_PLAN = {"qkv": ((2, GU, OWN, 2),), "attend": ((0, OD, OWN, 4), (4, GU, OWN, 3), (8, GU, OWN, 4))}
HEAD_PLAN = ((QKV, 1), (GU, 0), (QKV, 2), (OD, 1), (QKV, 3), (GU, 1), (QKV, 4))


def planned(act, entries):
    by_step = {}
    for when, *what in entries:
        by_step.setdefault(when, []).append(what)
    return {when: functools.partial(act, whats) for when, whats in by_step.items()}


def forward(ring, sizes, x, few, weights, spaces, h_s, few_s, table_s, packs_s, q_s, k_s, v_s, vt_s, o_s, lse_s, hm_s, top_s, mix_s,
            own_sem, in_sem, out_sem, gather_sems, handed_sems):
    layers, bq, rows = sizes
    me = ring.me
    wq, wk, wv, wo, wg, wu, wd = weights
    wide_q, r, ro, rd = wq.shape[2], wq.shape[1], wo.shape[1], wd.shape[1]
    half = wg.shape[2] // 2
    own = {}

    def fetch(i, group, pieces):
        for src, first, count, start, wide in pieces:
            copy = pltpu.make_async_copy(src, packs_s[i][group].part(me, first, count, slice(start, start + wide)), own_sem.at[sum(map(len, own.values()))])
            own.setdefault((i, group), []).append(copy)
            copy.start()

    for i in range(layers):
        fetch(i, QKV, [(wq.at[i], 0, r, 0, wide_q), (wk.at[i], 0, r, wide_q, HEAD), (wv.at[i], 0, r, wide_q + HEAD, HEAD)])
        fetch(i, OD, [(wo.at[i], 0, ro, 0, wo.shape[2]), (wd.at[i], ro, rd, 0, wd.shape[2])])
        if i == 0:
            brought = [pltpu.make_async_copy(x, h_s, in_sem.at[0]), pltpu.make_async_copy(few, few_s, in_sem.at[1])]
            for copy in brought:
                copy.start()
        fetch(i, GU, [(w.at[i, :, half * j : half * (j + 1)], 0, r, half * (2 * j + k), half) for j in (0, 1) for k, w in enumerate((wg, wu))])
    packs = {(g, i): Gather(ring, packs_s[i][g], gather_sems.at[3 * i + g], handed_sems.at[3 * i + g]) for g in (QKV, OD, GU) for i in range(layers)}
    begun = set()
    kept = {}

    def keep(name, src, i):
        kept[name] = pltpu.make_async_copy(src, spaces[name].at[i], out_sem.at[KEPT.index(name)])
        kept[name].start()

    def reuse(*names):
        for name in names:
            if name in kept:
                kept.pop(name).wait()

    def begin(group, i):
        if (group, i) not in begun:
            begun.add((group, i))
            for copy in own[i, group]:
                copy.wait()
            packs[group, i].begin()

    def act(i, whats):
        for group, which, stop in whats:
            if i + which < layers:
                begin(group, i + which)
                packs[group, i + which].now(stop)

    def plan(phase, i):
        return planned(functools.partial(act, i), (PLAN if i + 1 < layers else LAST_PLAN).get(phase, ()))

    def whole(group, i):
        begin(group, i)
        packs[group, i].finish()
        packs[group, i].complete()

    scoped('meet', ring.meet)
    begin(QKV, 0)
    begin(OD, 0)
    for copy in brought:
        copy.wait()
    table_phase(few_s, table_s)
    for group, stop in HEAD_PLAN:
        scoped(f'head{group}_{stop}', act, 0, [(group, OWN, stop)])
    for i in range(layers):
        qkv, od, gu = packs_s[i]
        last = i + 1 == layers
        keep("h", h_s, i)
        scoped('whole_QKV', whole, QKV, i)
        reuse("q", "k", "v")
        scoped('qkv_phase', qkv_phase, h_s, qkv.ref, table_s, q_s, k_s, v_s, vt_s, rows, plan("qkv", i))
        keep("q", q_s, i)
        keep("k", k_s, i)
        keep("v", v_s, i)
        reuse("o", "lse")
        scoped('attend_phase', attend_phase, q_s, k_s, vt_s, o_s, lse_s, top_s, mix_s, bq, plan("attend", i))
        keep("o", o_s, i)
        keep("lse", lse_s, i)
        scoped('whole_OD', whole, OD, i)
        if last:
            scoped('whole_GU', whole, GU, i)
        else:
            keep("od", od.ref, i)
        reuse("hm")
        scoped('mid_phase', mid_phase, h_s, o_s, od, hm_s, rows, ro)
        if not last:
            keep("hm", hm_s, i)
            scoped('whole_GU', whole, GU, i)
            keep("gu", gu.ref, i)
            reuse("h")
            scoped('ffn_phase', ffn_phase, hm_s, gu, od, h_s, rows, ro, plan("ffn", i))
    with jax.named_scope('flush'):
        reuse(*KEPT)
        for pack in packs.values():
            pack.drain()


KEPT = ("q", "k", "v", "o", "lse", "hm", "h", "od", "gu")
PACKS = 5
QKV_G, GA_G, GB_G, WD_G, WO_G = range(PACKS)
BACK = {
    "first": ((2, QKV_G, OLD, 2), (3, WD_G, OLD, 4), (3, WO_G, OLD, 4)),
    "second": ((0, QKV_G, OLD, 4), (2, GA_G, OWN, 1)),
    "downs": ((0, GA_G, OWN, 2),),
    "attend": ((0, GB_G, OWN, 1), (1, WD_G, OWN, 1), (2, GA_G, OWN, 3), (3, WO_G, OWN, 1), (4, GB_G, OWN, 2), (6, WD_G, OWN, 2), (7, GA_G, OWN, 4), (8, WO_G, OWN, 2),
               (9, GB_G, OWN, 3)),
    "late": ((0, WD_G, OWN, 3), (0, WO_G, OWN, 3)),
    "end": ((0, GB_G, OWN, 4),),
}
TAIL = ((GA_G, 4), (GB_G, 4), (QKV_G, 2), (WD_G, 4), (WO_G, 4))


def train(sizes, x, few, dy, *refs):
    layers, n, bq, rows, r = sizes
    weights, refs = refs[:SEVEN], refs[SEVEN:]
    results, refs = refs[:PACKS], refs[PACKS:]
    spaces, refs = dict(zip(KEPT, refs)), refs[len(KEPT) :]
    few_s, table_s, qkv_s, gu_s, od_s, k_s, v_s, lse_s, hm_s, dh_s, dhm_s, made_s, dgu_s, bt_s, db_s, mix_s, top_s, kt_s, delta_s = refs[:19]
    refs = refs[19:]
    terms, came_a, came_b, got = (refs[PACKS * i : PACKS * (i + 1)] for i in range(4))
    forward_sems, (in_sem, result_sem, scatter_sems, free_sems) = refs[PACKS * 4 : -4], refs[-4:]
    ring = Ring(n)
    split, heads = qkv_s.shape[2], spaces["q"].shape[2]
    d = dh_s.shape[1]
    depth = qkv_s.shape[1]
    early = Blocks(terms[QKV_G], depth), Blocks(made_s.at[:, :d], od_s.shape[0] // n), Blocks(dgu_s.at[: n * depth, :], depth)
    late = Blocks(qkv_s, depth), Blocks(od_s, od_s.shape[0] // n), Blocks(gu_s, depth)
    od = late[OD]
    dq_s = mix_s.at[:, :HEAD, :]
    dqkv_s, do_s = made_s.at[:, :split], made_s.at[:, split : split + heads]
    dk_s, dv_s = db_s.at[:, :HEAD], db_s.at[:, HEAD : 2 * HEAD]
    q_s, o_s, h_s = dgu_s.at[:, :heads], dgu_s.at[:, heads : 2 * heads], dgu_s.at[:, 2 * heads : 2 * heads + d]
    places = {"gu": gu_s, "hm": hm_s, "od": od_s, "q": q_s, "k": k_s, "v": v_s, "o": o_s, "lse": lse_s, "h": h_s}

    def copy_of(name, i):
        return pltpu.make_async_copy(spaces[name].at[i], places[name], in_sem.at[KEPT.index(name)])

    def bring(names, i):
        for name in names:
            copy_of(name, i).start()

    def need(names, i):
        for name in names:
            copy_of(name, i).wait()

    back = pltpu.make_async_copy(dy, dh_s, in_sem.at[len(KEPT)])
    back.start()
    forward(ring, (layers, bq, rows), x, few, weights, spaces, made_s.at[:, d : 2 * d], few_s, table_s, [early] * (layers - 1) + [late], dhm_s, k_s, v_s, bt_s.at[:HEAD, :],
            made_s.at[:, 2 * d : 2 * d + heads], lse_s, hm_s, top_s, mix_s, *forward_sems)
    back.wait()
    last = layers - 1

    def pack(group, i, signal, taken=(0, 0)):
        return (QuickScatter if group == QKV_G else Scatter)(ring, terms[group], came_a[group], came_b[group], scatter_sems.at[group], free_sems.at[group], got[group].at[i], signal, taken)

    reached = {}
    for entries in BACK.values():
        for _, group, old, stop in entries:
            if old == OWN:
                reached[group] = max(stop, reached.get(group, 0))
    taken = {group: (min(stop, ring.far_a), min(stop, ring.far_b)) for group, stop in reached.items()}

    def layer(step):
        i = last - step
        later = step > 0
        own = {group: pack(group, i, i > 0) for group in range(PACKS)}
        old = {group: pack(group, i + 1, i >= 0, taken.get(group, (0, 0))) for group in range(PACKS)}

        def act(whats):
            for group, which, stop in whats:
                if which == OWN:
                    own[group].now(stop)
                else:
                    pl.when(later)(functools.partial(old[group].now, stop))

        def plan(phase):
            return planned(act, BACK[phase])

        def before(group):
            pl.when(later)(old[group].finish)

        pl.when(later)(functools.partial(need, ("gu", "hm", "od"), i))
        for half, group, phase in ((0, GA_G, "first"), (1, GB_G, "second")):
            scoped('ffn_bwd', ffn_bwd_phase, half, hm_s, dh_s, gu_s, od, made_s, dgu_s, bt_s, db_s, dhm_s, rows, r, plan(phase))
            if half == 1:
                pl.when(i > 0)(functools.partial(bring, ("gu", "hm"), i - 1))
            before(group)
            scoped('units', units_phase, half, dgu_s, bt_s, terms[group])
            scoped('begin', own[group].begin, later)
        bring(("o", "q", "k", "v", "lse", "h"), i)
        before(WD_G)
        scoped('downs', downs_phase, made_s, dh_s, terms[WD_G])
        own[WD_G].begin(later)
        scoped('downs_ev', the_rest, plan("downs"), 0)
        need(("o",), i)
        before(WO_G)
        scoped('out_bwd', out_bwd_phase, dhm_s, o_s, od, terms[WO_G], do_s, delta_s, rows, r)
        own[WO_G].begin(later)
        pl.when(i > 0)(functools.partial(bring, ("od",), i - 1))
        need(("q", "k", "v", "lse"), i)
        scoped('attend_bwd', attend_bwd_phase, q_s, k_s, v_s, do_s, lse_s, delta_s, table_s, dqkv_s, dq_s, dk_s, dv_s, kt_s, bq, plan("attend"))
        scoped('late_ev', the_rest, plan("late"), 0)
        need(("h",), i)
        before(QKV_G)
        scoped('qkv_bwd', qkv_bwd_phase, h_s, dqkv_s, qkv_s, dhm_s, terms[QKV_G], do_s, dh_s, rows, i > 0)
        own[QKV_G].begin(later)
        scoped('end_ev', the_rest, plan("end"), 0)

    loop(layers, layer)
    final = {group: pack(group, 0, False, taken.get(group, (0, 0))) for group in range(PACKS)}
    out = []

    def leave(group, i):
        out.append(pltpu.make_async_copy(got[group].at[i], results[group].at[i], result_sem.at[group, i]))
        out[-1].start()

    for i in range(1, layers):
        for group in range(PACKS):
            leave(group, i)
    for group, stop in TAIL:
        scoped(f'tail{group}_{stop}', final[group].now, stop)
        if group != QKV_G:
            final[group].finish()
            leave(group, 0)
    scoped('tail0_4', final[QKV_G].finish)
    leave(QKV_G, 0)
    for copy in out:
        copy.wait()


def adamw(*refs):
    count = 3 * SEVEN
    grads, refs = refs[:PACKS], refs[PACKS:]
    ins, outs, refs = refs[:count], refs[count : 2 * count], refs[2 * count :]
    grads_s, refs = refs[:PACKS], refs[PACKS:]
    ins_s, outs_s, (grad_sem, in_sem, out_sem) = refs[:count], refs[count : 2 * count], refs[2 * count :]
    kinds = range(0, count, SEVEN)
    layers = ins[0].shape[0]
    heads, half, whole, few = ins[0].shape[2], ins[4].shape[2] // 2, ins[3].shape[2], FEW
    waits = []
    for i in range(layers):
        copies = [pltpu.make_async_copy(src.at[i], dst.at[i], grad_sem.at[g, i]) for g, (src, dst) in enumerate(zip(grads, grads_s, strict=True))]
        copies += [pltpu.make_async_copy(ins[a].at[i], ins_s[a].at[i], in_sem.at[a, i]) for w in range(SEVEN) for a in (w + kind for kind in kinds)]
        for copy in copies:
            copy.start()
        waits.append(copies)
    parts = (
        [(QKV_G, START, START, heads)], [(QKV_G, heads, START, HEAD)], [(QKV_G, heads + HEAD, START, HEAD)], [(WO_G, START, START, whole)],
        [(GA_G, START, START, half), (GB_G, START, half, half)], [(GA_G, half, START, half), (GB_G, half, half, half)], [(WD_G, START, START, whole)],
    )
    out = []
    for i in range(layers):
        for copy in waits[i][:PACKS]:
            copy.wait()
        for w in range(SEVEN):
            for copy in waits[i][PACKS + 3 * w : PACKS + 3 * (w + 1)]:
                copy.wait()

            def step(j, i=i, w=w):
                at = tile(j, few)
                for grad, first, start, wide in parts[w]:
                    here = slice(start, start + wide)
                    g = grads_s[grad][i, at, first : first + wide].astype(F32)
                    weight = ins_s[w][i, at, here].astype(F32)
                    of_m, of_v = w + SEVEN, w + 2 * SEVEN
                    m = 0.9 * ins_s[of_m][i, at, here] + 0.1 * g
                    v = 0.95 * ins_s[of_v][i, at, here] + 0.05 * g * g
                    outs_s[w][i, at, here] = (weight - 0.02 * (m * lax.rsqrt(v + 1e-8) + 0.1 * weight)).astype(BF16)
                    outs_s[of_m][i, at, here] = m
                    outs_s[of_v][i, at, here] = v

            loop(ins[w].shape[1] // few, step)
            for a in (w + kind for kind in kinds):
                out.append(pltpu.make_async_copy(outs_s[a].at[i], outs[a].at[i], out_sem.at[a, i]))
                out[-1].start()
    for copy in out:
        copy.wait()


def solution(mesh):
    n = mesh.shape["dp"]
    far_a, far_b = n // 2, n - 1 - n // 2

    def step(x, dy, *arrays):
        weights = arrays[:SEVEN]
        wq, wk, wv, wo, wg, wu, wd = weights
        layers, r, wide_q = wq.shape
        x, dy = x[0], dy[0]
        tokens, d = x.shape
        ff = wg.shape[2]
        bq, rows = (min(512, tokens),) * 2
        few = jnp.asarray(angles(tokens))
        wide = wide_q + 2 * HEAD
        heads = wide_q // HEAD
        ro = wo.shape[1]
        shapes = (r, wide), (r, 2 * ff), (ro + wd.shape[1], d)
        terms = (r, wide), (r, ff), (r, ff), (wd.shape[1], d), (ro, d)
        both = lambda *s: jax.ShapeDtypeStruct((layers, *s), BF16)
        some = lambda lead, s: pltpu.VMEM((*lead, *s), BF16)
        grads = pl.pallas_call(
            functools.partial(train, (layers, n, bq, rows, ro)),
            out_shape=[*(both(*s) for s in terms), both(tokens, wide_q), both(tokens, HEAD), both(tokens, HEAD), both(tokens, wide_q),
                       jax.ShapeDtypeStruct((layers, 8, tokens), F32), both(tokens, d), both(tokens, d),
                       jax.ShapeDtypeStruct((layers, n * shapes[2][0], d), BF16), jax.ShapeDtypeStruct((layers, n * r, 2 * ff), BF16)],
            in_specs=[ANY] * (3 + SEVEN),
            out_specs=[ANY] * (PACKS + len(KEPT)),
            scratch_shapes=[
                pltpu.VMEM(few.shape, F32), pltpu.VMEM((tokens, HEAD), F32), some((n,), shapes[0]), *(some((n * s[0],), s[1:]) for s in shapes[1:]),
                some((tokens,), (HEAD,)), some((tokens,), (HEAD,)), pltpu.VMEM((8, tokens), F32), *(some((tokens,), (d,)) for _ in terms[:3]),
                some((tokens,), (ff,)), some((tokens,), (2 * ff,)), some((d,), (tokens,)),
                pltpu.VMEM((tokens, d), F32), pltpu.VMEM((heads, HEAD + 8, bq), F32), pltpu.VMEM((heads, bq), F32), some((HEAD,), (tokens,)), pltpu.VMEM((heads, tokens), F32),
                *(some((lead,), s) for lead in (n, far_a, far_b, layers) for s in terms),
                pltpu.SemaphoreType.DMA((9 * layers,)), pltpu.SemaphoreType.DMA((2,)), pltpu.SemaphoreType.DMA((len(KEPT),)),
                pltpu.SemaphoreType.DMA((3 * layers, 4, far_a)), pltpu.SemaphoreType.DMA((3 * layers, n + 1)),
                pltpu.SemaphoreType.DMA((len(KEPT) + 1,)), pltpu.SemaphoreType.DMA((PACKS, layers)),
                pltpu.SemaphoreType.DMA((PACKS, 4, far_a)), pltpu.SemaphoreType.REGULAR((PACKS,)),
            ],
            compiler_params=pltpu.CompilerParams(vmem_limit_bytes=VMEM, collective_id=0, has_side_effects=True),
            name="train",
        )(x, few, dy, *weights)[:PACKS]
        in_vmem = lambda a: pltpu.VMEM(a.shape, a.dtype)
        return pl.pallas_call(
            adamw,
            out_shape=[jax.ShapeDtypeStruct(a.shape, a.dtype) for a in arrays],
            in_specs=[ANY] * (PACKS + 3 * SEVEN),
            out_specs=[ANY] * (3 * SEVEN),
            scratch_shapes=[*map(in_vmem, grads), *map(in_vmem, arrays), *map(in_vmem, arrays),
                            pltpu.SemaphoreType.DMA((PACKS, layers)), *(pltpu.SemaphoreType.DMA((3 * SEVEN, layers)) for _ in arrays[:2])],
            compiler_params=pltpu.CompilerParams(vmem_limit_bytes=VMEM),
            name="adamw",
        )(*grads, *arrays)

    states, cut = P(("rep", "dp"), None, None), P(None, "dp", None)
    return jax.shard_map(
        step,
        mesh=mesh,
        in_specs=(states, states) + (cut,) * (3 * SEVEN),
        out_specs=(P("rep", "dp", None),) * (3 * SEVEN),
        check_vma=False,
    )
```

```python
import functools

import jax
import jax.numpy as jnp
import numpy as np
from jax import lax
from jax.experimental import pallas as pl
from jax.experimental.pallas import tpu as pltpu
from jax.sharding import PartitionSpec as P

HEAD = 128
THETA = 10000
NEG = -1e30
HIDDEN = 2 * NEG
LOG2E = 1.4426950408889634
SCALE = HEAD**-0.5
E = SCALE * LOG2E
VMEM = 66_000_000
STRETCH = 64
F32, BF16 = jnp.float32, jnp.bfloat16
ANY = pl.BlockSpec(memory_space=pl.ANY)
MESH = pl.DeviceIdType.MESH
A, B = range(2)
FEW = 16


def dot(a, b, ca=1, cb=0):
    return lax.dot_general(a, b, (((ca,), (cb,)), ((), ())), preferred_element_type=F32)


def tile(i, n):
    return pl.ds(pl.multiple_of(i * n, n), n)


def loop(n, body):
    lax.fori_loop(0, n, lambda i, _: body(i), None)


def polled(events, i, steps):
    for when, what in events.items():
        if when < steps:
            pl.when(i == when)(what)


def the_rest(events, steps):
    for when, what in events.items():
        if when >= steps:
            what()


def scale_of(wide):
    return lax.rsqrt(jnp.mean(wide * wide, -1, keepdims=True) + 1e-6)


def norm_bwd(wide, scale, g):
    return scale * g - wide * (scale * scale * scale * jnp.mean(wide * g, -1, keepdims=True))


def angles(tokens):
    half = HEAD // 2
    turn = float(THETA) ** (-np.arange(half) / half)
    place = np.arange(STRETCH)[:, None] * turn
    start = np.arange(0, tokens, STRETCH)[:, None] * turn
    cos, sin = np.cos(start), np.sin(start)
    return np.concatenate([np.concatenate(p, 1) for p in ((np.cos(place), np.sin(place)), (cos, cos), (-sin, sin))]).astype(np.float32)


def table_phase(few, table):
    starts = table.shape[0] // STRETCH

    def step(i):
        place = few[:STRETCH, :]
        row = lambda first: few[pl.ds(first + i, 1), :]
        table[tile(i, STRETCH), :] = place * row(STRETCH) + pltpu.roll(place, HEAD // 2, 1) * row(STRETCH + starts)

    loop(starts, step)


def turns(t):
    swapped = pltpu.roll(t, HEAD // 2, 1)
    first = lax.broadcasted_iota(jnp.int32, t.shape, 1) < HEAD // 2
    return jnp.where(first, t, swapped), jnp.where(first, -swapped, t)


def rotated(t, cos, sin):
    return t * cos + pltpu.roll(t, HEAD // 2, 1) * sin


class Ring:
    def __init__(self, n):
        self.n, self.far_a = n, n // 2
        self.far_b = n - 1 - self.far_a
        self.me = lax.axis_index("dp")
        rep = lax.axis_index("rep")
        self.core = lax.rem(rep, 2)
        self.partner = {"rep": rep + 1 - 2 * self.core}
        self.turn = 1 - 2 * self.core
        self.beside = 1, -1
        self.near = *self.beside, 2, -2

    def at(self, k):
        return lax.rem(self.me + self.n + k * self.turn, self.n)

    def to(self, k):
        return {"dp": self.at(k)}

    def meet(self):
        barrier = pltpu.get_barrier_semaphore()
        others = [self.to(k) for k in self.beside] + [self.partner]
        for other in others:
            pl.semaphore_signal(barrier, inc=1, device_id=other, device_id_type=MESH)
        pl.semaphore_wait(barrier, len(others))


def remote(src, dst, send, recv, to):
    return pltpu.make_async_remote_copy(src_ref=src, dst_ref=dst, send_sem=send, recv_sem=recv, device_id=to, device_id_type=MESH)


class Chains:
    def far(self, chain):
        return self.ring.far_b if chain else self.ring.far_a

    def now(self, s):
        for count in range(1, s + 1):
            for chain in (A, B):
                if self.taken[chain] < min(count, self.far(chain)):
                    self.taken[chain] += 1
                    self.take(chain, self.taken[chain])

    def finish(self):
        self.now(self.ring.far_a)


class Blocks:
    def __init__(self, ref, rows):
        self.ref, self.rows = ref, rows

    def part(self, block, first, count, columns=slice(None)):
        if len(self.ref.shape) == 2:
            return self.ref.at[pl.ds(pl.multiple_of(block * self.rows + first, FEW), count), columns]
        return self.ref.at[block, pl.ds(pl.multiple_of(first, FEW), count), columns]

    def all(self, first, end, share=slice(None)):
        return jnp.concatenate([self.ref[at + first : at + end, :] for at in range(0, self.ref.shape[0], self.rows)[share]])


class Gather(Chains):
    def __init__(self, ring, blocks, sems, handed_sems):
        self.taken = [0, 0]
        self.ring, self.blocks, self.sems, self.handed_sems = ring, blocks, sems, handed_sems
        self.half = blocks.rows // 2
        self.last_handed = {}

    def piece(self, block, half):
        return self.blocks.part(block, half * self.half, self.half)

    def hop(self, chain, step):
        ring = self.ring
        along = 1 if chain == A else -1
        part = self.piece(ring.at(-along * step), ring.core)
        return remote(part, part, self.sems.at[2 * chain, step], self.sems.at[2 * chain + 1, step], ring.to(along))

    def handed(self, chain, step):
        ring = self.ring
        part = self.piece(ring.at(-step - 1 if chain == A else step + 1), ring.core)
        return remote(part, part, self.handed_sems.at[ring.n - 1 + chain], self.handed_sems.at[step + chain * ring.far_a], ring.partner)

    def begin(self):
        for chain in (A, B):
            self.hop(chain, 0).start()

    def take(self, chain, s):
        ring = self.ring
        part = self.piece(ring.at(-s if chain == A else s), ring.core)
        remote(part, part, self.sems.at[2 * chain, s - 1], self.sems.at[2 * chain + 1, s - 1], ring.to(1)).wait_recv()
        if s < self.far(chain):
            self.hop(chain, s).start()
        if chain in self.last_handed:
            self.handed(chain, self.last_handed[chain]).wait_send()
        self.last_handed[chain] = s - 1
        self.handed(chain, s - 1).start()

    def complete(self):
        ring = self.ring
        for chain in (A, B):
            for step in range(self.far(chain)):
                part = self.piece(ring.at(step + 1 if chain == A else -step - 1), 1 - ring.core)
                remote(part, part, self.handed_sems.at[ring.n - 1], self.handed_sems.at[step + chain * ring.far_a], ring.partner).wait_recv()

    def drain(self):
        for chain in (A, B):
            for step in range(self.far(chain)):
                self.hop(chain, step).wait_send()
        for chain, step in self.last_handed.items():
            self.handed(chain, step).wait_send()


class Scatter(Chains):
    def __init__(self, ring, p, came_a, came_b, sems, free, got, signal, taken=(0, 0)):
        self.signal = signal
        self.ring, self.p, self.came, self.sems, self.free, self.got = ring, p, (came_a, came_b), sems, free, got
        self.taken = list(taken)

    def hop(self, chain, step):
        ring = self.ring
        left = self.far(chain) - step
        block = ring.at(left if chain == 0 else -left)
        return remote(self.p.at[block], self.came[chain].at[step], self.sems.at[2 * chain, step], self.sems.at[2 * chain + 1, step],
                      ring.to(1 if chain == 0 else -1))

    def added(self, chain, step):
        ring = self.ring
        left = self.far(chain) - step
        block = ring.at(left if chain == 0 else -left)
        few = FEW

        def rows(i):
            at = tile(i, few)
            self.p[block, at, :] = (self.p[block, at, :].astype(F32) + self.came[chain][step - 1, at, :].astype(F32)).astype(BF16)

        loop(self.p.shape[1] // few, rows)

    def begin(self, wait):
        pl.when(wait)(lambda: pl.semaphore_wait(self.free, len(self.ring.near)))
        self.hop(A, 0).start()
        self.hop(B, 0).start()

    def take(self, chain, s):
        self.hop(chain, s - 1).wait_recv()
        if s < self.far(chain):
            self.added(chain, s)
            self.hop(chain, s).start()
        if self.taken == [self.far(A), self.far(B)]:
            self.end()

    def arrived(self):
        return [(chain, self.far(chain) - 1) for chain in (A, B)]

    def end(self):
        me, few = self.ring.me, FEW

        def rows(i):
            at = tile(i, few)
            total = self.p[me, at, :].astype(F32)
            for chain, slot in self.arrived():
                total += self.came[chain][slot, at, :].astype(F32)
            self.got[at, :] = total.astype(BF16)

        loop(self.p.shape[1] // few, rows)
        for chain in (A, B):
            for step in range(self.far(chain)):
                self.hop(chain, step).wait_send()

        @pl.when(self.signal)
        def _():
            for k in self.ring.near:
                pl.semaphore_signal(self.free, inc=1, device_id=self.ring.to(k), device_id_type=MESH)


class QuickScatter(Scatter):
    def hop(self, chain, step):
        ring = self.ring
        kind = step + self.far(A) - self.far(chain)
        block, reach = ((4, 2), (3, 1), (1, 1), (2, 2))[kind]
        along = 1 if chain == A else -1
        return remote(self.p.at[ring.at(along * block)], self.came[chain].at[step], self.sems.at[2 * chain, step], self.sems.at[2 * chain + 1, step],
                      ring.to(along * reach))

    def begin(self, wait):
        pl.when(wait)(lambda: pl.semaphore_wait(self.free, len(self.ring.near)))
        for step in range(self.far(A) - 1):
            for chain in (A, B):
                if step < self.far(chain) - 1:
                    self.hop(chain, step).start()

    def take(self, chain, s):
        self.hop(chain, s - 1).wait_recv()
        beyond = self.far(chain) - 2
        if s == beyond:
            block, few = self.ring.at(2 if chain == A else -2), FEW

            def rows(i):
                at = tile(i, few)
                total = self.p[block, at, :].astype(F32)
                for slot in range(beyond):
                    total += self.came[chain][slot, at, :].astype(F32)
                self.p[block, at, :] = total.astype(BF16)

            loop(self.p.shape[1] // few, rows)
            self.hop(chain, self.far(chain) - 1).start()
        if self.taken == [self.far(A), self.far(B)]:
            self.end()

    def arrived(self):
        return [(chain, self.far(chain) - back) for chain in (A, B) for back in (1, 2)]


def merged(w):
    return w.reshape(w.shape[0] * w.shape[1], w.shape[2])


def qkv_phase(h, w, table, q, k, v, vt, rows, events):
    wide_q = q.shape[1]

    def step(i):
        at = tile(i, rows)
        wide = h[at, :].astype(F32)
        a = (wide * scale_of(wide)).astype(BF16)
        y = dot(a, merged(w[...])).astype(BF16)
        cos, sin = turns(table[at, :])
        for n in range(wide_q // HEAD):
            part = slice(n * HEAD, (n + 1) * HEAD)
            q[at, part] = rotated(y[:, part].astype(F32), cos, sin).astype(BF16)
        k[at, :] = rotated(y[:, wide_q : wide_q + HEAD].astype(F32), cos, sin).astype(BF16)
        mine = y[:, wide_q + HEAD :]
        v[at, :] = mine
        vt[:, at] = mine.T
        polled(events, i, h.shape[0] // rows)

    loop(h.shape[0] // rows, step)
    the_rest(events, h.shape[0] // rows)


def spans(bq):
    half = bq // 2
    return [(0, half, 0), (half, half, half)]


def seen(keys, first_key, queries, first_query):
    key = lax.broadcasted_iota(jnp.int32, (keys, queries), 0) + first_key
    return lax.broadcasted_iota(jnp.int32, (keys, queries), 1) + first_query >= key


def blocks(tokens, bq):
    return (tokens // bq) * (tokens // bq + 1) // 2


def row_of_blocks(iq, bq, block, events, steps):
    def step(j):
        @pl.when(j < iq)
        def _():
            block(pl.multiple_of(j * bq, bq), bq, 0, None)

        @pl.when(j == iq)
        def _():
            for first, nk, lo in spans(bq):
                block(pl.multiple_of(iq * bq + first, nk), nk, lo, seen(nk, first, bq - lo, lo))

        polled(events, lax.div(iq * (iq + 1), 2) + j, steps)

    loop(iq + 1, step)


def attend_phase(q, k, vt, o, lse, top_s, mix_s, bq, events):
    heads = q.shape[1] // HEAD

    def block(iq, start, nk, lo, mask):
        here = pl.ds(start, nk)
        cols = pl.ds(pl.multiple_of(iq * bq + lo, bq - lo), bq - lo)
        keys = k[here, :]
        scores = [dot(keys, q[cols, n * HEAD : (n + 1) * HEAD], 1, 1) for n in range(heads)]
        values = jnp.concatenate([vt[:, here], jnp.ones((8, nk), BF16)], axis=0)
        for n, s in enumerate(scores):
            if mask is not None:
                s = jnp.where(mask, s, HIDDEN)
            old = top_s[n : n + 1, lo:]
            top = jnp.maximum(old, s.max(axis=0, keepdims=True))
            top_s[n : n + 1, lo:] = top
            p = jnp.exp2((s - top) * E).astype(BF16)
            mix_s[n, :, lo:] = mix_s[n, :, lo:] * jnp.exp2((old - top) * E) + dot(values, p)

    def step(iq):
        at = tile(iq, bq)
        top_s[...] = jnp.full(top_s.shape, NEG, F32)
        mix_s[...] = jnp.zeros(mix_s.shape, F32)
        row_of_blocks(iq, bq, functools.partial(block, iq), events, blocks(q.shape[0], bq))
        for n in range(heads):
            total = mix_s[n, HEAD : HEAD + 1, :]
            o[at, n * HEAD : (n + 1) * HEAD] = (mix_s[n, :HEAD, :] * (1 / total)).T.astype(BF16)
            lse[n : n + 1, at] = top_s[n : n + 1, :] * E + jnp.log2(total)

    loop(q.shape[0] // bq, step)
    the_rest(events, blocks(q.shape[0], bq))


def mid_phase(h, o, od, hm, rows, r):
    def step(i):
        at = tile(i, rows)
        hm[at, :] = h[at, :] + dot(o[at, :], od.all(0, r)).astype(BF16)

    loop(h.shape[0] // rows, step)


def ffn_phase(hm, gu, od, out, rows, r, events):
    def step(i):
        at = tile(i, rows)
        mid = hm[at, :]
        wide = mid.astype(F32)
        b = (wide * scale_of(wide)).astype(BF16)
        y = dot(b, gu.ref[...])
        part = y.shape[1] // 4
        pieces = []
        for n in (0, 2 * part):
            gate, up = y[:, n : n + part], y[:, n + part : n + 2 * part]
            pieces.append((gate * (1 / (1 + jnp.exp(-gate))) * up).astype(BF16))
        made = jnp.concatenate(pieces, axis=1)
        out[at, :] = mid + dot(made, od.all(r, od.rows)).astype(BF16)
        polled(events, i, hm.shape[0] // rows)

    loop(hm.shape[0] // rows, step)
    the_rest(events, hm.shape[0] // rows)


def ffn_bwd_phase(half, hm, dy, gu, od, made_s, dgu_s, bt_s, db_s, dhm, rows, r, events):
    part = dgu_s.shape[1] // 4
    lanes, units = slice(2 * part * half, 2 * part * (half + 1)), slice(part * half, part * (half + 1))
    some = od.ref.shape[0] // od.rows // 2
    share = slice(some * half, some * (half + 1))

    def step(i):
        at = tile(i, rows)
        wide = hm[at, :].astype(F32)
        scale = scale_of(wide)
        b = (wide * scale).astype(BF16)
        if half == 0:
            bt_s[:, at] = b.T
        y = dot(b, gu[:, lanes])
        gate, up = y[:, :part], y[:, part:]
        back = dy[at, :]
        d_made = dot(back, od.all(r, od.rows, share), 1, 1).astype(BF16).astype(F32)
        sig = 1 / (1 + jnp.exp(-gate))
        silu = gate * sig
        made_s[at, units] = (silu * up).astype(BF16)
        d_gate = (d_made * up * (sig * (1 + gate - silu))).astype(BF16)
        d_up = (d_made * silu).astype(BF16)
        both = jnp.concatenate([d_gate, d_up], axis=1)
        dgu_s[at, lanes] = both
        db = dot(both, gu[:, lanes], 1, 1)
        if half == 0:
            db_s[at, :] = db
        else:
            db = (db_s[at, :] + db).astype(BF16).astype(F32)
            dhm[at, :] = (back.astype(F32) + norm_bwd(wide, scale, db)).astype(BF16)
        polled(events, i, hm.shape[0] // rows)

    loop(hm.shape[0] // rows, step)
    the_rest(events, hm.shape[0] // rows)


def units_phase(half, dgu_s, bt_s, p):
    n, _, columns = p.shape
    wide = next(w for w in (512, 256, 128) if columns % w == 0)

    def units(i):
        here = pl.ds(pl.multiple_of(columns * half + i * wide, wide), wide)
        p[:, :, tile(i, wide)] = dot(bt_s[...], dgu_s[:, here]).astype(BF16).reshape(n, -1, wide)

    loop(columns // wide, units)


def downs_phase(made_s, dy, p):
    n, share, group = p.shape[0], p.shape[1], 2

    def downs(i):
        got = dot(made_s[:, tile(i, group * share)], dy[...], 0, 0).astype(BF16)
        p[pl.ds(i * group, group)] = got.reshape(group, share, -1)

    loop(n // group, downs)


def out_bwd_phase(dhm, o, od, p, do, delta, rows, r):
    def step(i):
        at = tile(i, rows)
        back = dot(dhm[at, :], od.all(0, r), 1, 1).astype(BF16)
        do[at, :] = back
        both = back.astype(F32) * o[at, :].astype(F32)
        for n in range(o.shape[1] // HEAD):
            delta[n : n + 1, at] = both[:, n * HEAD : (n + 1) * HEAD].T.sum(axis=0, keepdims=True)

    loop(dhm.shape[0] // rows, step)
    p[...] = dot(o[...], dhm[...], 0, 0).astype(BF16).reshape(p.shape)


def attend_bwd_phase(q, k, v, do, lse, delta, table, dqkv, dq_s, dk_s, dv_s, kt_s, bq, events):
    heads = q.shape[1] // HEAD
    wide_q = q.shape[1]
    dk_s[...] = jnp.zeros(dk_s.shape, F32)
    dv_s[...] = jnp.zeros(dv_s.shape, F32)
    kt_s[...] = k[...].T

    def block(iq, lses, deltas, start, nk, lo, mask):
        here = pl.ds(start, nk)
        cols = pl.ds(pl.multiple_of(iq * bq + lo, bq - lo), bq - lo)
        keys, values, keys_t = k[here, :], v[here, :], kt_s[:, here]
        for pair in range(0, heads, 2):
            some = range(pair, min(pair + 2, heads))
            qs = [q[cols, n * HEAD : (n + 1) * HEAD] for n in some]
            dos = [do[cols, n * HEAD : (n + 1) * HEAD] for n in some]
            products = [(dot(keys, x, 1, 1), dot(values, y, 1, 1)) for x, y in zip(qs, dos)]
            for n, x, y, (score, dp) in zip(some, qs, dos, products):
                p = jnp.exp2(score * E - lses[n][:, lo:])
                if mask is not None:
                    p = jnp.where(mask, p, 0.0)
                ds = (p * (dp - deltas[n][:, lo:])).astype(BF16)
                dv_s[here, :] += dot(p.astype(BF16), y)
                dk_s[here, :] += dot(ds, x)
                dq_s[n, :, lo:] += dot(keys_t, ds)

    def step(iq):
        at = tile(iq, bq)
        dq_s[...] = jnp.zeros(dq_s.shape, F32)
        lses = [lse[n : n + 1, at] for n in range(heads)]
        deltas = [delta[n : n + 1, at] for n in range(heads)]
        row_of_blocks(iq, bq, functools.partial(block, iq, lses, deltas), events, blocks(q.shape[0], bq))
        cos, sin = turns(table[at, :])
        for n in range(heads):
            back = (dq_s[n] * SCALE).T.astype(BF16).astype(F32)
            dqkv[at, n * HEAD : (n + 1) * HEAD] = rotated(back, cos, -sin).astype(BF16)

    loop(q.shape[0] // bq, step)
    the_rest(events, blocks(q.shape[0], bq))

    def finish(i):
        at = tile(i, bq)
        cos, sin = turns(table[at, :])
        dqkv[at, wide_q : wide_q + HEAD] = rotated((dk_s[at, :] * SCALE).astype(BF16).astype(F32), cos, -sin).astype(BF16)
        dqkv[at, wide_q + HEAD :] = dv_s[at, :].astype(BF16)

    loop(q.shape[0] // bq, finish)


def qkv_bwd_phase(h, dqkv, w, dhm, p_qkv, a_s, dh, rows, further):
    def normed(at):
        wide = h[at, :].astype(F32)
        scale = scale_of(wide)
        a_s[at, :] = (wide * scale).astype(BF16)
        return wide, scale

    def step(i):
        at = tile(i, rows)

        @pl.when(further)
        def _():
            wide, scale = normed(at)
            da = dot(dqkv[at, :], merged(w[...]), 1, 1).astype(BF16).astype(F32)
            dh[at, :] = (dhm[at, :].astype(F32) + norm_bwd(wide, scale, da)).astype(BF16)

        @pl.when(jnp.logical_not(further))
        def _():
            normed(at)

    loop(h.shape[0] // rows, step)
    p_qkv[...] = dot(a_s[...], dqkv[...], 0, 0).astype(BF16).reshape(p_qkv.shape)


SEVEN = 7
START = 0
QKV, OD, GU = range(3)
OWN, OLD = range(2)
NEXT = OLD
PLAN = {
    "qkv": ((0, OD, OWN, 2), (0, QKV, NEXT, 0), (3, GU, OWN, 2), (3, OD, NEXT, 0)),
    "attend": ((2, OD, OWN, 3), (2, QKV, NEXT, 1), (5, GU, OWN, 3), (6, QKV, NEXT, 2), (7, OD, NEXT, 1), (7, GU, NEXT, 0), (8, OD, OWN, 4), (9, GU, OWN, 4)),
    "ffn": ((0, QKV, NEXT, 3), (0, OD, NEXT, 2), (1, GU, NEXT, 1), (2, QKV, NEXT, 4), (3, OD, NEXT, 3)),
}
LAST_PLAN = {"qkv": ((2, GU, OWN, 2),), "attend": ((0, OD, OWN, 4), (4, GU, OWN, 3), (8, GU, OWN, 4))}
HEAD_PLAN = ((QKV, 1), (GU, 0), (QKV, 2), (OD, 1), (QKV, 3), (GU, 1), (QKV, 4))


def planned(act, entries):
    by_step = {}
    for when, *what in entries:
        by_step.setdefault(when, []).append(what)
    return {when: functools.partial(act, whats) for when, whats in by_step.items()}


def forward(ring, sizes, x, few, weights, spaces, h_s, few_s, table_s, packs_s, q_s, k_s, v_s, vt_s, o_s, lse_s, hm_s, top_s, mix_s,
            own_sem, in_sem, out_sem, gather_sems, handed_sems):
    layers, bq, rows = sizes
    me = ring.me
    wq, wk, wv, wo, wg, wu, wd = weights
    wide_q, r, ro, rd = wq.shape[2], wq.shape[1], wo.shape[1], wd.shape[1]
    half = wg.shape[2] // 2
    own = {}

    def fetch(i, group, pieces):
        for src, first, count, start, wide in pieces:
            copy = pltpu.make_async_copy(src, packs_s[i][group].part(me, first, count, slice(start, start + wide)), own_sem.at[sum(map(len, own.values()))])
            own.setdefault((i, group), []).append(copy)
            copy.start()

    for i in range(layers):
        fetch(i, QKV, [(wq.at[i], 0, r, 0, wide_q), (wk.at[i], 0, r, wide_q, HEAD), (wv.at[i], 0, r, wide_q + HEAD, HEAD)])
        fetch(i, OD, [(wo.at[i], 0, ro, 0, wo.shape[2]), (wd.at[i], ro, rd, 0, wd.shape[2])])
        if i == 0:
            brought = [pltpu.make_async_copy(x, h_s, in_sem.at[0]), pltpu.make_async_copy(few, few_s, in_sem.at[1])]
            for copy in brought:
                copy.start()
        fetch(i, GU, [(w.at[i, :, half * j : half * (j + 1)], 0, r, half * (2 * j + k), half) for j in (0, 1) for k, w in enumerate((wg, wu))])
    packs = {(g, i): Gather(ring, packs_s[i][g], gather_sems.at[3 * i + g], handed_sems.at[3 * i + g]) for g in (QKV, OD, GU) for i in range(layers)}
    begun = set()
    kept = {}

    def keep(name, src, i):
        kept[name] = pltpu.make_async_copy(src, spaces[name].at[i], out_sem.at[KEPT.index(name)])
        kept[name].start()

    def reuse(*names):
        for name in names:
            if name in kept:
                kept.pop(name).wait()

    def begin(group, i):
        if (group, i) not in begun:
            begun.add((group, i))
            for copy in own[i, group]:
                copy.wait()
            packs[group, i].begin()

    def act(i, whats):
        for group, which, stop in whats:
            if i + which < layers:
                begin(group, i + which)
                packs[group, i + which].now(stop)

    def plan(phase, i):
        return planned(functools.partial(act, i), (PLAN if i + 1 < layers else LAST_PLAN).get(phase, ()))

    def whole(group, i):
        begin(group, i)
        packs[group, i].finish()
        packs[group, i].complete()

    ring.meet()
    begin(QKV, 0)
    begin(OD, 0)
    for copy in brought:
        copy.wait()
    table_phase(few_s, table_s)
    act(0, [(group, OWN, stop) for group, stop in HEAD_PLAN])
    for i in range(layers):
        qkv, od, gu = packs_s[i]
        last = i + 1 == layers
        keep("h", h_s, i)
        whole(QKV, i)
        reuse("q", "k", "v")
        qkv_phase(h_s, qkv.ref, table_s, q_s, k_s, v_s, vt_s, rows, plan("qkv", i))
        keep("q", q_s, i)
        keep("k", k_s, i)
        keep("v", v_s, i)
        reuse("o", "lse")
        attend_phase(q_s, k_s, vt_s, o_s, lse_s, top_s, mix_s, bq, plan("attend", i))
        keep("o", o_s, i)
        keep("lse", lse_s, i)
        whole(OD, i)
        if last:
            whole(GU, i)
        else:
            keep("od", od.ref, i)
        reuse("hm")
        mid_phase(h_s, o_s, od, hm_s, rows, ro)
        if not last:
            keep("hm", hm_s, i)
            whole(GU, i)
            keep("gu", gu.ref, i)
            reuse("h")
            ffn_phase(hm_s, gu, od, h_s, rows, ro, plan("ffn", i))
    reuse(*KEPT)
    for pack in packs.values():
        pack.drain()


KEPT = ("q", "k", "v", "o", "lse", "hm", "h", "od", "gu")
PACKS = 5
QKV_G, GA_G, GB_G, WD_G, WO_G = range(PACKS)
BACK = {
    "first": ((2, QKV_G, OLD, 2), (3, WD_G, OLD, 4), (3, WO_G, OLD, 4)),
    "second": ((0, QKV_G, OLD, 4), (2, GA_G, OWN, 1)),
    "downs": ((0, GA_G, OWN, 2),),
    "out": ((0, GB_G, OWN, 1),),
    "attend": ((1, WD_G, OWN, 1), (2, GA_G, OWN, 3), (2, WO_G, OWN, 1), (4, GB_G, OWN, 2), (5, WD_G, OWN, 2), (7, GA_G, OWN, 4), (7, WO_G, OWN, 2), (9, GB_G, OWN, 3)),
    "late": ((0, WD_G, OWN, 3), (0, WO_G, OWN, 3)),
    "end": ((0, GB_G, OWN, 4),),
}
TAIL = ((GA_G, 4), (GB_G, 4), (QKV_G, 2), (WD_G, 4), (WO_G, 4))


def train(sizes, x, few, dy, *refs):
    layers, n, bq, rows, r = sizes
    weights, refs = refs[:SEVEN], refs[SEVEN:]
    results, refs = refs[:PACKS], refs[PACKS:]
    spaces, refs = dict(zip(KEPT, refs)), refs[len(KEPT) :]
    few_s, table_s, qkv_s, gu_s, od_s, k_s, v_s, lse_s, hm_s, dh_s, dhm_s, made_s, dgu_s, bt_s, db_s, mix_s, top_s, kt_s, delta_s = refs[:19]
    refs = refs[19:]
    terms, came_a, came_b, got = (refs[PACKS * i : PACKS * (i + 1)] for i in range(4))
    forward_sems, (in_sem, result_sem, scatter_sems, free_sems) = refs[PACKS * 4 : -4], refs[-4:]
    ring = Ring(n)
    split, heads = qkv_s.shape[2], spaces["q"].shape[2]
    d = dh_s.shape[1]
    depth = qkv_s.shape[1]
    early = Blocks(terms[QKV_G], depth), Blocks(made_s.at[:, :d], od_s.shape[0] // n), Blocks(dgu_s.at[: n * depth, :], depth)
    late = Blocks(qkv_s, depth), Blocks(od_s, od_s.shape[0] // n), Blocks(gu_s, depth)
    od = late[OD]
    dq_s = mix_s.at[:, :HEAD, :]
    dqkv_s, do_s = made_s.at[:, :split], made_s.at[:, split : split + heads]
    dk_s, dv_s = db_s.at[:, :HEAD], db_s.at[:, HEAD : 2 * HEAD]
    q_s, o_s, h_s = dgu_s.at[:, :heads], dgu_s.at[:, heads : 2 * heads], dgu_s.at[:, 2 * heads : 2 * heads + d]
    places = {"gu": gu_s, "hm": hm_s, "od": od_s, "q": q_s, "k": k_s, "v": v_s, "o": o_s, "lse": lse_s, "h": h_s}

    def copy_of(name, i):
        return pltpu.make_async_copy(spaces[name].at[i], places[name], in_sem.at[KEPT.index(name)])

    def bring(names, i):
        for name in names:
            copy_of(name, i).start()

    def need(names, i):
        for name in names:
            copy_of(name, i).wait()

    back = pltpu.make_async_copy(dy, dh_s, in_sem.at[len(KEPT)])
    back.start()
    forward(ring, (layers, bq, rows), x, few, weights, spaces, made_s.at[:, d : 2 * d], few_s, table_s, [early] * (layers - 1) + [late], dhm_s, k_s, v_s, bt_s.at[:HEAD, :],
            made_s.at[:, 2 * d : 2 * d + heads], lse_s, hm_s, top_s, mix_s, *forward_sems)
    back.wait()
    last = layers - 1

    def pack(group, i, signal, taken=(0, 0)):
        return (QuickScatter if group == QKV_G else Scatter)(ring, terms[group], came_a[group], came_b[group], scatter_sems.at[group], free_sems.at[group], got[group].at[i], signal, taken)

    reached = {}
    for entries in BACK.values():
        for _, group, old, stop in entries:
            if old == OWN:
                reached[group] = max(stop, reached.get(group, 0))
    taken = {group: (min(stop, ring.far_a), min(stop, ring.far_b)) for group, stop in reached.items()}

    def layer(step):
        i = last - step
        later = step > 0
        own = {group: pack(group, i, i > 0) for group in range(PACKS)}
        old = {group: pack(group, i + 1, i >= 0, taken.get(group, (0, 0))) for group in range(PACKS)}

        def act(whats):
            for group, which, stop in whats:
                if which == OWN:
                    own[group].now(stop)
                else:
                    pl.when(later)(functools.partial(old[group].now, stop))

        def plan(phase):
            return planned(act, BACK[phase])

        def before(group):
            pl.when(later)(old[group].finish)

        pl.when(later)(functools.partial(need, ("gu", "hm", "od"), i))
        for half, group, phase in ((0, GA_G, "first"), (1, GB_G, "second")):
            ffn_bwd_phase(half, hm_s, dh_s, gu_s, od, made_s, dgu_s, bt_s, db_s, dhm_s, rows, r, plan(phase))
            if half == 1:
                pl.when(i > 0)(functools.partial(bring, ("gu", "hm"), i - 1))
            before(group)
            units_phase(half, dgu_s, bt_s, terms[group])
            own[group].begin(later)
        bring(("o", "q", "k", "v", "lse", "h"), i)
        before(WD_G)
        downs_phase(made_s, dh_s, terms[WD_G])
        own[WD_G].begin(later)
        the_rest(plan("downs"), 0)
        need(("o",), i)
        before(WO_G)
        out_bwd_phase(dhm_s, o_s, od, terms[WO_G], do_s, delta_s, rows, r)
        own[WO_G].begin(later)
        the_rest(plan("out"), 0)
        pl.when(i > 0)(functools.partial(bring, ("od",), i - 1))
        need(("q", "k", "v", "lse"), i)
        attend_bwd_phase(q_s, k_s, v_s, do_s, lse_s, delta_s, table_s, dqkv_s, dq_s, dk_s, dv_s, kt_s, bq, plan("attend"))
        the_rest(plan("late"), 0)
        need(("h",), i)
        before(QKV_G)
        qkv_bwd_phase(h_s, dqkv_s, qkv_s, dhm_s, terms[QKV_G], do_s, dh_s, rows, i > 0)
        own[QKV_G].begin(later)
        the_rest(plan("end"), 0)

    loop(layers, layer)
    final = {group: pack(group, 0, False, taken.get(group, (0, 0))) for group in range(PACKS)}
    out = []

    def leave(group, i):
        out.append(pltpu.make_async_copy(got[group].at[i], results[group].at[i], result_sem.at[group, i]))
        out[-1].start()

    for i in range(1, layers):
        for group in range(PACKS):
            leave(group, i)
    for group, stop in TAIL:
        final[group].now(stop)
        if group != QKV_G:
            final[group].finish()
            leave(group, 0)
    final[QKV_G].finish()
    leave(QKV_G, 0)
    for copy in out:
        copy.wait()


def adamw(*refs):
    count = 3 * SEVEN
    grads, refs = refs[:PACKS], refs[PACKS:]
    ins, outs, refs = refs[:count], refs[count : 2 * count], refs[2 * count :]
    grads_s, refs = refs[:PACKS], refs[PACKS:]
    ins_s, outs_s, (grad_sem, in_sem, out_sem) = refs[:count], refs[count : 2 * count], refs[2 * count :]
    kinds = range(0, count, SEVEN)
    layers = ins[0].shape[0]
    heads, half, whole, few = ins[0].shape[2], ins[4].shape[2] // 2, ins[3].shape[2], FEW
    waits = []
    for i in range(layers):
        copies = [pltpu.make_async_copy(src.at[i], dst.at[i], grad_sem.at[g, i]) for g, (src, dst) in enumerate(zip(grads, grads_s, strict=True))]
        copies += [pltpu.make_async_copy(ins[a].at[i], ins_s[a].at[i], in_sem.at[a, i]) for w in range(SEVEN) for a in (w + kind for kind in kinds)]
        for copy in copies:
            copy.start()
        waits.append(copies)
    parts = (
        [(QKV_G, START, START, heads)], [(QKV_G, heads, START, HEAD)], [(QKV_G, heads + HEAD, START, HEAD)], [(WO_G, START, START, whole)],
        [(GA_G, START, START, half), (GB_G, START, half, half)], [(GA_G, half, START, half), (GB_G, half, half, half)], [(WD_G, START, START, whole)],
    )
    out = []
    for i in range(layers):
        for copy in waits[i][:PACKS]:
            copy.wait()
        for w in range(SEVEN):
            for copy in waits[i][PACKS + 3 * w : PACKS + 3 * (w + 1)]:
                copy.wait()

            def step(j, i=i, w=w):
                at = tile(j, few)
                for grad, first, start, wide in parts[w]:
                    here = slice(start, start + wide)
                    g = grads_s[grad][i, at, first : first + wide].astype(F32)
                    weight = ins_s[w][i, at, here].astype(F32)
                    of_m, of_v = w + SEVEN, w + 2 * SEVEN
                    m = 0.9 * ins_s[of_m][i, at, here] + 0.1 * g
                    v = 0.95 * ins_s[of_v][i, at, here] + 0.05 * g * g
                    outs_s[w][i, at, here] = (weight - 0.02 * (m * lax.rsqrt(v + 1e-8) + 0.1 * weight)).astype(BF16)
                    outs_s[of_m][i, at, here] = m
                    outs_s[of_v][i, at, here] = v

            loop(ins[w].shape[1] // few, step)
            for a in (w + kind for kind in kinds):
                out.append(pltpu.make_async_copy(outs_s[a].at[i], outs[a].at[i], out_sem.at[a, i]))
                out[-1].start()
    for copy in out:
        copy.wait()


def solution(mesh):
    n = mesh.shape["dp"]
    far_a, far_b = n // 2, n - 1 - n // 2

    def step(x, dy, *arrays):
        weights = arrays[:SEVEN]
        wq, wk, wv, wo, wg, wu, wd = weights
        layers, r, wide_q = wq.shape
        x, dy = x[0], dy[0]
        tokens, d = x.shape
        ff = wg.shape[2]
        bq, rows = (min(512, tokens),) * 2
        few = jnp.asarray(angles(tokens))
        wide = wide_q + 2 * HEAD
        heads = wide_q // HEAD
        ro = wo.shape[1]
        shapes = (r, wide), (r, 2 * ff), (ro + wd.shape[1], d)
        terms = (r, wide), (r, ff), (r, ff), (wd.shape[1], d), (ro, d)
        both = lambda *s: jax.ShapeDtypeStruct((layers, *s), BF16)
        some = lambda lead, s: pltpu.VMEM((*lead, *s), BF16)
        grads = pl.pallas_call(
            functools.partial(train, (layers, n, bq, rows, ro)),
            out_shape=[*(both(*s) for s in terms), both(tokens, wide_q), both(tokens, HEAD), both(tokens, HEAD), both(tokens, wide_q),
                       jax.ShapeDtypeStruct((layers, 8, tokens), F32), both(tokens, d), both(tokens, d),
                       jax.ShapeDtypeStruct((layers, n * shapes[2][0], d), BF16), jax.ShapeDtypeStruct((layers, n * r, 2 * ff), BF16)],
            in_specs=[ANY] * (3 + SEVEN),
            out_specs=[ANY] * (PACKS + len(KEPT)),
            scratch_shapes=[
                pltpu.VMEM(few.shape, F32), pltpu.VMEM((tokens, HEAD), F32), some((n,), shapes[0]), *(some((n * s[0],), s[1:]) for s in shapes[1:]),
                some((tokens,), (HEAD,)), some((tokens,), (HEAD,)), pltpu.VMEM((8, tokens), F32), *(some((tokens,), (d,)) for _ in terms[:3]),
                some((tokens,), (ff,)), some((tokens,), (2 * ff,)), some((d,), (tokens,)),
                pltpu.VMEM((tokens, d), F32), pltpu.VMEM((heads, HEAD + 8, bq), F32), pltpu.VMEM((heads, bq), F32), some((HEAD,), (tokens,)), pltpu.VMEM((heads, tokens), F32),
                *(some((lead,), s) for lead in (n, far_a, far_b, layers) for s in terms),
                pltpu.SemaphoreType.DMA((9 * layers,)), pltpu.SemaphoreType.DMA((2,)), pltpu.SemaphoreType.DMA((len(KEPT),)),
                pltpu.SemaphoreType.DMA((3 * layers, 4, far_a)), pltpu.SemaphoreType.DMA((3 * layers, n + 1)),
                pltpu.SemaphoreType.DMA((len(KEPT) + 1,)), pltpu.SemaphoreType.DMA((PACKS, layers)),
                pltpu.SemaphoreType.DMA((PACKS, 4, far_a)), pltpu.SemaphoreType.REGULAR((PACKS,)),
            ],
            compiler_params=pltpu.CompilerParams(vmem_limit_bytes=VMEM, collective_id=0, has_side_effects=True),
            name="train",
        )(x, few, dy, *weights)[:PACKS]
        in_vmem = lambda a: pltpu.VMEM(a.shape, a.dtype)
        return pl.pallas_call(
            adamw,
            out_shape=[jax.ShapeDtypeStruct(a.shape, a.dtype) for a in arrays],
            in_specs=[ANY] * (PACKS + 3 * SEVEN),
            out_specs=[ANY] * (3 * SEVEN),
            scratch_shapes=[*map(in_vmem, grads), *map(in_vmem, arrays), *map(in_vmem, arrays),
                            pltpu.SemaphoreType.DMA((PACKS, layers)), *(pltpu.SemaphoreType.DMA((3 * SEVEN, layers)) for _ in arrays[:2])],
            compiler_params=pltpu.CompilerParams(vmem_limit_bytes=VMEM),
            name="adamw",
        )(*grads, *arrays)

    states, cut = P(("rep", "dp"), None, None), P(None, "dp", None)
    return jax.shard_map(
        step,
        mesh=mesh,
        in_specs=(states, states) + (cut,) * (3 * SEVEN),
        out_specs=(P("rep", "dp", None),) * (3 * SEVEN),
        check_vma=False,
    )
```

```python
import functools

import jax
import jax.numpy as jnp
import numpy as np
from jax import lax
from jax.experimental import pallas as pl
from jax.experimental.pallas import tpu as pltpu
from jax.sharding import PartitionSpec as P

HEAD = 128
THETA = 10000
NEG = -1e30
HIDDEN = 2 * NEG
LOG2E = 1.4426950408889634
SCALE = HEAD**-0.5
E = SCALE * LOG2E
VMEM = 66_000_000
STRETCH = 64
F32, BF16 = jnp.float32, jnp.bfloat16
ANY = pl.BlockSpec(memory_space=pl.ANY)
MESH = pl.DeviceIdType.MESH
A, B = range(2)
FEW = 16


def dot(a, b, ca=1, cb=0):
    return lax.dot_general(a, b, (((ca,), (cb,)), ((), ())), preferred_element_type=F32)


def tile(i, n):
    return pl.ds(pl.multiple_of(i * n, n), n)


def loop(n, body):
    lax.fori_loop(0, n, lambda i, _: body(i), None)


def polled(events, i, steps):
    for when, what in events.items():
        if when < steps:
            pl.when(i == when)(what)


def the_rest(events, steps):
    for when, what in events.items():
        if when >= steps:
            what()


def scale_of(wide):
    return lax.rsqrt(jnp.mean(wide * wide, -1, keepdims=True) + 1e-6)


def norm_bwd(wide, scale, g):
    return scale * g - wide * (scale * scale * scale * jnp.mean(wide * g, -1, keepdims=True))


def angles(tokens):
    half = HEAD // 2
    turn = float(THETA) ** (-np.arange(half) / half)
    place = np.arange(STRETCH)[:, None] * turn
    start = np.arange(0, tokens, STRETCH)[:, None] * turn
    cos, sin = np.cos(start), np.sin(start)
    return np.concatenate([np.concatenate(p, 1) for p in ((np.cos(place), np.sin(place)), (cos, cos), (-sin, sin))]).astype(np.float32)


def table_phase(few, table):
    starts = table.shape[0] // STRETCH

    def step(i):
        place = few[:STRETCH, :]
        row = lambda first: few[pl.ds(first + i, 1), :]
        table[tile(i, STRETCH), :] = place * row(STRETCH) + pltpu.roll(place, HEAD // 2, 1) * row(STRETCH + starts)

    loop(starts, step)


def turns(t):
    swapped = pltpu.roll(t, HEAD // 2, 1)
    first = lax.broadcasted_iota(jnp.int32, t.shape, 1) < HEAD // 2
    return jnp.where(first, t, swapped), jnp.where(first, -swapped, t)


def rotated(t, cos, sin):
    return t * cos + pltpu.roll(t, HEAD // 2, 1) * sin


class Ring:
    def __init__(self, n):
        self.n, self.far_a = n, n // 2
        self.far_b = n - 1 - self.far_a
        self.me = lax.axis_index("dp")
        rep = lax.axis_index("rep")
        self.core = lax.rem(rep, 2)
        self.partner = {"rep": rep + 1 - 2 * self.core}
        self.turn = 1 - 2 * self.core
        self.beside = 1, -1
        self.near = *self.beside, 2, -2

    def at(self, k):
        return lax.rem(self.me + self.n + k * self.turn, self.n)

    def to(self, k):
        return {"dp": self.at(k)}

    def meet(self):
        barrier = pltpu.get_barrier_semaphore()
        others = [self.to(k) for k in self.beside] + [self.partner]
        for other in others:
            pl.semaphore_signal(barrier, inc=1, device_id=other, device_id_type=MESH)
        pl.semaphore_wait(barrier, len(others))


def remote(src, dst, send, recv, to):
    return pltpu.make_async_remote_copy(src_ref=src, dst_ref=dst, send_sem=send, recv_sem=recv, device_id=to, device_id_type=MESH)


class Chains:
    def far(self, chain):
        return self.ring.far_b if chain else self.ring.far_a

    def now(self, s):
        for count in range(1, s + 1):
            for chain in (A, B):
                if self.taken[chain] < min(count, self.far(chain)):
                    self.taken[chain] += 1
                    self.take(chain, self.taken[chain])

    def finish(self):
        self.now(self.ring.far_a)


class Blocks:
    def __init__(self, ref, rows):
        self.ref, self.rows = ref, rows

    def part(self, block, first, count, columns=slice(None)):
        if len(self.ref.shape) == 2:
            return self.ref.at[pl.ds(pl.multiple_of(block * self.rows + first, FEW), count), columns]
        return self.ref.at[block, pl.ds(pl.multiple_of(first, FEW), count), columns]

    def all(self, first, end, share=slice(None)):
        return jnp.concatenate([self.ref[at + first : at + end, :] for at in range(0, self.ref.shape[0], self.rows)[share]])


class Gather(Chains):
    def __init__(self, ring, blocks, sems, handed_sems):
        self.taken = [0, 0]
        self.ring, self.blocks, self.sems, self.handed_sems = ring, blocks, sems, handed_sems
        self.half = blocks.rows // 2
        self.last_handed = {}

    def piece(self, block, half):
        return self.blocks.part(block, half * self.half, self.half)

    def hop(self, chain, step):
        ring = self.ring
        along = 1 if chain == A else -1
        part = self.piece(ring.at(-along * step), ring.core)
        return remote(part, part, self.sems.at[2 * chain, step], self.sems.at[2 * chain + 1, step], ring.to(along))

    def handed(self, chain, step):
        ring = self.ring
        part = self.piece(ring.at(-step - 1 if chain == A else step + 1), ring.core)
        return remote(part, part, self.handed_sems.at[ring.n - 1 + chain], self.handed_sems.at[step + chain * ring.far_a], ring.partner)

    def begin(self):
        for chain in (A, B):
            self.hop(chain, 0).start()

    def take(self, chain, s):
        ring = self.ring
        part = self.piece(ring.at(-s if chain == A else s), ring.core)
        remote(part, part, self.sems.at[2 * chain, s - 1], self.sems.at[2 * chain + 1, s - 1], ring.to(1)).wait_recv()
        if s < self.far(chain):
            self.hop(chain, s).start()
        if chain in self.last_handed:
            self.handed(chain, self.last_handed[chain]).wait_send()
        self.last_handed[chain] = s - 1
        self.handed(chain, s - 1).start()

    def complete(self):
        ring = self.ring
        for chain in (A, B):
            for step in range(self.far(chain)):
                part = self.piece(ring.at(step + 1 if chain == A else -step - 1), 1 - ring.core)
                remote(part, part, self.handed_sems.at[ring.n - 1], self.handed_sems.at[step + chain * ring.far_a], ring.partner).wait_recv()

    def drain(self):
        for chain in (A, B):
            for step in range(self.far(chain)):
                self.hop(chain, step).wait_send()
        for chain, step in self.last_handed.items():
            self.handed(chain, step).wait_send()


class Scatter(Chains):
    def __init__(self, ring, p, came_a, came_b, sems, free, got, signal, taken=(0, 0)):
        self.signal = signal
        self.ring, self.p, self.came, self.sems, self.free, self.got = ring, p, (came_a, came_b), sems, free, got
        self.taken = list(taken)

    def hop(self, chain, step):
        ring = self.ring
        left = self.far(chain) - step
        block = ring.at(left if chain == 0 else -left)
        return remote(self.p.at[block], self.came[chain].at[step], self.sems.at[2 * chain, step], self.sems.at[2 * chain + 1, step],
                      ring.to(1 if chain == 0 else -1))

    def added(self, chain, step):
        ring = self.ring
        left = self.far(chain) - step
        block = ring.at(left if chain == 0 else -left)
        few = FEW

        def rows(i):
            at = tile(i, few)
            self.p[block, at, :] = (self.p[block, at, :].astype(F32) + self.came[chain][step - 1, at, :].astype(F32)).astype(BF16)

        loop(self.p.shape[1] // few, rows)

    def begin(self, wait):
        pl.when(wait)(lambda: pl.semaphore_wait(self.free, len(self.ring.near)))
        self.hop(A, 0).start()
        self.hop(B, 0).start()

    def take(self, chain, s):
        self.hop(chain, s - 1).wait_recv()
        if s < self.far(chain):
            self.added(chain, s)
            self.hop(chain, s).start()
        if self.taken == [self.far(A), self.far(B)]:
            self.end()

    def arrived(self):
        return [(chain, self.far(chain) - 1) for chain in (A, B)]

    def end(self):
        me, few = self.ring.me, FEW

        def rows(i):
            at = tile(i, few)
            total = self.p[me, at, :].astype(F32)
            for chain, slot in self.arrived():
                total += self.came[chain][slot, at, :].astype(F32)
            self.got[at, :] = total.astype(BF16)

        loop(self.p.shape[1] // few, rows)
        for chain in (A, B):
            for step in range(self.far(chain)):
                self.hop(chain, step).wait_send()

        @pl.when(self.signal)
        def _():
            for k in self.ring.near:
                pl.semaphore_signal(self.free, inc=1, device_id=self.ring.to(k), device_id_type=MESH)


class QuickScatter(Scatter):
    def hop(self, chain, step):
        ring = self.ring
        kind = step + self.far(A) - self.far(chain)
        block, reach = ((4, 2), (3, 1), (1, 1), (2, 2))[kind]
        along = 1 if chain == A else -1
        return remote(self.p.at[ring.at(along * block)], self.came[chain].at[step], self.sems.at[2 * chain, step], self.sems.at[2 * chain + 1, step],
                      ring.to(along * reach))

    def begin(self, wait):
        pl.when(wait)(lambda: pl.semaphore_wait(self.free, len(self.ring.near)))
        for step in range(self.far(A) - 1):
            for chain in (A, B):
                if step < self.far(chain) - 1:
                    self.hop(chain, step).start()

    def take(self, chain, s):
        self.hop(chain, s - 1).wait_recv()
        beyond = self.far(chain) - 2
        if s == beyond:
            block, few = self.ring.at(2 if chain == A else -2), FEW

            def rows(i):
                at = tile(i, few)
                total = self.p[block, at, :].astype(F32)
                for slot in range(beyond):
                    total += self.came[chain][slot, at, :].astype(F32)
                self.p[block, at, :] = total.astype(BF16)

            loop(self.p.shape[1] // few, rows)
            self.hop(chain, self.far(chain) - 1).start()
        if self.taken == [self.far(A), self.far(B)]:
            self.end()

    def arrived(self):
        return [(chain, self.far(chain) - back) for chain in (A, B) for back in (1, 2)]


def merged(w):
    return w.reshape(w.shape[0] * w.shape[1], w.shape[2])


def qkv_phase(h, w, table, q, k, v, vt, rows, events):
    wide_q = q.shape[1]

    def step(i):
        at = tile(i, rows)
        wide = h[at, :].astype(F32)
        a = (wide * scale_of(wide)).astype(BF16)
        y = dot(a, merged(w[...])).astype(BF16)
        cos, sin = turns(table[at, :])
        for n in range(wide_q // HEAD):
            part = slice(n * HEAD, (n + 1) * HEAD)
            q[at, part] = rotated(y[:, part].astype(F32), cos, sin).astype(BF16)
        k[at, :] = rotated(y[:, wide_q : wide_q + HEAD].astype(F32), cos, sin).astype(BF16)
        mine = y[:, wide_q + HEAD :]
        v[at, :] = mine
        vt[:, at] = mine.T
        polled(events, i, h.shape[0] // rows)

    loop(h.shape[0] // rows, step)
    the_rest(events, h.shape[0] // rows)


def spans(bq):
    half = bq // 2
    return [(0, half, 0), (half, half, half)]


def seen(keys, first_key, queries, first_query):
    key = lax.broadcasted_iota(jnp.int32, (keys, queries), 0) + first_key
    return lax.broadcasted_iota(jnp.int32, (keys, queries), 1) + first_query >= key


def blocks(tokens, bq):
    return (tokens // bq) * (tokens // bq + 1) // 2


def row_of_blocks(iq, bq, block, events, steps):
    def step(j):
        @pl.when(j < iq)
        def _():
            block(pl.multiple_of(j * bq, bq), bq, 0, None)

        @pl.when(j == iq)
        def _():
            for first, nk, lo in spans(bq):
                block(pl.multiple_of(iq * bq + first, nk), nk, lo, seen(nk, first, bq - lo, lo))

        polled(events, lax.div(iq * (iq + 1), 2) + j, steps)

    loop(iq + 1, step)


def attend_phase(q, k, vt, o, lse, top_s, mix_s, bq, events):
    heads = q.shape[1] // HEAD

    def block(iq, start, nk, lo, mask):
        here = pl.ds(start, nk)
        cols = pl.ds(pl.multiple_of(iq * bq + lo, bq - lo), bq - lo)
        keys = k[here, :]
        scores = [dot(keys, q[cols, n * HEAD : (n + 1) * HEAD], 1, 1) for n in range(heads)]
        values = jnp.concatenate([vt[:, here], jnp.ones((8, nk), BF16)], axis=0)
        for n, s in enumerate(scores):
            if mask is not None:
                s = jnp.where(mask, s, HIDDEN)
            old = top_s[n : n + 1, lo:]
            top = jnp.maximum(old, s.max(axis=0, keepdims=True))
            top_s[n : n + 1, lo:] = top
            p = jnp.exp2((s - top) * E).astype(BF16)
            mix_s[n, :, lo:] = mix_s[n, :, lo:] * jnp.exp2((old - top) * E) + dot(values, p)

    def step(iq):
        at = tile(iq, bq)
        top_s[...] = jnp.full(top_s.shape, NEG, F32)
        mix_s[...] = jnp.zeros(mix_s.shape, F32)
        row_of_blocks(iq, bq, functools.partial(block, iq), events, blocks(q.shape[0], bq))
        for n in range(heads):
            total = mix_s[n, HEAD : HEAD + 1, :]
            o[at, n * HEAD : (n + 1) * HEAD] = (mix_s[n, :HEAD, :] * (1 / total)).T.astype(BF16)
            lse[n : n + 1, at] = top_s[n : n + 1, :] * E + jnp.log2(total)

    loop(q.shape[0] // bq, step)
    the_rest(events, blocks(q.shape[0], bq))


def mid_phase(h, o, od, hm, rows, r):
    def step(i):
        at = tile(i, rows)
        hm[at, :] = h[at, :] + dot(o[at, :], od.all(0, r)).astype(BF16)

    loop(h.shape[0] // rows, step)


def ffn_phase(hm, gu, od, out, rows, r, events):
    def step(i):
        at = tile(i, rows)
        mid = hm[at, :]
        wide = mid.astype(F32)
        b = (wide * scale_of(wide)).astype(BF16)
        y = dot(b, gu.ref[...])
        part = y.shape[1] // 4
        pieces = []
        for n in (0, 2 * part):
            gate, up = y[:, n : n + part], y[:, n + part : n + 2 * part]
            pieces.append((gate * (1 / (1 + jnp.exp(-gate))) * up).astype(BF16))
        made = jnp.concatenate(pieces, axis=1)
        out[at, :] = mid + dot(made, od.all(r, od.rows)).astype(BF16)
        polled(events, i, hm.shape[0] // rows)

    loop(hm.shape[0] // rows, step)
    the_rest(events, hm.shape[0] // rows)


def ffn_bwd_phase(half, hm, dy, gu, od, made_s, dgu_s, bt_s, db_s, dhm, rows, r, events):
    part = dgu_s.shape[1] // 4
    lanes, units = slice(2 * part * half, 2 * part * (half + 1)), slice(part * half, part * (half + 1))
    some = od.ref.shape[0] // od.rows // 2
    share = slice(some * half, some * (half + 1))

    def step(i):
        at = tile(i, rows)
        wide = hm[at, :].astype(F32)
        scale = scale_of(wide)
        b = (wide * scale).astype(BF16)
        if half == 0:
            bt_s[:, at] = b.T
        y = dot(b, gu[:, lanes])
        gate, up = y[:, :part], y[:, part:]
        back = dy[at, :]
        d_made = dot(back, od.all(r, od.rows, share), 1, 1).astype(BF16).astype(F32)
        sig = 1 / (1 + jnp.exp(-gate))
        silu = gate * sig
        made_s[at, units] = (silu * up).astype(BF16)
        d_gate = (d_made * up * (sig * (1 + gate - silu))).astype(BF16)
        d_up = (d_made * silu).astype(BF16)
        both = jnp.concatenate([d_gate, d_up], axis=1)
        dgu_s[at, lanes] = both
        db = dot(both, gu[:, lanes], 1, 1)
        if half == 0:
            db_s[at, :] = db
        else:
            db = (db_s[at, :] + db).astype(BF16).astype(F32)
            dhm[at, :] = (back.astype(F32) + norm_bwd(wide, scale, db)).astype(BF16)
        polled(events, i, hm.shape[0] // rows)

    loop(hm.shape[0] // rows, step)
    the_rest(events, hm.shape[0] // rows)


def units_phase(half, dgu_s, bt_s, p):
    n, _, columns = p.shape
    wide = next(w for w in (512, 256, 128) if columns % w == 0)

    def units(i):
        here = pl.ds(pl.multiple_of(columns * half + i * wide, wide), wide)
        p[:, :, tile(i, wide)] = dot(bt_s[...], dgu_s[:, here]).astype(BF16).reshape(n, -1, wide)

    loop(columns // wide, units)


def downs_phase(made_s, dy, p):
    n, share, group = p.shape[0], p.shape[1], 2

    def downs(i):
        got = dot(made_s[:, tile(i, group * share)], dy[...], 0, 0).astype(BF16)
        p[pl.ds(i * group, group)] = got.reshape(group, share, -1)

    loop(n // group, downs)


def out_bwd_phase(dhm, o, od, p, do, delta, rows, r):
    def step(i):
        at = tile(i, rows)
        back = dot(dhm[at, :], od.all(0, r), 1, 1).astype(BF16)
        do[at, :] = back
        both = back.astype(F32) * o[at, :].astype(F32)
        for n in range(o.shape[1] // HEAD):
            delta[n : n + 1, at] = both[:, n * HEAD : (n + 1) * HEAD].T.sum(axis=0, keepdims=True)

    loop(dhm.shape[0] // rows, step)
    p[...] = dot(o[...], dhm[...], 0, 0).astype(BF16).reshape(p.shape)


def attend_bwd_phase(q, k, v, do, lse, delta, table, dqkv, dq_s, dk_s, dv_s, kt_s, bq, events):
    heads = q.shape[1] // HEAD
    wide_q = q.shape[1]
    dk_s[...] = jnp.zeros(dk_s.shape, F32)
    dv_s[...] = jnp.zeros(dv_s.shape, F32)
    kt_s[...] = k[...].T

    def block(iq, lses, deltas, start, nk, lo, mask):
        here = pl.ds(start, nk)
        cols = pl.ds(pl.multiple_of(iq * bq + lo, bq - lo), bq - lo)
        keys, values, keys_t = k[here, :], v[here, :], kt_s[:, here]
        for pair in range(0, heads, 2):
            some = range(pair, min(pair + 2, heads))
            qs = [q[cols, n * HEAD : (n + 1) * HEAD] for n in some]
            dos = [do[cols, n * HEAD : (n + 1) * HEAD] for n in some]
            products = [(dot(keys, x, 1, 1), dot(values, y, 1, 1)) for x, y in zip(qs, dos)]
            for n, x, y, (score, dp) in zip(some, qs, dos, products):
                p = jnp.exp2(score * E - lses[n][:, lo:])
                if mask is not None:
                    p = jnp.where(mask, p, 0.0)
                ds = (p * (dp - deltas[n][:, lo:])).astype(BF16)
                dv_s[here, :] += dot(p.astype(BF16), y)
                dk_s[here, :] += dot(ds, x)
                dq_s[n, :, lo:] += dot(keys_t, ds)

    def step(iq):
        at = tile(iq, bq)
        dq_s[...] = jnp.zeros(dq_s.shape, F32)
        lses = [lse[n : n + 1, at] for n in range(heads)]
        deltas = [delta[n : n + 1, at] for n in range(heads)]
        row_of_blocks(iq, bq, functools.partial(block, iq, lses, deltas), events, blocks(q.shape[0], bq))
        cos, sin = turns(table[at, :])
        for n in range(heads):
            back = (dq_s[n] * SCALE).T.astype(BF16).astype(F32)
            dqkv[at, n * HEAD : (n + 1) * HEAD] = rotated(back, cos, -sin).astype(BF16)

    loop(q.shape[0] // bq, step)
    the_rest(events, blocks(q.shape[0], bq))

    def finish(i):
        at = tile(i, bq)
        cos, sin = turns(table[at, :])
        dqkv[at, wide_q : wide_q + HEAD] = rotated((dk_s[at, :] * SCALE).astype(BF16).astype(F32), cos, -sin).astype(BF16)
        dqkv[at, wide_q + HEAD :] = dv_s[at, :].astype(BF16)

    loop(q.shape[0] // bq, finish)


def qkv_bwd_phase(h, dqkv, w, dhm, p_qkv, a_s, dh, rows, further):
    def normed(at):
        wide = h[at, :].astype(F32)
        scale = scale_of(wide)
        a_s[at, :] = (wide * scale).astype(BF16)
        return wide, scale

    def step(i):
        at = tile(i, rows)

        @pl.when(further)
        def _():
            wide, scale = normed(at)
            da = dot(dqkv[at, :], merged(w[...]), 1, 1).astype(BF16).astype(F32)
            dh[at, :] = (dhm[at, :].astype(F32) + norm_bwd(wide, scale, da)).astype(BF16)

        @pl.when(jnp.logical_not(further))
        def _():
            normed(at)

    loop(h.shape[0] // rows, step)
    p_qkv[...] = dot(a_s[...], dqkv[...], 0, 0).astype(BF16).reshape(p_qkv.shape)


SEVEN = 7
START = 0
QKV, OD, GU = range(3)
OWN, OLD = range(2)
NEXT = OLD
PLAN = {
    "qkv": ((0, OD, OWN, 2), (0, QKV, NEXT, 0), (3, GU, OWN, 2), (3, OD, NEXT, 0)),
    "attend": ((2, OD, OWN, 3), (2, QKV, NEXT, 1), (5, GU, OWN, 3), (6, QKV, NEXT, 2), (7, OD, NEXT, 1), (7, GU, NEXT, 0), (8, OD, OWN, 4), (9, GU, OWN, 4)),
    "ffn": ((0, QKV, NEXT, 3), (0, OD, NEXT, 2), (1, GU, NEXT, 1), (2, QKV, NEXT, 4), (3, OD, NEXT, 3)),
}
LAST_PLAN = {"qkv": ((2, GU, OWN, 2),), "attend": ((0, OD, OWN, 4), (4, GU, OWN, 3), (8, GU, OWN, 4))}
HEAD_PLAN = ((QKV, 1), (GU, 0), (QKV, 2), (OD, 1), (QKV, 3), (GU, 1), (QKV, 4))


def planned(act, entries):
    by_step = {}
    for when, *what in entries:
        by_step.setdefault(when, []).append(what)
    return {when: functools.partial(act, whats) for when, whats in by_step.items()}


def forward(ring, sizes, x, few, weights, spaces, h_s, few_s, table_s, packs_s, q_s, k_s, v_s, vt_s, o_s, lse_s, hm_s, top_s, mix_s,
            own_sem, in_sem, out_sem, gather_sems, handed_sems):
    layers, bq, rows = sizes
    me = ring.me
    wq, wk, wv, wo, wg, wu, wd = weights
    wide_q, r, ro, rd = wq.shape[2], wq.shape[1], wo.shape[1], wd.shape[1]
    half = wg.shape[2] // 2
    own = {}

    def fetch(i, group, pieces):
        for src, first, count, start, wide in pieces:
            copy = pltpu.make_async_copy(src, packs_s[i][group].part(me, first, count, slice(start, start + wide)), own_sem.at[sum(map(len, own.values()))])
            own.setdefault((i, group), []).append(copy)
            copy.start()

    for i in range(layers):
        fetch(i, QKV, [(wq.at[i], 0, r, 0, wide_q), (wk.at[i], 0, r, wide_q, HEAD), (wv.at[i], 0, r, wide_q + HEAD, HEAD)])
        fetch(i, OD, [(wo.at[i], 0, ro, 0, wo.shape[2]), (wd.at[i], ro, rd, 0, wd.shape[2])])
        if i == 0:
            brought = [pltpu.make_async_copy(x, h_s, in_sem.at[0]), pltpu.make_async_copy(few, few_s, in_sem.at[1])]
            for copy in brought:
                copy.start()
        fetch(i, GU, [(w.at[i, :, half * j : half * (j + 1)], 0, r, half * (2 * j + k), half) for j in (0, 1) for k, w in enumerate((wg, wu))])
    packs = {(g, i): Gather(ring, packs_s[i][g], gather_sems.at[3 * i + g], handed_sems.at[3 * i + g]) for g in (QKV, OD, GU) for i in range(layers)}
    begun = set()
    kept = {}

    def keep(name, src, i):
        kept[name] = pltpu.make_async_copy(src, spaces[name].at[i], out_sem.at[KEPT.index(name)])
        kept[name].start()

    def reuse(*names):
        for name in names:
            if name in kept:
                kept.pop(name).wait()

    def begin(group, i):
        if (group, i) not in begun:
            begun.add((group, i))
            for copy in own[i, group]:
                copy.wait()
            packs[group, i].begin()

    def act(i, whats):
        for group, which, stop in whats:
            if i + which < layers:
                begin(group, i + which)
                packs[group, i + which].now(stop)

    def plan(phase, i):
        return planned(functools.partial(act, i), (PLAN if i + 1 < layers else LAST_PLAN).get(phase, ()))

    def whole(group, i):
        begin(group, i)
        packs[group, i].finish()
        packs[group, i].complete()

    ring.meet()
    begin(QKV, 0)
    begin(OD, 0)
    for copy in brought:
        copy.wait()
    table_phase(few_s, table_s)
    act(0, [(group, OWN, stop) for group, stop in HEAD_PLAN])
    for i in range(layers):
        qkv, od, gu = packs_s[i]
        last = i + 1 == layers
        keep("h", h_s, i)
        whole(QKV, i)
        reuse("q", "k", "v")
        qkv_phase(h_s, qkv.ref, table_s, q_s, k_s, v_s, vt_s, rows, plan("qkv", i))
        keep("q", q_s, i)
        keep("k", k_s, i)
        keep("v", v_s, i)
        reuse("o", "lse")
        attend_phase(q_s, k_s, vt_s, o_s, lse_s, top_s, mix_s, bq, plan("attend", i))
        keep("o", o_s, i)
        keep("lse", lse_s, i)
        whole(OD, i)
        if last:
            whole(GU, i)
        else:
            keep("od", od.ref, i)
        reuse("hm")
        mid_phase(h_s, o_s, od, hm_s, rows, ro)
        if not last:
            keep("hm", hm_s, i)
            whole(GU, i)
            keep("gu", gu.ref, i)
            reuse("h")
            ffn_phase(hm_s, gu, od, h_s, rows, ro, plan("ffn", i))
    reuse(*KEPT)
    for pack in packs.values():
        pack.drain()


KEPT = ("q", "k", "v", "o", "lse", "hm", "h", "od", "gu")
PACKS = 5
QKV_G, GA_G, GB_G, WD_G, WO_G = range(PACKS)
BACK = {
    "first": ((2, QKV_G, OLD, 2), (3, WD_G, OLD, 4), (3, WO_G, OLD, 4)),
    "second": ((0, QKV_G, OLD, 4), (2, GA_G, OWN, 1)),
    "downs": ((0, GA_G, OWN, 2),),
    "out": ((0, GB_G, OWN, 1),),
    "attend": ((1, WD_G, OWN, 1), (2, GA_G, OWN, 3), (2, WO_G, OWN, 1), (4, GB_G, OWN, 2), (5, WD_G, OWN, 2), (7, GA_G, OWN, 4), (7, WO_G, OWN, 2), (9, GB_G, OWN, 3)),
    "late": ((0, WD_G, OWN, 3), (0, WO_G, OWN, 3)),
    "end": ((0, GB_G, OWN, 4),),
}
TAIL = ((GA_G, 4), (GB_G, 4), (QKV_G, 2), (WD_G, 4), (WO_G, 4))


def train(sizes, x, few, dy, *refs):
    layers, n, bq, rows, r = sizes
    weights, refs = refs[:SEVEN], refs[SEVEN:]
    results, refs = refs[:PACKS], refs[PACKS:]
    spaces, refs = dict(zip(KEPT, refs)), refs[len(KEPT) :]
    few_s, table_s, qkv_s, gu_s, od_s, k_s, v_s, lse_s, hm_s, dh_s, dhm_s, made_s, dgu_s, bt_s, db_s, mix_s, top_s, kt_s, delta_s = refs[:19]
    refs = refs[19:]
    terms, came_a, came_b, got = (refs[PACKS * i : PACKS * (i + 1)] for i in range(4))
    forward_sems, (in_sem, result_sem, free_sems) = refs[PACKS * 4 : -3], refs[-3:]
    scatter_sems = forward_sems[3]
    ring = Ring(n)
    split, heads = qkv_s.shape[2], spaces["q"].shape[2]
    d = dh_s.shape[1]
    depth = qkv_s.shape[1]
    early = Blocks(terms[QKV_G], depth), Blocks(made_s.at[:, :d], od_s.shape[0] // n), Blocks(dgu_s.at[: n * depth, :], depth)
    late = Blocks(qkv_s, depth), Blocks(od_s, od_s.shape[0] // n), Blocks(gu_s, depth)
    od = late[OD]
    dq_s = mix_s.at[:, :HEAD, :]
    dqkv_s, do_s = made_s.at[:, :split], made_s.at[:, split : split + heads]
    dk_s, dv_s = db_s.at[:, :HEAD], db_s.at[:, HEAD : 2 * HEAD]
    q_s, o_s, h_s = dgu_s.at[:, :heads], dgu_s.at[:, heads : 2 * heads], dgu_s.at[:, 2 * heads : 2 * heads + d]
    places = {"gu": gu_s, "hm": hm_s, "od": od_s, "q": q_s, "k": k_s, "v": v_s, "o": o_s, "lse": lse_s, "h": h_s}

    def copy_of(name, i):
        return pltpu.make_async_copy(spaces[name].at[i], places[name], in_sem.at[KEPT.index(name)])

    def bring(names, i):
        for name in names:
            copy_of(name, i).start()

    def need(names, i):
        for name in names:
            copy_of(name, i).wait()

    back = pltpu.make_async_copy(dy, dh_s, in_sem.at[len(KEPT)])
    back.start()
    forward(ring, (layers, bq, rows), x, few, weights, spaces, made_s.at[:, d : 2 * d], few_s, table_s, [early] * (layers - 1) + [late], dhm_s, k_s, v_s, bt_s.at[:HEAD, :],
            made_s.at[:, 2 * d : 2 * d + heads], lse_s, hm_s, top_s, mix_s, *forward_sems)
    back.wait()
    last = layers - 1

    def pack(group, i, signal, taken=(0, 0)):
        return (QuickScatter if group == QKV_G else Scatter)(ring, terms[group], came_a[group], came_b[group], scatter_sems.at[group], free_sems.at[group], got[group].at[i], signal, taken)

    reached = {}
    for entries in BACK.values():
        for _, group, old, stop in entries:
            if old == OWN:
                reached[group] = max(stop, reached.get(group, 0))
    taken = {group: (min(stop, ring.far_a), min(stop, ring.far_b)) for group, stop in reached.items()}

    def layer(step):
        i = last - step
        later = step > 0
        own = {group: pack(group, i, i > 0) for group in range(PACKS)}
        old = {group: pack(group, i + 1, i >= 0, taken.get(group, (0, 0))) for group in range(PACKS)}

        def act(whats):
            for group, which, stop in whats:
                if which == OWN:
                    own[group].now(stop)
                else:
                    pl.when(later)(functools.partial(old[group].now, stop))

        def plan(phase):
            return planned(act, BACK[phase])

        def before(group):
            pl.when(later)(old[group].finish)

        pl.when(later)(functools.partial(need, ("gu", "hm", "od"), i))
        for half, group, phase in ((0, GA_G, "first"), (1, GB_G, "second")):
            ffn_bwd_phase(half, hm_s, dh_s, gu_s, od, made_s, dgu_s, bt_s, db_s, dhm_s, rows, r, plan(phase))
            if half == 1:
                pl.when(i > 0)(functools.partial(bring, ("gu", "hm"), i - 1))
            before(group)
            units_phase(half, dgu_s, bt_s, terms[group])
            own[group].begin(later)
        bring(("o", "q", "k", "v", "lse", "h"), i)
        before(WD_G)
        downs_phase(made_s, dh_s, terms[WD_G])
        own[WD_G].begin(later)
        the_rest(plan("downs"), 0)
        need(("o",), i)
        before(WO_G)
        out_bwd_phase(dhm_s, o_s, od, terms[WO_G], do_s, delta_s, rows, r)
        own[WO_G].begin(later)
        the_rest(plan("out"), 0)
        pl.when(i > 0)(functools.partial(bring, ("od",), i - 1))
        need(("q", "k", "v", "lse"), i)
        attend_bwd_phase(q_s, k_s, v_s, do_s, lse_s, delta_s, table_s, dqkv_s, dq_s, dk_s, dv_s, kt_s, bq, plan("attend"))
        the_rest(plan("late"), 0)
        need(("h",), i)
        before(QKV_G)
        qkv_bwd_phase(h_s, dqkv_s, qkv_s, dhm_s, terms[QKV_G], do_s, dh_s, rows, i > 0)
        own[QKV_G].begin(later)
        the_rest(plan("end"), 0)

    loop(layers, layer)
    final = {group: pack(group, 0, False, taken.get(group, (0, 0))) for group in range(PACKS)}
    out = []

    def leave(group, i):
        out.append(pltpu.make_async_copy(got[group].at[i], results[group].at[i], result_sem.at[group, i]))
        out[-1].start()

    for i in range(1, layers):
        for group in range(PACKS):
            leave(group, i)
    for group, stop in TAIL:
        final[group].now(stop)
        if group != QKV_G:
            final[group].finish()
            leave(group, 0)
    final[QKV_G].finish()
    leave(QKV_G, 0)
    for copy in out:
        copy.wait()


def adamw(*refs):
    count = 3 * SEVEN
    grads, refs = refs[:PACKS], refs[PACKS:]
    ins, outs, refs = refs[:count], refs[count : 2 * count], refs[2 * count :]
    grads_s, refs = refs[:PACKS], refs[PACKS:]
    ins_s, outs_s, (grad_sem, in_sem, out_sem) = refs[:count], refs[count : 2 * count], refs[2 * count :]
    kinds = range(0, count, SEVEN)
    layers = ins[0].shape[0]
    heads, half, whole, few = ins[0].shape[2], ins[4].shape[2] // 2, ins[3].shape[2], FEW
    waits = []
    for i in range(layers):
        copies = [pltpu.make_async_copy(src.at[i], dst.at[i], grad_sem.at[g, i]) for g, (src, dst) in enumerate(zip(grads, grads_s, strict=True))]
        copies += [pltpu.make_async_copy(ins[a].at[i], ins_s[a].at[i], in_sem.at[a, i]) for w in range(SEVEN) for a in (w + kind for kind in kinds)]
        for copy in copies:
            copy.start()
        waits.append(copies)
    parts = (
        [(QKV_G, START, START, heads)], [(QKV_G, heads, START, HEAD)], [(QKV_G, heads + HEAD, START, HEAD)], [(WO_G, START, START, whole)],
        [(GA_G, START, START, half), (GB_G, START, half, half)], [(GA_G, half, START, half), (GB_G, half, half, half)], [(WD_G, START, START, whole)],
    )
    out = []
    for i in range(layers):
        for copy in waits[i][:PACKS]:
            copy.wait()
        for w in range(SEVEN):
            for copy in waits[i][PACKS + 3 * w : PACKS + 3 * (w + 1)]:
                copy.wait()

            def step(j, i=i, w=w):
                at = tile(j, few)
                for grad, first, start, wide in parts[w]:
                    here = slice(start, start + wide)
                    g = grads_s[grad][i, at, first : first + wide].astype(F32)
                    weight = ins_s[w][i, at, here].astype(F32)
                    of_m, of_v = w + SEVEN, w + 2 * SEVEN
                    m = 0.9 * ins_s[of_m][i, at, here] + 0.1 * g
                    v = 0.95 * ins_s[of_v][i, at, here] + 0.05 * g * g
                    outs_s[w][i, at, here] = (weight - 0.02 * (m * lax.rsqrt(v + 1e-8) + 0.1 * weight)).astype(BF16)
                    outs_s[of_m][i, at, here] = m
                    outs_s[of_v][i, at, here] = v

            loop(ins[w].shape[1] // few, step)
            for a in (w + kind for kind in kinds):
                out.append(pltpu.make_async_copy(outs_s[a].at[i], outs[a].at[i], out_sem.at[a, i]))
                out[-1].start()
    for copy in out:
        copy.wait()


def solution(mesh):
    n = mesh.shape["dp"]
    far_a, far_b = n // 2, n - 1 - n // 2

    def step(x, dy, *arrays):
        weights = arrays[:SEVEN]
        wq, wk, wv, wo, wg, wu, wd = weights
        layers, r, wide_q = wq.shape
        x, dy = x[0], dy[0]
        tokens, d = x.shape
        ff = wg.shape[2]
        bq, rows = (min(512, tokens),) * 2
        few = jnp.asarray(angles(tokens))
        wide = wide_q + 2 * HEAD
        heads = wide_q // HEAD
        ro = wo.shape[1]
        shapes = (r, wide), (r, 2 * ff), (ro + wd.shape[1], d)
        terms = (r, wide), (r, ff), (r, ff), (wd.shape[1], d), (ro, d)
        both = lambda *s: jax.ShapeDtypeStruct((layers, *s), BF16)
        some = lambda lead, s: pltpu.VMEM((*lead, *s), BF16)
        grads = pl.pallas_call(
            functools.partial(train, (layers, n, bq, rows, ro)),
            out_shape=[*(both(*s) for s in terms), both(tokens, wide_q), both(tokens, HEAD), both(tokens, HEAD), both(tokens, wide_q),
                       jax.ShapeDtypeStruct((layers, 8, tokens), F32), both(tokens, d), both(tokens, d),
                       jax.ShapeDtypeStruct((layers, n * shapes[2][0], d), BF16), jax.ShapeDtypeStruct((layers, n * r, 2 * ff), BF16)],
            in_specs=[ANY] * (3 + SEVEN),
            out_specs=[ANY] * (PACKS + len(KEPT)),
            scratch_shapes=[
                pltpu.VMEM(few.shape, F32), pltpu.VMEM((tokens, HEAD), F32), some((n,), shapes[0]), *(some((n * s[0],), s[1:]) for s in shapes[1:]),
                some((tokens,), (HEAD,)), some((tokens,), (HEAD,)), pltpu.VMEM((8, tokens), F32), *(some((tokens,), (d,)) for _ in terms[:3]),
                some((tokens,), (ff,)), some((tokens,), (2 * ff,)), some((d,), (tokens,)),
                pltpu.VMEM((tokens, d), F32), pltpu.VMEM((heads, HEAD + 8, bq), F32), pltpu.VMEM((heads, bq), F32), some((HEAD,), (tokens,)), pltpu.VMEM((heads, tokens), F32),
                *(some((lead,), s) for lead in (n, far_a, far_b, layers) for s in terms),
                pltpu.SemaphoreType.DMA((9 * layers,)), pltpu.SemaphoreType.DMA((2,)), pltpu.SemaphoreType.DMA((len(KEPT),)),
                pltpu.SemaphoreType.DMA((3 * layers, 4, far_a)), pltpu.SemaphoreType.DMA((3 * layers, n + 1)),
                pltpu.SemaphoreType.DMA((len(KEPT) + 1,)), pltpu.SemaphoreType.DMA((PACKS, layers)),
                pltpu.SemaphoreType.REGULAR((PACKS,)),
            ],
            compiler_params=pltpu.CompilerParams(vmem_limit_bytes=VMEM, collective_id=0, has_side_effects=True),
            name="train",
        )(x, few, dy, *weights)[:PACKS]
        in_vmem = lambda a: pltpu.VMEM(a.shape, a.dtype)
        return pl.pallas_call(
            adamw,
            out_shape=[jax.ShapeDtypeStruct(a.shape, a.dtype) for a in arrays],
            in_specs=[ANY] * (PACKS + 3 * SEVEN),
            out_specs=[ANY] * (3 * SEVEN),
            scratch_shapes=[*map(in_vmem, grads), *map(in_vmem, arrays), *map(in_vmem, arrays),
                            pltpu.SemaphoreType.DMA((PACKS, layers)), *(pltpu.SemaphoreType.DMA((3 * SEVEN, layers)) for _ in arrays[:2])],
            compiler_params=pltpu.CompilerParams(vmem_limit_bytes=VMEM),
            name="adamw",
        )(*grads, *arrays)

    states, cut = P(("rep", "dp"), None, None), P(None, "dp", None)
    return jax.shard_map(
        step,
        mesh=mesh,
        in_specs=(states, states) + (cut,) * (3 * SEVEN),
        out_specs=(P("rep", "dp", None),) * (3 * SEVEN),
        check_vma=False,
    )
```
